32 devices in a mesh: dp: 8 (over z, core), tensor: 4 (over y, x).
Axes of the slice: x: 2, y: 2, z: 4, core: 2. Of those that a mesh axis runs over, the one named last changes fastest.
Arguments:
- tokens: bfloat16 [16, 512, 1024], P('dp', 'tensor'), may hold values from -8.5 to 8.5
- segment_ids: int32 [16, 512], P('dp'), may hold values from 0 to 5, never falling along the last dimension, each value on 1 to 128 neighbouring positions
- w_qkv: bfloat16 [3, 1024, 1024], P(None, 'dp', 'tensor'), may hold values from -0.2625 to 0.2625
- w_out: bfloat16 [1024, 1024], P('tensor', 'dp'), may hold values from -1.75 to 1.75
- w_up: bfloat16 [1024, 4096], P('dp', 'tensor'), may hold values from -0.1875 to 0.1875
- w_down: bfloat16 [4096, 1024], P('tensor', 'dp'), may hold values from -0.09375 to 0.09375
- vectors: bfloat16 [12, 1024], P(None, 'dp'), may hold values from -3 to 3
- cotangent: bfloat16 [16, 512, 1024], P('dp', 'tensor'), may hold values from -6 to 6
Outputs:
- out_tokens: bfloat16 [16, 512, 1024], P('dp', 'tensor')
- grad_tokens: float32 [16, 512, 1024], P('dp', 'tensor')
- grad_qkv: float32 [3, 1024, 1024], P(None, 'dp', 'tensor')
- grad_out: float32 [1024, 1024], P('tensor', 'dp')
- grad_up: float32 [1024, 4096], P('dp', 'tensor')
- grad_down: float32 [4096, 1024], P('tensor', 'dp')
- grad_vectors: float32 [12, 1024], P(None, 'dp')
The draws below stay inside these ranges and needn't reach their ends.
Inputs may be any that keep to these rules, and one draw needn't show every extreme that they name: `segment_ids`: within a sequence the ids never fall; each document has 1 to 128 tokens and one has exactly that many.
All inputs are finite; a program needn't handle non-finite values.
Results may differ from the reference program's by a relative error of at most 0.02.
Values may be sent and summed in bfloat16 or wider, within the bound.
A program may use at most 128 MiB of HBM per device.

```python
import math
import jax
import jax.numpy as jnp
import numpy as np
from jax import lax

D = 1024
FF = 4096
HD = 64
HEADS = 16
SEQ = 512
DOCS = 6
SEQS = 16


def draw_tokens(key, part):
    first_key = jax.random.fold_in(key, 0)
    base = jnp.clip(jax.random.normal(first_key, (SEQS, SEQ, D), jnp.float32), -6.0, 6.0)
    return base.astype(jnp.bfloat16)


def draw_w_qkv(key, part):
    first_key = jax.random.fold_in(key, 0)
    spread = D ** (-0.5)
    base = jnp.clip(jax.random.normal(first_key, (3, D, D), jnp.float32), -6.0, 6.0) * spread
    return base.astype(jnp.bfloat16)


def draw_vectors(key, part):
    noise = jnp.clip(jax.random.normal(key, (12, D), jnp.float32), -6.0, 6.0)
    row_num = jax.lax.broadcasted_iota(jnp.int32, (12, D), 0)
    is_gain = (row_num == 3) | (row_num == 6)
    return jnp.where(is_gain, 1.0 + 0.15 * noise, 0.5 * noise).astype(jnp.bfloat16)


def block_levels(own_key, dims, cuts, low, largest):
    def one(position, shards_of):
        heights = jax.random.uniform(jax.random.fold_in(jax.random.fold_in(own_key, 6), position), (shards_of,), jnp.float32, low / len(cuts), largest / len(cuts))
        return jnp.repeat(jnp.exp(heights), dims[position] // shards_of).reshape((-1,) + (1,) * (len(dims) - position - 1))

    level = one(*cuts[0])
    for cut in cuts[1:]:
        level = level * one(*cut)
    return level


def split_up(amount, total, limit, skew):
    portions = [(1 << 20) // math.isqrt(standing ** skew) + 1 for standing in range(2, amount + 1)]
    surplus, holding = total - limit - (amount - 1), [1] * (amount - 1)
    while surplus > 0:
        candidates = [i for i in range(amount - 1) if holding[i] < limit]
        whole, remaining = sum([portions[i] for i in candidates]), surplus
        for i in candidates:
            more = min(limit - holding[i], max(1, remaining * portions[i] // whole), surplus)
            holding[i] = holding[i] + more
            surplus = surplus - more
    return np.array([limit] + holding)


def ragged_sizes(rng, count, total, reach, lean):
    if count == 2:
        one = jax.random.randint(rng, (), max(1, total - reach), min(reach, total - 1) + 1)
        return jnp.stack([one, total - one])
    tallies = jnp.asarray(split_up(count, total, reach, lean), jnp.int32)
    pairs = (count - 1) // 2
    donor, sink = tallies[1:1 + 2 * pairs:2], tallies[2:2 + 2 * pairs:2]
    slack = jnp.minimum(donor - 1, reach - sink)
    shifted = jax.random.randint(jax.random.fold_in(rng, 1), (pairs,), 0, 1 << 20) % (slack + 1)
    tallies = tallies.at[1:1 + 2 * pairs:2].set(donor - shifted).at[2:2 + 2 * pairs:2].set(sink + shifted)
    return tallies[jax.random.permutation(jax.random.fold_in(rng, 2), count)]


def bell_draw(stream_key, dims, deviation, limit, cuts=(), held_as=jnp.bfloat16):
    result = jax.random.normal(stream_key, dims, jnp.float32) * deviation
    if len(cuts) > 0:
        result = block_levels(stream_key, dims, cuts, -0.22, 0.18) * result
    return jnp.clip(result, min=-limit, max=limit).astype(held_as)


def setup_inputs(seed: int = 0) -> dict:
    seeds = jax.random.split(jax.random.key(seed), 9)
    tokens = draw_tokens(jax.random.fold_in(seeds[8], 71), 0)
    segment_ids = jax.vmap(lambda own: jnp.searchsorted(jnp.cumsum(ragged_sizes(own, DOCS, SEQ, SEQ // 4, 0)), jnp.arange(SEQ), side="right"))(jax.random.split(seeds[1], SEQS)).reshape((SEQS, SEQ)).astype(jnp.int32)
    w_qkv = draw_w_qkv(jax.random.fold_in(seeds[8], 71), 0)
    w_out = bell_draw(seeds[3], (D, D), (D * 6 // SEQ) ** -0.5, 1.75, ((0, 4), (1, 8)))
    w_up = bell_draw(seeds[4], (D, FF), D ** -0.5, 0.1875, ((0, 8), (1, 4)))
    w_down = bell_draw(seeds[5], (FF, D), FF ** -0.5, 0.09375, ((0, 4), (1, 8)))
    vectors = draw_vectors(jax.random.fold_in(seeds[8], 71), 0)
    cotangent = bell_draw(seeds[7], (SEQS, SEQ, D), 1.0, 6.0, ((0, 8), (1, 4)))
    return {"tokens": tokens, "segment_ids": segment_ids, "w_qkv": w_qkv, "w_out": w_out, "w_up": w_up, "w_down": w_down, "vectors": vectors, "cotangent": cotangent}


NORM_EPS = 1e-06
SQRT_HALF = 0.7071067811865476
INV_ROOT_TAU = 0.3989422804014327
MASKED = -1e+30

def gelu_value(pre_act):
    return 0.5 * pre_act * (1.0 + lax.erf(pre_act * SQRT_HALF))

def gelu_slope(pre_act):
    return 0.5 * (1.0 + lax.erf(pre_act * SQRT_HALF)) + pre_act * INV_ROOT_TAU * jnp.exp(-0.5 * pre_act * pre_act)

def norm_forward(summed, gain, shift):
    centred = summed - lax.optimization_barrier(jnp.mean(summed, axis=-1, keepdims=True))
    inverse = lax.rsqrt(lax.optimization_barrier(jnp.mean(centred * centred, axis=-1, keepdims=True)) + NORM_EPS)
    normed = centred * inverse
    return (normed * gain + shift, normed, inverse)

def norm_backward(normed, inverse, grad_normed):
    first_mean = lax.optimization_barrier(jnp.mean(grad_normed, axis=-1, keepdims=True))
    second_mean = lax.optimization_barrier(jnp.mean(grad_normed * normed, axis=-1, keepdims=True))
    return inverse * (grad_normed - first_mean - normed * second_mean)

def reference(tokens, segment_ids, w_qkv, w_out, w_up, w_down, vectors, cotangent):
    vec_f32 = vectors.astype(jnp.float32)
    score_scale = HD ** (-0.5)

    def single(carried, batch_item):
        tok_block, segments, grad_block = batch_item
        proj_q = jnp.dot(tok_block, w_qkv[0], preferred_element_type=jnp.float32)
        proj_k = jnp.dot(tok_block, w_qkv[1], preferred_element_type=jnp.float32)
        proj_v = jnp.dot(tok_block, w_qkv[2], preferred_element_type=jnp.float32)
        query_b = (proj_q + vec_f32[0]).astype(jnp.bfloat16)
        key_b = proj_k.astype(jnp.bfloat16)
        value_b = (proj_v + vec_f32[1]).astype(jnp.bfloat16)
        query_f = query_b.astype(jnp.float32).reshape(SEQ, HEADS, HD)
        key_f = key_b.astype(jnp.float32).reshape(SEQ, HEADS, HD)
        value_f = value_b.astype(jnp.float32).reshape(SEQ, HEADS, HD)
        same_doc = segments[:, None] == segments[None, :]
        scores = jnp.einsum('qhe,khe->hqk', query_f, key_f) * score_scale
        scores = jnp.where(same_doc[None], scores, MASKED)
        row_top = lax.optimization_barrier(jnp.max(scores, axis=-1, keepdims=True))
        log_total = row_top + jnp.log(lax.optimization_barrier(jnp.sum(jnp.exp(scores - row_top), axis=-1, keepdims=True)))
        attn_exact = jnp.exp(scores - log_total)
        attn_probs = attn_exact.astype(jnp.bfloat16)
        context = jnp.einsum('hqk,khe->qhe', attn_probs.astype(jnp.float32), value_f).reshape(SEQ, D).astype(jnp.bfloat16)
        summed_one = tok_block.astype(jnp.float32) + jnp.dot(context, w_out, preferred_element_type=jnp.float32) + vec_f32[2]
        normed_out, normed_one, inverse_one = norm_forward(summed_one, vec_f32[3], vec_f32[4])
        normed_b = normed_out.astype(jnp.bfloat16)
        pre_act = jnp.dot(normed_b, w_up, preferred_element_type=jnp.float32) + vec_f32[8:12].reshape(FF)
        activated = gelu_value(pre_act).astype(jnp.bfloat16)
        summed_two = normed_out + jnp.dot(activated, w_down, preferred_element_type=jnp.float32) + vec_f32[5]
        final, normed_two, inverse_two = norm_forward(summed_two, vec_f32[6], vec_f32[7])
        grad_final = grad_block.astype(jnp.float32)
        g_gain2 = lax.optimization_barrier(jnp.sum(grad_final * normed_two, axis=0))
        g_shift2 = lax.optimization_barrier(jnp.sum(grad_final, axis=0))
        grad_two = norm_backward(normed_two, inverse_two, grad_final * vec_f32[6])
        grad_two_b = grad_two.astype(jnp.bfloat16)
        g_bdown = lax.optimization_barrier(jnp.sum(grad_two, axis=0))
        g_down = jnp.dot(activated.T, grad_two_b, preferred_element_type=jnp.float32)
        grad_pre = jnp.dot(grad_two_b, w_down.T, preferred_element_type=jnp.float32) * gelu_slope(pre_act)
        grad_pre_b = grad_pre.astype(jnp.bfloat16)
        g_bup = lax.optimization_barrier(jnp.sum(grad_pre, axis=0))
        g_up = jnp.dot(normed_b.T, grad_pre_b, preferred_element_type=jnp.float32)
        grad_one_in = grad_two + jnp.dot(grad_pre_b, w_up.T, preferred_element_type=jnp.float32)
        g_gain1 = lax.optimization_barrier(jnp.sum(grad_one_in * normed_one, axis=0))
        g_shift1 = lax.optimization_barrier(jnp.sum(grad_one_in, axis=0))
        grad_one = norm_backward(normed_one, inverse_one, grad_one_in * vec_f32[3])
        grad_one_b = grad_one.astype(jnp.bfloat16)
        g_bout = lax.optimization_barrier(jnp.sum(grad_one, axis=0))
        g_out = jnp.dot(context.T, grad_one_b, preferred_element_type=jnp.float32)
        grad_context = jnp.dot(grad_one_b, w_out.T, preferred_element_type=jnp.float32).astype(jnp.bfloat16)
        grad_ctx_f = grad_context.astype(jnp.float32).reshape(SEQ, HEADS, HD)
        grad_probs = jnp.einsum('qhe,khe->hqk', grad_ctx_f, value_f)
        row_dot = lax.optimization_barrier(jnp.sum(attn_exact * grad_probs, axis=-1, keepdims=True))
        grad_scores = (attn_exact * (grad_probs - row_dot) * score_scale).astype(jnp.bfloat16).astype(jnp.float32)
        grad_value = jnp.einsum('hqk,qhe->khe', attn_probs.astype(jnp.float32), grad_ctx_f).reshape(SEQ, D)
        grad_query = jnp.einsum('hqk,khe->qhe', grad_scores, key_f).reshape(SEQ, D)
        grad_key = jnp.einsum('hqk,qhe->khe', grad_scores, query_f).reshape(SEQ, D)
        grad_qkv = jnp.stack([grad_query, grad_key, grad_value]).astype(jnp.bfloat16)
        g_qkv = jnp.einsum('sd,tsc->tdc', tok_block.astype(jnp.float32), grad_qkv.astype(jnp.float32))
        grad_input = grad_one + jnp.dot(grad_qkv[0], w_qkv[0].T, preferred_element_type=jnp.float32)
        grad_input = grad_input + jnp.dot(grad_qkv[1], w_qkv[1].T, preferred_element_type=jnp.float32)
        grad_input = grad_input + jnp.dot(grad_qkv[2], w_qkv[2].T, preferred_element_type=jnp.float32)
        g_bq = lax.optimization_barrier(jnp.sum(grad_query, axis=0))
        g_bv = lax.optimization_barrier(jnp.sum(grad_value, axis=0))
        first_rows = jnp.stack([g_bq, g_bv, g_bout, g_gain1, g_shift1, g_bdown, g_gain2, g_shift2])
        g_vec = jnp.concatenate([first_rows, g_bup.reshape(4, D)], axis=0)
        updated = jax.tree.map(jnp.add, carried, (g_qkv, g_out, g_up, g_down, g_vec))
        return (updated, (final.astype(jnp.bfloat16), grad_input))
    initial = (jnp.zeros((3, D, D), jnp.float32), jnp.zeros((D, D), jnp.float32), jnp.zeros((D, FF), jnp.float32), jnp.zeros((FF, D), jnp.float32), jnp.zeros((12, D), jnp.float32))
    totals, stacked = lax.scan(single, initial, (tokens, segment_ids, cotangent))
    return (stacked[0], stacked[1], totals[0], totals[1], totals[2], totals[3], totals[4])
```

```python
import jax
import jax.numpy as jnp
from jax import lax
from jax.experimental import pallas as pl
from jax.experimental.pallas import tpu as pltpu
from jax.sharding import PartitionSpec as P

D = 1024
FF = 4096
HD = 64


NORM_EPS = 1e-06
SQRT_HALF = 0.7071067811865476
INV_ROOT_TAU = 0.3989422804014327
MASKED = -1e30


def gelu_value(pre_act):
    return 0.5 * pre_act * (1.0 + lax.erf(pre_act * SQRT_HALF))


def gelu_slope(pre_act):
    return 0.5 * (1.0 + lax.erf(pre_act * SQRT_HALF)) + pre_act * INV_ROOT_TAU * jnp.exp(
        -0.5 * pre_act * pre_act
    )


def norm_forward(summed, gain, shift):
    centred = summed - jnp.mean(summed, axis=-1, keepdims=True)
    inverse = lax.rsqrt(jnp.mean(centred * centred, axis=-1, keepdims=True) + NORM_EPS)
    normed = centred * inverse
    return (normed * gain + shift, normed, inverse)


def norm_backward(normed, inverse, grad_normed):
    first_mean = jnp.mean(grad_normed, axis=-1, keepdims=True)
    second_mean = jnp.mean(grad_normed * normed, axis=-1, keepdims=True)
    return inverse * (grad_normed - first_mean - normed * second_mean)


def attention_scores(query_heads, key_heads, segments):
    same_doc = segments[:, None] == segments[None, :]
    scores = jnp.einsum(
        "qhe,khe->hqk", query_heads, key_heads, preferred_element_type=jnp.float32
    ) * HD ** (-0.5)
    return jnp.where(same_doc[None], scores, MASKED)


def collect(w_qkv, w_out, w_up, w_down, vectors):
    return (
        lax.all_gather(w_qkv, "dp", axis=1, tiled=True),
        lax.all_gather(w_out, "dp", axis=1, tiled=True),
        lax.all_gather(w_up, "dp", axis=0, tiled=True),
        lax.all_gather(w_down, "dp", axis=1, tiled=True),
        lax.all_gather(vectors, "dp", axis=1, tiled=True),
    )


def share(gradients):
    return (
        lax.psum_scatter(
            gradients[0].astype(jnp.bfloat16), "dp", scatter_dimension=1, tiled=True
        ).astype(jnp.float32),
        lax.psum_scatter(
            gradients[1].astype(jnp.bfloat16), "dp", scatter_dimension=1, tiled=True
        ).astype(jnp.float32),
        lax.psum_scatter(
            gradients[2].astype(jnp.bfloat16), "dp", scatter_dimension=0, tiled=True
        ).astype(jnp.float32),
        lax.psum_scatter(
            gradients[3].astype(jnp.bfloat16), "dp", scatter_dimension=1, tiled=True
        ).astype(jnp.float32),
        lax.psum_scatter(
            gradients[4].astype(jnp.bfloat16), "dp", scatter_dimension=1, tiled=True
        ).astype(jnp.float32),
    )


def body(tokens, segment_ids, w_qkv, w_out, w_up, w_down, vectors, cotangent):
    tensor_rank = lax.axis_index("tensor")
    local_cols = w_qkv.shape[2]
    head_count = local_cols // HD
    hidden = w_up.shape[1]
    col_start = tensor_rank * local_cols
    ffn_start = tensor_rank * hidden

    def forward(weights, tok_block, segments):
        qkv_w, out_w, up_w, down_w, vec_b = weights
        vec_f32 = vec_b.astype(jnp.float32)
        whole = lax.all_gather(tok_block, "tensor", axis=0, tiled=True)
        seq_len = whole.shape[0]
        projected = jnp.einsum("sd,tdc->tsc", whole, qkv_w, preferred_element_type=jnp.float32)
        bias_q = lax.dynamic_slice_in_dim(vec_f32[0], col_start, local_cols)
        bias_v = lax.dynamic_slice_in_dim(vec_f32[1], col_start, local_cols)
        query_heads = (projected[0] + bias_q).astype(jnp.bfloat16).reshape(seq_len, head_count, HD)
        key_heads = projected[1].astype(jnp.bfloat16).reshape(seq_len, head_count, HD)
        value_heads = (projected[2] + bias_v).astype(jnp.bfloat16).reshape(seq_len, head_count, HD)
        scores = attention_scores(query_heads, key_heads, segments)
        row_top = jnp.max(scores, axis=-1, keepdims=True)
        log_total = row_top + jnp.log(jnp.sum(jnp.exp(scores - row_top), axis=-1, keepdims=True))
        attn_probs = jnp.exp(scores - log_total).astype(jnp.bfloat16)
        context = jnp.einsum(
            "hqk,khe->qhe", attn_probs, value_heads, preferred_element_type=jnp.float32
        )
        context = context.reshape(seq_len, local_cols).astype(jnp.bfloat16)
        piece = context
        attn_mixed = lax.psum_scatter(
            jnp.dot(piece, out_w, preferred_element_type=jnp.float32).astype(jnp.bfloat16),
            "tensor",
            scatter_dimension=0,
            tiled=True,
        ).astype(jnp.float32)
        summed_one = tok_block.astype(jnp.float32) + attn_mixed + vec_f32[2]
        normed_out, normed_one, inverse_one = norm_forward(summed_one, vec_f32[3], vec_f32[4])
        normed_b = normed_out.astype(jnp.bfloat16)
        normed_whole = lax.all_gather(normed_b, "tensor", axis=0, tiled=True)
        bias_up = lax.dynamic_slice_in_dim(vec_f32[8:12].reshape(FF), ffn_start, hidden)
        pre_act = jnp.dot(normed_whole, up_w, preferred_element_type=jnp.float32) + bias_up
        activated = gelu_value(pre_act).astype(jnp.bfloat16)
        piece = activated
        summed_two = (
            normed_out
            + lax.psum_scatter(
                jnp.dot(piece, down_w, preferred_element_type=jnp.float32).astype(jnp.bfloat16),
                "tensor",
                scatter_dimension=0,
                tiled=True,
            ).astype(jnp.float32)
            + vec_f32[5]
        )
        final, normed_two, inverse_two = norm_forward(summed_two, vec_f32[6], vec_f32[7])
        saved = (
            whole,
            query_heads,
            key_heads,
            value_heads,
            log_total,
            context,
            normed_one,
            inverse_one,
            normed_whole,
            pre_act,
            activated,
            normed_two,
            inverse_two,
        )
        return (final.astype(jnp.bfloat16), saved)

    def backward(weights, saved, segments, grad_block):
        qkv_w, out_w, up_w, down_w, vec_b = weights
        vec_f32 = vec_b.astype(jnp.float32)
        (
            whole,
            query_heads,
            key_heads,
            value_heads,
            log_total,
            context,
            normed_one,
            inverse_one,
            normed_whole,
            pre_act,
            activated,
            normed_two,
            inverse_two,
        ) = saved
        seq_len = whole.shape[0]
        grad_final = grad_block.astype(jnp.float32)
        g_gain2 = jnp.sum(grad_final * normed_two, axis=0)
        g_shift2 = jnp.sum(grad_final, axis=0)
        grad_two = norm_backward(normed_two, inverse_two, grad_final * vec_f32[6])
        grad_two_b = grad_two.astype(jnp.bfloat16)
        g_bdown = jnp.sum(grad_two, axis=0)
        grad_two_whole = lax.all_gather(grad_two_b, "tensor", axis=0, tiled=True)
        g_down = jnp.dot(activated.T, grad_two_whole, preferred_element_type=jnp.float32)
        grad_pre = jnp.dot(
            grad_two_whole, down_w.T, preferred_element_type=jnp.float32
        ) * gelu_slope(pre_act)
        grad_pre_b = grad_pre.astype(jnp.bfloat16)
        g_bup = jnp.sum(grad_pre, axis=0)
        g_up = jnp.dot(normed_whole.T, grad_pre_b, preferred_element_type=jnp.float32)
        piece = grad_pre_b
        grad_one_in = grad_two + lax.psum_scatter(
            jnp.dot(piece, up_w.T, preferred_element_type=jnp.float32).astype(jnp.bfloat16),
            "tensor",
            scatter_dimension=0,
            tiled=True,
        ).astype(jnp.float32)
        g_gain1 = jnp.sum(grad_one_in * normed_one, axis=0)
        g_shift1 = jnp.sum(grad_one_in, axis=0)
        grad_one = norm_backward(normed_one, inverse_one, grad_one_in * vec_f32[3])
        grad_one_b = grad_one.astype(jnp.bfloat16)
        g_bout = jnp.sum(grad_one, axis=0)
        grad_one_whole = lax.all_gather(grad_one_b, "tensor", axis=0, tiled=True)
        g_out = jnp.dot(context.T, grad_one_whole, preferred_element_type=jnp.float32)
        grad_context = jnp.dot(grad_one_whole, out_w.T, preferred_element_type=jnp.float32).astype(
            jnp.bfloat16
        )
        grad_context = grad_context.reshape(seq_len, head_count, HD)
        scores = attention_scores(query_heads, key_heads, segments)
        attn_exact = jnp.exp(scores - log_total)
        attn_probs = attn_exact.astype(jnp.bfloat16)
        grad_probs = jnp.einsum(
            "qhe,khe->hqk", grad_context, value_heads, preferred_element_type=jnp.float32
        )
        row_dot = jnp.sum(attn_exact * grad_probs, axis=-1, keepdims=True)
        grad_scores = (attn_exact * (grad_probs - row_dot) * HD ** (-0.5)).astype(jnp.bfloat16)
        grad_value = jnp.einsum(
            "hqk,qhe->khe", attn_probs, grad_context, preferred_element_type=jnp.float32
        )
        grad_value = grad_value.reshape(seq_len, local_cols)
        grad_query = jnp.einsum(
            "hqk,khe->qhe", grad_scores, key_heads, preferred_element_type=jnp.float32
        )
        grad_query = grad_query.reshape(seq_len, local_cols)
        grad_key = jnp.einsum(
            "hqk,qhe->khe", grad_scores, query_heads, preferred_element_type=jnp.float32
        )
        grad_key = grad_key.reshape(seq_len, local_cols)
        grad_qkv = jnp.stack([grad_query, grad_key, grad_value]).astype(jnp.bfloat16)
        g_qkv = jnp.einsum("sd,tsc->tdc", whole, grad_qkv, preferred_element_type=jnp.float32)
        piece = grad_qkv
        grad_input = grad_one + lax.psum_scatter(
            jnp.einsum("tsc,tdc->sd", piece, qkv_w, preferred_element_type=jnp.float32).astype(
                jnp.bfloat16
            ),
            "tensor",
            scatter_dimension=0,
            tiled=True,
        ).astype(jnp.float32)
        zero_row = jnp.zeros((D,), jnp.float32)
        row_q = lax.dynamic_update_slice_in_dim(zero_row, jnp.sum(grad_query, axis=0), col_start, 0)
        row_v = lax.dynamic_update_slice_in_dim(zero_row, jnp.sum(grad_value, axis=0), col_start, 0)
        up_rows = lax.dynamic_update_slice_in_dim(
            jnp.zeros((FF,), jnp.float32), g_bup, ffn_start, 0
        ).reshape(4, D)
        first_rows = jnp.stack(
            [row_q, row_v, g_bout, g_gain1, g_shift1, g_bdown, g_gain2, g_shift2]
        )
        g_vec = jnp.concatenate([first_rows, up_rows], axis=0)
        return ((g_qkv, g_out, g_up, g_down, g_vec), grad_input)

    def one_batch(carried, batch_item):
        tok_block, segments, grad_block = batch_item
        forward_w = collect(w_qkv, w_out, w_up, w_down, vectors)
        final_b, saved = forward(forward_w, tok_block, segments)
        second = collect(w_qkv, w_out, w_up, w_down, vectors)
        gradients, grad_input = backward(second, saved, segments, grad_block)
        updated = jax.tree.map(jnp.add, carried, gradients)
        return (updated, (final_b, grad_input))

    initial = (
        jnp.zeros((3, D, local_cols), jnp.float32),
        jnp.zeros((local_cols, D), jnp.float32),
        jnp.zeros((D, hidden), jnp.float32),
        jnp.zeros((hidden, D), jnp.float32),
        jnp.zeros((12, D), jnp.float32),
    )
    carried, stacked = lax.scan(one_batch, initial, (tokens, segment_ids, cotangent))
    totals = share(carried)
    vector_grads = lax.psum(totals[4], "tensor")
    return (stacked[0], stacked[1], totals[0], totals[1], totals[2], totals[3], vector_grads)


Y_TOK, Y_COT, Y_OUT, Y_GTOK = range(4)
X_TOK, X_MIX, X_NORM, X_FFN, X_DA2, X_DH, X_DA1, X_DX = range(8)
QKV, OUT, UP, DOWN, VEC = range(5)
U_DOWN, U_UP, U_OUT, U_V, U_K, U_Q = range(6)
R_BQ, R_BV, R_BO, R_G1, R_C1, R_BD, R_G2, R_C2, R_BU = range(9)
ZS = 4
SEQ = 512
ROWS = 256
CHUNK = 128
TILE = 32
COLS = 512
HID = 2048
WINDOW = 384
BF = jnp.bfloat16
F32 = jnp.float32
MESH = pl.DeviceIdType.MESH


def span(index, size):
    return pl.ds(pl.multiple_of(index * size, size), size)


def contract(a, b, a_dim, b_dim):
    return lax.dot_general(a, b, (((a_dim,), (b_dim,)), ((), ())), preferred_element_type=F32)


def fold_rows(value):
    return jnp.sum(value.reshape(value.shape[0] // 8, 8, value.shape[1]), axis=0)


def layer_kernel(
    tok, seg, wq, wo, wu, wd, vec, cot,
    out, gtok, gq, go, gu, gd, gv,
    w_qkv, w_out, w_up, w_down, w_vec, vf,
    g_down, g_up, g_out, g_qkv,
    c_down, c_up, c_out, c_qkv,
    y_down, y_up, y_out, y_qkv,
    z_down, z_up, z_out, z_qkv,
    o_qkv, o_out, o_up, o_down,
    xw, qkv, ctx, prob, bias, hw, act, slope, aw, a1w, dctx,
    own, n1, da, inv1, recv, stage, cotb, outb, gts, gtr, gtf,
    acc, vg, vgx, vgc, vgy, vgz, gvb, acc_k, acc_v,
    wsz, wrz, wsy, wry, wsc, wrc, xs, xr, ys, yr,
    gsc, grc, gsy, gry, gsz, grz, vs, vr, ls, os,
):
    dp = lax.axis_index("dp")
    tensor = lax.axis_index("tensor")
    z, c = dp // 2, dp % 2
    y, x = tensor // 2, tensor % 2
    at_x = {"dp": dp, "tensor": y * 2 + (1 - x)}
    at_y = {"dp": dp, "tensor": (1 - y) * 2 + x}
    at_c = {"dp": z * 2 + (1 - c), "tensor": tensor}
    at_z = [{"dp": lax.rem(z + k, ZS) * 2 + c, "tensor": tensor} for k in range(1, ZS)]

    def remote(src, dst, send, recv_sem, where):
        return pltpu.make_async_remote_copy(
            src_ref=src, dst_ref=dst, send_sem=send, recv_sem=recv_sem,
            device_id=where, device_id_type=MESH,
        )

    barrier = pltpu.get_barrier_semaphore()
    for where in [at_x, at_y, at_c] + at_z:
        pl.semaphore_signal(barrier, inc=1, device_id=where, device_id_type=MESH)
    pl.semaphore_wait(barrier, 6)

    sent = []

    def go_on(copy):
        copy.start()
        sent.append(copy)

    args = [wq, wo, wu, wd, vec]

    def place(m, yy, d):
        if m == QKV:
            return w_qkv.at[:, span(d, 128), span(yy, 256)]
        if m == OUT:
            return w_out.at[span(yy, 256), span(d, 128)]
        if m == UP:
            return w_up.at[span(d, 128), span(yy, 1024)]
        if m == DOWN:
            return w_down.at[span(yy, 1024), span(d, 128)]
        return w_vec.at[d]

    def from_z(k):
        return lax.rem(z + ZS - k, ZS)

    def z_copy(m, k):
        return remote(args[m], place(m, y, dp), wsz.at[m, k - 1], wrz.at[m, k - 1], at_z[k - 1])

    def z_arrived(m, k):
        here = place(m, y, from_z(k) * 2 + c)
        remote(args[m], here, wsz.at[m, k - 1], wrz.at[m, k - 1], at_z[k - 1]).wait_recv()

    def y_copy(m, j):
        if j == 0:
            return remote(args[m], place(m, y, dp), wsy.at[m, 0], wry.at[m, 0], at_y)
        here = place(m, y, from_z(j) * 2 + c)
        return remote(here, here, wsy.at[m, j], wry.at[m, j], at_y)

    def y_place(m, j):
        return place(m, 1 - y, (z if j == 0 else from_z(j)) * 2 + c)

    def y_arrived(m, j):
        here = y_place(m, j)
        remote(here, here, wsy.at[m, j], wry.at[m, j], at_y).wait_recv()

    def c_copy(m, j):
        if j == 0:
            return remote(args[m], place(m, y, dp), wsc.at[m, 0], wrc.at[m, 0], at_c)
        here = place(m, y, from_z(j) * 2 + c) if j < 4 else y_place(m, j - 4)
        return remote(here, here, wsc.at[m, j], wrc.at[m, j], at_c)

    def c_arrived(m, j):
        d = (z if j == 0 or j == 4 else from_z(j % 4)) * 2 + 1 - c
        here = place(m, y if j < 4 else 1 - y, d)
        remote(here, here, wsc.at[m, j], wrc.at[m, j], at_c).wait_recv()

    def serve_z(m, ks=(1, 2, 3)):
        for k in ks:
            z_arrived(m, k)
            if m != VEC:
                go_on(y_copy(m, k))
            go_on(c_copy(m, k))

    def serve_y(m):
        for j in range(4):
            y_arrived(m, j)
            go_on(c_copy(m, j + 4))

    def wait_weight(m):
        if m != VEC:
            pltpu.make_async_copy(args[m], place(m, y, dp), ls.at[m]).wait()
        else:
            pltpu.make_async_copy(args[m], place(m, y, dp), ls.at[m]).wait()
        for j in range(4 if m == VEC else 8):
            c_arrived(m, j)

    def x_copy(kind, j, src, dst):
        return remote(src, dst, xs.at[kind, j], xr.at[kind, j], at_x)

    def tok_rows(xx, yy):
        return pl.ds(pl.multiple_of(xx * ROWS + yy * CHUNK, CHUNK), CHUNK)

    y_tok = remote(tok.at[1 - y], xw.at[tok_rows(x, y)], ys.at[Y_TOK], yr.at[Y_TOK], at_y)
    go_on(y_tok)
    go_on(x_copy(X_TOK, 0, tok.at[y], xw.at[tok_rows(x, y)]))
    local_x = pltpu.make_async_copy(tok.at[y], xw.at[tok_rows(x, y)], ls.at[5])
    local_x.start()
    for m in (QKV, VEC, OUT, UP, DOWN):
        for k in range(1, ZS):
            go_on(z_copy(m, k))
        if m == QKV:
            go_on(y_copy(m, 0))
        go_on(c_copy(m, 0))
        pltpu.make_async_copy(args[m], place(m, y, dp), ls.at[m]).start()
    local_cot = pltpu.make_async_copy(cot.at[y], cotb.at[span(y, CHUNK)], ls.at[6])
    local_cot.start()

    seg_row = seg[pl.ds(y, 1), :].astype(F32)
    blocks = [(p % 2) * 2 + p // 2 for p in range(4)]
    across = [jnp.broadcast_to(seg_row[:, n * 128:(n + 1) * 128], (128, 128)) for n in blocks]
    down = [b.T for b in across]
    for t in range(2):
        for i, q in enumerate((t, t + 2)):
            for j in range(3):
                same = down[q] == across[t + j]
                bias[t, i * 128:(i + 1) * 128, j * 128:(j + 1) * 128] = jnp.where(same, 0.0, MASKED)
    acc[...] = jnp.zeros_like(acc)
    vg[...] = jnp.zeros_like(vg)

    y_tok_here = xw.at[tok_rows(x, 1 - y)]
    remote(tok.at[1 - y], y_tok_here, ys.at[Y_TOK], yr.at[Y_TOK], at_y).wait_recv()
    go_on(x_copy(X_TOK, 1, y_tok_here, y_tok_here))
    serve_z(QKV)
    serve_z(VEC)
    go_on(y_copy(OUT, 0))
    serve_z(OUT)
    go_on(y_copy(UP, 0))
    serve_y(QKV)
    wait_weight(VEC)
    for d in range(8):
        vf[0:12, d * 128:(d + 1) * 128] = w_vec[d].astype(F32)
    local_x.wait()
    for j, yy in ((0, y), (1, 1 - y)):
        there = xw.at[tok_rows(1 - x, yy)]
        x_copy(X_TOK, j, there, there).wait_recv()
    wait_weight(QKV)

    zero_bias = jnp.zeros((1, COLS), F32)

    def head_bias(row):
        parts = [vf[row:row + 1, pl.ds(pl.multiple_of(yy * 512 + x * 256, 256), 256)] for yy in range(2)]
        return jnp.concatenate(parts, axis=1)

    for i in range(3):
        value = contract(xw[...], w_qkv[i], 1, 0)
        if i == 0:
            value = (value + head_bias(0)).astype(BF) * BF(HD ** -0.5)
        elif i == 2:
            value = value + head_bias(1)
        qkv[i] = value.astype(BF)

    low_half = lax.broadcasted_iota(jnp.int32, (1, 128), 1) < HD
    halves = (low_half, jnp.logical_not(low_half))
    none = jnp.zeros((), BF)

    def two_blocks(ref, t, lanes):
        return jnp.concatenate([ref[span(t, 128), lanes], ref[span(t + 2, 128), lanes]], axis=0)

    def attend(index, carry):
        pair, t = index // 2, index % 2
        lanes = span(pair, 128)
        keys = pl.ds(pl.multiple_of(t * 128, 128), WINDOW)
        query = two_blocks(qkv.at[0], t, lanes)
        key, value = qkv[1, keys, lanes], qkv[2, keys, lanes]
        total = jnp.zeros((ROWS, 128), F32)
        for h, half in enumerate(halves):
            scores = contract(jnp.where(half, query, none), key, 1, 1) + bias[t]
            top = jnp.max(scores, axis=1, keepdims=True)
            weight = jnp.exp(scores - top)
            share_of = 1.0 / jnp.sum(weight, axis=1, keepdims=True)
            weight = (weight * share_of).astype(BF)
            prob[pair * 4 + t * 2 + h] = weight
            total = total + contract(weight, jnp.where(half, value, none), 1, 0)
        total = total.astype(BF)
        ctx[span(t, 128), lanes] = total[:128]
        ctx[span(t + 2, 128), lanes] = total[128:]
        return carry

    lax.fori_loop(0, 8, attend, 0)

    def rows_of(s):
        mine = jnp.where(s < 2, x, 1 - x)
        return pl.ds(pl.multiple_of(mine * ROWS + lax.rem(s, 2) * CHUNK, CHUNK), CHUNK)

    def x_sum(kind, j):
        return x_copy(kind, j, stage.at[span(j, CHUNK)], recv.at[span(j, CHUNK)])

    def x_rows(kind, j, buf):
        here = buf.at[pl.ds(pl.multiple_of(x * ROWS + j * CHUNK, CHUNK), CHUNK)]
        return x_copy(kind, j, here, here)

    def hand_over(kind, before, s, value):
        @pl.when(s < 2)
        def _():
            own[span(s, CHUNK), :] = value

        @pl.when(s >= 2)
        def _():
            if before is not None:
                x_sum(before, s - 2).wait_send()
            stage[span(s - 2, CHUNK), :] = value.astype(BF)
            x_sum(kind, s - 2).start()

    serve_y(OUT)
    serve_z(UP, (1,))
    wait_weight(OUT)

    def mix(i, carry):
        s = lax.rem(i + 2, 4)
        hand_over(X_MIX, None, s, contract(ctx[rows_of(s), :], w_out[...], 1, 0))
        return carry

    lax.fori_loop(0, 4, mix, 0)
    serve_z(UP, (2, 3))
    go_on(y_copy(DOWN, 0))

    def row_of(row):
        return vf[row:row + 1, :]

    def normed(value):
        centred = value - jnp.mean(value, axis=1, keepdims=True)
        inverse = lax.rsqrt(jnp.mean(centred * centred, axis=1, keepdims=True) + NORM_EPS)
        return centred * inverse, inverse

    def norm_back(normal, inverse, grad):
        first = jnp.mean(grad, axis=1, keepdims=True)
        second = jnp.mean(grad * normal, axis=1, keepdims=True)
        return inverse * (grad - first - normal * second)

    def tiles(j, body):
        def step(i, carry):
            body(pl.ds(pl.multiple_of(j * CHUNK + i * TILE, TILE), TILE),
                 pl.ds(pl.multiple_of(x * ROWS + j * CHUNK + i * TILE, TILE), TILE))
            return carry
        lax.fori_loop(0, CHUNK // TILE, step, 0)

    def first_norm(r, g):
        summed = xw[g, :].astype(F32) + own[r, :] + recv[r, :].astype(F32) + row_of(R_BO)
        normal, inverse = normed(summed)
        n1[r, :] = normal
        inv1[r, :] = jnp.broadcast_to(inverse, (TILE, 128))
        hw[g, :] = (normal * row_of(R_G1) + row_of(R_C1)).astype(BF)

    for j in range(2):
        x_sum(X_MIX, j).wait_recv()
        tiles(j, first_norm)
        x_rows(X_NORM, j, hw).start()

    serve_y(UP)
    serve_z(DOWN)
    wait_weight(UP)

    def arrived(kind, s, buf):
        @pl.when(s >= 2)
        def _():
            there = buf.at[rows_of(s)]
            x_copy(kind, s - 2, there, there).wait_recv()

    def up_bias(n):
        return vf[pl.ds(8 + n * 2 + x, 1), :]

    def ffn_up(s, carry):
        rows = rows_of(s)
        arrived(X_NORM, s, hw)
        for n in range(2):
            pre = contract(hw[rows, :], w_up[:, n * 1024:(n + 1) * 1024], 1, 0) + up_bias(n)
            cdf = 0.5 * (1.0 + lax.erf(pre * SQRT_HALF))
            act[rows, n * 1024:(n + 1) * 1024] = (pre * cdf).astype(BF)
            slope[rows, n * 1024:(n + 1) * 1024] = (
                cdf + pre * INV_ROOT_TAU * jnp.exp(-0.5 * pre * pre)
            ).astype(BF)
        return carry

    lax.fori_loop(0, 4, ffn_up, 0)
    go_on(remote(cot.at[1 - y], cotb.at[span(y, CHUNK)], ys.at[Y_COT], yr.at[Y_COT], at_y))
    serve_y(DOWN)
    wait_weight(DOWN)

    def ffn_down(i, carry):
        s = lax.rem(i + 2, 4)
        hand_over(X_FFN, X_MIX, s, contract(act[rows_of(s), :], w_down[...], 1, 0))
        return carry

    lax.fori_loop(0, 4, ffn_down, 0)

    def bump(row, value):
        acc[row] += fold_rows(value)

    def second_norm(r, g):
        h1 = n1[r, :] * row_of(R_G1) + row_of(R_C1)
        normal, inverse = normed(h1 + own[r, :] + recv[r, :].astype(F32) + row_of(R_BD))
        outb[r, :] = (normal * row_of(R_G2) + row_of(R_C2)).astype(BF)
        dy = cotb[r, :].astype(F32)
        bump(R_G2, dy * normal)
        bump(R_C2, dy)
        grad = norm_back(normal, inverse, dy * row_of(R_G2))
        bump(R_BD, grad)
        da[r, :] = grad
        aw[g, :] = grad.astype(BF)

    local_cot.wait()
    cot_here = cotb.at[span(1 - y, CHUNK)]
    remote(cot.at[1 - y], cot_here, ys.at[Y_COT], yr.at[Y_COT], at_y).wait_recv()
    for j in range(2):
        x_sum(X_FFN, j).wait_recv()
        tiles(j, second_norm)
        x_rows(X_DA2, j, aw).start()
    out_here = pltpu.make_async_copy(outb.at[span(y, CHUNK)], out.at[y], os.at[0])
    out_here.start()
    go_on(remote(outb.at[span(1 - y, CHUNK)], out.at[y], ys.at[Y_OUT], yr.at[Y_OUT], at_y))

    def ffn_back(s, carry):
        rows = rows_of(s)
        arrived(X_DA2, s, aw)
        for n in range(2):
            cols = slice(n * 1024, (n + 1) * 1024)
            grad = contract(aw[rows, :], w_down[cols, :], 1, 1) * slope[rows, cols].astype(F32)
            bump(R_BU + n, grad)
            slope[rows, cols] = grad.astype(BF)
        hand_over(X_DH, X_FFN, s, contract(slope[rows, :], w_up[...], 1, 1))
        return carry

    lax.fori_loop(0, 4, ffn_back, 0)

    units = {
        U_DOWN: (g_down, c_down, y_down, z_down, o_down, gd),
        U_UP: (g_up, c_up, y_up, z_up, o_up, gu),
        U_OUT: (g_out, c_out, y_out, z_out, o_out, go),
        U_Q: tuple(r.at[0] for r in (g_qkv, c_qkv, y_qkv, z_qkv, o_qkv, gq)),
        U_K: tuple(r.at[1] for r in (g_qkv, c_qkv, y_qkv, z_qkv, o_qkv, gq)),
        U_V: tuple(r.at[2] for r in (g_qkv, c_qkv, y_qkv, z_qkv, o_qkv, gq)),
    }

    def core_copy(u):
        g, rc = units[u][0], units[u][1]
        return remote(g.at[1 - c], rc, gsc.at[u], grc.at[u], at_c)

    def y_part(u):
        g, ry = units[u][0], units[u][2]
        return remote(g.at[c, 1 - y], ry, gsy.at[u], gry.at[u], at_y)

    def z_part(u, k):
        g, rz = units[u][0], units[u][3]
        to = lax.rem(z + k, ZS)
        return remote(g.at[c, y, to], rz.at[k - 1], gsz.at[u, k - 1], grz.at[u, k - 1], at_z[k - 1])

    def add_pieces(g, yy, other):
        for zz in range(ZS):
            rows = g.shape[3]
            def step(i, carry):
                r = span(i, TILE)
                g[c, yy, zz, r, :] = (
                    g[c, yy, zz, r, :].astype(F32) + other[zz, r, :].astype(F32)
                ).astype(BF)
                return carry
            lax.fori_loop(0, rows // TILE, step, 0)

    def send_core(u):
        go_on(core_copy(u))

    def send_y(u):
        g, rc = units[u][0], units[u][1]
        core_copy(u).wait_recv()
        add_pieces(g, 1 - y, rc.at[1 - y])
        go_on(y_part(u))
        add_pieces(g, y, rc.at[y])

    def send_z(u):
        g, ry = units[u][0], units[u][2]
        y_part(u).wait_recv()
        add_pieces(g, y, ry)
        for k in range(1, ZS):
            go_on(z_part(u, k))

    finals = []

    def finish(u):
        g, _, _, rz, o, dest = units[u]
        for k in range(1, ZS):
            z_part(u, k).wait_recv()
        rows = g.shape[3]
        def step(i, carry):
            r = span(i, TILE)
            value = g[c, y, z, r, :].astype(F32)
            for k in range(ZS - 1):
                value = value + rz[k, r, :].astype(F32)
            o[r, :] = value
            return carry
        lax.fori_loop(0, rows // TILE, step, 0)
        copy = pltpu.make_async_copy(o, dest, os.at[1 + u])
        copy.start()
        finals.append(copy)

    def grad_down(i, carry):
        value = contract(act[:, span(i, 512)], aw[...], 0, 0).astype(BF)
        for d in range(8):
            g_down[d % 2, i // 2, d // 2, span(i % 2, 512), :] = value[:, d * 128:(d + 1) * 128]
        return carry

    lax.fori_loop(0, 4, grad_down, 0)
    send_core(U_DOWN)

    def grad_up(index, carry):
        i, n = index // 2, index % 2
        value = contract(hw[:, span(i, 512)], slope[:, span(n, 1024)], 0, 0).astype(BF)
        for d in range(4):
            g_up[d % 2, n, i * 2 + d // 2] = value[d * 128:(d + 1) * 128, :]
        return carry

    lax.fori_loop(0, 4, grad_up, 0)
    send_core(U_UP)
    send_y(U_DOWN)

    def back_norm(r, g):
        grad = da[r, :] + own[r, :] + recv[r, :].astype(F32)
        normal = n1[r, :]
        bump(R_G1, grad * normal)
        bump(R_C1, grad)
        grad = norm_back(normal, inv1[r, 0:1], grad * row_of(R_G1))
        bump(R_BO, grad)
        da[r, :] = grad
        a1w[g, :] = grad.astype(BF)

    for j in range(2):
        x_sum(X_DH, j).wait_recv()
        tiles(j, back_norm)
        x_rows(X_DA1, j, a1w).start()

    send_y(U_UP)

    def ctx_back(s, carry):
        rows = rows_of(s)
        arrived(X_DA1, s, a1w)
        dctx[rows, :] = contract(a1w[rows, :], w_out[...], 1, 1).astype(BF)
        return carry

    lax.fori_loop(0, 4, ctx_back, 0)

    def attend_back(pair, carry):
        lanes = span(pair, 128)
        for t in range(2):
            keys = pl.ds(t * 128, WINDOW)
            query = two_blocks(qkv.at[0], t, lanes)
            key, value = qkv[1, keys, lanes], qkv[2, keys, lanes]
            grad = two_blocks(dctx, t, lanes)
            product = grad.astype(F32) * two_blocks(ctx, t, lanes).astype(F32)
            grad_q = jnp.zeros((ROWS, 128), F32)
            grad_k = jnp.zeros((WINDOW, 128), F32)
            grad_v = jnp.zeros((WINDOW, 128), F32)
            for h, half in enumerate(halves):
                grad_h = jnp.where(half, grad, none)
                weight = prob[pair * 4 + t * 2 + h]
                row_dot = jnp.sum(jnp.where(half, product, 0.0), axis=1, keepdims=True)
                score = (weight.astype(F32) * (contract(grad_h, value, 1, 1) - row_dot)).astype(BF)
                grad_q = grad_q + contract(score, jnp.where(half, key, none), 1, 0)
                grad_k = grad_k + contract(score, jnp.where(half, query, none), 0, 0)
                grad_v = grad_v + contract(weight, grad_h, 0, 0)
            grad_q = grad_q * (HD ** -0.5)
            acc[R_BQ, :, lanes] += fold_rows(grad_q)
            acc[R_BV, :, lanes] += fold_rows(grad_v)
            grad_q = grad_q.astype(BF)
            qkv[0, t * 128:t * 128 + 128, lanes] = grad_q[:128]
            qkv[0, t * 128 + 256:t * 128 + 384, lanes] = grad_q[128:]
            if t == 0:
                acc_k[0:WINDOW, :] = grad_k
                acc_v[0:WINDOW, :] = grad_v
                acc_k[WINDOW:SEQ, :] = jnp.zeros((128, 128), F32)
                acc_v[WINDOW:SEQ, :] = jnp.zeros((128, 128), F32)
            else:
                for i, total, more in ((1, acc_k, grad_k), (2, acc_v, grad_v)):
                    qkv[i, 0:128, lanes] = total[0:128, :].astype(BF)
                    qkv[i, 128:SEQ, lanes] = (total[128:SEQ, :] + more).astype(BF)
        return carry

    lax.fori_loop(0, 4, attend_back, 0)

    def input_back(i, carry):
        s = lax.rem(i + 2, 4)
        rows = rows_of(s)
        value = contract(qkv[0, rows, :], w_qkv[0], 1, 1)
        value = value + contract(qkv[1, rows, :], w_qkv[1], 1, 1)
        value = value + contract(qkv[2, rows, :], w_qkv[2], 1, 1)
        hand_over(X_DX, X_DH, s, value)
        return carry

    lax.fori_loop(0, 4, input_back, 0)

    def grad_qkv(index, carry):
        kind, i = index // 2, index % 2
        value = contract(xw[:, span(i, 512)], qkv[kind], 0, 0).astype(BF)
        for d in range(4):
            for yy in range(2):
                g_qkv[kind, d % 2, yy, i * 2 + d // 2] = (
                    value[d * 128:(d + 1) * 128, yy * 256:(yy + 1) * 256]
                )
        return carry

    def grad_out():
        value = contract(ctx[...], a1w[...], 0, 0).astype(BF)
        for d in range(8):
            for yy in range(2):
                g_out[d % 2, yy, d // 2] = value[yy * 256:(yy + 1) * 256, d * 128:(d + 1) * 128]

    grad_out()
    send_core(U_OUT)
    for kind, u in ((0, U_Q), (1, U_K), (2, U_V)):
        lax.fori_loop(kind * 2, kind * 2 + 2, grad_qkv, 0)
        send_core(u)

    def vec_piece(d):
        return vg.at[d % 2, d // 2]

    for row in range(2, 8):
        line = jnp.sum(acc[row], axis=0, keepdims=True)
        for d in range(8):
            vg[d % 2, d // 2, row:row + 1, :] = line[:, d * 128:(d + 1) * 128]
    for n in range(2):
        line = jnp.sum(acc[R_BU + n], axis=0, keepdims=True)
        for d in range(8):
            vg[d % 2, d // 2, pl.ds(8 + n * 2 + x, 1), :] = line[:, d * 128:(d + 1) * 128]
    for row, source in ((0, R_BQ), (1, R_BV)):
        line = jnp.sum(acc[source], axis=0, keepdims=True)
        for yy in range(2):
            for half in range(2):
                vg[half, 2 * yy + x, row:row + 1, :] = (
                    line[:, yy * 256 + half * 128:yy * 256 + (half + 1) * 128]
                )
    vec_x = remote(vg, vgx, vs.at[0], vr.at[0], at_x)
    vec_c = remote(vg.at[1 - c], vgc, vs.at[1], vr.at[1], at_c)
    vec_y = remote(vg.at[c], vgy, vs.at[2], vr.at[2], at_y)

    def vec_z(k):
        to = lax.rem(z + k, ZS)
        return remote(vg.at[c, to], vgz.at[k - 1], vs.at[2 + k], vr.at[2 + k], at_z[k - 1])

    vec_x.start()
    send_y(U_OUT)
    send_z(U_DOWN)
    send_y(U_Q)
    vec_x.wait()
    vg[...] = vg[...] + vgx[...]
    vec_c.start()
    send_y(U_K)
    send_y(U_V)
    vec_c.wait()
    vg[c] = vg[c] + vgc[...]
    vec_y.start()
    send_z(U_UP)

    def last_sum(j, other):
        x_sum(X_DX, j).wait_recv()

        def body(r, g):
            value = da[r, :] + own[r, :] + recv[r, :].astype(F32)
            if other:
                gts[pl.ds(pl.multiple_of(r.start - j * CHUNK, TILE), TILE), :] = value.astype(BF)
            else:
                da[r, :] = value
        tiles(j, body)

    last_sum(1 - y, True)
    go_on(remote(gts, gtr, ys.at[Y_GTOK], yr.at[Y_GTOK], at_y))
    last_sum(y, False)
    gtok_here = pltpu.make_async_copy(da.at[span(y, CHUNK)], gtok.at[y], os.at[7])
    gtok_here.start()
    vec_y.wait()
    vg[c] = vg[c] + vgy[...]
    for k in range(1, ZS):
        vec_z(k).start()
    send_z(U_OUT)
    send_z(U_Q)
    send_z(U_K)
    send_z(U_V)
    finish(U_DOWN)
    finish(U_UP)
    for k in range(1, ZS):
        vec_z(k).wait()
    gvb[...] = vg[c, z] + vgz[0] + vgz[1] + vgz[2]
    vec_here = pltpu.make_async_copy(gvb.at[0:12], gv, os.at[8])
    vec_here.start()
    remote(gts, gtr, ys.at[Y_GTOK], yr.at[Y_GTOK], at_y).wait_recv()
    gtf[...] = gtr[...].astype(F32)
    gtok_there = pltpu.make_async_copy(gtf, gtok.at[1 - y], os.at[9])
    gtok_there.start()
    finish(U_OUT)
    finish(U_Q)
    finish(U_K)
    finish(U_V)
    remote(outb.at[span(1 - y, CHUNK)], out.at[1 - y], ys.at[Y_OUT], yr.at[Y_OUT], at_y).wait_recv()
    for kind, buf in ((X_NORM, hw), (X_DA2, aw), (X_DA1, a1w)):
        for j in range(2):
            x_rows(kind, j, buf).wait_send()
    for j in range(2):
        x_sum(X_DX, j).wait_send()
    for copy in sent:
        copy.wait_send()
    for copy in finals + [out_here, gtok_here, gtok_there, vec_here]:
        copy.wait()


def layer(tokens, segment_ids, w_qkv, w_out, w_up, w_down, vectors, cotangent):
    vmem, dma = pltpu.VMEM, pltpu.SemaphoreType.DMA
    outs = (
        jax.ShapeDtypeStruct(tokens.shape, BF),
        jax.ShapeDtypeStruct(tokens.shape, F32),
        jax.ShapeDtypeStruct(w_qkv.shape, F32),
        jax.ShapeDtypeStruct(w_out.shape, F32),
        jax.ShapeDtypeStruct(w_up.shape, F32),
        jax.ShapeDtypeStruct(w_down.shape, F32),
        jax.ShapeDtypeStruct(vectors.shape, F32),
    )
    pieces = ((1024, 128), (128, 1024), (256, 128), (128, 256))
    lead = ((), (), (), (3,))
    scratch = [
        vmem((3, D, COLS), BF), vmem((COLS, D), BF), vmem((D, HID), BF), vmem((HID, D), BF),
        vmem((8, 12, 128), BF), vmem((16, D), F32),
    ]
    for shape in ((2, 2, 4), (2, 4), (4,), (3,)):
        scratch += [vmem(first + shape + piece, BF) for first, piece in zip(lead, pieces)]
    scratch += [vmem((3, 128, 256), F32), vmem((256, 128), F32), vmem((128, 1024), F32), vmem((1024, 128), F32)]
    scratch += [
        vmem((SEQ, D), BF), vmem((3, SEQ, COLS), BF), vmem((SEQ, COLS), BF),
        vmem((16, ROWS, WINDOW), BF), vmem((2, ROWS, WINDOW), F32), vmem((SEQ, D), BF),
        vmem((SEQ, HID), BF), vmem((SEQ, HID), BF), vmem((SEQ, D), BF), vmem((SEQ, D), BF),
        vmem((SEQ, COLS), BF),
        vmem((ROWS, D), F32), vmem((ROWS, D), F32), vmem((ROWS, D), F32), vmem((ROWS, 128), F32),
        vmem((ROWS, D), BF), vmem((ROWS, D), BF), vmem((ROWS, D), BF), vmem((ROWS, D), BF),
        vmem((CHUNK, D), BF), vmem((CHUNK, D), BF), vmem((CHUNK, D), F32),
        vmem((12, 8, D), F32),
        vmem((2, 4, 16, 128), F32), vmem((2, 4, 16, 128), F32), vmem((4, 16, 128), F32),
        vmem((4, 16, 128), F32), vmem((3, 16, 128), F32), vmem((16, 128), F32),
        vmem((SEQ, 128), F32), vmem((SEQ, 128), F32),
        dma((5, 3)), dma((5, 3)), dma((4, 4)), dma((4, 4)), dma((5, 8)), dma((5, 8)),
        dma((8, 2)), dma((8, 2)), dma((4,)), dma((4,)),
        dma((6,)), dma((6,)), dma((6,)), dma((6,)), dma((6, 3)), dma((6, 3)),
        dma((6,)), dma((6,)), dma((7,)), dma((10,)),
    ]
    hbm = pl.BlockSpec(memory_space=pl.ANY)
    return pl.pallas_call(
        layer_kernel,
        out_shape=outs,
        in_specs=[hbm, pl.BlockSpec(memory_space=pltpu.VMEM)] + [hbm] * 6,
        out_specs=[hbm] * 7,
        scratch_shapes=scratch,
        compiler_params=pltpu.CompilerParams(
            collective_id=0, has_side_effects=True, vmem_limit_bytes=67043328
        ),
    )(tokens, segment_ids, w_qkv, w_out, w_up, w_down, vectors, cotangent)


def solution(mesh):
    step = layer if (mesh.shape["dp"], mesh.shape["tensor"]) == (8, 4) else body
    return jax.shard_map(
        step,
        mesh=mesh,
        in_specs=(
            P("dp", "tensor", None),
            P("dp", None),
            P(None, "dp", "tensor"),
            P("tensor", "dp"),
            P("dp", "tensor"),
            P("tensor", "dp"),
            P(None, "dp"),
            P("dp", "tensor", None),
        ),
        out_specs=(
            P("dp", "tensor", None),
            P("dp", "tensor", None),
            P(None, "dp", "tensor"),
            P("tensor", "dp"),
            P("dp", "tensor"),
            P("tensor", "dp"),
            P(None, "dp"),
        ),
        check_vma=False,
    )
```

```python
import jax
import jax.numpy as jnp
from jax import lax
from jax.experimental import pallas as pl
from jax.experimental.pallas import tpu as pltpu
from jax.sharding import PartitionSpec as P

D = 1024
FF = 4096
HD = 64


NORM_EPS = 1e-06
SQRT_HALF = 0.7071067811865476
INV_ROOT_TAU = 0.3989422804014327
MASKED = -1e30


def gelu_value(pre_act):
    return 0.5 * pre_act * (1.0 + lax.erf(pre_act * SQRT_HALF))


def gelu_slope(pre_act):
    return 0.5 * (1.0 + lax.erf(pre_act * SQRT_HALF)) + pre_act * INV_ROOT_TAU * jnp.exp(
        -0.5 * pre_act * pre_act
    )


def norm_forward(summed, gain, shift):
    centred = summed - jnp.mean(summed, axis=-1, keepdims=True)
    inverse = lax.rsqrt(jnp.mean(centred * centred, axis=-1, keepdims=True) + NORM_EPS)
    normed = centred * inverse
    return (normed * gain + shift, normed, inverse)


def norm_backward(normed, inverse, grad_normed):
    first_mean = jnp.mean(grad_normed, axis=-1, keepdims=True)
    second_mean = jnp.mean(grad_normed * normed, axis=-1, keepdims=True)
    return inverse * (grad_normed - first_mean - normed * second_mean)


def attention_scores(query_heads, key_heads, segments):
    same_doc = segments[:, None] == segments[None, :]
    scores = jnp.einsum(
        "qhe,khe->hqk", query_heads, key_heads, preferred_element_type=jnp.float32
    ) * HD ** (-0.5)
    return jnp.where(same_doc[None], scores, MASKED)


def collect(w_qkv, w_out, w_up, w_down, vectors):
    return (
        lax.all_gather(w_qkv, "dp", axis=1, tiled=True),
        lax.all_gather(w_out, "dp", axis=1, tiled=True),
        lax.all_gather(w_up, "dp", axis=0, tiled=True),
        lax.all_gather(w_down, "dp", axis=1, tiled=True),
        lax.all_gather(vectors, "dp", axis=1, tiled=True),
    )


def share(gradients):
    return (
        lax.psum_scatter(
            gradients[0].astype(jnp.bfloat16), "dp", scatter_dimension=1, tiled=True
        ).astype(jnp.float32),
        lax.psum_scatter(
            gradients[1].astype(jnp.bfloat16), "dp", scatter_dimension=1, tiled=True
        ).astype(jnp.float32),
        lax.psum_scatter(
            gradients[2].astype(jnp.bfloat16), "dp", scatter_dimension=0, tiled=True
        ).astype(jnp.float32),
        lax.psum_scatter(
            gradients[3].astype(jnp.bfloat16), "dp", scatter_dimension=1, tiled=True
        ).astype(jnp.float32),
        lax.psum_scatter(
            gradients[4].astype(jnp.bfloat16), "dp", scatter_dimension=1, tiled=True
        ).astype(jnp.float32),
    )


def body(tokens, segment_ids, w_qkv, w_out, w_up, w_down, vectors, cotangent):
    tensor_rank = lax.axis_index("tensor")
    local_cols = w_qkv.shape[2]
    head_count = local_cols // HD
    hidden = w_up.shape[1]
    col_start = tensor_rank * local_cols
    ffn_start = tensor_rank * hidden

    def forward(weights, tok_block, segments):
        qkv_w, out_w, up_w, down_w, vec_b = weights
        vec_f32 = vec_b.astype(jnp.float32)
        whole = lax.all_gather(tok_block, "tensor", axis=0, tiled=True)
        seq_len = whole.shape[0]
        projected = jnp.einsum("sd,tdc->tsc", whole, qkv_w, preferred_element_type=jnp.float32)
        bias_q = lax.dynamic_slice_in_dim(vec_f32[0], col_start, local_cols)
        bias_v = lax.dynamic_slice_in_dim(vec_f32[1], col_start, local_cols)
        query_heads = (projected[0] + bias_q).astype(jnp.bfloat16).reshape(seq_len, head_count, HD)
        key_heads = projected[1].astype(jnp.bfloat16).reshape(seq_len, head_count, HD)
        value_heads = (projected[2] + bias_v).astype(jnp.bfloat16).reshape(seq_len, head_count, HD)
        scores = attention_scores(query_heads, key_heads, segments)
        row_top = jnp.max(scores, axis=-1, keepdims=True)
        log_total = row_top + jnp.log(jnp.sum(jnp.exp(scores - row_top), axis=-1, keepdims=True))
        attn_probs = jnp.exp(scores - log_total).astype(jnp.bfloat16)
        context = jnp.einsum(
            "hqk,khe->qhe", attn_probs, value_heads, preferred_element_type=jnp.float32
        )
        context = context.reshape(seq_len, local_cols).astype(jnp.bfloat16)
        piece = context
        attn_mixed = lax.psum_scatter(
            jnp.dot(piece, out_w, preferred_element_type=jnp.float32).astype(jnp.bfloat16),
            "tensor",
            scatter_dimension=0,
            tiled=True,
        ).astype(jnp.float32)
        summed_one = tok_block.astype(jnp.float32) + attn_mixed + vec_f32[2]
        normed_out, normed_one, inverse_one = norm_forward(summed_one, vec_f32[3], vec_f32[4])
        normed_b = normed_out.astype(jnp.bfloat16)
        normed_whole = lax.all_gather(normed_b, "tensor", axis=0, tiled=True)
        bias_up = lax.dynamic_slice_in_dim(vec_f32[8:12].reshape(FF), ffn_start, hidden)
        pre_act = jnp.dot(normed_whole, up_w, preferred_element_type=jnp.float32) + bias_up
        activated = gelu_value(pre_act).astype(jnp.bfloat16)
        piece = activated
        summed_two = (
            normed_out
            + lax.psum_scatter(
                jnp.dot(piece, down_w, preferred_element_type=jnp.float32).astype(jnp.bfloat16),
                "tensor",
                scatter_dimension=0,
                tiled=True,
            ).astype(jnp.float32)
            + vec_f32[5]
        )
        final, normed_two, inverse_two = norm_forward(summed_two, vec_f32[6], vec_f32[7])
        saved = (
            whole,
            query_heads,
            key_heads,
            value_heads,
            log_total,
            context,
            normed_one,
            inverse_one,
            normed_whole,
            pre_act,
            activated,
            normed_two,
            inverse_two,
        )
        return (final.astype(jnp.bfloat16), saved)

    def backward(weights, saved, segments, grad_block):
        qkv_w, out_w, up_w, down_w, vec_b = weights
        vec_f32 = vec_b.astype(jnp.float32)
        (
            whole,
            query_heads,
            key_heads,
            value_heads,
            log_total,
            context,
            normed_one,
            inverse_one,
            normed_whole,
            pre_act,
            activated,
            normed_two,
            inverse_two,
        ) = saved
        seq_len = whole.shape[0]
        grad_final = grad_block.astype(jnp.float32)
        g_gain2 = jnp.sum(grad_final * normed_two, axis=0)
        g_shift2 = jnp.sum(grad_final, axis=0)
        grad_two = norm_backward(normed_two, inverse_two, grad_final * vec_f32[6])
        grad_two_b = grad_two.astype(jnp.bfloat16)
        g_bdown = jnp.sum(grad_two, axis=0)
        grad_two_whole = lax.all_gather(grad_two_b, "tensor", axis=0, tiled=True)
        g_down = jnp.dot(activated.T, grad_two_whole, preferred_element_type=jnp.float32)
        grad_pre = jnp.dot(
            grad_two_whole, down_w.T, preferred_element_type=jnp.float32
        ) * gelu_slope(pre_act)
        grad_pre_b = grad_pre.astype(jnp.bfloat16)
        g_bup = jnp.sum(grad_pre, axis=0)
        g_up = jnp.dot(normed_whole.T, grad_pre_b, preferred_element_type=jnp.float32)
        piece = grad_pre_b
        grad_one_in = grad_two + lax.psum_scatter(
            jnp.dot(piece, up_w.T, preferred_element_type=jnp.float32).astype(jnp.bfloat16),
            "tensor",
            scatter_dimension=0,
            tiled=True,
        ).astype(jnp.float32)
        g_gain1 = jnp.sum(grad_one_in * normed_one, axis=0)
        g_shift1 = jnp.sum(grad_one_in, axis=0)
        grad_one = norm_backward(normed_one, inverse_one, grad_one_in * vec_f32[3])
        grad_one_b = grad_one.astype(jnp.bfloat16)
        g_bout = jnp.sum(grad_one, axis=0)
        grad_one_whole = lax.all_gather(grad_one_b, "tensor", axis=0, tiled=True)
        g_out = jnp.dot(context.T, grad_one_whole, preferred_element_type=jnp.float32)
        grad_context = jnp.dot(grad_one_whole, out_w.T, preferred_element_type=jnp.float32).astype(
            jnp.bfloat16
        )
        grad_context = grad_context.reshape(seq_len, head_count, HD)
        scores = attention_scores(query_heads, key_heads, segments)
        attn_exact = jnp.exp(scores - log_total)
        attn_probs = attn_exact.astype(jnp.bfloat16)
        grad_probs = jnp.einsum(
            "qhe,khe->hqk", grad_context, value_heads, preferred_element_type=jnp.float32
        )
        row_dot = jnp.sum(attn_exact * grad_probs, axis=-1, keepdims=True)
        grad_scores = (attn_exact * (grad_probs - row_dot) * HD ** (-0.5)).astype(jnp.bfloat16)
        grad_value = jnp.einsum(
            "hqk,qhe->khe", attn_probs, grad_context, preferred_element_type=jnp.float32
        )
        grad_value = grad_value.reshape(seq_len, local_cols)
        grad_query = jnp.einsum(
            "hqk,khe->qhe", grad_scores, key_heads, preferred_element_type=jnp.float32
        )
        grad_query = grad_query.reshape(seq_len, local_cols)
        grad_key = jnp.einsum(
            "hqk,qhe->khe", grad_scores, query_heads, preferred_element_type=jnp.float32
        )
        grad_key = grad_key.reshape(seq_len, local_cols)
        grad_qkv = jnp.stack([grad_query, grad_key, grad_value]).astype(jnp.bfloat16)
        g_qkv = jnp.einsum("sd,tsc->tdc", whole, grad_qkv, preferred_element_type=jnp.float32)
        piece = grad_qkv
        grad_input = grad_one + lax.psum_scatter(
            jnp.einsum("tsc,tdc->sd", piece, qkv_w, preferred_element_type=jnp.float32).astype(
                jnp.bfloat16
            ),
            "tensor",
            scatter_dimension=0,
            tiled=True,
        ).astype(jnp.float32)
        zero_row = jnp.zeros((D,), jnp.float32)
        row_q = lax.dynamic_update_slice_in_dim(zero_row, jnp.sum(grad_query, axis=0), col_start, 0)
        row_v = lax.dynamic_update_slice_in_dim(zero_row, jnp.sum(grad_value, axis=0), col_start, 0)
        up_rows = lax.dynamic_update_slice_in_dim(
            jnp.zeros((FF,), jnp.float32), g_bup, ffn_start, 0
        ).reshape(4, D)
        first_rows = jnp.stack(
            [row_q, row_v, g_bout, g_gain1, g_shift1, g_bdown, g_gain2, g_shift2]
        )
        g_vec = jnp.concatenate([first_rows, up_rows], axis=0)
        return ((g_qkv, g_out, g_up, g_down, g_vec), grad_input)

    def one_batch(carried, batch_item):
        tok_block, segments, grad_block = batch_item
        forward_w = collect(w_qkv, w_out, w_up, w_down, vectors)
        final_b, saved = forward(forward_w, tok_block, segments)
        second = collect(w_qkv, w_out, w_up, w_down, vectors)
        gradients, grad_input = backward(second, saved, segments, grad_block)
        updated = jax.tree.map(jnp.add, carried, gradients)
        return (updated, (final_b, grad_input))

    initial = (
        jnp.zeros((3, D, local_cols), jnp.float32),
        jnp.zeros((local_cols, D), jnp.float32),
        jnp.zeros((D, hidden), jnp.float32),
        jnp.zeros((hidden, D), jnp.float32),
        jnp.zeros((12, D), jnp.float32),
    )
    carried, stacked = lax.scan(one_batch, initial, (tokens, segment_ids, cotangent))
    totals = share(carried)
    vector_grads = lax.psum(totals[4], "tensor")
    return (stacked[0], stacked[1], totals[0], totals[1], totals[2], totals[3], vector_grads)


Y_TOK, Y_COT, Y_OUT, Y_GTOK = range(4)
X_TOK, X_MIX, X_NORM, X_FFN, X_DA2, X_DH, X_DA1, X_DX = range(8)
W_Q, W_K, W_V, W_OUT, W_UP, W_DOWN, W_VEC = range(7)
Y_FIRST = (W_Q, W_OUT)
Z_FIRST = (0,)
U_DOWN, U_UP, U_OUT, U_V, U_K, U_Q = range(6)
R_BQ, R_BV, R_BO, R_G1, R_C1, R_BD, R_G2, R_C2, R_BU = range(9)
ZS = 4
SEQ = 512
ROWS = 256
CHUNK = 128
TILE = 32
COLS = 512
HID = 2048
WINDOW = 384
BF = jnp.bfloat16
F32 = jnp.float32
MESH = pl.DeviceIdType.MESH


def span(index, size):
    return pl.ds(pl.multiple_of(index * size, size), size)


def contract(a, b, a_dim, b_dim):
    return lax.dot_general(a, b, (((a_dim,), (b_dim,)), ((), ())), preferred_element_type=F32)


def fold_rows(value):
    return jnp.sum(value.reshape(value.shape[0] // 8, 8, value.shape[1]), axis=0)


def layer_kernel(
    tok, seg, wq, wo, wu, wd, vec, cot,
    out, gtok, gq, go, gu, gd, gv,
    w_qkv, w_out, w_up, w_down, w_vec, vf,
    g_down, g_up, g_out, g_qkv,
    c_down, c_up, c_out, c_qkv,
    y_down, y_up, y_out, y_qkv,
    z_down, z_up, z_out, z_qkv,
    h_down, h_up, h_out, h_qkv,
    o_qkv, o_out, o_up, o_down,
    xw, qkv, ctx, prob, bias, hw, act, slope, aw, a1w, dctx,
    own, n1, da, inv1, recv, stage, cotb, outb, gts, gtr, gtf,
    acc, vg, vgx, vgc, vgy, vgz, gvb, acc_k, acc_v,
    wsz, wrz, wsy, wry, wsc, wrc, xs, xr, ys, yr,
    gsc, grc, gsy, gry, gsz, grz, vs, vr, ls, os,
):
    dp = lax.axis_index("dp")
    tensor = lax.axis_index("tensor")
    z, c = dp // 2, dp % 2
    y, x = tensor // 2, tensor % 2
    at_x = {"dp": dp, "tensor": y * 2 + (1 - x)}
    at_y = {"dp": dp, "tensor": (1 - y) * 2 + x}
    at_c = {"dp": z * 2 + (1 - c), "tensor": tensor}

    def remote(src, dst, send, recv_sem, where):
        return pltpu.make_async_remote_copy(
            src_ref=src, dst_ref=dst, send_sem=send, recv_sem=recv_sem,
            device_id=where, device_id_type=MESH,
        )

    barrier = pltpu.get_barrier_semaphore()
    for where in [at_x, at_y, at_c] + [{"dp": lax.rem(z + k, ZS) * 2 + c, "tensor": tensor} for k in range(1, ZS)]:
        pl.semaphore_signal(barrier, inc=1, device_id=where, device_id_type=MESH)
    pl.semaphore_wait(barrier, 6)

    sent = []

    def go_on(copy):
        copy.start()
        sent.append(copy)

    args = [wq.at[0], wq.at[1], wq.at[2], wo, wu, wd, vec]
    edge = jnp.logical_or(z == 0, z == ZS - 1)
    middle = jnp.logical_not(edge)
    later = []

    def z_device(where):
        return {"dp": where * 2 + c, "tensor": tensor}

    def go_if(condition, copy):
        @pl.when(condition)
        def _():
            copy.start()
        later.append((condition, copy))

    def place(m, yy, d):
        if m <= W_V:
            return w_qkv.at[m, span(d, 128), span(yy, 256)]
        if m == W_OUT:
            return w_out.at[span(yy, 256), span(d, 128)]
        if m == W_UP:
            return w_up.at[span(d, 128), span(yy, 1024)]
        if m == W_DOWN:
            return w_down.at[span(yy, 1024), span(d, 128)]
        return w_vec.at[d]

    def from_z(k):
        return lax.rem(z + ZS - k, ZS)

    def column(r):
        return y if r == 0 else 1 - y

    def z_send(m, r):
        source = args[m] if r == 0 else place(m, 1 - y, dp)
        for k, there in ((1, z != ZS - 1), (3, z != 0), (2, None)):
            there = None if m == W_VEC else there
            copy = remote(
                source, place(m, column(r), dp), wsz.at[m, r, k - 1], wrz.at[m, r, k - 1],
                z_device(lax.rem(z + k, ZS)),
            )
            if there is None:
                go_on(copy)
            else:
                go_if(there, copy)

    def z_serve(m, r, step):
        k = (jnp.where(z == 0, 3, 1), 2, jnp.where(z == 0, 1, 3))[step]
        here = place(m, column(r), from_z(k) * 2 + c)
        remote(here, here, wsz.at[m, r, k - 1], wrz.at[m, r, k - 1], at_x).wait_recv()
        if step == 1 and m != W_VEC:
            slot = jnp.where(z == 1, 0, 2)
            go_if(middle, remote(
                here, here, wsz.at[m, r, 3], wrz.at[m, r, slot], z_device(jnp.where(z == 1, 0, 3)),
            ))
        if r == 0 and m not in Y_FIRST and m != W_VEC:
            go_on(remote(here, here, wsy.at[m, k], wry.at[m, from_z(k)], at_y))
        c_send(m, here)

    def y_send(m):
        go_on(remote(args[m], place(m, y, dp), wsy.at[m, 0], wry.at[m, z], at_y))

    def y_serve(m, step):
        zz = lax.rem(z + step, ZS)
        here = place(m, 1 - y, zz * 2 + c)
        remote(here, here, wsy.at[m, 0], wry.at[m, zz], at_y).wait_recv()
        c_send(m, here)

    def c_send(m, source, dest=None):
        dest = source if dest is None else dest
        remote(source, dest, wsc.at[m], wrc.at[m], at_c).start()

    def own_send(m):
        c_send(m, args[m], place(m, y, dp))
        pltpu.make_async_copy(args[m], place(m, y, dp), ls.at[m]).start()

    def half_of(m):
        if m <= W_V:
            return w_qkv.at[m, :, 0:256]
        return (w_out.at[0:256], w_up.at[:, 0:1024], w_down.at[0:1024], w_vec.at[0:4])[m - W_OUT]

    def wait_weight(m):
        pltpu.make_async_copy(args[m], place(m, y, dp), ls.at[m]).wait()
        remote(half_of(m), half_of(m), wsc.at[m], wrc.at[m], at_c).wait_recv()

    def x_copy(kind, j, src, dst):
        return remote(src, dst, xs.at[kind, j], xr.at[kind, j], at_x)

    def tok_rows(xx, yy):
        return pl.ds(pl.multiple_of(xx * ROWS + yy * CHUNK, CHUNK), CHUNK)

    for m in (W_Q, W_K, W_V):
        y_send(m)
        z_send(m, 0)
    y_send(W_OUT)
    go_on(remote(tok.at[1 - y], xw.at[tok_rows(x, y)], ys.at[Y_TOK], yr.at[Y_TOK], at_y))
    go_on(x_copy(X_TOK, 0, tok.at[y], xw.at[tok_rows(x, y)]))
    z_send(W_VEC, 0)
    for m in range(7):
        own_send(m)
    local_x = pltpu.make_async_copy(tok.at[y], xw.at[tok_rows(x, y)], ls.at[7])
    local_x.start()
    local_cot = pltpu.make_async_copy(cot.at[y], cotb.at[span(y, CHUNK)], ls.at[8])
    local_cot.start()

    seg_row = seg[pl.ds(y, 1), :].astype(F32)
    blocks = [(p % 2) * 2 + p // 2 for p in range(4)]
    across = [jnp.broadcast_to(seg_row[:, n * 128:(n + 1) * 128], (128, 128)) for n in blocks]
    down = [b.T for b in across]
    for t in range(2):
        for i, q in enumerate((t, t + 2)):
            for j in range(3):
                same = down[q] == across[t + j]
                bias[t, i * 128:(i + 1) * 128, j * 128:(j + 1) * 128] = jnp.where(same, 0.0, MASKED)
    acc[...] = jnp.zeros_like(acc)
    vg[...] = jnp.zeros_like(vg)

    y_serve(W_Q, 0)
    z_send(W_Q, 1)
    y_serve(W_OUT, 0)
    for step in range(2):
        for m in (W_K, W_V, W_Q):
            z_serve(m, 0, step)
    z_send(W_OUT, 0)
    z_send(W_OUT, 1)
    y_tok_here = xw.at[tok_rows(x, 1 - y)]
    remote(tok.at[1 - y], y_tok_here, ys.at[Y_TOK], yr.at[Y_TOK], at_y).wait_recv()
    go_on(x_copy(X_TOK, 1, y_tok_here, y_tok_here))
    z_serve(W_Q, 1, 0)
    z_serve(W_Q, 1, 1)
    for m in (W_K, W_V, W_Q):
        z_serve(m, 0, 2)
    z_serve(W_Q, 1, 2)
    z_send(W_UP, 0)
    y_send(W_UP)
    for r in range(2):
        for step in range(2):
            z_serve(W_OUT, r, step)
    for step in range(3):
        z_serve(W_VEC, 0, step)
    for step in range(4):
        y_serve(W_K, step)
        y_serve(W_V, step)
    wait_weight(W_VEC)
    for d in range(8):
        vf[0:12, d * 128:(d + 1) * 128] = w_vec[d].astype(F32)
    local_x.wait()
    for j, yy in ((0, y), (1, 1 - y)):
        there = xw.at[tok_rows(1 - x, yy)]
        x_copy(X_TOK, j, there, there).wait_recv()
    for m in (W_Q, W_K, W_V):
        wait_weight(m)

    def head_bias(row):
        parts = [vf[row:row + 1, pl.ds(pl.multiple_of(yy * 512 + x * 256, 256), 256)] for yy in range(2)]
        return jnp.concatenate(parts, axis=1)

    for i in range(3):
        value = contract(xw[...], w_qkv[i], 1, 0)
        if i == 0:
            value = (value + head_bias(0)).astype(BF) * BF(HD ** -0.5)
        elif i == 2:
            value = value + head_bias(1)
        qkv[i] = value.astype(BF)

    low_half = lax.broadcasted_iota(jnp.int32, (1, 128), 1) < HD
    halves = (low_half, jnp.logical_not(low_half))
    none = jnp.zeros((), BF)

    def two_blocks(ref, t, lanes):
        return jnp.concatenate([ref[span(t, 128), lanes], ref[span(t + 2, 128), lanes]], axis=0)

    def attend(index, carry):
        pair, t = index // 2, index % 2
        lanes = span(pair, 128)
        keys = pl.ds(pl.multiple_of(t * 128, 128), WINDOW)
        query = two_blocks(qkv.at[0], t, lanes)
        key, value = qkv[1, keys, lanes], qkv[2, keys, lanes]
        total = jnp.zeros((ROWS, 128), F32)
        for h, half in enumerate(halves):
            scores = contract(jnp.where(half, query, none), key, 1, 1) + bias[t]
            top = jnp.max(scores, axis=1, keepdims=True)
            weight = jnp.exp(scores - top)
            share_of = 1.0 / jnp.sum(weight, axis=1, keepdims=True)
            weight = (weight * share_of).astype(BF)
            prob[pair * 4 + t * 2 + h] = weight
            total = total + contract(weight, jnp.where(half, value, none), 1, 0)
        total = total.astype(BF)
        ctx[span(t, 128), lanes] = total[:128]
        ctx[span(t + 2, 128), lanes] = total[128:]
        return carry

    z_serve(W_UP, 0, 0)
    lax.fori_loop(0, 4, attend, 0)
    z_serve(W_UP, 0, 1)
    z_send(W_DOWN, 0)
    z_serve(W_OUT, 0, 2)
    z_serve(W_OUT, 1, 2)
    lax.fori_loop(4, 8, attend, 0)
    z_serve(W_UP, 0, 2)
    y_send(W_DOWN)

    def rows_of(s):
        mine = jnp.where(s < 2, x, 1 - x)
        return pl.ds(pl.multiple_of(mine * ROWS + lax.rem(s, 2) * CHUNK, CHUNK), CHUNK)

    def x_sum(kind, j):
        return x_copy(kind, j, stage.at[span(j, CHUNK)], recv.at[span(j, CHUNK)])

    def x_rows(kind, j, buf):
        here = buf.at[pl.ds(pl.multiple_of(x * ROWS + j * CHUNK, CHUNK), CHUNK)]
        return x_copy(kind, j, here, here)

    def hand_over(kind, before, s, value):
        @pl.when(s < 2)
        def _():
            own[span(s, CHUNK), :] = value

        @pl.when(s >= 2)
        def _():
            if before is not None:
                x_sum(before, s - 2).wait_send()
            stage[span(s - 2, CHUNK), :] = value.astype(BF)
            x_sum(kind, s - 2).start()

    wait_weight(W_OUT)

    def mix(i, carry):
        s = lax.rem(i + 2, 4)
        hand_over(X_MIX, None, s, contract(ctx[rows_of(s), :], w_out[...], 1, 0))
        return carry

    lax.fori_loop(0, 4, mix, 0)
    z_serve(W_DOWN, 0, 0)
    y_serve(W_UP, 0)
    y_serve(W_UP, 1)

    def row_of(row):
        return vf[row:row + 1, :]

    def normed(value):
        centred = value - jnp.mean(value, axis=1, keepdims=True)
        inverse = lax.rsqrt(jnp.mean(centred * centred, axis=1, keepdims=True) + NORM_EPS)
        return centred * inverse, inverse

    def norm_back(normal, inverse, grad):
        first = jnp.mean(grad, axis=1, keepdims=True)
        second = jnp.mean(grad * normal, axis=1, keepdims=True)
        return inverse * (grad - first - normal * second)

    def tiles(j, body):
        def step(i, carry):
            body(pl.ds(pl.multiple_of(j * CHUNK + i * TILE, TILE), TILE),
                 pl.ds(pl.multiple_of(x * ROWS + j * CHUNK + i * TILE, TILE), TILE))
            return carry
        lax.fori_loop(0, CHUNK // TILE, step, 0)

    def first_norm(r, g):
        summed = xw[g, :].astype(F32) + own[r, :] + recv[r, :].astype(F32) + row_of(R_BO)
        normal, inverse = normed(summed)
        n1[r, :] = normal
        inv1[r, :] = jnp.broadcast_to(inverse, (TILE, 128))
        hw[g, :] = (normal * row_of(R_G1) + row_of(R_C1)).astype(BF)

    for j in range(2):
        x_sum(X_MIX, j).wait_recv()
        tiles(j, first_norm)
        x_rows(X_NORM, j, hw).start()

    z_serve(W_DOWN, 0, 1)
    y_serve(W_UP, 2)
    y_serve(W_UP, 3)
    wait_weight(W_UP)

    def arrived(kind, s, buf):
        @pl.when(s >= 2)
        def _():
            there = buf.at[rows_of(s)]
            x_copy(kind, s - 2, there, there).wait_recv()

    def up_bias(n):
        return vf[pl.ds(8 + n * 2 + x, 1), :]

    def ffn_up(s, carry):
        rows = rows_of(s)
        arrived(X_NORM, s, hw)
        for n in range(2):
            pre = contract(hw[rows, :], w_up[:, n * 1024:(n + 1) * 1024], 1, 0) + up_bias(n)
            cdf = 0.5 * (1.0 + lax.erf(pre * SQRT_HALF))
            act[rows, n * 1024:(n + 1) * 1024] = (pre * cdf).astype(BF)
            slope[rows, n * 1024:(n + 1) * 1024] = (
                cdf + pre * INV_ROOT_TAU * jnp.exp(-0.5 * pre * pre)
            ).astype(BF)
        return carry

    lax.fori_loop(0, 2, ffn_up, 0)
    z_serve(W_DOWN, 0, 2)
    lax.fori_loop(2, 4, ffn_up, 0)
    go_on(remote(cot.at[1 - y], cotb.at[span(y, CHUNK)], ys.at[Y_COT], yr.at[Y_COT], at_y))
    for step in range(4):
        y_serve(W_DOWN, step)
    wait_weight(W_DOWN)

    def ffn_down(i, carry):
        s = lax.rem(i + 2, 4)
        hand_over(X_FFN, X_MIX, s, contract(act[rows_of(s), :], w_down[...], 1, 0))
        return carry

    lax.fori_loop(0, 4, ffn_down, 0)

    def bump(row, value):
        acc[row] += fold_rows(value)

    def second_norm(r, g):
        h1 = n1[r, :] * row_of(R_G1) + row_of(R_C1)
        normal, inverse = normed(h1 + own[r, :] + recv[r, :].astype(F32) + row_of(R_BD))
        outb[r, :] = (normal * row_of(R_G2) + row_of(R_C2)).astype(BF)
        dy = cotb[r, :].astype(F32)
        bump(R_G2, dy * normal)
        bump(R_C2, dy)
        grad = norm_back(normal, inverse, dy * row_of(R_G2))
        bump(R_BD, grad)
        da[r, :] = grad
        aw[g, :] = grad.astype(BF)

    local_cot.wait()
    cot_here = cotb.at[span(1 - y, CHUNK)]
    remote(cot.at[1 - y], cot_here, ys.at[Y_COT], yr.at[Y_COT], at_y).wait_recv()
    for j in range(2):
        x_sum(X_FFN, j).wait_recv()
        tiles(j, second_norm)
        x_rows(X_DA2, j, aw).start()
    out_here = pltpu.make_async_copy(outb.at[span(y, CHUNK)], out.at[y], os.at[0])
    out_here.start()
    go_on(remote(outb.at[span(1 - y, CHUNK)], out.at[y], ys.at[Y_OUT], yr.at[Y_OUT], at_y))

    def ffn_back(s, carry):
        rows = rows_of(s)
        arrived(X_DA2, s, aw)
        for n in range(2):
            cols = slice(n * 1024, (n + 1) * 1024)
            grad = contract(aw[rows, :], w_down[cols, :], 1, 1) * slope[rows, cols].astype(F32)
            bump(R_BU + n, grad)
            slope[rows, cols] = grad.astype(BF)
        hand_over(X_DH, X_FFN, s, contract(slope[rows, :], w_up[...], 1, 1))
        return carry

    lax.fori_loop(0, 4, ffn_back, 0)

    units = {
        U_DOWN: (g_down, c_down, y_down, z_down, h_down, o_down, gd),
        U_UP: (g_up, c_up, y_up, z_up, h_up, o_up, gu),
        U_OUT: (g_out, c_out, y_out, z_out, h_out, o_out, go),
    }
    for u, i in ((U_Q, 0), (U_K, 1), (U_V, 2)):
        units[u] = tuple(r.at[i] for r in (g_qkv, c_qkv, y_qkv, z_qkv, h_qkv, o_qkv, gq))

    def piece_loop(rows, body):
        size = min(rows, CHUNK)

        def step(i, carry):
            body(span(i, size))
            return carry
        lax.fori_loop(0, rows // size, step, 0)

    def add_piece(g, yy, zz, other):
        def body(r):
            g[c, yy, zz, r, :] = (g[c, yy, zz, r, :].astype(F32) + other[r, :].astype(F32)).astype(BF)
        piece_loop(g.shape[3], body)

    def core_copy(u):
        g, rc = units[u][0], units[u][1]
        return remote(g.at[1 - c], rc, gsc.at[u], grc.at[u], at_c)

    def core_send(u):
        go_on(core_copy(u))

    def core_add(u, r):
        g, rc = units[u][0], units[u][1]
        for zz in range(ZS):
            add_piece(g, column(r), zz, rc.at[column(r), zz])

    def rs_y_copy(u):
        g, ry = units[u][0], units[u][2]
        source = g.at[c, 1 - y, pl.ds(z, 1)] if u in Z_FIRST else g.at[c, 1 - y]
        return remote(source, ry, gsy.at[u], gry.at[u], at_y)

    def rs_z_copy(u, r, k):
        g, rz = units[u][0], units[u][3]
        to = lax.rem(z + k, ZS)
        return remote(g.at[c, column(r), to], rz.at[r, k - 1], gsz.at[u, r, k - 1], grz.at[u, r, k - 1], z_device(to))

    def rs_hand_on(u, r):
        g, rh = units[u][0], units[u][4]
        far = jnp.where(z == 0, ZS - 1, 0)
        return remote(g.at[c, column(r), far], rh.at[r], gsz.at[u, r, 3], grz.at[u, r, 3], z_device(jnp.where(z == 0, 1, 2)))

    def z_hand_on(u, r):
        go_if(edge, rs_hand_on(u, r))

    def z_begin(u, r):
        go_if(z != ZS - 1, rs_z_copy(u, r, 1))
        go_if(z != 0, rs_z_copy(u, r, 3))
        go_if(edge, rs_z_copy(u, r, 2))

    def z_relay(u, r):
        g, rh = units[u][0], units[u][4]

        @pl.when(middle)
        def _():
            rs_hand_on(u, r).wait_recv()
            add_piece(g, column(r), lax.rem(z + 2, ZS), rh.at[r])
        go_if(middle, rs_z_copy(u, r, 2))

    def start(u):
        core_copy(u).wait_recv()
        core_add(u, 1)
        if u in Z_FIRST:
            z_hand_on(u, 1)
            core_add(u, 0)
            z_hand_on(u, 0)
            z_begin(u, 1)
            z_begin(u, 0)
        else:
            go_on(rs_y_copy(u))
            core_add(u, 0)

    def y_to_z(u):
        g, ry = units[u][0], units[u][2]
        rs_y_copy(u).wait_recv()
        for zz in range(ZS):
            add_piece(g, y, zz, ry.at[zz])
        z_hand_on(u, 0)
        z_begin(u, 0)

    def wait_z(u, r):
        rs_z_copy(u, r, 2).wait_recv()

        @pl.when(z != 0)
        def _():
            rs_z_copy(u, r, 1).wait_recv()

        @pl.when(z != ZS - 1)
        def _():
            rs_z_copy(u, r, 3).wait_recv()

    def z_total(u, r, rows):
        g, rz = units[u][0], units[u][3]
        value = g[c, column(r), z, rows, :].astype(F32)
        for k in range(ZS - 1):
            value = value + rz[r, k, rows, :].astype(F32)
        return value

    def z_to_y(u):
        g = units[u][0]
        wait_z(u, 1)

        def body(rows):
            g[c, 1 - y, z, rows, :] = z_total(u, 1, rows).astype(BF)
        piece_loop(g.shape[3], body)
        go_on(rs_y_copy(u))

    finals = []

    def finish(u):
        g, _, ry, _, _, o, dest = units[u]
        wait_z(u, 0)
        if u in Z_FIRST:
            rs_y_copy(u).wait_recv()

        def body(rows):
            value = z_total(u, 0, rows)
            if u in Z_FIRST:
                value = value + ry[0, rows, :].astype(F32)
            o[rows, :] = value
        piece_loop(g.shape[3], body)
        copy = pltpu.make_async_copy(o, dest, os.at[1 + u])
        copy.start()
        finals.append(copy)

    for u in units:
        for r in range(2 if u in Z_FIRST else 1):
            for k, alone in ((1, z == 0), (3, z == ZS - 1)):
                @pl.when(alone)
                def _(u=u, r=r, k=k):
                    rz = units[u][3]
                    rz[r, k - 1] = jnp.zeros(rz.shape[2:], BF)

    def grad_down(i, carry):
        value = contract(act[:, span(i, 512)], aw[...], 0, 0).astype(BF)
        for d in range(8):
            g_down[d % 2, i // 2, d // 2, span(i % 2, 512), :] = value[:, d * 128:(d + 1) * 128]
        return carry

    lax.fori_loop(0, 4, grad_down, 0)
    core_send(U_DOWN)

    def grad_up(index, carry):
        i, n = index // 2, index % 2
        value = contract(hw[:, span(i, 512)], slope[:, span(n, 1024)], 0, 0).astype(BF)
        for d in range(4):
            g_up[d % 2, n, i * 2 + d // 2] = value[d * 128:(d + 1) * 128, :]
        return carry

    lax.fori_loop(0, 4, grad_up, 0)
    core_send(U_UP)
    start(U_DOWN)
    start(U_UP)

    def back_norm(r, g):
        grad = da[r, :] + own[r, :] + recv[r, :].astype(F32)
        normal = n1[r, :]
        bump(R_G1, grad * normal)
        bump(R_C1, grad)
        grad = norm_back(normal, inv1[r, 0:1], grad * row_of(R_G1))
        bump(R_BO, grad)
        da[r, :] = grad
        a1w[g, :] = grad.astype(BF)

    for j in range(2):
        x_sum(X_DH, j).wait_recv()
        tiles(j, back_norm)
        x_rows(X_DA1, j, a1w).start()

    z_relay(U_DOWN, 1)
    z_relay(U_DOWN, 0)

    def ctx_back(s, carry):
        rows = rows_of(s)
        arrived(X_DA1, s, a1w)
        dctx[rows, :] = contract(a1w[rows, :], w_out[...], 1, 1).astype(BF)
        return carry

    lax.fori_loop(0, 4, ctx_back, 0)

    def attend_back(pair, carry):
        lanes = span(pair, 128)
        for t in range(2):
            keys = pl.ds(t * 128, WINDOW)
            query = two_blocks(qkv.at[0], t, lanes)
            key, value = qkv[1, keys, lanes], qkv[2, keys, lanes]
            grad = two_blocks(dctx, t, lanes)
            product = grad.astype(F32) * two_blocks(ctx, t, lanes).astype(F32)
            grad_q = jnp.zeros((ROWS, 128), F32)
            grad_k = jnp.zeros((WINDOW, 128), F32)
            grad_v = jnp.zeros((WINDOW, 128), F32)
            for h, half in enumerate(halves):
                grad_h = jnp.where(half, grad, none)
                weight = prob[pair * 4 + t * 2 + h]
                row_dot = jnp.sum(jnp.where(half, product, 0.0), axis=1, keepdims=True)
                score = (weight.astype(F32) * (contract(grad_h, value, 1, 1) - row_dot)).astype(BF)
                grad_q = grad_q + contract(score, jnp.where(half, key, none), 1, 0)
                grad_k = grad_k + contract(score, jnp.where(half, query, none), 0, 0)
                grad_v = grad_v + contract(weight, grad_h, 0, 0)
            grad_q = grad_q * (HD ** -0.5)
            acc[R_BQ, :, lanes] += fold_rows(grad_q)
            acc[R_BV, :, lanes] += fold_rows(grad_v)
            grad_q = grad_q.astype(BF)
            qkv[0, t * 128:t * 128 + 128, lanes] = grad_q[:128]
            qkv[0, t * 128 + 256:t * 128 + 384, lanes] = grad_q[128:]
            if t == 0:
                acc_k[0:WINDOW, :] = grad_k
                acc_v[0:WINDOW, :] = grad_v
                acc_k[WINDOW:SEQ, :] = jnp.zeros((128, 128), F32)
                acc_v[WINDOW:SEQ, :] = jnp.zeros((128, 128), F32)
            else:
                for i, total, more in ((1, acc_k, grad_k), (2, acc_v, grad_v)):
                    qkv[i, 0:128, lanes] = total[0:128, :].astype(BF)
                    qkv[i, 128:SEQ, lanes] = (total[128:SEQ, :] + more).astype(BF)
        return carry

    lax.fori_loop(0, 4, attend_back, 0)
    y_to_z(U_UP)

    for row in range(2, 8):
        line = jnp.sum(acc[row], axis=0, keepdims=True)
        for d in range(8):
            vg[d % 2, d // 2, row:row + 1, :] = line[:, d * 128:(d + 1) * 128]
    for n in range(2):
        line = jnp.sum(acc[R_BU + n], axis=0, keepdims=True)
        for d in range(8):
            vg[d % 2, d // 2, pl.ds(8 + n * 2 + x, 1), :] = line[:, d * 128:(d + 1) * 128]
    for row, source in ((0, R_BQ), (1, R_BV)):
        line = jnp.sum(acc[source], axis=0, keepdims=True)
        for yy in range(2):
            for half in range(2):
                vg[half, 2 * yy + x, row:row + 1, :] = (
                    line[:, yy * 256 + half * 128:yy * 256 + (half + 1) * 128]
                )
    vec_x = remote(vg, vgx, vs.at[0], vr.at[0], at_x)
    vec_c = remote(vg.at[1 - c], vgc, vs.at[1], vr.at[1], at_c)
    vec_y = remote(vg.at[c], vgy, vs.at[2], vr.at[2], at_y)

    def vec_z(k):
        to = lax.rem(z + k, ZS)
        return remote(vg.at[c, to], vgz.at[k - 1], vs.at[2 + k], vr.at[2 + k], z_device(to))

    vec_x.start()

    def input_back(i, carry):
        s = lax.rem(i + 2, 4)
        rows = rows_of(s)
        value = contract(qkv[0, rows, :], w_qkv[0], 1, 1)
        value = value + contract(qkv[1, rows, :], w_qkv[1], 1, 1)
        value = value + contract(qkv[2, rows, :], w_qkv[2], 1, 1)
        hand_over(X_DX, X_DH, s, value)
        return carry

    lax.fori_loop(0, 2, input_back, 0)
    vec_x.wait()
    vg[...] = vg[...] + vgx[...]
    vec_c.start()

    def grad_qkv(index, carry):
        kind, i = index // 2, index % 2
        value = contract(xw[:, span(i, 512)], qkv[kind], 0, 0).astype(BF)
        for d in range(4):
            for yy in range(2):
                g_qkv[kind, d % 2, yy, i * 2 + d // 2] = (
                    value[d * 128:(d + 1) * 128, yy * 256:(yy + 1) * 256]
                )
        return carry

    def grad_out():
        value = contract(ctx[...], a1w[...], 0, 0).astype(BF)
        for d in range(8):
            for yy in range(2):
                g_out[d % 2, yy, d // 2] = value[yy * 256:(yy + 1) * 256, d * 128:(d + 1) * 128]

    grad_out()
    core_send(U_OUT)
    for kind, u in ((0, U_Q), (1, U_K), (2, U_V)):
        lax.fori_loop(kind * 2, kind * 2 + 2, grad_qkv, 0)
        core_send(u)
    vec_c.wait()
    vg[c] = vg[c] + vgc[...]
    vec_y.start()
    start(U_OUT)
    start(U_Q)
    start(U_K)
    start(U_V)
    lax.fori_loop(2, 4, input_back, 0)
    z_relay(U_UP, 0)
    vec_y.wait()
    vg[c] = vg[c] + vgy[...]
    for k in range(1, ZS):
        vec_z(k).start()
    y_to_z(U_OUT)

    def last_sum(j, other):
        x_sum(X_DX, j).wait_recv()

        def body(r, g):
            value = da[r, :] + own[r, :] + recv[r, :].astype(F32)
            if other:
                gts[pl.ds(pl.multiple_of(r.start - j * CHUNK, TILE), TILE), :] = value.astype(BF)
            else:
                da[r, :] = value
        tiles(j, body)

    last_sum(1 - y, True)
    z_to_y(U_DOWN)
    go_on(remote(gts, gtr, ys.at[Y_GTOK], yr.at[Y_GTOK], at_y))
    last_sum(y, False)
    gtok_here = pltpu.make_async_copy(da.at[span(y, CHUNK)], gtok.at[y], os.at[7])
    gtok_here.start()
    z_relay(U_OUT, 0)
    for u in (U_Q, U_K, U_V):
        y_to_z(u)
    for u in (U_Q, U_K, U_V):
        z_relay(u, 0)
    for k in range(1, ZS):
        vec_z(k).wait()
    gvb[...] = vg[c, z] + vgz[0] + vgz[1] + vgz[2]
    vec_here = pltpu.make_async_copy(gvb.at[0:12], gv, os.at[8])
    vec_here.start()
    finish(U_DOWN)
    finish(U_UP)
    remote(gts, gtr, ys.at[Y_GTOK], yr.at[Y_GTOK], at_y).wait_recv()
    gtf[...] = gtr[...].astype(F32)
    gtok_there = pltpu.make_async_copy(gtf, gtok.at[1 - y], os.at[9])
    gtok_there.start()
    finish(U_OUT)
    finish(U_Q)
    finish(U_K)
    finish(U_V)
    remote(outb.at[span(1 - y, CHUNK)], out.at[1 - y], ys.at[Y_OUT], yr.at[Y_OUT], at_y).wait_recv()
    for kind, buf in ((X_NORM, hw), (X_DA2, aw), (X_DA1, a1w)):
        for j in range(2):
            x_rows(kind, j, buf).wait_send()
    for j in range(2):
        x_sum(X_DX, j).wait_send()
    for copy in sent:
        copy.wait_send()
    for condition, copy in later:
        @pl.when(condition)
        def _(copy=copy):
            copy.wait_send()
    for m in range(7):
        remote(half_of(m), half_of(m), wsc.at[m], wrc.at[m], at_c).wait_send()
    for copy in finals + [out_here, gtok_here, gtok_there, vec_here]:
        copy.wait()


def layer(tokens, segment_ids, w_qkv, w_out, w_up, w_down, vectors, cotangent):
    vmem, dma = pltpu.VMEM, pltpu.SemaphoreType.DMA
    outs = (
        jax.ShapeDtypeStruct(tokens.shape, BF),
        jax.ShapeDtypeStruct(tokens.shape, F32),
        jax.ShapeDtypeStruct(w_qkv.shape, F32),
        jax.ShapeDtypeStruct(w_out.shape, F32),
        jax.ShapeDtypeStruct(w_up.shape, F32),
        jax.ShapeDtypeStruct(w_down.shape, F32),
        jax.ShapeDtypeStruct(vectors.shape, F32),
    )
    pieces = ((1024, 128), (128, 1024), (256, 128), (128, 256))
    lead = ((), (), (), (3,))
    scratch = [
        vmem((3, D, COLS), BF), vmem((COLS, D), BF), vmem((D, HID), BF), vmem((HID, D), BF),
        vmem((8, 12, 128), BF), vmem((16, D), F32),
    ]
    ways = [2 if u in Z_FIRST else 1 for u in (U_DOWN, U_UP, U_OUT, U_Q)]
    for shapes in (
        [(2, 2, 4)] * 4, [(2, 4)] * 4, [(4,) if way == 1 else (1,) for way in ways],
        [(way, 3) for way in ways], [(way,) for way in ways],
    ):
        scratch += [vmem(first + shape + piece, BF) for first, shape, piece in zip(lead, shapes, pieces)]
    scratch += [vmem((3, 128, 256), F32), vmem((256, 128), F32), vmem((128, 1024), F32), vmem((1024, 128), F32)]
    scratch += [
        vmem((SEQ, D), BF), vmem((3, SEQ, COLS), BF), vmem((SEQ, COLS), BF),
        vmem((16, ROWS, WINDOW), BF), vmem((2, ROWS, WINDOW), F32), vmem((SEQ, D), BF),
        vmem((SEQ, HID), BF), vmem((SEQ, HID), BF), vmem((SEQ, D), BF), vmem((SEQ, D), BF),
        vmem((SEQ, COLS), BF),
        vmem((ROWS, D), F32), vmem((ROWS, D), F32), vmem((ROWS, D), F32), vmem((ROWS, 128), F32),
        vmem((ROWS, D), BF), vmem((ROWS, D), BF), vmem((ROWS, D), BF), vmem((ROWS, D), BF),
        vmem((CHUNK, D), BF), vmem((CHUNK, D), BF), vmem((CHUNK, D), F32),
        vmem((12, 8, D), F32),
        vmem((2, 4, 16, 128), F32), vmem((2, 4, 16, 128), F32), vmem((4, 16, 128), F32),
        vmem((4, 16, 128), F32), vmem((3, 16, 128), F32), vmem((16, 128), F32),
        vmem((SEQ, 128), F32), vmem((SEQ, 128), F32),
        dma((7, 2, 4)), dma((7, 2, 3)), dma((7, 4)), dma((7, 4)), dma((7,)), dma((7,)),
        dma((8, 2)), dma((8, 2)), dma((4,)), dma((4,)),
        dma((6,)), dma((6,)), dma((6,)), dma((6,)), dma((6, 2, 4)), dma((6, 2, 4)),
        dma((6,)), dma((6,)), dma((9,)), dma((10,)),
    ]
    hbm = pl.BlockSpec(memory_space=pl.ANY)
    return pl.pallas_call(
        layer_kernel,
        out_shape=outs,
        in_specs=[hbm, pl.BlockSpec(memory_space=pltpu.VMEM)] + [hbm] * 6,
        out_specs=[hbm] * 7,
        scratch_shapes=scratch,
        compiler_params=pltpu.CompilerParams(
            collective_id=0, has_side_effects=True, vmem_limit_bytes=67043328
        ),
    )(tokens, segment_ids, w_qkv, w_out, w_up, w_down, vectors, cotangent)


def solution(mesh):
    step = layer if (mesh.shape["dp"], mesh.shape["tensor"]) == (8, 4) else body
    return jax.shard_map(
        step,
        mesh=mesh,
        in_specs=(
            P("dp", "tensor", None),
            P("dp", None),
            P(None, "dp", "tensor"),
            P("tensor", "dp"),
            P("dp", "tensor"),
            P("tensor", "dp"),
            P(None, "dp"),
            P("dp", "tensor", None),
        ),
        out_specs=(
            P("dp", "tensor", None),
            P("dp", "tensor", None),
            P(None, "dp", "tensor"),
            P("tensor", "dp"),
            P("dp", "tensor"),
            P("tensor", "dp"),
            P(None, "dp"),
        ),
        check_vma=False,
    )
```

```python
import jax
import jax.numpy as jnp
from jax import lax
from jax.experimental import pallas as pl
from jax.experimental.pallas import tpu as pltpu
from jax.sharding import PartitionSpec as P

D = 1024
FF = 4096
HD = 64


NORM_EPS = 1e-06
SQRT_HALF = 0.7071067811865476
INV_ROOT_TAU = 0.3989422804014327
MASKED = -1e30


def gelu_value(pre_act):
    return 0.5 * pre_act * (1.0 + lax.erf(pre_act * SQRT_HALF))


def gelu_slope(pre_act):
    return 0.5 * (1.0 + lax.erf(pre_act * SQRT_HALF)) + pre_act * INV_ROOT_TAU * jnp.exp(
        -0.5 * pre_act * pre_act
    )


def norm_forward(summed, gain, shift):
    centred = summed - jnp.mean(summed, axis=-1, keepdims=True)
    inverse = lax.rsqrt(jnp.mean(centred * centred, axis=-1, keepdims=True) + NORM_EPS)
    normed = centred * inverse
    return (normed * gain + shift, normed, inverse)


def norm_backward(normed, inverse, grad_normed):
    first_mean = jnp.mean(grad_normed, axis=-1, keepdims=True)
    second_mean = jnp.mean(grad_normed * normed, axis=-1, keepdims=True)
    return inverse * (grad_normed - first_mean - normed * second_mean)


def attention_scores(query_heads, key_heads, segments):
    same_doc = segments[:, None] == segments[None, :]
    scores = jnp.einsum(
        "qhe,khe->hqk", query_heads, key_heads, preferred_element_type=jnp.float32
    ) * HD ** (-0.5)
    return jnp.where(same_doc[None], scores, MASKED)


def collect(w_qkv, w_out, w_up, w_down, vectors):
    return (
        lax.all_gather(w_qkv, "dp", axis=1, tiled=True),
        lax.all_gather(w_out, "dp", axis=1, tiled=True),
        lax.all_gather(w_up, "dp", axis=0, tiled=True),
        lax.all_gather(w_down, "dp", axis=1, tiled=True),
        lax.all_gather(vectors, "dp", axis=1, tiled=True),
    )


def share(gradients):
    return (
        lax.psum_scatter(
            gradients[0].astype(jnp.bfloat16), "dp", scatter_dimension=1, tiled=True
        ).astype(jnp.float32),
        lax.psum_scatter(
            gradients[1].astype(jnp.bfloat16), "dp", scatter_dimension=1, tiled=True
        ).astype(jnp.float32),
        lax.psum_scatter(
            gradients[2].astype(jnp.bfloat16), "dp", scatter_dimension=0, tiled=True
        ).astype(jnp.float32),
        lax.psum_scatter(
            gradients[3].astype(jnp.bfloat16), "dp", scatter_dimension=1, tiled=True
        ).astype(jnp.float32),
        lax.psum_scatter(
            gradients[4].astype(jnp.bfloat16), "dp", scatter_dimension=1, tiled=True
        ).astype(jnp.float32),
    )


def body(tokens, segment_ids, w_qkv, w_out, w_up, w_down, vectors, cotangent):
    tensor_rank = lax.axis_index("tensor")
    local_cols = w_qkv.shape[2]
    head_count = local_cols // HD
    hidden = w_up.shape[1]
    col_start = tensor_rank * local_cols
    ffn_start = tensor_rank * hidden

    def forward(weights, tok_block, segments):
        qkv_w, out_w, up_w, down_w, vec_b = weights
        vec_f32 = vec_b.astype(jnp.float32)
        whole = lax.all_gather(tok_block, "tensor", axis=0, tiled=True)
        seq_len = whole.shape[0]
        projected = jnp.einsum("sd,tdc->tsc", whole, qkv_w, preferred_element_type=jnp.float32)
        bias_q = lax.dynamic_slice_in_dim(vec_f32[0], col_start, local_cols)
        bias_v = lax.dynamic_slice_in_dim(vec_f32[1], col_start, local_cols)
        query_heads = (projected[0] + bias_q).astype(jnp.bfloat16).reshape(seq_len, head_count, HD)
        key_heads = projected[1].astype(jnp.bfloat16).reshape(seq_len, head_count, HD)
        value_heads = (projected[2] + bias_v).astype(jnp.bfloat16).reshape(seq_len, head_count, HD)
        scores = attention_scores(query_heads, key_heads, segments)
        row_top = jnp.max(scores, axis=-1, keepdims=True)
        log_total = row_top + jnp.log(jnp.sum(jnp.exp(scores - row_top), axis=-1, keepdims=True))
        attn_probs = jnp.exp(scores - log_total).astype(jnp.bfloat16)
        context = jnp.einsum(
            "hqk,khe->qhe", attn_probs, value_heads, preferred_element_type=jnp.float32
        )
        context = context.reshape(seq_len, local_cols).astype(jnp.bfloat16)
        piece = context
        attn_mixed = lax.psum_scatter(
            jnp.dot(piece, out_w, preferred_element_type=jnp.float32).astype(jnp.bfloat16),
            "tensor",
            scatter_dimension=0,
            tiled=True,
        ).astype(jnp.float32)
        summed_one = tok_block.astype(jnp.float32) + attn_mixed + vec_f32[2]
        normed_out, normed_one, inverse_one = norm_forward(summed_one, vec_f32[3], vec_f32[4])
        normed_b = normed_out.astype(jnp.bfloat16)
        normed_whole = lax.all_gather(normed_b, "tensor", axis=0, tiled=True)
        bias_up = lax.dynamic_slice_in_dim(vec_f32[8:12].reshape(FF), ffn_start, hidden)
        pre_act = jnp.dot(normed_whole, up_w, preferred_element_type=jnp.float32) + bias_up
        activated = gelu_value(pre_act).astype(jnp.bfloat16)
        piece = activated
        summed_two = (
            normed_out
            + lax.psum_scatter(
                jnp.dot(piece, down_w, preferred_element_type=jnp.float32).astype(jnp.bfloat16),
                "tensor",
                scatter_dimension=0,
                tiled=True,
            ).astype(jnp.float32)
            + vec_f32[5]
        )
        final, normed_two, inverse_two = norm_forward(summed_two, vec_f32[6], vec_f32[7])
        saved = (
            whole,
            query_heads,
            key_heads,
            value_heads,
            log_total,
            context,
            normed_one,
            inverse_one,
            normed_whole,
            pre_act,
            activated,
            normed_two,
            inverse_two,
        )
        return (final.astype(jnp.bfloat16), saved)

    def backward(weights, saved, segments, grad_block):
        qkv_w, out_w, up_w, down_w, vec_b = weights
        vec_f32 = vec_b.astype(jnp.float32)
        (
            whole,
            query_heads,
            key_heads,
            value_heads,
            log_total,
            context,
            normed_one,
            inverse_one,
            normed_whole,
            pre_act,
            activated,
            normed_two,
            inverse_two,
        ) = saved
        seq_len = whole.shape[0]
        grad_final = grad_block.astype(jnp.float32)
        g_gain2 = jnp.sum(grad_final * normed_two, axis=0)
        g_shift2 = jnp.sum(grad_final, axis=0)
        grad_two = norm_backward(normed_two, inverse_two, grad_final * vec_f32[6])
        grad_two_b = grad_two.astype(jnp.bfloat16)
        g_bdown = jnp.sum(grad_two, axis=0)
        grad_two_whole = lax.all_gather(grad_two_b, "tensor", axis=0, tiled=True)
        g_down = jnp.dot(activated.T, grad_two_whole, preferred_element_type=jnp.float32)
        grad_pre = jnp.dot(
            grad_two_whole, down_w.T, preferred_element_type=jnp.float32
        ) * gelu_slope(pre_act)
        grad_pre_b = grad_pre.astype(jnp.bfloat16)
        g_bup = jnp.sum(grad_pre, axis=0)
        g_up = jnp.dot(normed_whole.T, grad_pre_b, preferred_element_type=jnp.float32)
        piece = grad_pre_b
        grad_one_in = grad_two + lax.psum_scatter(
            jnp.dot(piece, up_w.T, preferred_element_type=jnp.float32).astype(jnp.bfloat16),
            "tensor",
            scatter_dimension=0,
            tiled=True,
        ).astype(jnp.float32)
        g_gain1 = jnp.sum(grad_one_in * normed_one, axis=0)
        g_shift1 = jnp.sum(grad_one_in, axis=0)
        grad_one = norm_backward(normed_one, inverse_one, grad_one_in * vec_f32[3])
        grad_one_b = grad_one.astype(jnp.bfloat16)
        g_bout = jnp.sum(grad_one, axis=0)
        grad_one_whole = lax.all_gather(grad_one_b, "tensor", axis=0, tiled=True)
        g_out = jnp.dot(context.T, grad_one_whole, preferred_element_type=jnp.float32)
        grad_context = jnp.dot(grad_one_whole, out_w.T, preferred_element_type=jnp.float32).astype(
            jnp.bfloat16
        )
        grad_context = grad_context.reshape(seq_len, head_count, HD)
        scores = attention_scores(query_heads, key_heads, segments)
        attn_exact = jnp.exp(scores - log_total)
        attn_probs = attn_exact.astype(jnp.bfloat16)
        grad_probs = jnp.einsum(
            "qhe,khe->hqk", grad_context, value_heads, preferred_element_type=jnp.float32
        )
        row_dot = jnp.sum(attn_exact * grad_probs, axis=-1, keepdims=True)
        grad_scores = (attn_exact * (grad_probs - row_dot) * HD ** (-0.5)).astype(jnp.bfloat16)
        grad_value = jnp.einsum(
            "hqk,qhe->khe", attn_probs, grad_context, preferred_element_type=jnp.float32
        )
        grad_value = grad_value.reshape(seq_len, local_cols)
        grad_query = jnp.einsum(
            "hqk,khe->qhe", grad_scores, key_heads, preferred_element_type=jnp.float32
        )
        grad_query = grad_query.reshape(seq_len, local_cols)
        grad_key = jnp.einsum(
            "hqk,qhe->khe", grad_scores, query_heads, preferred_element_type=jnp.float32
        )
        grad_key = grad_key.reshape(seq_len, local_cols)
        grad_qkv = jnp.stack([grad_query, grad_key, grad_value]).astype(jnp.bfloat16)
        g_qkv = jnp.einsum("sd,tsc->tdc", whole, grad_qkv, preferred_element_type=jnp.float32)
        piece = grad_qkv
        grad_input = grad_one + lax.psum_scatter(
            jnp.einsum("tsc,tdc->sd", piece, qkv_w, preferred_element_type=jnp.float32).astype(
                jnp.bfloat16
            ),
            "tensor",
            scatter_dimension=0,
            tiled=True,
        ).astype(jnp.float32)
        zero_row = jnp.zeros((D,), jnp.float32)
        row_q = lax.dynamic_update_slice_in_dim(zero_row, jnp.sum(grad_query, axis=0), col_start, 0)
        row_v = lax.dynamic_update_slice_in_dim(zero_row, jnp.sum(grad_value, axis=0), col_start, 0)
        up_rows = lax.dynamic_update_slice_in_dim(
            jnp.zeros((FF,), jnp.float32), g_bup, ffn_start, 0
        ).reshape(4, D)
        first_rows = jnp.stack(
            [row_q, row_v, g_bout, g_gain1, g_shift1, g_bdown, g_gain2, g_shift2]
        )
        g_vec = jnp.concatenate([first_rows, up_rows], axis=0)
        return ((g_qkv, g_out, g_up, g_down, g_vec), grad_input)

    def one_batch(carried, batch_item):
        tok_block, segments, grad_block = batch_item
        forward_w = collect(w_qkv, w_out, w_up, w_down, vectors)
        final_b, saved = forward(forward_w, tok_block, segments)
        second = collect(w_qkv, w_out, w_up, w_down, vectors)
        gradients, grad_input = backward(second, saved, segments, grad_block)
        updated = jax.tree.map(jnp.add, carried, gradients)
        return (updated, (final_b, grad_input))

    initial = (
        jnp.zeros((3, D, local_cols), jnp.float32),
        jnp.zeros((local_cols, D), jnp.float32),
        jnp.zeros((D, hidden), jnp.float32),
        jnp.zeros((hidden, D), jnp.float32),
        jnp.zeros((12, D), jnp.float32),
    )
    carried, stacked = lax.scan(one_batch, initial, (tokens, segment_ids, cotangent))
    totals = share(carried)
    vector_grads = lax.psum(totals[4], "tensor")
    return (stacked[0], stacked[1], totals[0], totals[1], totals[2], totals[3], vector_grads)


Y_TOK, Y_COT, Y_OUT, Y_GTOK = range(4)
X_TOK, X_MIX, X_NORM, X_FFN, X_DA2, X_DH, X_DA1, X_DX = range(8)
W_Q, W_K, W_V, W_OUT, W_UP, W_DOWN, W_REST, W_VEC = range(8)
W_KINDS = 8
Y_FIRST = (W_REST,)
DIRECT = (W_VEC,)
FAR_FIRST = ()
U_DA, U_DB, U_UA, U_UB, U_OUT, U_V, U_K, U_Q = range(8)
Z_FIRST = (U_DA, U_OUT)
R_BQ, R_BV, R_BO, R_G1, R_C1, R_BD, R_G2, R_C2, R_BU = range(9)
ZS = 4
SEQ = 512
ROWS = 256
CHUNK = 128
TILE = 32
COLS = 512
HID = 2048
WINDOW = 384
BF = jnp.bfloat16
F32 = jnp.float32
MESH = pl.DeviceIdType.MESH


def span(index, size):
    return pl.ds(pl.multiple_of(index * size, size), size)


def contract(a, b, a_dim, b_dim):
    return lax.dot_general(a, b, (((a_dim,), (b_dim,)), ((), ())), preferred_element_type=F32)


def fold_rows(value):
    return jnp.sum(value.reshape(value.shape[0] // 8, 8, value.shape[1]), axis=0)


def layer_kernel(
    tok, seg, wq, wo, wu, wd, vec, cot,
    out, gtok, gq, go, gu, gd, gv,
    w_qkv, w_out, w_up, w_down, w_vec, vf,
    g_down, g_up, g_out, g_qkv,
    c_down, c_up, c_out, c_qkv,
    y_da, y_db, y_up, y_out, y_qkv,
    z_da, z_db, z_up, z_out, z_qkv,
    h_da, h_db, h_up, h_out, h_qkv,
    o_qkv, o_out, o_up, o_down,
    xw, qkv, ctx, prob, bias, hw, act, slope, aw, a1w, dctx,
    own, n1, da, inv1, recv, stage, cotb, outb, gts, gtr, gtf,
    acc, vg, vgx, vgc, vgy, vgz, gvb, acc_k, acc_v,
    done, wrz, wry, wsc, wrc, wrd, fs, fr, xs, xr, yr,
    grc, gry, grz, vs, vr, ls, os,
):
    dp = lax.axis_index("dp")
    tensor = lax.axis_index("tensor")
    z, c = dp // 2, dp % 2
    y, x = tensor // 2, tensor % 2
    at_x = {"dp": dp, "tensor": y * 2 + (1 - x)}
    at_y = {"dp": dp, "tensor": (1 - y) * 2 + x}
    at_c = {"dp": z * 2 + (1 - c), "tensor": tensor}

    def remote(src, dst, send, recv_sem, where):
        return pltpu.make_async_remote_copy(
            src_ref=src, dst_ref=dst, send_sem=send, recv_sem=recv_sem,
            device_id=where, device_id_type=MESH,
        )

    barrier = pltpu.get_barrier_semaphore()
    for where in [at_x, at_y, at_c] + [{"dp": lax.rem(z + k, ZS) * 2 + c, "tensor": tensor} for k in range(1, ZS)]:
        pl.semaphore_signal(barrier, inc=1, device_id=where, device_id_type=MESH)
    pl.semaphore_wait(barrier, 6)

    sent = []

    def go_on(copy):
        copy.start()
        sent.append(copy)

    args = [wq.at[0], wq.at[1], wq.at[2], wo, wu, wd.at[0:512], wd.at[512:1024], vec]
    edge = jnp.logical_or(z == 0, z == ZS - 1)
    middle = jnp.logical_not(edge)
    later = []

    def z_device(where):
        return {"dp": where * 2 + c, "tensor": tensor}

    def go_if(condition, copy):
        @pl.when(condition)
        def _():
            copy.start()
        later.append((condition, copy))

    def place(m, yy, d):
        if m <= W_V:
            return w_qkv.at[m, span(d, 128), span(yy, 256)]
        if m == W_OUT:
            return w_out.at[span(yy, 256), span(d, 128)]
        if m == W_UP:
            return w_up.at[span(d, 128), span(yy, 1024)]
        if m == W_DOWN or m == W_REST:
            return w_down.at[span(yy * 2 + m - W_DOWN, 512), span(d, 128)]
        return w_vec.at[d]

    def from_z(k):
        return lax.rem(z + ZS - k, ZS)

    def column(r):
        return y if r == 0 else 1 - y

    def z_send(m, r):
        source = args[m] if r == 0 else place(m, 1 - y, dp)
        steps = ((1, z != ZS - 1), (3, z != 0), (2, None))
        for k, there in (steps[2:] + steps[:2] if m in FAR_FIRST else steps):
            there = None if m in DIRECT else there
            copy = remote(
                source, place(m, column(r), dp), done.at[0], wrz.at[m, r, k - 1],
                z_device(lax.rem(z + k, ZS)),
            )
            if there is None:
                go_on(copy)
            else:
                go_if(there, copy)

    def z_serve(m, r, step, keep=False):
        z_take(m, r, step, keep)
        z_note(m, r, step)

    def z_serve_split(m, r, step, early, late):
        def first():
            @pl.when(early)
            def _():
                z_take(m, r, step)

        def second():
            @pl.when(late)
            def _():
                z_take(m, r, step)
            z_note(m, r, step)
        return first, second

    def z_parts(m, r, step):
        k = (jnp.where(z == 0, 3, 1), 2, jnp.where(z == 0, 1, 3))[step]
        here = place(m, column(r), from_z(k) * 2 + c)
        slot = jnp.where(z == 1, 0, 2)
        hand_on = None
        if step == 1 and m not in DIRECT:
            hand_on = remote(
                here, here, done.at[0], wrz.at[m, r, slot], z_device(jnp.where(z == 1, 0, 3)),
            )
        over_y = None
        if r == 0 and m not in Y_FIRST and m != W_VEC:
            over_y = remote(here, here, done.at[0], wry.at[m, from_z(k)], at_y)
        return k, here, hand_on, over_y

    def z_over(m, step):
        z_parts(m, 0, step)[3].start()

    def z_take(m, r, step, keep=False):
        k, here, hand_on, over_y = z_parts(m, r, step)
        remote(here, here, done.at[0], wrz.at[m, r, k - 1], at_x).wait_recv()
        if hand_on is not None:
            @pl.when(middle)
            def _():
                hand_on.start()
        if over_y is not None and not keep:
            over_y.start()
        c_send(m, here, step + 1)

    def z_note(m, r, step):
        _, _, hand_on, over_y = z_parts(m, r, step)
        if hand_on is not None:
            later.append((middle, hand_on))
        if over_y is not None:
            sent.append(over_y)

    def y_send(m):
        go_on(remote(args[m], place(m, y, dp), done.at[0], wry.at[m, z], at_y))

    def source_of(step):
        return z if step == 0 else from_z((jnp.where(z == 0, 3, 1), 2, jnp.where(z == 0, 1, 3))[step - 1])

    def y_serve(m, step):
        zz = source_of(step)
        here = place(m, 1 - y, zz * 2 + c)
        remote(here, here, done.at[0], wry.at[m, zz], at_y).wait_recv()
        c_send(m, here, step)

    def c_send(m, source, step, dest=None):
        dest = source if dest is None else dest
        into = wrd.at[m - W_DOWN, step] if m in (W_DOWN, W_REST) else wrc.at[m]
        remote(source, dest, wsc.at[m], into, at_c).start()

    def own_send(m):
        c_send(m, args[m], 0, place(m, y, dp))
        pltpu.make_async_copy(args[m], place(m, y, dp), ls.at[m]).start()

    def half_of(m):
        if m <= W_V:
            return w_qkv.at[m, :, 0:256]
        return (
            w_out.at[0:256], w_up.at[:, 0:1024], w_down.at[0:512], w_down.at[0:512], w_vec.at[0:4]
        )[m - W_OUT]

    def wait_down(step):
        for m in (W_DOWN, W_REST):
            if step == 0:
                pltpu.make_async_copy(args[m], place(m, y, dp), ls.at[m]).wait()
            two = w_down.at[0:1024, 0:128]
            remote(two, two, wsc.at[m], wrd.at[m - W_DOWN, step], at_c).wait_recv()

    def wait_weight(m):
        pltpu.make_async_copy(args[m], place(m, y, dp), ls.at[m]).wait()
        remote(half_of(m), half_of(m), wsc.at[m], wrc.at[m], at_c).wait_recv()

    def x_copy(kind, j, src, dst):
        return remote(src, dst, xs.at[kind, j], xr.at[kind, j], at_x)

    def tok_rows(xx, yy):
        return pl.ds(pl.multiple_of(xx * ROWS + yy * CHUNK, CHUNK), CHUNK)

    for m in (W_Q, W_K, W_V):
        y_send(m)
        z_send(m, 0)
    go_on(remote(tok.at[1 - y], xw.at[tok_rows(x, y)], done.at[0], yr.at[Y_TOK], at_y))
    go_on(x_copy(X_TOK, 0, tok.at[y], xw.at[tok_rows(x, y)]))
    z_send(W_VEC, 0)
    for m in range(W_KINDS):
        own_send(m)
    local_x = pltpu.make_async_copy(tok.at[y], xw.at[tok_rows(x, y)], ls.at[8])
    local_x.start()
    local_cot = pltpu.make_async_copy(cot.at[y], cotb.at[span(y, CHUNK)], ls.at[9])
    local_cot.start()

    seg_row = seg[pl.ds(y, 1), :].astype(F32)
    blocks = [(p % 2) * 2 + p // 2 for p in range(4)]
    across = [jnp.broadcast_to(seg_row[:, n * 128:(n + 1) * 128], (128, 128)) for n in blocks]
    down = [b.T for b in across]
    for t in range(2):
        for i, q in enumerate((t, t + 2)):
            for j in range(3):
                same = down[q] == across[t + j]
                bias[t, i * 128:(i + 1) * 128, j * 128:(j + 1) * 128] = jnp.where(same, 0.0, MASKED)
    acc[...] = jnp.zeros_like(acc)
    vg[...] = jnp.zeros_like(vg)

    for step in range(2):
        for m in (W_Q, W_K, W_V):
            z_serve(m, 0, step)
    z_send(W_OUT, 0)
    y_tok_here = xw.at[tok_rows(x, 1 - y)]
    remote(tok.at[1 - y], y_tok_here, done.at[0], yr.at[Y_TOK], at_y).wait_recv()
    go_on(x_copy(X_TOK, 1, y_tok_here, y_tok_here))
    for m in (W_Q, W_K, W_V):
        z_serve(m, 0, 2)
    y_send(W_OUT)
    z_serve(W_OUT, 0, 0)
    z_serve(W_OUT, 0, 1)
    z_send(W_UP, 0)
    for step in range(3):
        z_serve(W_VEC, 0, step)
    z_serve(W_OUT, 0, 2)
    y_send(W_UP)
    y_send(W_REST)
    for step in range(4):
        for m in (W_Q, W_K, W_V):
            y_serve(m, step)
    wait_weight(W_VEC)
    for d in range(8):
        vf[0:12, d * 128:(d + 1) * 128] = w_vec[d].astype(F32)
    local_x.wait()
    for j, yy in ((0, y), (1, 1 - y)):
        there = xw.at[tok_rows(1 - x, yy)]
        x_copy(X_TOK, j, there, there).wait_recv()
    for m in (W_Q, W_K, W_V):
        wait_weight(m)

    def head_bias(row):
        parts = [vf[row:row + 1, pl.ds(pl.multiple_of(yy * 512 + x * 256, 256), 256)] for yy in range(2)]
        return jnp.concatenate(parts, axis=1)

    for i in range(3):
        value = contract(xw[...], w_qkv[i], 1, 0)
        if i == 0:
            value = (value + head_bias(0)).astype(BF) * BF(HD ** -0.5)
        elif i == 2:
            value = value + head_bias(1)
        qkv[i] = value.astype(BF)

    low_half = lax.broadcasted_iota(jnp.int32, (1, 128), 1) < HD
    halves = (low_half, jnp.logical_not(low_half))
    none = jnp.zeros((), BF)

    def two_blocks(ref, t, lanes):
        return jnp.concatenate([ref[span(t, 128), lanes], ref[span(t + 2, 128), lanes]], axis=0)

    def attend(index, carry):
        pair, t = index // 2, index % 2
        lanes = span(pair, 128)
        keys = pl.ds(pl.multiple_of(t * 128, 128), WINDOW)
        query = two_blocks(qkv.at[0], t, lanes)
        key, value = qkv[1, keys, lanes], qkv[2, keys, lanes]
        total = jnp.zeros((ROWS, 128), F32)
        for h, half in enumerate(halves):
            scores = contract(jnp.where(half, query, none), key, 1, 1) + bias[t]
            top = jnp.max(scores, axis=1, keepdims=True)
            weight = jnp.exp(scores - top)
            share_of = 1.0 / jnp.sum(weight, axis=1, keepdims=True)
            weight = (weight * share_of).astype(BF)
            prob[pair * 4 + t * 2 + h] = weight
            total = total + contract(weight, jnp.where(half, value, none), 1, 0)
        total = total.astype(BF)
        ctx[span(t, 128), lanes] = total[:128]
        ctx[span(t + 2, 128), lanes] = total[128:]
        return carry

    z_serve(W_UP, 0, 0)
    lax.fori_loop(0, 4, attend, 0)
    for step in range(4):
        y_serve(W_OUT, step)
    lax.fori_loop(4, 8, attend, 0)
    up_early, up_late = z_serve_split(W_UP, 0, 1, middle, edge)
    up_early()
    z_send(W_DOWN, 0)

    def rows_of(s):
        mine = jnp.where(s < 2, x, 1 - x)
        return pl.ds(pl.multiple_of(mine * ROWS + lax.rem(s, 2) * CHUNK, CHUNK), CHUNK)

    def x_sum(kind, j):
        return x_copy(kind, j, stage.at[span(j, CHUNK)], recv.at[span(j, CHUNK)])

    def x_rows(kind, j, buf):
        here = buf.at[pl.ds(pl.multiple_of(x * ROWS + j * CHUNK, CHUNK), CHUNK)]
        return x_copy(kind, j, here, here)

    def hand_over(kind, before, s, value):
        @pl.when(s < 2)
        def _():
            own[span(s, CHUNK), :] = value

        @pl.when(s >= 2)
        def _():
            if before is not None:
                x_sum(before, s - 2).wait_send()
            stage[span(s - 2, CHUNK), :] = value.astype(BF)
            x_sum(kind, s - 2).start()

    wait_weight(W_OUT)

    def mix(i, carry):
        s = lax.rem(i + 2, 4)
        hand_over(X_MIX, None, s, contract(ctx[rows_of(s), :], w_out[...], 1, 0))
        return carry

    lax.fori_loop(0, 4, mix, 0)
    up_late()
    z_serve(W_UP, 0, 2)
    y_serve(W_REST, 0)
    z_send(W_REST, 0)
    z_send(W_REST, 1)
    y_serve(W_UP, 0)
    z_serve(W_DOWN, 0, 0, keep=True)
    z_serve(W_DOWN, 0, 1, keep=True)

    def row_of(row):
        return vf[row:row + 1, :]

    def normed(value):
        centred = value - jnp.mean(value, axis=1, keepdims=True)
        inverse = lax.rsqrt(jnp.mean(centred * centred, axis=1, keepdims=True) + NORM_EPS)
        return centred * inverse, inverse

    def norm_back(normal, inverse, grad):
        first = jnp.mean(grad, axis=1, keepdims=True)
        second = jnp.mean(grad * normal, axis=1, keepdims=True)
        return inverse * (grad - first - normal * second)

    def tiles(j, body):
        def step(i, carry):
            body(pl.ds(pl.multiple_of(j * CHUNK + i * TILE, TILE), TILE),
                 pl.ds(pl.multiple_of(x * ROWS + j * CHUNK + i * TILE, TILE), TILE))
            return carry
        lax.fori_loop(0, CHUNK // TILE, step, 0)

    def first_norm(r, g):
        summed = xw[g, :].astype(F32) + own[r, :] + recv[r, :].astype(F32) + row_of(R_BO)
        normal, inverse = normed(summed)
        n1[r, :] = normal
        inv1[r, :] = jnp.broadcast_to(inverse, (TILE, 128))
        hw[g, :] = (normal * row_of(R_G1) + row_of(R_C1)).astype(BF)

    for j in range(2):
        x_sum(X_MIX, j).wait_recv()
        tiles(j, first_norm)
        x_rows(X_NORM, j, hw).start()

    y_send(W_DOWN)
    z_over(W_DOWN, 0)
    z_over(W_DOWN, 1)
    for step in range(1, 4):
        y_serve(W_UP, step)
    z_serve(W_DOWN, 0, 2)
    for r in range(2):
        z_serve(W_REST, r, 0)
        z_serve(W_REST, r, 1)
    wait_weight(W_UP)

    def arrived(kind, s, buf):
        @pl.when(s >= 2)
        def _():
            there = buf.at[rows_of(s)]
            x_copy(kind, s - 2, there, there).wait_recv()

    def up_bias(n):
        return vf[pl.ds(8 + n * 2 + x, 1), :]

    def ffn_up(s, carry):
        rows = rows_of(s)
        arrived(X_NORM, s, hw)
        for n in range(2):
            pre = contract(hw[rows, :], w_up[:, n * 1024:(n + 1) * 1024], 1, 0) + up_bias(n)
            cdf = 0.5 * (1.0 + lax.erf(pre * SQRT_HALF))
            act[rows, n * 1024:(n + 1) * 1024] = (pre * cdf).astype(BF)
            slope[rows, n * 1024:(n + 1) * 1024] = (
                cdf + pre * INV_ROOT_TAU * jnp.exp(-0.5 * pre * pre)
            ).astype(BF)
        return carry

    lax.fori_loop(0, 2, ffn_up, 0)
    y_serve(W_DOWN, 0)
    y_serve(W_DOWN, 1)
    lax.fori_loop(2, 3, ffn_up, 0)
    z_serve(W_REST, 0, 2)
    z_serve(W_REST, 1, 2)
    y_serve(W_DOWN, 2)
    lax.fori_loop(3, 4, ffn_up, 0)
    y_serve(W_DOWN, 3)
    go_on(remote(cot.at[1 - y], cotb.at[span(y, CHUNK)], done.at[0], yr.at[Y_COT], at_y))

    def ffn_copy(step):
        cols = span(source_of(step), 256)
        return remote(stage.at[:, cols], recv.at[:, cols], fs.at[step], fr.at[step], at_x)

    for j in range(2):
        x_sum(X_MIX, j).wait_send()
    for step in range(4):
        wait_down(step)
        cols = span(source_of(step), 256)
        stage[:, cols] = contract(act[span(1 - x, ROWS), :], w_down[:, cols], 1, 0).astype(BF)
        ffn_copy(step).start()
        own[:, cols] = contract(act[span(x, ROWS), :], w_down[:, cols], 1, 0)

    def bump(row, value):
        acc[row] += fold_rows(value)

    def second_norm(r, g):
        h1 = n1[r, :] * row_of(R_G1) + row_of(R_C1)
        normal, inverse = normed(h1 + own[r, :] + recv[r, :].astype(F32) + row_of(R_BD))
        outb[r, :] = (normal * row_of(R_G2) + row_of(R_C2)).astype(BF)
        dy = cotb[r, :].astype(F32)
        bump(R_G2, dy * normal)
        bump(R_C2, dy)
        grad = norm_back(normal, inverse, dy * row_of(R_G2))
        bump(R_BD, grad)
        da[r, :] = grad
        aw[g, :] = grad.astype(BF)

    local_cot.wait()
    cot_here = cotb.at[span(1 - y, CHUNK)]
    remote(cot.at[1 - y], cot_here, done.at[0], yr.at[Y_COT], at_y).wait_recv()
    for step in range(4):
        ffn_copy(step).wait()
    for j in range(2):
        tiles(j, second_norm)
        x_rows(X_DA2, j, aw).start()
    out_here = pltpu.make_async_copy(outb.at[span(y, CHUNK)], out.at[y], os.at[0])
    out_here.start()
    go_on(remote(outb.at[span(1 - y, CHUNK)], out.at[y], done.at[0], yr.at[Y_OUT], at_y))

    def ffn_back(s, carry):
        rows = rows_of(s)
        arrived(X_DA2, s, aw)
        for n in range(2):
            cols = slice(n * 1024, (n + 1) * 1024)
            grad = contract(aw[rows, :], w_down[cols, :], 1, 1) * slope[rows, cols].astype(F32)
            bump(R_BU + n, grad)
            slope[rows, cols] = grad.astype(BF)
        hand_over(X_DH, None, s, contract(slope[rows, :], w_up[...], 1, 1))
        return carry

    lax.fori_loop(0, 4, ffn_back, 0)

    units = {
        U_DA: (g_down.at[0], c_down.at[0], y_da, z_da, h_da, o_down.at[0:512], gd.at[0:512]),
        U_DB: (g_down.at[1], c_down.at[1], y_db, z_db, h_db, o_down.at[512:1024], gd.at[512:1024]),
        U_OUT: (g_out, c_out, y_out, z_out, h_out, o_out, go),
    }
    for u, i in ((U_UA, 0), (U_UB, 1)):
        rows = slice(i * 64, (i + 1) * 64)
        units[u] = tuple(r.at[i] for r in (g_up, c_up, y_up, z_up, h_up)) + (o_up.at[rows], gu.at[rows])
    for u, i in ((U_Q, 0), (U_K, 1), (U_V, 2)):
        units[u] = tuple(r.at[i] for r in (g_qkv, c_qkv, y_qkv, z_qkv, h_qkv, o_qkv, gq))

    def piece_loop(rows, body):
        size = min(rows, CHUNK)

        def step(i, carry):
            body(span(i, size))
            return carry
        lax.fori_loop(0, rows // size, step, 0)

    def add_piece(g, yy, zz, other):
        def body(r):
            g[c, yy, zz, r, :] = (g[c, yy, zz, r, :].astype(F32) + other[r, :].astype(F32)).astype(BF)
        piece_loop(g.shape[3], body)

    def core_copy(u):
        g, rc = units[u][0], units[u][1]
        return remote(g.at[1 - c], rc, done.at[0], grc.at[u], at_c)

    def core_send(u):
        go_on(core_copy(u))

    def core_add(u, r):
        g, rc = units[u][0], units[u][1]
        for zz in range(ZS):
            add_piece(g, column(r), zz, rc.at[column(r), zz])

    def rs_y_copy(u):
        g, ry = units[u][0], units[u][2]
        source = g.at[c, 1 - y, pl.ds(z, 1)] if u in Z_FIRST else g.at[c, 1 - y]
        return remote(source, ry, done.at[0], gry.at[u], at_y)

    def rs_z_copy(u, r, k):
        g, rz = units[u][0], units[u][3]
        to = lax.rem(z + k, ZS)
        return remote(g.at[c, column(r), to], rz.at[r, k - 1], done.at[0], grz.at[u, r, k - 1], z_device(to))

    def rs_hand_on(u, r):
        g, rh = units[u][0], units[u][4]
        far = jnp.where(z == 0, ZS - 1, 0)
        return remote(g.at[c, column(r), far], rh.at[r], done.at[0], grz.at[u, r, 3], z_device(jnp.where(z == 0, 1, 2)))

    def z_hand_on(u, r):
        go_if(edge, rs_hand_on(u, r))

    def z_begin(u, r):
        go_if(z != ZS - 1, rs_z_copy(u, r, 1))
        go_if(z != 0, rs_z_copy(u, r, 3))
        go_if(edge, rs_z_copy(u, r, 2))

    def z_relay(u, r):
        g, rh = units[u][0], units[u][4]

        @pl.when(middle)
        def _():
            rs_hand_on(u, r).wait_recv()
            add_piece(g, column(r), lax.rem(z + 2, ZS), rh.at[r])
        go_if(middle, rs_z_copy(u, r, 2))

    def start(u):
        core_copy(u).wait_recv()
        core_add(u, 1)
        if u in Z_FIRST:
            z_hand_on(u, 1)
            core_add(u, 0)
            z_hand_on(u, 0)
            z_begin(u, 1)
            z_begin(u, 0)
        else:
            go_on(rs_y_copy(u))
            core_add(u, 0)

    def y_to_z(u):
        g, ry = units[u][0], units[u][2]
        rs_y_copy(u).wait_recv()
        for zz in range(ZS):
            add_piece(g, y, zz, ry.at[zz])
        z_hand_on(u, 0)
        z_begin(u, 0)

    def wait_z(u, r):
        rs_z_copy(u, r, 2).wait_recv()

        @pl.when(z != 0)
        def _():
            rs_z_copy(u, r, 1).wait_recv()

        @pl.when(z != ZS - 1)
        def _():
            rs_z_copy(u, r, 3).wait_recv()

    def z_total(u, r, rows):
        g, rz = units[u][0], units[u][3]
        value = g[c, column(r), z, rows, :].astype(F32)
        for k in range(ZS - 1):
            value = value + rz[r, k, rows, :].astype(F32)
        return value

    def z_to_y(u):
        g = units[u][0]
        wait_z(u, 1)

        def body(rows):
            g[c, 1 - y, z, rows, :] = z_total(u, 1, rows).astype(BF)
        piece_loop(g.shape[3], body)
        go_on(rs_y_copy(u))

    finals = []

    def finish(u):
        g, _, ry, _, _, o, dest = units[u]
        wait_z(u, 0)
        if u in Z_FIRST:
            rs_y_copy(u).wait_recv()

        def body(rows):
            value = z_total(u, 0, rows)
            if u in Z_FIRST:
                value = value + ry[0, rows, :].astype(F32)
            o[rows, :] = value
        piece_loop(g.shape[3], body)
        copy = pltpu.make_async_copy(o, dest, os.at[1 + u])
        copy.start()
        finals.append(copy)

    for u in units:
        for r in range(2 if u in Z_FIRST else 1):
            for k, alone in ((1, z == 0), (3, z == ZS - 1)):
                @pl.when(alone)
                def _(u=u, r=r, k=k):
                    rz = units[u][3]
                    rz[r, k - 1] = jnp.zeros(rz.shape[2:], BF)

    def grad_down(i, carry):
        half, yy = 1 - i // 2, i % 2
        value = contract(act[:, span(yy * 2 + half, 512)], aw[...], 0, 0).astype(BF)
        for d in range(8):
            g_down[half, d % 2, yy, d // 2] = value[:, d * 128:(d + 1) * 128]
        return carry

    lax.fori_loop(0, 2, grad_down, 0)
    core_send(U_DB)
    lax.fori_loop(2, 4, grad_down, 0)
    core_send(U_DA)
    start(U_DB)

    def grad_up(index, carry):
        i, n = index // 2, index % 2
        value = contract(hw[:, span(i, 512)], slope[:, span(n, 1024)], 0, 0).astype(BF)
        for d in range(4):
            for part in range(2):
                r = d * 128 + part * 64
                g_up[part, d % 2, n, i * 2 + d // 2] = value[r:r + 64, :]
        return carry

    lax.fori_loop(0, 4, grad_up, 0)
    core_send(U_UA)
    core_send(U_UB)
    for u in (U_DA, U_UA, U_UB):
        start(u)

    def back_norm(r, g):
        grad = da[r, :] + own[r, :] + recv[r, :].astype(F32)
        normal = n1[r, :]
        bump(R_G1, grad * normal)
        bump(R_C1, grad)
        grad = norm_back(normal, inv1[r, 0:1], grad * row_of(R_G1))
        bump(R_BO, grad)
        da[r, :] = grad
        a1w[g, :] = grad.astype(BF)

    for j in range(2):
        x_sum(X_DH, j).wait_recv()
        tiles(j, back_norm)
        x_rows(X_DA1, j, a1w).start()

    z_relay(U_DA, 1)
    z_relay(U_DA, 0)

    def ctx_back(s, carry):
        rows = rows_of(s)
        arrived(X_DA1, s, a1w)
        dctx[rows, :] = contract(a1w[rows, :], w_out[...], 1, 1).astype(BF)
        return carry

    lax.fori_loop(0, 4, ctx_back, 0)

    def attend_back(pair, carry):
        lanes = span(pair, 128)
        for t in range(2):
            keys = pl.ds(t * 128, WINDOW)
            query = two_blocks(qkv.at[0], t, lanes)
            key, value = qkv[1, keys, lanes], qkv[2, keys, lanes]
            grad = two_blocks(dctx, t, lanes)
            product = grad.astype(F32) * two_blocks(ctx, t, lanes).astype(F32)
            grad_q = jnp.zeros((ROWS, 128), F32)
            grad_k = jnp.zeros((WINDOW, 128), F32)
            grad_v = jnp.zeros((WINDOW, 128), F32)
            for h, half in enumerate(halves):
                grad_h = jnp.where(half, grad, none)
                weight = prob[pair * 4 + t * 2 + h]
                row_dot = jnp.sum(jnp.where(half, product, 0.0), axis=1, keepdims=True)
                score = (weight.astype(F32) * (contract(grad_h, value, 1, 1) - row_dot)).astype(BF)
                grad_q = grad_q + contract(score, jnp.where(half, key, none), 1, 0)
                grad_k = grad_k + contract(score, jnp.where(half, query, none), 0, 0)
                grad_v = grad_v + contract(weight, grad_h, 0, 0)
            grad_q = grad_q * (HD ** -0.5)
            acc[R_BQ, :, lanes] += fold_rows(grad_q)
            acc[R_BV, :, lanes] += fold_rows(grad_v)
            grad_q = grad_q.astype(BF)
            qkv[0, t * 128:t * 128 + 128, lanes] = grad_q[:128]
            qkv[0, t * 128 + 256:t * 128 + 384, lanes] = grad_q[128:]
            if t == 0:
                acc_k[0:WINDOW, :] = grad_k
                acc_v[0:WINDOW, :] = grad_v
                acc_k[WINDOW:SEQ, :] = jnp.zeros((128, 128), F32)
                acc_v[WINDOW:SEQ, :] = jnp.zeros((128, 128), F32)
            else:
                for i, total, more in ((1, acc_k, grad_k), (2, acc_v, grad_v)):
                    qkv[i, 0:128, lanes] = total[0:128, :].astype(BF)
                    qkv[i, 128:SEQ, lanes] = (total[128:SEQ, :] + more).astype(BF)
        return carry

    def grad_out():
        value = contract(ctx[...], a1w[...], 0, 0).astype(BF)
        for d in range(8):
            for yy in range(2):
                g_out[d % 2, yy, d // 2] = value[yy * 256:(yy + 1) * 256, d * 128:(d + 1) * 128]

    grad_out()
    core_send(U_OUT)
    y_to_z(U_DB)
    lax.fori_loop(0, 4, attend_back, 0)

    for row in range(2, 8):
        line = jnp.sum(acc[row], axis=0, keepdims=True)
        for d in range(8):
            vg[d % 2, d // 2, row:row + 1, :] = line[:, d * 128:(d + 1) * 128]
    for n in range(2):
        line = jnp.sum(acc[R_BU + n], axis=0, keepdims=True)
        for d in range(8):
            vg[d % 2, d // 2, pl.ds(8 + n * 2 + x, 1), :] = line[:, d * 128:(d + 1) * 128]
    for row, source in ((0, R_BQ), (1, R_BV)):
        line = jnp.sum(acc[source], axis=0, keepdims=True)
        for yy in range(2):
            for half in range(2):
                vg[half, 2 * yy + x, row:row + 1, :] = (
                    line[:, yy * 256 + half * 128:yy * 256 + (half + 1) * 128]
                )
    vec_x = remote(vg, vgx, vs.at[0], vr.at[0], at_x)
    vec_c = remote(vg.at[1 - c], vgc, vs.at[1], vr.at[1], at_c)
    vec_y = remote(vg.at[c], vgy, vs.at[2], vr.at[2], at_y)

    def vec_z(k):
        to = lax.rem(z + k, ZS)
        return remote(vg.at[c, to], vgz.at[k - 1], vs.at[2 + k], vr.at[2 + k], z_device(to))

    vec_x.start()

    def input_back(i, carry):
        s = lax.rem(i + 2, 4)
        rows = rows_of(s)
        value = contract(qkv[0, rows, :], w_qkv[0], 1, 1)
        value = value + contract(qkv[1, rows, :], w_qkv[1], 1, 1)
        value = value + contract(qkv[2, rows, :], w_qkv[2], 1, 1)
        hand_over(X_DX, X_DH, s, value)
        return carry

    lax.fori_loop(0, 2, input_back, 0)
    start(U_OUT)
    z_relay(U_DB, 0)
    y_to_z(U_UA)
    vec_x.wait()
    vg[...] = vg[...] + vgx[...]
    vec_c.start()

    def grad_qkv(index, carry):
        kind, i = index // 2, index % 2
        value = contract(xw[:, span(i, 512)], qkv[kind], 0, 0).astype(BF)
        for d in range(4):
            for yy in range(2):
                g_qkv[kind, d % 2, yy, i * 2 + d // 2] = (
                    value[d * 128:(d + 1) * 128, yy * 256:(yy + 1) * 256]
                )
        return carry

    for kind, u in ((0, U_Q), (1, U_K), (2, U_V)):
        lax.fori_loop(kind * 2, kind * 2 + 2, grad_qkv, 0)
        core_send(u)
    vec_c.wait()
    vg[c] = vg[c] + vgc[...]
    vec_y.start()
    for u in (U_Q, U_K, U_V):
        start(u)
    y_to_z(U_UB)
    lax.fori_loop(2, 4, input_back, 0)
    z_relay(U_OUT, 1)
    z_relay(U_OUT, 0)
    vec_y.wait()
    vg[c] = vg[c] + vgy[...]
    for k in range(1, ZS):
        vec_z(k).start()

    def last_sum(j, other):
        x_sum(X_DX, j).wait_recv()

        def body(r, g):
            value = da[r, :] + own[r, :] + recv[r, :].astype(F32)
            if other:
                gts[pl.ds(pl.multiple_of(r.start - j * CHUNK, TILE), TILE), :] = value.astype(BF)
            else:
                da[r, :] = value
        tiles(j, body)

    last_sum(1 - y, True)
    go_on(remote(gts, gtr, done.at[0], yr.at[Y_GTOK], at_y))
    last_sum(y, False)
    gtok_here = pltpu.make_async_copy(da.at[span(y, CHUNK)], gtok.at[y], os.at[9])
    gtok_here.start()
    z_relay(U_UA, 0)
    y_to_z(U_Q)
    z_to_y(U_DA)
    y_to_z(U_K)
    z_relay(U_UB, 0)
    z_to_y(U_OUT)
    y_to_z(U_V)
    for u in (U_Q, U_K, U_V):
        z_relay(u, 0)
    for k in range(1, ZS):
        vec_z(k).wait()
    gvb[...] = vg[c, z] + vgz[0] + vgz[1] + vgz[2]
    vec_here = pltpu.make_async_copy(gvb.at[0:12], gv, os.at[10])
    vec_here.start()
    for u in (U_DA, U_DB, U_UA, U_UB):
        finish(u)
    remote(gts, gtr, done.at[0], yr.at[Y_GTOK], at_y).wait_recv()
    gtf[...] = gtr[...].astype(F32)
    gtok_there = pltpu.make_async_copy(gtf, gtok.at[1 - y], os.at[11])
    gtok_there.start()
    finish(U_OUT)
    finish(U_Q)
    finish(U_K)
    finish(U_V)
    remote(outb.at[span(1 - y, CHUNK)], out.at[1 - y], done.at[0], yr.at[Y_OUT], at_y).wait_recv()
    for kind, buf in ((X_NORM, hw), (X_DA2, aw), (X_DA1, a1w)):
        for j in range(2):
            x_rows(kind, j, buf).wait_send()
    for j in range(2):
        x_sum(X_DX, j).wait_send()
    for copy in sent:
        copy.wait_send()
    for condition, copy in later:
        @pl.when(condition)
        def _(copy=copy):
            copy.wait_send()
    for m in range(W_KINDS):
        remote(half_of(m), half_of(m), wsc.at[m], wrc.at[m], at_c).wait_send()
    for copy in finals + [out_here, gtok_here, gtok_there, vec_here]:
        copy.wait()


def layer(tokens, segment_ids, w_qkv, w_out, w_up, w_down, vectors, cotangent):
    vmem, dma = pltpu.VMEM, pltpu.SemaphoreType.DMA
    outs = (
        jax.ShapeDtypeStruct(tokens.shape, BF),
        jax.ShapeDtypeStruct(tokens.shape, F32),
        jax.ShapeDtypeStruct(w_qkv.shape, F32),
        jax.ShapeDtypeStruct(w_out.shape, F32),
        jax.ShapeDtypeStruct(w_up.shape, F32),
        jax.ShapeDtypeStruct(w_down.shape, F32),
        jax.ShapeDtypeStruct(vectors.shape, F32),
    )
    scratch = [
        vmem((3, D, COLS), BF), vmem((COLS, D), BF), vmem((D, HID), BF), vmem((HID, D), BF),
        vmem((8, 12, 128), BF), vmem((16, D), F32),
    ]
    half_down, half_up, piece_out, piece_qkv = (512, 128), (64, 1024), (256, 128), (128, 256)
    for shape in ((2, 2, 4), (2, 4)):
        scratch += [
            vmem((2,) + shape + half_down, BF), vmem((2,) + shape + half_up, BF),
            vmem(shape + piece_out, BF), vmem((3,) + shape + piece_qkv, BF),
        ]
    for y_shape, z_shape in (((4,), (1,)), ((1, 3), (2, 3)), ((1,), (2,))):
        scratch += [
            vmem(z_shape + half_down, BF), vmem(y_shape + half_down, BF),
            vmem((2,) + y_shape + half_up, BF), vmem(z_shape + piece_out, BF),
            vmem((3,) + y_shape + piece_qkv, BF),
        ]
    scratch += [vmem((3, 128, 256), F32), vmem((256, 128), F32), vmem((128, 1024), F32), vmem((1024, 128), F32)]
    scratch += [
        vmem((SEQ, D), BF), vmem((3, SEQ, COLS), BF), vmem((SEQ, COLS), BF),
        vmem((16, ROWS, WINDOW), BF), vmem((2, ROWS, WINDOW), F32), vmem((SEQ, D), BF),
        vmem((SEQ, HID), BF), vmem((SEQ, HID), BF), vmem((SEQ, D), BF), vmem((SEQ, D), BF),
        vmem((SEQ, COLS), BF),
        vmem((ROWS, D), F32), vmem((ROWS, D), F32), vmem((ROWS, D), F32), vmem((ROWS, 128), F32),
        vmem((ROWS, D), BF), vmem((ROWS, D), BF), vmem((ROWS, D), BF), vmem((ROWS, D), BF),
        vmem((CHUNK, D), BF), vmem((CHUNK, D), BF), vmem((CHUNK, D), F32),
        vmem((12, 8, D), F32),
        vmem((2, 4, 16, 128), F32), vmem((2, 4, 16, 128), F32), vmem((4, 16, 128), F32),
        vmem((4, 16, 128), F32), vmem((3, 16, 128), F32), vmem((16, 128), F32),
        vmem((SEQ, 128), F32), vmem((SEQ, 128), F32),
        dma((1,)), dma((8, 2, 3)), dma((8, 4)), dma((8,)), dma((8,)), dma((2, 4)), dma((4,)), dma((4,)),
        dma((8, 2)), dma((8, 2)), dma((4,)),
        dma((8,)), dma((8,)), dma((8, 2, 4)),
        dma((6,)), dma((6,)), dma((10,)), dma((12,)),
    ]
    hbm = pl.BlockSpec(memory_space=pl.ANY)
    return pl.pallas_call(
        layer_kernel,
        out_shape=outs,
        in_specs=[hbm, pl.BlockSpec(memory_space=pltpu.VMEM)] + [hbm] * 6,
        out_specs=[hbm] * 7,
        scratch_shapes=scratch,
        compiler_params=pltpu.CompilerParams(
            collective_id=0, has_side_effects=True, vmem_limit_bytes=67043328
        ),
    )(tokens, segment_ids, w_qkv, w_out, w_up, w_down, vectors, cotangent)


def solution(mesh):
    step = layer if (mesh.shape["dp"], mesh.shape["tensor"]) == (8, 4) else body
    return jax.shard_map(
        step,
        mesh=mesh,
        in_specs=(
            P("dp", "tensor", None),
            P("dp", None),
            P(None, "dp", "tensor"),
            P("tensor", "dp"),
            P("dp", "tensor"),
            P("tensor", "dp"),
            P(None, "dp"),
            P("dp", "tensor", None),
        ),
        out_specs=(
            P("dp", "tensor", None),
            P("dp", "tensor", None),
            P(None, "dp", "tensor"),
            P("tensor", "dp"),
            P("dp", "tensor"),
            P("tensor", "dp"),
            P(None, "dp"),
        ),
        check_vma=False,
    )
```

```python
import jax
import jax.numpy as jnp
from jax import lax
from jax.experimental import pallas as pl
from jax.experimental.pallas import tpu as pltpu
from jax.sharding import PartitionSpec as P

D = 1024
FF = 4096
HD = 64


NORM_EPS = 1e-06
SQRT_HALF = 0.7071067811865476
INV_ROOT_TAU = 0.3989422804014327
MASKED = -1e30


def gelu_value(pre_act):
    return 0.5 * pre_act * (1.0 + lax.erf(pre_act * SQRT_HALF))


def gelu_slope(pre_act):
    return 0.5 * (1.0 + lax.erf(pre_act * SQRT_HALF)) + pre_act * INV_ROOT_TAU * jnp.exp(
        -0.5 * pre_act * pre_act
    )


def norm_forward(summed, gain, shift):
    centred = summed - jnp.mean(summed, axis=-1, keepdims=True)
    inverse = lax.rsqrt(jnp.mean(centred * centred, axis=-1, keepdims=True) + NORM_EPS)
    normed = centred * inverse
    return (normed * gain + shift, normed, inverse)


def norm_backward(normed, inverse, grad_normed):
    first_mean = jnp.mean(grad_normed, axis=-1, keepdims=True)
    second_mean = jnp.mean(grad_normed * normed, axis=-1, keepdims=True)
    return inverse * (grad_normed - first_mean - normed * second_mean)


def attention_scores(query_heads, key_heads, segments):
    same_doc = segments[:, None] == segments[None, :]
    scores = jnp.einsum(
        "qhe,khe->hqk", query_heads, key_heads, preferred_element_type=jnp.float32
    ) * HD ** (-0.5)
    return jnp.where(same_doc[None], scores, MASKED)


def collect(w_qkv, w_out, w_up, w_down, vectors):
    return (
        lax.all_gather(w_qkv, "dp", axis=1, tiled=True),
        lax.all_gather(w_out, "dp", axis=1, tiled=True),
        lax.all_gather(w_up, "dp", axis=0, tiled=True),
        lax.all_gather(w_down, "dp", axis=1, tiled=True),
        lax.all_gather(vectors, "dp", axis=1, tiled=True),
    )


def share(gradients):
    return (
        lax.psum_scatter(
            gradients[0].astype(jnp.bfloat16), "dp", scatter_dimension=1, tiled=True
        ).astype(jnp.float32),
        lax.psum_scatter(
            gradients[1].astype(jnp.bfloat16), "dp", scatter_dimension=1, tiled=True
        ).astype(jnp.float32),
        lax.psum_scatter(
            gradients[2].astype(jnp.bfloat16), "dp", scatter_dimension=0, tiled=True
        ).astype(jnp.float32),
        lax.psum_scatter(
            gradients[3].astype(jnp.bfloat16), "dp", scatter_dimension=1, tiled=True
        ).astype(jnp.float32),
        lax.psum_scatter(
            gradients[4].astype(jnp.bfloat16), "dp", scatter_dimension=1, tiled=True
        ).astype(jnp.float32),
    )


def body(tokens, segment_ids, w_qkv, w_out, w_up, w_down, vectors, cotangent):
    tensor_rank = lax.axis_index("tensor")
    local_cols = w_qkv.shape[2]
    head_count = local_cols // HD
    hidden = w_up.shape[1]
    col_start = tensor_rank * local_cols
    ffn_start = tensor_rank * hidden

    def forward(weights, tok_block, segments):
        qkv_w, out_w, up_w, down_w, vec_b = weights
        vec_f32 = vec_b.astype(jnp.float32)
        whole = lax.all_gather(tok_block, "tensor", axis=0, tiled=True)
        seq_len = whole.shape[0]
        projected = jnp.einsum("sd,tdc->tsc", whole, qkv_w, preferred_element_type=jnp.float32)
        bias_q = lax.dynamic_slice_in_dim(vec_f32[0], col_start, local_cols)
        bias_v = lax.dynamic_slice_in_dim(vec_f32[1], col_start, local_cols)
        query_heads = (projected[0] + bias_q).astype(jnp.bfloat16).reshape(seq_len, head_count, HD)
        key_heads = projected[1].astype(jnp.bfloat16).reshape(seq_len, head_count, HD)
        value_heads = (projected[2] + bias_v).astype(jnp.bfloat16).reshape(seq_len, head_count, HD)
        scores = attention_scores(query_heads, key_heads, segments)
        row_top = jnp.max(scores, axis=-1, keepdims=True)
        log_total = row_top + jnp.log(jnp.sum(jnp.exp(scores - row_top), axis=-1, keepdims=True))
        attn_probs = jnp.exp(scores - log_total).astype(jnp.bfloat16)
        context = jnp.einsum(
            "hqk,khe->qhe", attn_probs, value_heads, preferred_element_type=jnp.float32
        )
        context = context.reshape(seq_len, local_cols).astype(jnp.bfloat16)
        piece = context
        attn_mixed = lax.psum_scatter(
            jnp.dot(piece, out_w, preferred_element_type=jnp.float32).astype(jnp.bfloat16),
            "tensor",
            scatter_dimension=0,
            tiled=True,
        ).astype(jnp.float32)
        summed_one = tok_block.astype(jnp.float32) + attn_mixed + vec_f32[2]
        normed_out, normed_one, inverse_one = norm_forward(summed_one, vec_f32[3], vec_f32[4])
        normed_b = normed_out.astype(jnp.bfloat16)
        normed_whole = lax.all_gather(normed_b, "tensor", axis=0, tiled=True)
        bias_up = lax.dynamic_slice_in_dim(vec_f32[8:12].reshape(FF), ffn_start, hidden)
        pre_act = jnp.dot(normed_whole, up_w, preferred_element_type=jnp.float32) + bias_up
        activated = gelu_value(pre_act).astype(jnp.bfloat16)
        piece = activated
        summed_two = (
            normed_out
            + lax.psum_scatter(
                jnp.dot(piece, down_w, preferred_element_type=jnp.float32).astype(jnp.bfloat16),
                "tensor",
                scatter_dimension=0,
                tiled=True,
            ).astype(jnp.float32)
            + vec_f32[5]
        )
        final, normed_two, inverse_two = norm_forward(summed_two, vec_f32[6], vec_f32[7])
        saved = (
            whole,
            query_heads,
            key_heads,
            value_heads,
            log_total,
            context,
            normed_one,
            inverse_one,
            normed_whole,
            pre_act,
            activated,
            normed_two,
            inverse_two,
        )
        return (final.astype(jnp.bfloat16), saved)

    def backward(weights, saved, segments, grad_block):
        qkv_w, out_w, up_w, down_w, vec_b = weights
        vec_f32 = vec_b.astype(jnp.float32)
        (
            whole,
            query_heads,
            key_heads,
            value_heads,
            log_total,
            context,
            normed_one,
            inverse_one,
            normed_whole,
            pre_act,
            activated,
            normed_two,
            inverse_two,
        ) = saved
        seq_len = whole.shape[0]
        grad_final = grad_block.astype(jnp.float32)
        g_gain2 = jnp.sum(grad_final * normed_two, axis=0)
        g_shift2 = jnp.sum(grad_final, axis=0)
        grad_two = norm_backward(normed_two, inverse_two, grad_final * vec_f32[6])
        grad_two_b = grad_two.astype(jnp.bfloat16)
        g_bdown = jnp.sum(grad_two, axis=0)
        grad_two_whole = lax.all_gather(grad_two_b, "tensor", axis=0, tiled=True)
        g_down = jnp.dot(activated.T, grad_two_whole, preferred_element_type=jnp.float32)
        grad_pre = jnp.dot(
            grad_two_whole, down_w.T, preferred_element_type=jnp.float32
        ) * gelu_slope(pre_act)
        grad_pre_b = grad_pre.astype(jnp.bfloat16)
        g_bup = jnp.sum(grad_pre, axis=0)
        g_up = jnp.dot(normed_whole.T, grad_pre_b, preferred_element_type=jnp.float32)
        piece = grad_pre_b
        grad_one_in = grad_two + lax.psum_scatter(
            jnp.dot(piece, up_w.T, preferred_element_type=jnp.float32).astype(jnp.bfloat16),
            "tensor",
            scatter_dimension=0,
            tiled=True,
        ).astype(jnp.float32)
        g_gain1 = jnp.sum(grad_one_in * normed_one, axis=0)
        g_shift1 = jnp.sum(grad_one_in, axis=0)
        grad_one = norm_backward(normed_one, inverse_one, grad_one_in * vec_f32[3])
        grad_one_b = grad_one.astype(jnp.bfloat16)
        g_bout = jnp.sum(grad_one, axis=0)
        grad_one_whole = lax.all_gather(grad_one_b, "tensor", axis=0, tiled=True)
        g_out = jnp.dot(context.T, grad_one_whole, preferred_element_type=jnp.float32)
        grad_context = jnp.dot(grad_one_whole, out_w.T, preferred_element_type=jnp.float32).astype(
            jnp.bfloat16
        )
        grad_context = grad_context.reshape(seq_len, head_count, HD)
        scores = attention_scores(query_heads, key_heads, segments)
        attn_exact = jnp.exp(scores - log_total)
        attn_probs = attn_exact.astype(jnp.bfloat16)
        grad_probs = jnp.einsum(
            "qhe,khe->hqk", grad_context, value_heads, preferred_element_type=jnp.float32
        )
        row_dot = jnp.sum(attn_exact * grad_probs, axis=-1, keepdims=True)
        grad_scores = (attn_exact * (grad_probs - row_dot) * HD ** (-0.5)).astype(jnp.bfloat16)
        grad_value = jnp.einsum(
            "hqk,qhe->khe", attn_probs, grad_context, preferred_element_type=jnp.float32
        )
        grad_value = grad_value.reshape(seq_len, local_cols)
        grad_query = jnp.einsum(
            "hqk,khe->qhe", grad_scores, key_heads, preferred_element_type=jnp.float32
        )
        grad_query = grad_query.reshape(seq_len, local_cols)
        grad_key = jnp.einsum(
            "hqk,qhe->khe", grad_scores, query_heads, preferred_element_type=jnp.float32
        )
        grad_key = grad_key.reshape(seq_len, local_cols)
        grad_qkv = jnp.stack([grad_query, grad_key, grad_value]).astype(jnp.bfloat16)
        g_qkv = jnp.einsum("sd,tsc->tdc", whole, grad_qkv, preferred_element_type=jnp.float32)
        piece = grad_qkv
        grad_input = grad_one + lax.psum_scatter(
            jnp.einsum("tsc,tdc->sd", piece, qkv_w, preferred_element_type=jnp.float32).astype(
                jnp.bfloat16
            ),
            "tensor",
            scatter_dimension=0,
            tiled=True,
        ).astype(jnp.float32)
        zero_row = jnp.zeros((D,), jnp.float32)
        row_q = lax.dynamic_update_slice_in_dim(zero_row, jnp.sum(grad_query, axis=0), col_start, 0)
        row_v = lax.dynamic_update_slice_in_dim(zero_row, jnp.sum(grad_value, axis=0), col_start, 0)
        up_rows = lax.dynamic_update_slice_in_dim(
            jnp.zeros((FF,), jnp.float32), g_bup, ffn_start, 0
        ).reshape(4, D)
        first_rows = jnp.stack(
            [row_q, row_v, g_bout, g_gain1, g_shift1, g_bdown, g_gain2, g_shift2]
        )
        g_vec = jnp.concatenate([first_rows, up_rows], axis=0)
        return ((g_qkv, g_out, g_up, g_down, g_vec), grad_input)

    def one_batch(carried, batch_item):
        tok_block, segments, grad_block = batch_item
        forward_w = collect(w_qkv, w_out, w_up, w_down, vectors)
        final_b, saved = forward(forward_w, tok_block, segments)
        second = collect(w_qkv, w_out, w_up, w_down, vectors)
        gradients, grad_input = backward(second, saved, segments, grad_block)
        updated = jax.tree.map(jnp.add, carried, gradients)
        return (updated, (final_b, grad_input))

    initial = (
        jnp.zeros((3, D, local_cols), jnp.float32),
        jnp.zeros((local_cols, D), jnp.float32),
        jnp.zeros((D, hidden), jnp.float32),
        jnp.zeros((hidden, D), jnp.float32),
        jnp.zeros((12, D), jnp.float32),
    )
    carried, stacked = lax.scan(one_batch, initial, (tokens, segment_ids, cotangent))
    totals = share(carried)
    vector_grads = lax.psum(totals[4], "tensor")
    return (stacked[0], stacked[1], totals[0], totals[1], totals[2], totals[3], vector_grads)


Y_TOK, Y_COT, Y_OUT, Y_GTOK = range(4)
X_TOK, X_MIX, X_NORM, X_FFN, X_DA2, X_DH, X_DA1, X_DX = range(8)
W_Q, W_K, W_V, W_OUT, W_UP, W_DOWN, W_REST, W_VEC = range(8)
W_KINDS = 8
Y_FIRST = (W_REST,)
DIRECT = (W_VEC,)
FAR_FIRST = ()
U_DA, U_DB, U_UA, U_UB, U_OUT, U_V, U_K, U_Q = range(8)
Z_FIRST = (U_DA, U_OUT)
R_BQ, R_BV, R_BO, R_G1, R_C1, R_BD, R_G2, R_C2, R_BU = range(9)
ZS = 4
SEQ = 512
ROWS = 256
CHUNK = 128
TILE = 32
COLS = 512
HID = 2048
WINDOW = 384
BF = jnp.bfloat16
F32 = jnp.float32
MESH = pl.DeviceIdType.MESH


def span(index, size):
    return pl.ds(pl.multiple_of(index * size, size), size)


def contract(a, b, a_dim, b_dim):
    return lax.dot_general(a, b, (((a_dim,), (b_dim,)), ((), ())), preferred_element_type=F32)


def fold_rows(value):
    return jnp.sum(value.reshape(value.shape[0] // 8, 8, value.shape[1]), axis=0)


def layer_kernel(
    tok, seg, wq, wo, wu, wd, vec, cot,
    out, gtok, gq, go, gu, gd, gv,
    w_qkv, w_out, w_up, w_down, w_vec, vf,
    g_down, g_up, g_out, g_qkv,
    c_down, c_up, c_out, c_qkv,
    y_da, y_db, y_up, y_out, y_qkv,
    z_da, z_db, z_up, z_out, z_qkv,
    h_da, h_db, h_up, h_out, h_qkv,
    o_qkv, o_out, o_up, o_down,
    xw, qkv, ctx, prob, bias, hw, act, slope, aw, a1w, dctx,
    own, n1, da, inv1, recv, stage, cotb, outb, gts, gtr, gtf,
    acc, vg, vgx, vgc, vgy, vgz, gvb, acc_k, acc_v,
    done, wrz, wry, wrc, wrd, fs, fr, xs, xr, yr,
    grc, gry, grz, vs, vr, ls, os,
):
    dp = lax.axis_index("dp")
    tensor = lax.axis_index("tensor")
    z, c = dp // 2, dp % 2
    y, x = tensor // 2, tensor % 2
    at_x = {"dp": dp, "tensor": y * 2 + (1 - x)}
    at_y = {"dp": dp, "tensor": (1 - y) * 2 + x}
    at_c = {"dp": z * 2 + (1 - c), "tensor": tensor}

    def remote(src, dst, send, recv_sem, where):
        return pltpu.make_async_remote_copy(
            src_ref=src, dst_ref=dst, send_sem=send, recv_sem=recv_sem,
            device_id=where, device_id_type=MESH,
        )

    barrier = pltpu.get_barrier_semaphore()
    for where in [at_x, at_y, at_c] + [{"dp": lax.rem(z + k, ZS) * 2 + c, "tensor": tensor} for k in range(1, ZS)]:
        pl.semaphore_signal(barrier, inc=1, device_id=where, device_id_type=MESH)
    pl.semaphore_wait(barrier, 6)

    sent = []

    def go_on(copy):
        copy.start()
        sent.append(copy)

    args = [wq.at[0], wq.at[1], wq.at[2], wo, wu, wd.at[0:512], wd.at[512:1024], vec]
    edge = jnp.logical_or(z == 0, z == ZS - 1)
    middle = jnp.logical_not(edge)
    later = []

    def z_device(where):
        return {"dp": where * 2 + c, "tensor": tensor}

    def go_if(condition, copy):
        @pl.when(condition)
        def _():
            copy.start()
        later.append((condition, copy))

    def place(m, yy, d):
        if m <= W_V:
            return w_qkv.at[m, span(d, 128), span(yy, 256)]
        if m == W_OUT:
            return w_out.at[span(yy, 256), span(d, 128)]
        if m == W_UP:
            return w_up.at[span(d, 128), span(yy, 1024)]
        if m == W_DOWN or m == W_REST:
            return w_down.at[span(yy * 2 + m - W_DOWN, 512), span(d, 128)]
        return w_vec.at[d]

    even = lax.rem(z, 2) == 0
    near_first = (jnp.where(even, 3, 1), 2, jnp.where(even, 1, 3))

    def from_z(k):
        return lax.rem(z + ZS - k, ZS)

    def column(r):
        return y if r == 0 else 1 - y

    def z_send(m, r):
        source = args[m] if r == 0 else place(m, 1 - y, dp)
        steps = ((1, z != ZS - 1), (3, z != 0), (2, None))
        for k, there in (steps[2:] + steps[:2] if m in FAR_FIRST else steps):
            there = None if m in DIRECT else there
            copy = remote(
                source, place(m, column(r), dp), done.at[0], wrz.at[m, r, k - 1],
                z_device(lax.rem(z + k, ZS)),
            )
            if there is None:
                go_on(copy)
            else:
                go_if(there, copy)

    def z_serve(m, r, step, keep=False):
        z_take(m, r, step, keep)
        z_note(m, r, step)

    def z_serve_split(m, r, step, early, late):
        def first():
            @pl.when(early)
            def _():
                z_take(m, r, step)

        def second():
            @pl.when(late)
            def _():
                z_take(m, r, step)
            z_note(m, r, step)
        return first, second

    def z_parts(m, r, step):
        k = near_first[step]
        here = place(m, column(r), from_z(k) * 2 + c)
        slot = jnp.where(z == 1, 0, 2)
        hand_on = None
        if step == 1 and m not in DIRECT:
            hand_on = remote(
                here, here, done.at[0], wrz.at[m, r, slot], z_device(jnp.where(z == 1, 0, 3)),
            )
        over_y = None
        if r == 0 and m not in Y_FIRST and m != W_VEC:
            over_y = remote(here, here, done.at[0], wry.at[m, from_z(k)], at_y)
        return k, here, hand_on, over_y

    def z_over(m, step):
        z_parts(m, 0, step)[3].start()

    def z_take(m, r, step, keep=False):
        k, here, hand_on, over_y = z_parts(m, r, step)
        remote(here, here, done.at[0], wrz.at[m, r, k - 1], at_x).wait_recv()
        if hand_on is not None:
            @pl.when(middle)
            def _():
                hand_on.start()
        if over_y is not None and not keep:
            over_y.start()
        c_send(m, here, step + 1)

    def z_note(m, r, step):
        _, _, hand_on, over_y = z_parts(m, r, step)
        if hand_on is not None:
            later.append((middle, hand_on))
        if over_y is not None:
            sent.append(over_y)

    def y_send(m):
        go_on(remote(args[m], place(m, y, dp), done.at[0], wry.at[m, z], at_y))

    def source_of(step):
        return z if step == 0 else from_z(near_first[step - 1])

    def y_serve(m, step):
        zz = source_of(step)
        here = place(m, 1 - y, zz * 2 + c)
        remote(here, here, done.at[0], wry.at[m, zz], at_y).wait_recv()
        c_send(m, here, step)

    def c_send(m, source, step, dest=None):
        dest = source if dest is None else dest
        into = wrd.at[m - W_DOWN, step] if m in (W_DOWN, W_REST) else wrc.at[m]
        remote(source, dest, done.at[0], into, at_c).start()

    def own_send(m):
        c_send(m, args[m], 0, place(m, y, dp))
        pltpu.make_async_copy(args[m], place(m, y, dp), ls.at[m]).start()

    def half_of(m):
        if m <= W_V:
            return w_qkv.at[m, :, 0:256]
        return (
            w_out.at[0:256], w_up.at[:, 0:1024], w_down.at[0:512], w_down.at[0:512], w_vec.at[0:4]
        )[m - W_OUT]

    def wait_down(step):
        for m in (W_DOWN, W_REST):
            if step == 0:
                pltpu.make_async_copy(args[m], place(m, y, dp), ls.at[m]).wait()
            two = w_down.at[0:1024, 0:128]
            remote(two, two, done.at[0], wrd.at[m - W_DOWN, step], at_c).wait_recv()

    def wait_weight(m):
        pltpu.make_async_copy(args[m], place(m, y, dp), ls.at[m]).wait()
        remote(half_of(m), half_of(m), done.at[0], wrc.at[m], at_c).wait_recv()

    def x_copy(kind, j, src, dst):
        return remote(src, dst, xs.at[kind, j], xr.at[kind, j], at_x)

    def tok_rows(xx, yy):
        return pl.ds(pl.multiple_of(xx * ROWS + yy * CHUNK, CHUNK), CHUNK)

    for m in (W_Q, W_K, W_V):
        y_send(m)
        z_send(m, 0)
    go_on(remote(tok.at[1 - y], xw.at[tok_rows(x, y)], done.at[0], yr.at[Y_TOK], at_y))
    go_on(x_copy(X_TOK, 0, tok.at[y], xw.at[tok_rows(x, y)]))
    z_send(W_VEC, 0)
    for m in range(W_KINDS):
        own_send(m)
    local_x = pltpu.make_async_copy(tok.at[y], xw.at[tok_rows(x, y)], ls.at[8])
    local_x.start()
    local_cot = pltpu.make_async_copy(cot.at[y], cotb.at[span(y, CHUNK)], ls.at[9])
    local_cot.start()

    seg_row = seg[pl.ds(y, 1), :].astype(F32)
    blocks = [(p % 2) * 2 + p // 2 for p in range(4)]
    across = [jnp.broadcast_to(seg_row[:, n * 128:(n + 1) * 128], (128, 128)) for n in blocks]
    down = [b.T for b in across]
    for t in range(2):
        for i, q in enumerate((t, t + 2)):
            for j in range(3):
                same = down[q] == across[t + j]
                bias[t, i * 128:(i + 1) * 128, j * 128:(j + 1) * 128] = jnp.where(same, 0.0, MASKED)
    acc[...] = jnp.zeros_like(acc)
    vg[...] = jnp.zeros_like(vg)

    for step in range(2):
        for m in (W_Q, W_K, W_V):
            z_serve(m, 0, step)
    z_send(W_OUT, 0)
    y_tok_here = xw.at[tok_rows(x, 1 - y)]
    remote(tok.at[1 - y], y_tok_here, done.at[0], yr.at[Y_TOK], at_y).wait_recv()
    go_on(x_copy(X_TOK, 1, y_tok_here, y_tok_here))
    for m in (W_Q, W_K, W_V):
        z_serve(m, 0, 2)
    y_send(W_OUT)
    z_serve(W_OUT, 0, 0)
    z_serve(W_OUT, 0, 1)
    z_send(W_UP, 0)
    for step in range(3):
        z_serve(W_VEC, 0, step)
    z_serve(W_OUT, 0, 2)
    y_send(W_UP)
    y_send(W_REST)
    for step in range(4):
        for m in (W_Q, W_K, W_V):
            y_serve(m, step)
    wait_weight(W_VEC)
    for d in range(8):
        vf[0:12, d * 128:(d + 1) * 128] = w_vec[d].astype(F32)
    local_x.wait()
    for j, yy in ((0, y), (1, 1 - y)):
        there = xw.at[tok_rows(1 - x, yy)]
        x_copy(X_TOK, j, there, there).wait_recv()
    for m in (W_Q, W_K, W_V):
        wait_weight(m)

    def head_bias(row):
        parts = [vf[row:row + 1, pl.ds(pl.multiple_of(yy * 512 + x * 256, 256), 256)] for yy in range(2)]
        return jnp.concatenate(parts, axis=1)

    for i in range(3):
        value = contract(xw[...], w_qkv[i], 1, 0)
        if i == 0:
            value = (value + head_bias(0)).astype(BF) * BF(HD ** -0.5)
        elif i == 2:
            value = value + head_bias(1)
        qkv[i] = value.astype(BF)

    low_half = lax.broadcasted_iota(jnp.int32, (1, 128), 1) < HD
    halves = (low_half, jnp.logical_not(low_half))
    none = jnp.zeros((), BF)

    def two_blocks(ref, t, lanes):
        return jnp.concatenate([ref[span(t, 128), lanes], ref[span(t + 2, 128), lanes]], axis=0)

    def attend(index, carry):
        pair, t = index // 2, index % 2
        lanes = span(pair, 128)
        keys = pl.ds(pl.multiple_of(t * 128, 128), WINDOW)
        query = two_blocks(qkv.at[0], t, lanes)
        key, value = qkv[1, keys, lanes], qkv[2, keys, lanes]
        total = jnp.zeros((ROWS, 128), F32)
        for h, half in enumerate(halves):
            scores = contract(jnp.where(half, query, none), key, 1, 1) + bias[t]
            top = jnp.max(scores, axis=1, keepdims=True)
            weight = jnp.exp(scores - top)
            share_of = 1.0 / jnp.sum(weight, axis=1, keepdims=True)
            weight = (weight * share_of).astype(BF)
            prob[pair * 4 + t * 2 + h] = weight
            total = total + contract(weight, jnp.where(half, value, none), 1, 0)
        total = total.astype(BF)
        ctx[span(t, 128), lanes] = total[:128]
        ctx[span(t + 2, 128), lanes] = total[128:]
        return carry

    z_serve(W_UP, 0, 0)
    lax.fori_loop(0, 4, attend, 0)
    for step in range(4):
        y_serve(W_OUT, step)
    lax.fori_loop(4, 8, attend, 0)
    up_early, up_late = z_serve_split(W_UP, 0, 1, middle, edge)
    up_early()
    z_send(W_DOWN, 0)

    def rows_of(s):
        mine = jnp.where(s < 2, x, 1 - x)
        return pl.ds(pl.multiple_of(mine * ROWS + lax.rem(s, 2) * CHUNK, CHUNK), CHUNK)

    def x_sum(kind, j):
        return x_copy(kind, j, stage.at[span(j, CHUNK)], recv.at[span(j, CHUNK)])

    def x_rows(kind, j, buf):
        here = buf.at[pl.ds(pl.multiple_of(x * ROWS + j * CHUNK, CHUNK), CHUNK)]
        return x_copy(kind, j, here, here)

    def hand_over(kind, before, s, value):
        @pl.when(s < 2)
        def _():
            own[span(s, CHUNK), :] = value

        @pl.when(s >= 2)
        def _():
            if before is not None:
                x_sum(before, s - 2).wait_send()
            stage[span(s - 2, CHUNK), :] = value.astype(BF)
            x_sum(kind, s - 2).start()

    wait_weight(W_OUT)

    def mix(i, carry):
        s = lax.rem(i + 2, 4)
        hand_over(X_MIX, None, s, contract(ctx[rows_of(s), :], w_out[...], 1, 0))
        return carry

    lax.fori_loop(0, 4, mix, 0)
    up_late()
    z_serve(W_UP, 0, 2)
    y_serve(W_REST, 0)
    z_send(W_REST, 0)
    z_send(W_REST, 1)
    y_serve(W_UP, 0)
    z_serve(W_DOWN, 0, 0, keep=True)
    z_serve(W_DOWN, 0, 1, keep=True)

    def row_of(row):
        return vf[row:row + 1, :]

    def normed(value):
        centred = value - jnp.mean(value, axis=1, keepdims=True)
        inverse = lax.rsqrt(jnp.mean(centred * centred, axis=1, keepdims=True) + NORM_EPS)
        return centred * inverse, inverse

    def norm_back(normal, inverse, grad):
        first = jnp.mean(grad, axis=1, keepdims=True)
        second = jnp.mean(grad * normal, axis=1, keepdims=True)
        return inverse * (grad - first - normal * second)

    def tiles(j, body):
        def step(i, carry):
            body(pl.ds(pl.multiple_of(j * CHUNK + i * TILE, TILE), TILE),
                 pl.ds(pl.multiple_of(x * ROWS + j * CHUNK + i * TILE, TILE), TILE))
            return carry
        lax.fori_loop(0, CHUNK // TILE, step, 0)

    def first_norm(r, g):
        summed = xw[g, :].astype(F32) + own[r, :] + recv[r, :].astype(F32) + row_of(R_BO)
        normal, inverse = normed(summed)
        n1[r, :] = normal
        inv1[r, :] = jnp.broadcast_to(inverse, (TILE, 128))
        hw[g, :] = (normal * row_of(R_G1) + row_of(R_C1)).astype(BF)

    for j in range(2):
        x_sum(X_MIX, j).wait_recv()
        tiles(j, first_norm)
        x_rows(X_NORM, j, hw).start()

    y_send(W_DOWN)
    z_over(W_DOWN, 0)
    z_over(W_DOWN, 1)
    for step in range(1, 4):
        y_serve(W_UP, step)
    wait_weight(W_UP)

    def arrived(kind, s, buf):
        @pl.when(s >= 2)
        def _():
            there = buf.at[rows_of(s)]
            x_copy(kind, s - 2, there, there).wait_recv()

    def up_bias(n):
        return vf[pl.ds(8 + n * 2 + x, 1), :]

    def ffn_up(s, carry):
        rows = rows_of(s)
        arrived(X_NORM, s, hw)
        for n in range(2):
            pre = contract(hw[rows, :], w_up[:, n * 1024:(n + 1) * 1024], 1, 0) + up_bias(n)
            cdf = 0.5 * (1.0 + lax.erf(pre * SQRT_HALF))
            act[rows, n * 1024:(n + 1) * 1024] = (pre * cdf).astype(BF)
            slope[rows, n * 1024:(n + 1) * 1024] = (
                cdf + pre * INV_ROOT_TAU * jnp.exp(-0.5 * pre * pre)
            ).astype(BF)
        return carry

    lax.fori_loop(0, 2, ffn_up, 0)
    z_serve(W_DOWN, 0, 2)
    for r in range(2):
        z_serve(W_REST, r, 0)
        z_serve(W_REST, r, 1)
    y_serve(W_DOWN, 0)
    lax.fori_loop(2, 3, ffn_up, 0)
    y_serve(W_DOWN, 1)
    lax.fori_loop(3, 4, ffn_up, 0)
    y_serve(W_DOWN, 2)
    z_serve(W_REST, 0, 2)
    z_serve(W_REST, 1, 2)
    go_on(remote(cot.at[1 - y], cotb.at[span(y, CHUNK)], done.at[0], yr.at[Y_COT], at_y))

    def ffn_copy(step, j):
        cols = span(source_of(step), 256)
        return remote(
            stage.at[span(j, CHUNK), cols], recv.at[span(j, CHUNK), cols],
            fs.at[step, j], fr.at[step, j], at_x,
        )

    for j in range(2):
        x_sum(X_MIX, j).wait_send()
    for step in range(4):
        if step == 2:
            y_serve(W_DOWN, 3)
        wait_down(step)
        cols = span(source_of(step), 256)
        stage[:, cols] = contract(act[span(1 - x, ROWS), :], w_down[:, cols], 1, 0).astype(BF)
        for j in range(2):
            ffn_copy(step, j).start()
    for step in range(2):
        cols = span(step, 512)
        own[:, cols] = contract(act[span(x, ROWS), :], w_down[:, cols], 1, 0)

    def bump(row, value):
        acc[row] += fold_rows(value)

    def second_norm(r, g):
        h1 = n1[r, :] * row_of(R_G1) + row_of(R_C1)
        normal, inverse = normed(h1 + own[r, :] + recv[r, :].astype(F32) + row_of(R_BD))
        outb[r, :] = (normal * row_of(R_G2) + row_of(R_C2)).astype(BF)
        dy = cotb[r, :].astype(F32)
        bump(R_G2, dy * normal)
        bump(R_C2, dy)
        grad = norm_back(normal, inverse, dy * row_of(R_G2))
        bump(R_BD, grad)
        da[r, :] = grad
        aw[g, :] = grad.astype(BF)

    local_cot.wait()
    cot_here = cotb.at[span(1 - y, CHUNK)]
    remote(cot.at[1 - y], cot_here, done.at[0], yr.at[Y_COT], at_y).wait_recv()
    for j in range(2):
        for step in range(4):
            ffn_copy(step, j).wait()
        tiles(j, second_norm)
        x_rows(X_DA2, j, aw).start()
    out_here = pltpu.make_async_copy(outb.at[span(y, CHUNK)], out.at[y], os.at[0])
    out_here.start()
    go_on(remote(outb.at[span(1 - y, CHUNK)], out.at[y], done.at[0], yr.at[Y_OUT], at_y))

    def ffn_back(s, carry):
        rows = rows_of(s)
        arrived(X_DA2, s, aw)
        for n in range(2):
            cols = slice(n * 1024, (n + 1) * 1024)
            grad = contract(aw[rows, :], w_down[cols, :], 1, 1) * slope[rows, cols].astype(F32)
            bump(R_BU + n, grad)
            slope[rows, cols] = grad.astype(BF)
        hand_over(X_DH, None, s, contract(slope[rows, :], w_up[...], 1, 1))
        return carry

    lax.fori_loop(0, 4, ffn_back, 0)

    units = {
        U_DA: (g_down.at[0], c_down.at[0], y_da, z_da, h_da, o_down.at[0:512], gd.at[0:512]),
        U_DB: (g_down.at[1], c_down.at[1], y_db, z_db, h_db, o_down.at[512:1024], gd.at[512:1024]),
        U_OUT: (g_out, c_out, y_out, z_out, h_out, o_out, go),
    }
    for u, i in ((U_UA, 0), (U_UB, 1)):
        rows = slice(i * 64, (i + 1) * 64)
        units[u] = tuple(r.at[i] for r in (g_up, c_up, y_up, z_up, h_up)) + (o_up.at[rows], gu.at[rows])
    for u, i in ((U_Q, 0), (U_K, 1), (U_V, 2)):
        units[u] = tuple(r.at[i] for r in (g_qkv, c_qkv, y_qkv, z_qkv, h_qkv, o_qkv, gq))

    def piece_loop(rows, body):
        size = min(rows, CHUNK)

        def step(i, carry):
            body(span(i, size))
            return carry
        lax.fori_loop(0, rows // size, step, 0)

    def add_piece(g, yy, zz, other):
        def body(r):
            g[c, yy, zz, r, :] = (g[c, yy, zz, r, :].astype(F32) + other[r, :].astype(F32)).astype(BF)
        piece_loop(g.shape[3], body)

    def core_copy(u):
        g, rc = units[u][0], units[u][1]
        return remote(g.at[1 - c], rc, done.at[0], grc.at[u], at_c)

    def core_send(u):
        go_on(core_copy(u))

    def core_add(u, r):
        g, rc = units[u][0], units[u][1]
        for zz in range(ZS):
            add_piece(g, column(r), zz, rc.at[column(r), zz])

    def rs_y_copy(u):
        g, ry = units[u][0], units[u][2]
        source = g.at[c, 1 - y, pl.ds(z, 1)] if u in Z_FIRST else g.at[c, 1 - y]
        return remote(source, ry, done.at[0], gry.at[u], at_y)

    def rs_z_copy(u, r, k):
        g, rz = units[u][0], units[u][3]
        to = lax.rem(z + k, ZS)
        return remote(g.at[c, column(r), to], rz.at[r, k - 1], done.at[0], grz.at[u, r, k - 1], z_device(to))

    def rs_hand_on(u, r):
        g, rh = units[u][0], units[u][4]
        far = jnp.where(z == 0, ZS - 1, 0)
        return remote(g.at[c, column(r), far], rh.at[r], done.at[0], grz.at[u, r, 3], z_device(jnp.where(z == 0, 1, 2)))

    def z_hand_on(u, r):
        go_if(edge, rs_hand_on(u, r))

    def z_begin(u, r):
        go_if(z != ZS - 1, rs_z_copy(u, r, 1))
        go_if(z != 0, rs_z_copy(u, r, 3))
        go_if(edge, rs_z_copy(u, r, 2))

    def z_relay(u, r):
        g, rh = units[u][0], units[u][4]

        @pl.when(middle)
        def _():
            rs_hand_on(u, r).wait_recv()
            add_piece(g, column(r), lax.rem(z + 2, ZS), rh.at[r])
        go_if(middle, rs_z_copy(u, r, 2))

    def start(u):
        core_copy(u).wait_recv()
        core_add(u, 1)
        if u in Z_FIRST:
            z_hand_on(u, 1)
            core_add(u, 0)
            z_hand_on(u, 0)
            z_begin(u, 1)
            z_begin(u, 0)
        else:
            go_on(rs_y_copy(u))
            core_add(u, 0)

    def y_to_z(u):
        g, ry = units[u][0], units[u][2]
        rs_y_copy(u).wait_recv()
        for zz in range(ZS):
            add_piece(g, y, zz, ry.at[zz])
        z_hand_on(u, 0)
        z_begin(u, 0)

    def wait_z(u, r):
        rs_z_copy(u, r, 2).wait_recv()

        @pl.when(z != 0)
        def _():
            rs_z_copy(u, r, 1).wait_recv()

        @pl.when(z != ZS - 1)
        def _():
            rs_z_copy(u, r, 3).wait_recv()

    def z_total(u, r, rows):
        g, rz = units[u][0], units[u][3]
        value = g[c, column(r), z, rows, :].astype(F32)
        for k in range(ZS - 1):
            value = value + rz[r, k, rows, :].astype(F32)
        return value

    def z_to_y(u):
        g = units[u][0]
        wait_z(u, 1)

        def body(rows):
            g[c, 1 - y, z, rows, :] = z_total(u, 1, rows).astype(BF)
        piece_loop(g.shape[3], body)
        go_on(rs_y_copy(u))

    finals = []

    def finish(u):
        g, _, ry, _, _, o, dest = units[u]
        wait_z(u, 0)
        if u in Z_FIRST:
            rs_y_copy(u).wait_recv()

        def body(rows):
            value = z_total(u, 0, rows)
            if u in Z_FIRST:
                value = value + ry[0, rows, :].astype(F32)
            o[rows, :] = value
        piece_loop(g.shape[3], body)
        copy = pltpu.make_async_copy(o, dest, os.at[1 + u])
        copy.start()
        finals.append(copy)

    for u in units:
        for r in range(2 if u in Z_FIRST else 1):
            for k, alone in ((1, z == 0), (3, z == ZS - 1)):
                @pl.when(alone)
                def _(u=u, r=r, k=k):
                    rz = units[u][3]
                    rz[r, k - 1] = jnp.zeros(rz.shape[2:], BF)

    def grad_down(i, carry):
        half, yy = i // 2, i % 2
        value = contract(act[:, span(yy * 2 + half, 512)], aw[...], 0, 0).astype(BF)
        for d in range(8):
            g_down[half, d % 2, yy, d // 2] = value[:, d * 128:(d + 1) * 128]
        return carry

    lax.fori_loop(0, 2, grad_down, 0)
    core_send(U_DA)
    lax.fori_loop(2, 4, grad_down, 0)
    core_send(U_DB)
    start(U_DA)
    start(U_DB)

    def grad_up(index, carry):
        i, n = index // 2, index % 2
        value = contract(hw[:, span(i, 512)], slope[:, span(n, 1024)], 0, 0).astype(BF)
        for d in range(4):
            for part in range(2):
                r = d * 128 + part * 64
                g_up[part, d % 2, n, i * 2 + d // 2] = value[r:r + 64, :]
        return carry

    lax.fori_loop(0, 4, grad_up, 0)
    core_send(U_UA)
    core_send(U_UB)
    for u in (U_UA, U_UB):
        start(u)

    def back_norm(r, g):
        grad = da[r, :] + own[r, :] + recv[r, :].astype(F32)
        normal = n1[r, :]
        bump(R_G1, grad * normal)
        bump(R_C1, grad)
        grad = norm_back(normal, inv1[r, 0:1], grad * row_of(R_G1))
        bump(R_BO, grad)
        da[r, :] = grad
        a1w[g, :] = grad.astype(BF)

    for j in range(2):
        x_sum(X_DH, j).wait_recv()
        tiles(j, back_norm)
        x_rows(X_DA1, j, a1w).start()

    z_relay(U_DA, 1)
    z_relay(U_DA, 0)

    def ctx_back(s, carry):
        rows = rows_of(s)
        arrived(X_DA1, s, a1w)
        dctx[rows, :] = contract(a1w[rows, :], w_out[...], 1, 1).astype(BF)
        return carry

    lax.fori_loop(0, 2, ctx_back, 0)
    y_to_z(U_DB)
    lax.fori_loop(2, 4, ctx_back, 0)

    def attend_back(pair, carry):
        lanes = span(pair, 128)
        for t in range(2):
            keys = pl.ds(t * 128, WINDOW)
            query = two_blocks(qkv.at[0], t, lanes)
            key, value = qkv[1, keys, lanes], qkv[2, keys, lanes]
            grad = two_blocks(dctx, t, lanes)
            product = grad.astype(F32) * two_blocks(ctx, t, lanes).astype(F32)
            grad_q = jnp.zeros((ROWS, 128), F32)
            grad_k = jnp.zeros((WINDOW, 128), F32)
            grad_v = jnp.zeros((WINDOW, 128), F32)
            for h, half in enumerate(halves):
                grad_h = jnp.where(half, grad, none)
                weight = prob[pair * 4 + t * 2 + h]
                row_dot = jnp.sum(jnp.where(half, product, 0.0), axis=1, keepdims=True)
                score = (weight.astype(F32) * (contract(grad_h, value, 1, 1) - row_dot)).astype(BF)
                grad_q = grad_q + contract(score, jnp.where(half, key, none), 1, 0)
                grad_k = grad_k + contract(score, jnp.where(half, query, none), 0, 0)
                grad_v = grad_v + contract(weight, grad_h, 0, 0)
            grad_q = grad_q * (HD ** -0.5)
            acc[R_BQ, :, lanes] += fold_rows(grad_q)
            acc[R_BV, :, lanes] += fold_rows(grad_v)
            grad_q = grad_q.astype(BF)
            qkv[0, t * 128:t * 128 + 128, lanes] = grad_q[:128]
            qkv[0, t * 128 + 256:t * 128 + 384, lanes] = grad_q[128:]
            if t == 0:
                acc_k[0:WINDOW, :] = grad_k
                acc_v[0:WINDOW, :] = grad_v
                acc_k[WINDOW:SEQ, :] = jnp.zeros((128, 128), F32)
                acc_v[WINDOW:SEQ, :] = jnp.zeros((128, 128), F32)
            else:
                for i, total, more in ((1, acc_k, grad_k), (2, acc_v, grad_v)):
                    qkv[i, 0:128, lanes] = total[0:128, :].astype(BF)
                    qkv[i, 128:SEQ, lanes] = (total[128:SEQ, :] + more).astype(BF)
        return carry

    def grad_out():
        value = contract(ctx[...], a1w[...], 0, 0).astype(BF)
        for d in range(8):
            for yy in range(2):
                g_out[d % 2, yy, d // 2] = value[yy * 256:(yy + 1) * 256, d * 128:(d + 1) * 128]

    grad_out()
    core_send(U_OUT)
    lax.fori_loop(0, 2, attend_back, 0)
    z_relay(U_DB, 0)
    y_to_z(U_UA)
    lax.fori_loop(2, 4, attend_back, 0)

    for row in range(2, 8):
        line = jnp.sum(acc[row], axis=0, keepdims=True)
        for d in range(8):
            vg[d % 2, d // 2, row:row + 1, :] = line[:, d * 128:(d + 1) * 128]
    for n in range(2):
        line = jnp.sum(acc[R_BU + n], axis=0, keepdims=True)
        for d in range(8):
            vg[d % 2, d // 2, pl.ds(8 + n * 2 + x, 1), :] = line[:, d * 128:(d + 1) * 128]
    for row, source in ((0, R_BQ), (1, R_BV)):
        line = jnp.sum(acc[source], axis=0, keepdims=True)
        for yy in range(2):
            for half in range(2):
                vg[half, 2 * yy + x, row:row + 1, :] = (
                    line[:, yy * 256 + half * 128:yy * 256 + (half + 1) * 128]
                )
    vec_x = remote(vg, vgx, vs.at[0], vr.at[0], at_x)
    vec_c = remote(vg.at[1 - c], vgc, vs.at[1], vr.at[1], at_c)
    vec_y = remote(vg.at[c], vgy, vs.at[2], vr.at[2], at_y)

    def vec_z(k):
        to = lax.rem(z + k, ZS)
        return remote(vg.at[c, to], vgz.at[k - 1], vs.at[2 + k], vr.at[2 + k], z_device(to))

    vec_x.start()

    def input_back(i, carry):
        s = lax.rem(i + 2, 4)
        rows = rows_of(s)
        value = contract(qkv[0, rows, :], w_qkv[0], 1, 1)
        value = value + contract(qkv[1, rows, :], w_qkv[1], 1, 1)
        value = value + contract(qkv[2, rows, :], w_qkv[2], 1, 1)
        hand_over(X_DX, X_DH, s, value)
        return carry

    lax.fori_loop(0, 2, input_back, 0)
    start(U_OUT)
    z_to_y(U_DA)
    vec_x.wait()
    vg[...] = vg[...] + vgx[...]
    vec_c.start()

    def grad_qkv(index, carry):
        kind, i = index // 2, index % 2
        value = contract(xw[:, span(i, 512)], qkv[kind], 0, 0).astype(BF)
        for d in range(4):
            for yy in range(2):
                g_qkv[kind, d % 2, yy, i * 2 + d // 2] = (
                    value[d * 128:(d + 1) * 128, yy * 256:(yy + 1) * 256]
                )
        return carry

    for kind, u in ((0, U_Q), (1, U_K), (2, U_V)):
        lax.fori_loop(kind * 2, kind * 2 + 2, grad_qkv, 0)
        core_send(u)
    vec_c.wait()
    vg[c] = vg[c] + vgc[...]
    vec_y.start()
    for u in (U_Q, U_K, U_V):
        start(u)
    z_relay(U_UA, 0)
    y_to_z(U_UB)
    lax.fori_loop(2, 4, input_back, 0)
    z_relay(U_OUT, 1)
    z_relay(U_OUT, 0)
    vec_y.wait()
    vg[c] = vg[c] + vgy[...]
    for k in range(1, ZS):
        vec_z(k).start()

    def last_sum(j, other):
        x_sum(X_DX, j).wait_recv()

        def body(r, g):
            value = da[r, :] + own[r, :] + recv[r, :].astype(F32)
            if other:
                gts[pl.ds(pl.multiple_of(r.start - j * CHUNK, TILE), TILE), :] = value.astype(BF)
            else:
                da[r, :] = value
        tiles(j, body)

    last_sum(1 - y, True)
    go_on(remote(gts, gtr, done.at[0], yr.at[Y_GTOK], at_y))
    last_sum(y, False)
    gtok_here = pltpu.make_async_copy(da.at[span(y, CHUNK)], gtok.at[y], os.at[9])
    gtok_here.start()
    z_relay(U_UB, 0)
    y_to_z(U_Q)
    z_to_y(U_OUT)
    y_to_z(U_K)
    y_to_z(U_V)
    for u in (U_Q, U_K, U_V):
        z_relay(u, 0)
    for k in range(1, ZS):
        vec_z(k).wait()
    gvb[...] = vg[c, z] + vgz[0] + vgz[1] + vgz[2]
    vec_here = pltpu.make_async_copy(gvb.at[0:12], gv, os.at[10])
    vec_here.start()
    for u in (U_DA, U_DB, U_UA, U_UB):
        finish(u)
    remote(gts, gtr, done.at[0], yr.at[Y_GTOK], at_y).wait_recv()
    gtf[...] = gtr[...].astype(F32)
    gtok_there = pltpu.make_async_copy(gtf, gtok.at[1 - y], os.at[11])
    gtok_there.start()
    finish(U_OUT)
    finish(U_Q)
    finish(U_K)
    finish(U_V)
    remote(outb.at[span(1 - y, CHUNK)], out.at[1 - y], done.at[0], yr.at[Y_OUT], at_y).wait_recv()
    for kind, buf in ((X_NORM, hw), (X_DA2, aw), (X_DA1, a1w)):
        for j in range(2):
            x_rows(kind, j, buf).wait_send()
    for j in range(2):
        x_sum(X_DX, j).wait_send()
    for copy in sent:
        copy.wait_send()
    for condition, copy in later:
        @pl.when(condition)
        def _(copy=copy):
            copy.wait_send()
    for m in range(W_KINDS):
        remote(half_of(m), half_of(m), done.at[0], wrc.at[m], at_c).wait_send()
    for copy in finals + [out_here, gtok_here, gtok_there, vec_here]:
        copy.wait()


def settle_kernel(*refs):
    count = (len(refs) - 2) // 3
    sources, dests, held = refs[:count], refs[count:2 * count], refs[2 * count:3 * count]
    into, out_of = refs[3 * count:]
    first = [pltpu.make_async_copy(s, h, into.at[i]) for i, (s, h) in enumerate(zip(sources, held))]
    second = [pltpu.make_async_copy(h, d, out_of.at[i]) for i, (h, d) in enumerate(zip(held, dests))]
    for copy in first:
        copy.start()
    for before, after in zip(first, second):
        before.wait()
        after.start()
    for copy in second:
        copy.wait()


def settle(results):
    shapes = [jax.ShapeDtypeStruct(r.shape, r.dtype) for r in results]
    count = len(shapes)
    hbm = pl.BlockSpec(memory_space=pl.ANY)
    return pl.pallas_call(
        settle_kernel,
        out_shape=shapes,
        in_specs=[hbm] * count,
        out_specs=[hbm] * count,
        scratch_shapes=[pltpu.VMEM(r.shape, r.dtype) for r in shapes]
        + [pltpu.SemaphoreType.DMA((count,))] * 2,
    )(*results)


def layer(tokens, segment_ids, w_qkv, w_out, w_up, w_down, vectors, cotangent):
    vmem, dma = pltpu.VMEM, pltpu.SemaphoreType.DMA
    outs = (
        jax.ShapeDtypeStruct(tokens.shape, BF),
        jax.ShapeDtypeStruct(tokens.shape, F32),
        jax.ShapeDtypeStruct(w_qkv.shape, F32),
        jax.ShapeDtypeStruct(w_out.shape, F32),
        jax.ShapeDtypeStruct(w_up.shape, F32),
        jax.ShapeDtypeStruct(w_down.shape, F32),
        jax.ShapeDtypeStruct(vectors.shape, F32),
    )
    scratch = [
        vmem((3, D, COLS), BF), vmem((COLS, D), BF), vmem((D, HID), BF), vmem((HID, D), BF),
        vmem((8, 12, 128), BF), vmem((16, D), F32),
    ]
    half_down, half_up, piece_out, piece_qkv = (512, 128), (64, 1024), (256, 128), (128, 256)
    for shape in ((2, 2, 4), (2, 4)):
        scratch += [
            vmem((2,) + shape + half_down, BF), vmem((2,) + shape + half_up, BF),
            vmem(shape + piece_out, BF), vmem((3,) + shape + piece_qkv, BF),
        ]
    for y_shape, z_shape in (((4,), (1,)), ((1, 3), (2, 3)), ((1,), (2,))):
        scratch += [
            vmem(z_shape + half_down, BF), vmem(y_shape + half_down, BF),
            vmem((2,) + y_shape + half_up, BF), vmem(z_shape + piece_out, BF),
            vmem((3,) + y_shape + piece_qkv, BF),
        ]
    scratch += [vmem((3, 128, 256), F32), vmem((256, 128), F32), vmem((128, 1024), F32), vmem((1024, 128), F32)]
    scratch += [
        vmem((SEQ, D), BF), vmem((3, SEQ, COLS), BF), vmem((SEQ, COLS), BF),
        vmem((16, ROWS, WINDOW), BF), vmem((2, ROWS, WINDOW), F32), vmem((SEQ, D), BF),
        vmem((SEQ, HID), BF), vmem((SEQ, HID), BF), vmem((SEQ, D), BF), vmem((SEQ, D), BF),
        vmem((SEQ, COLS), BF),
        vmem((ROWS, D), F32), vmem((ROWS, D), F32), vmem((ROWS, D), F32), vmem((ROWS, 128), F32),
        vmem((ROWS, D), BF), vmem((ROWS, D), BF), vmem((ROWS, D), BF), vmem((ROWS, D), BF),
        vmem((CHUNK, D), BF), vmem((CHUNK, D), BF), vmem((CHUNK, D), F32),
        vmem((12, 8, D), F32),
        vmem((2, 4, 16, 128), F32), vmem((2, 4, 16, 128), F32), vmem((4, 16, 128), F32),
        vmem((4, 16, 128), F32), vmem((3, 16, 128), F32), vmem((16, 128), F32),
        vmem((SEQ, 128), F32), vmem((SEQ, 128), F32),
        dma((1,)), dma((8, 2, 3)), dma((8, 4)), dma((8,)), dma((2, 4)), dma((4, 2)), dma((4, 2)),
        dma((8, 2)), dma((8, 2)), dma((4,)),
        dma((8,)), dma((8,)), dma((8, 2, 4)),
        dma((6,)), dma((6,)), dma((10,)), dma((12,)),
    ]
    hbm = pl.BlockSpec(memory_space=pl.ANY)
    results = pl.pallas_call(
        layer_kernel,
        out_shape=outs,
        in_specs=[hbm, pl.BlockSpec(memory_space=pltpu.VMEM)] + [hbm] * 6,
        out_specs=[hbm] * 7,
        scratch_shapes=scratch,
        compiler_params=pltpu.CompilerParams(
            collective_id=0, has_side_effects=True, vmem_limit_bytes=67043328
        ),
    )(tokens, segment_ids, w_qkv, w_out, w_up, w_down, vectors, cotangent)
    return settle(results)


def solution(mesh):
    step = layer if (mesh.shape["dp"], mesh.shape["tensor"]) == (8, 4) else body
    return jax.shard_map(
        step,
        mesh=mesh,
        in_specs=(
            P("dp", "tensor", None),
            P("dp", None),
            P(None, "dp", "tensor"),
            P("tensor", "dp"),
            P("dp", "tensor"),
            P("tensor", "dp"),
            P(None, "dp"),
            P("dp", "tensor", None),
        ),
        out_specs=(
            P("dp", "tensor", None),
            P("dp", "tensor", None),
            P(None, "dp", "tensor"),
            P("tensor", "dp"),
            P("dp", "tensor"),
            P("tensor", "dp"),
            P(None, "dp"),
        ),
        check_vma=False,
    )
```

```python
import jax
import jax.numpy as jnp
from jax import lax
from jax.experimental import pallas as pl
from jax.experimental.pallas import tpu as pltpu
from jax.sharding import PartitionSpec as P

D = 1024
FF = 4096
HD = 64


NORM_EPS = 1e-06
SQRT_HALF = 0.7071067811865476
INV_ROOT_TAU = 0.3989422804014327
MASKED = -1e30


def gelu_value(pre_act):
    return 0.5 * pre_act * (1.0 + lax.erf(pre_act * SQRT_HALF))


def gelu_slope(pre_act):
    return 0.5 * (1.0 + lax.erf(pre_act * SQRT_HALF)) + pre_act * INV_ROOT_TAU * jnp.exp(
        -0.5 * pre_act * pre_act
    )


def norm_forward(summed, gain, shift):
    centred = summed - jnp.mean(summed, axis=-1, keepdims=True)
    inverse = lax.rsqrt(jnp.mean(centred * centred, axis=-1, keepdims=True) + NORM_EPS)
    normed = centred * inverse
    return (normed * gain + shift, normed, inverse)


def norm_backward(normed, inverse, grad_normed):
    first_mean = jnp.mean(grad_normed, axis=-1, keepdims=True)
    second_mean = jnp.mean(grad_normed * normed, axis=-1, keepdims=True)
    return inverse * (grad_normed - first_mean - normed * second_mean)


def attention_scores(query_heads, key_heads, segments):
    same_doc = segments[:, None] == segments[None, :]
    scores = jnp.einsum(
        "qhe,khe->hqk", query_heads, key_heads, preferred_element_type=jnp.float32
    ) * HD ** (-0.5)
    return jnp.where(same_doc[None], scores, MASKED)


def collect(w_qkv, w_out, w_up, w_down, vectors):
    return (
        lax.all_gather(w_qkv, "dp", axis=1, tiled=True),
        lax.all_gather(w_out, "dp", axis=1, tiled=True),
        lax.all_gather(w_up, "dp", axis=0, tiled=True),
        lax.all_gather(w_down, "dp", axis=1, tiled=True),
        lax.all_gather(vectors, "dp", axis=1, tiled=True),
    )


def share(gradients):
    return (
        lax.psum_scatter(
            gradients[0].astype(jnp.bfloat16), "dp", scatter_dimension=1, tiled=True
        ).astype(jnp.float32),
        lax.psum_scatter(
            gradients[1].astype(jnp.bfloat16), "dp", scatter_dimension=1, tiled=True
        ).astype(jnp.float32),
        lax.psum_scatter(
            gradients[2].astype(jnp.bfloat16), "dp", scatter_dimension=0, tiled=True
        ).astype(jnp.float32),
        lax.psum_scatter(
            gradients[3].astype(jnp.bfloat16), "dp", scatter_dimension=1, tiled=True
        ).astype(jnp.float32),
        lax.psum_scatter(
            gradients[4].astype(jnp.bfloat16), "dp", scatter_dimension=1, tiled=True
        ).astype(jnp.float32),
    )


def body(tokens, segment_ids, w_qkv, w_out, w_up, w_down, vectors, cotangent):
    tensor_rank = lax.axis_index("tensor")
    local_cols = w_qkv.shape[2]
    head_count = local_cols // HD
    hidden = w_up.shape[1]
    col_start = tensor_rank * local_cols
    ffn_start = tensor_rank * hidden

    def forward(weights, tok_block, segments):
        qkv_w, out_w, up_w, down_w, vec_b = weights
        vec_f32 = vec_b.astype(jnp.float32)
        whole = lax.all_gather(tok_block, "tensor", axis=0, tiled=True)
        seq_len = whole.shape[0]
        projected = jnp.einsum("sd,tdc->tsc", whole, qkv_w, preferred_element_type=jnp.float32)
        bias_q = lax.dynamic_slice_in_dim(vec_f32[0], col_start, local_cols)
        bias_v = lax.dynamic_slice_in_dim(vec_f32[1], col_start, local_cols)
        query_heads = (projected[0] + bias_q).astype(jnp.bfloat16).reshape(seq_len, head_count, HD)
        key_heads = projected[1].astype(jnp.bfloat16).reshape(seq_len, head_count, HD)
        value_heads = (projected[2] + bias_v).astype(jnp.bfloat16).reshape(seq_len, head_count, HD)
        scores = attention_scores(query_heads, key_heads, segments)
        row_top = jnp.max(scores, axis=-1, keepdims=True)
        log_total = row_top + jnp.log(jnp.sum(jnp.exp(scores - row_top), axis=-1, keepdims=True))
        attn_probs = jnp.exp(scores - log_total).astype(jnp.bfloat16)
        context = jnp.einsum(
            "hqk,khe->qhe", attn_probs, value_heads, preferred_element_type=jnp.float32
        )
        context = context.reshape(seq_len, local_cols).astype(jnp.bfloat16)
        piece = context
        attn_mixed = lax.psum_scatter(
            jnp.dot(piece, out_w, preferred_element_type=jnp.float32).astype(jnp.bfloat16),
            "tensor",
            scatter_dimension=0,
            tiled=True,
        ).astype(jnp.float32)
        summed_one = tok_block.astype(jnp.float32) + attn_mixed + vec_f32[2]
        normed_out, normed_one, inverse_one = norm_forward(summed_one, vec_f32[3], vec_f32[4])
        normed_b = normed_out.astype(jnp.bfloat16)
        normed_whole = lax.all_gather(normed_b, "tensor", axis=0, tiled=True)
        bias_up = lax.dynamic_slice_in_dim(vec_f32[8:12].reshape(FF), ffn_start, hidden)
        pre_act = jnp.dot(normed_whole, up_w, preferred_element_type=jnp.float32) + bias_up
        activated = gelu_value(pre_act).astype(jnp.bfloat16)
        piece = activated
        summed_two = (
            normed_out
            + lax.psum_scatter(
                jnp.dot(piece, down_w, preferred_element_type=jnp.float32).astype(jnp.bfloat16),
                "tensor",
                scatter_dimension=0,
                tiled=True,
            ).astype(jnp.float32)
            + vec_f32[5]
        )
        final, normed_two, inverse_two = norm_forward(summed_two, vec_f32[6], vec_f32[7])
        saved = (
            whole,
            query_heads,
            key_heads,
            value_heads,
            log_total,
            context,
            normed_one,
            inverse_one,
            normed_whole,
            pre_act,
            activated,
            normed_two,
            inverse_two,
        )
        return (final.astype(jnp.bfloat16), saved)

    def backward(weights, saved, segments, grad_block):
        qkv_w, out_w, up_w, down_w, vec_b = weights
        vec_f32 = vec_b.astype(jnp.float32)
        (
            whole,
            query_heads,
            key_heads,
            value_heads,
            log_total,
            context,
            normed_one,
            inverse_one,
            normed_whole,
            pre_act,
            activated,
            normed_two,
            inverse_two,
        ) = saved
        seq_len = whole.shape[0]
        grad_final = grad_block.astype(jnp.float32)
        g_gain2 = jnp.sum(grad_final * normed_two, axis=0)
        g_shift2 = jnp.sum(grad_final, axis=0)
        grad_two = norm_backward(normed_two, inverse_two, grad_final * vec_f32[6])
        grad_two_b = grad_two.astype(jnp.bfloat16)
        g_bdown = jnp.sum(grad_two, axis=0)
        grad_two_whole = lax.all_gather(grad_two_b, "tensor", axis=0, tiled=True)
        g_down = jnp.dot(activated.T, grad_two_whole, preferred_element_type=jnp.float32)
        grad_pre = jnp.dot(
            grad_two_whole, down_w.T, preferred_element_type=jnp.float32
        ) * gelu_slope(pre_act)
        grad_pre_b = grad_pre.astype(jnp.bfloat16)
        g_bup = jnp.sum(grad_pre, axis=0)
        g_up = jnp.dot(normed_whole.T, grad_pre_b, preferred_element_type=jnp.float32)
        piece = grad_pre_b
        grad_one_in = grad_two + lax.psum_scatter(
            jnp.dot(piece, up_w.T, preferred_element_type=jnp.float32).astype(jnp.bfloat16),
            "tensor",
            scatter_dimension=0,
            tiled=True,
        ).astype(jnp.float32)
        g_gain1 = jnp.sum(grad_one_in * normed_one, axis=0)
        g_shift1 = jnp.sum(grad_one_in, axis=0)
        grad_one = norm_backward(normed_one, inverse_one, grad_one_in * vec_f32[3])
        grad_one_b = grad_one.astype(jnp.bfloat16)
        g_bout = jnp.sum(grad_one, axis=0)
        grad_one_whole = lax.all_gather(grad_one_b, "tensor", axis=0, tiled=True)
        g_out = jnp.dot(context.T, grad_one_whole, preferred_element_type=jnp.float32)
        grad_context = jnp.dot(grad_one_whole, out_w.T, preferred_element_type=jnp.float32).astype(
            jnp.bfloat16
        )
        grad_context = grad_context.reshape(seq_len, head_count, HD)
        scores = attention_scores(query_heads, key_heads, segments)
        attn_exact = jnp.exp(scores - log_total)
        attn_probs = attn_exact.astype(jnp.bfloat16)
        grad_probs = jnp.einsum(
            "qhe,khe->hqk", grad_context, value_heads, preferred_element_type=jnp.float32
        )
        row_dot = jnp.sum(attn_exact * grad_probs, axis=-1, keepdims=True)
        grad_scores = (attn_exact * (grad_probs - row_dot) * HD ** (-0.5)).astype(jnp.bfloat16)
        grad_value = jnp.einsum(
            "hqk,qhe->khe", attn_probs, grad_context, preferred_element_type=jnp.float32
        )
        grad_value = grad_value.reshape(seq_len, local_cols)
        grad_query = jnp.einsum(
            "hqk,khe->qhe", grad_scores, key_heads, preferred_element_type=jnp.float32
        )
        grad_query = grad_query.reshape(seq_len, local_cols)
        grad_key = jnp.einsum(
            "hqk,qhe->khe", grad_scores, query_heads, preferred_element_type=jnp.float32
        )
        grad_key = grad_key.reshape(seq_len, local_cols)
        grad_qkv = jnp.stack([grad_query, grad_key, grad_value]).astype(jnp.bfloat16)
        g_qkv = jnp.einsum("sd,tsc->tdc", whole, grad_qkv, preferred_element_type=jnp.float32)
        piece = grad_qkv
        grad_input = grad_one + lax.psum_scatter(
            jnp.einsum("tsc,tdc->sd", piece, qkv_w, preferred_element_type=jnp.float32).astype(
                jnp.bfloat16
            ),
            "tensor",
            scatter_dimension=0,
            tiled=True,
        ).astype(jnp.float32)
        zero_row = jnp.zeros((D,), jnp.float32)
        row_q = lax.dynamic_update_slice_in_dim(zero_row, jnp.sum(grad_query, axis=0), col_start, 0)
        row_v = lax.dynamic_update_slice_in_dim(zero_row, jnp.sum(grad_value, axis=0), col_start, 0)
        up_rows = lax.dynamic_update_slice_in_dim(
            jnp.zeros((FF,), jnp.float32), g_bup, ffn_start, 0
        ).reshape(4, D)
        first_rows = jnp.stack(
            [row_q, row_v, g_bout, g_gain1, g_shift1, g_bdown, g_gain2, g_shift2]
        )
        g_vec = jnp.concatenate([first_rows, up_rows], axis=0)
        return ((g_qkv, g_out, g_up, g_down, g_vec), grad_input)

    def one_batch(carried, batch_item):
        tok_block, segments, grad_block = batch_item
        forward_w = collect(w_qkv, w_out, w_up, w_down, vectors)
        final_b, saved = forward(forward_w, tok_block, segments)
        second = collect(w_qkv, w_out, w_up, w_down, vectors)
        gradients, grad_input = backward(second, saved, segments, grad_block)
        updated = jax.tree.map(jnp.add, carried, gradients)
        return (updated, (final_b, grad_input))

    initial = (
        jnp.zeros((3, D, local_cols), jnp.float32),
        jnp.zeros((local_cols, D), jnp.float32),
        jnp.zeros((D, hidden), jnp.float32),
        jnp.zeros((hidden, D), jnp.float32),
        jnp.zeros((12, D), jnp.float32),
    )
    carried, stacked = lax.scan(one_batch, initial, (tokens, segment_ids, cotangent))
    totals = share(carried)
    vector_grads = lax.psum(totals[4], "tensor")
    return (stacked[0], stacked[1], totals[0], totals[1], totals[2], totals[3], vector_grads)


Y_TOK, Y_COT, Y_OUT, Y_GTOK = range(4)
X_TOK, X_MIX, X_NORM, X_FFN, X_DA2, X_DH, X_DA1, X_DX = range(8)
W_Q, W_K, W_V, W_OUT, W_UP, W_DOWN, W_REST, W_VEC = range(8)
W_KINDS = 8
Y_FIRST = (W_REST,)
DIRECT = (W_VEC,)
FAR_FIRST = ()
U_DA, U_DB, U_UA, U_UB, U_OUT, U_V, U_K, U_Q = range(8)
Z_FIRST = (U_DA,)
R_BQ, R_BV, R_BO, R_G1, R_C1, R_BD, R_G2, R_C2, R_BU = range(9)
ZS = 4
SEQ = 512
ROWS = 256
CHUNK = 128
TILE = 32
COLS = 512
HID = 2048
WINDOW = 384
BF = jnp.bfloat16
F32 = jnp.float32
MESH = pl.DeviceIdType.MESH


def span(index, size):
    return pl.ds(pl.multiple_of(index * size, size), size)


def contract(a, b, a_dim, b_dim):
    return lax.dot_general(a, b, (((a_dim,), (b_dim,)), ((), ())), preferred_element_type=F32)


def fold_rows(value):
    return jnp.sum(value.reshape(value.shape[0] // 8, 8, value.shape[1]), axis=0)


def layer_kernel(
    tok, seg, wq, wo, wu, wd, vec, cot,
    out, gtok, gq, go, gu, gd, gv,
    w_qkv, w_out, w_up, w_down, w_vec, vf,
    g_down, g_up, g_out, g_qkv,
    c_down, c_up, c_out, c_qkv,
    y_da, y_db, y_up, y_out, y_qkv,
    z_da, z_db, z_up, z_out, z_qkv,
    h_da, h_db, h_up, h_out, h_qkv,
    o_qkv, o_out, o_up, o_down,
    xw, qkv, ctx, prob, bias, hw, act, slope, aw, a1w, dctx,
    own, n1, da, inv1, recv, stage, cotb, outb, gts, gtr, gtf,
    acc, vg, vgx, vgc, vgy, vgz, gvb, acc_k, acc_v,
    done, wrz, wry, wrc, wrd, fs, fr, xs, xr, yr,
    grc, gry, grz, vs, vr, ls, os,
):
    dp = lax.axis_index("dp")
    tensor = lax.axis_index("tensor")
    z, c = dp // 2, dp % 2
    y, x = tensor // 2, tensor % 2
    at_x = {"dp": dp, "tensor": y * 2 + (1 - x)}
    at_y = {"dp": dp, "tensor": (1 - y) * 2 + x}
    at_c = {"dp": z * 2 + (1 - c), "tensor": tensor}

    def remote(src, dst, send, recv_sem, where):
        return pltpu.make_async_remote_copy(
            src_ref=src, dst_ref=dst, send_sem=send, recv_sem=recv_sem,
            device_id=where, device_id_type=MESH,
        )

    barrier = pltpu.get_barrier_semaphore()
    for where in [at_x, at_y, at_c] + [{"dp": lax.rem(z + k, ZS) * 2 + c, "tensor": tensor} for k in range(1, ZS)]:
        pl.semaphore_signal(barrier, inc=1, device_id=where, device_id_type=MESH)
    pl.semaphore_wait(barrier, 6)

    sent = []

    def go_on(copy):
        copy.start()
        sent.append(copy)

    args = [wq.at[0], wq.at[1], wq.at[2], wo, wu, wd.at[0:512], wd.at[512:1024], vec]
    edge = jnp.logical_or(z == 0, z == ZS - 1)
    middle = jnp.logical_not(edge)
    later = []

    def z_device(where):
        return {"dp": where * 2 + c, "tensor": tensor}

    def go_if(condition, copy):
        @pl.when(condition)
        def _():
            copy.start()
        later.append((condition, copy))

    def place(m, yy, d):
        if m <= W_V:
            return w_qkv.at[m, span(d, 128), span(yy, 256)]
        if m == W_OUT:
            return w_out.at[span(yy, 256), span(d, 128)]
        if m == W_UP:
            return w_up.at[span(d, 128), span(yy, 1024)]
        if m == W_DOWN or m == W_REST:
            return w_down.at[span(yy * 2 + m - W_DOWN, 512), span(d, 128)]
        return w_vec.at[d]

    even = lax.rem(z, 2) == 0
    near_first = (jnp.where(even, 3, 1), 2, jnp.where(even, 1, 3))

    def from_z(k):
        return lax.rem(z + ZS - k, ZS)

    def column(r):
        return y if r == 0 else 1 - y

    def z_send(m, r):
        source = args[m] if r == 0 else place(m, 1 - y, dp)
        steps = ((1, z != ZS - 1), (3, z != 0), (2, None))
        for k, there in (steps[2:] + steps[:2] if m in FAR_FIRST else steps):
            there = None if m in DIRECT else there
            copy = remote(
                source, place(m, column(r), dp), done.at[0], wrz.at[m, r, k - 1],
                z_device(lax.rem(z + k, ZS)),
            )
            if there is None:
                go_on(copy)
            else:
                go_if(there, copy)

    def z_serve(m, r, step, keep=False):
        z_take(m, r, step, keep)
        z_note(m, r, step)

    def z_serve_split(m, r, step, early, late):
        def first():
            @pl.when(early)
            def _():
                z_take(m, r, step)

        def second():
            @pl.when(late)
            def _():
                z_take(m, r, step)
            z_note(m, r, step)
        return first, second

    def z_parts(m, r, step):
        k = near_first[step]
        here = place(m, column(r), from_z(k) * 2 + c)
        slot = jnp.where(z == 1, 0, 2)
        hand_on = None
        if step == 1 and m not in DIRECT:
            hand_on = remote(
                here, here, done.at[0], wrz.at[m, r, slot], z_device(jnp.where(z == 1, 0, 3)),
            )
        over_y = None
        if r == 0 and m not in Y_FIRST and m != W_VEC:
            over_y = remote(here, here, done.at[0], wry.at[m, from_z(k)], at_y)
        return k, here, hand_on, over_y

    def z_over(m, step):
        z_parts(m, 0, step)[3].start()

    def z_take(m, r, step, keep=False):
        k, here, hand_on, over_y = z_parts(m, r, step)
        remote(here, here, done.at[0], wrz.at[m, r, k - 1], at_x).wait_recv()
        if hand_on is not None:
            @pl.when(middle)
            def _():
                hand_on.start()
        if over_y is not None and not keep:
            over_y.start()
        c_send(m, here, step + 1)

    def z_note(m, r, step):
        _, _, hand_on, over_y = z_parts(m, r, step)
        if hand_on is not None:
            later.append((middle, hand_on))
        if over_y is not None:
            sent.append(over_y)

    def y_send(m):
        go_on(remote(args[m], place(m, y, dp), done.at[0], wry.at[m, z], at_y))

    def source_of(step):
        return z if step == 0 else from_z(near_first[step - 1])

    def y_serve(m, step):
        zz = source_of(step)
        here = place(m, 1 - y, zz * 2 + c)
        remote(here, here, done.at[0], wry.at[m, zz], at_y).wait_recv()
        c_send(m, here, step)

    def c_send(m, source, step, dest=None):
        dest = source if dest is None else dest
        into = wrd.at[m - W_DOWN, step] if m in (W_DOWN, W_REST) else wrc.at[m]
        remote(source, dest, done.at[0], into, at_c).start()

    def own_send(m):
        c_send(m, args[m], 0, place(m, y, dp))
        pltpu.make_async_copy(args[m], place(m, y, dp), ls.at[m]).start()

    def half_of(m):
        if m <= W_V:
            return w_qkv.at[m, :, 0:256]
        return (
            w_out.at[0:256], w_up.at[:, 0:1024], w_down.at[0:512], w_down.at[0:512], w_vec.at[0:4]
        )[m - W_OUT]

    def wait_down(step):
        for m in (W_DOWN, W_REST):
            if step == 0:
                pltpu.make_async_copy(args[m], place(m, y, dp), ls.at[m]).wait()
            two = w_down.at[0:1024, 0:128]
            remote(two, two, done.at[0], wrd.at[m - W_DOWN, step], at_c).wait_recv()

    def wait_weight(m):
        pltpu.make_async_copy(args[m], place(m, y, dp), ls.at[m]).wait()
        remote(half_of(m), half_of(m), done.at[0], wrc.at[m], at_c).wait_recv()

    def x_copy(kind, j, src, dst):
        return remote(src, dst, xs.at[kind, j], xr.at[kind, j], at_x)

    def tok_rows(xx, yy):
        return pl.ds(pl.multiple_of(xx * ROWS + yy * CHUNK, CHUNK), CHUNK)

    for m in (W_Q, W_K, W_V):
        y_send(m)
        z_send(m, 0)
    go_on(remote(tok.at[1 - y], xw.at[tok_rows(x, y)], done.at[0], yr.at[Y_TOK], at_y))
    go_on(x_copy(X_TOK, 0, tok.at[y], xw.at[tok_rows(x, y)]))
    z_send(W_VEC, 0)
    for m in range(W_KINDS):
        own_send(m)
    local_x = pltpu.make_async_copy(tok.at[y], xw.at[tok_rows(x, y)], ls.at[8])
    local_x.start()
    local_cot = pltpu.make_async_copy(cot.at[y], cotb.at[span(y, CHUNK)], ls.at[9])
    local_cot.start()

    seg_row = seg[pl.ds(y, 1), :].astype(F32)
    blocks = [(p % 2) * 2 + p // 2 for p in range(4)]
    across = [jnp.broadcast_to(seg_row[:, n * 128:(n + 1) * 128], (128, 128)) for n in blocks]
    down = [b.T for b in across]
    for t in range(2):
        for i, q in enumerate((t, t + 2)):
            for j in range(3):
                same = down[q] == across[t + j]
                bias[t, i * 128:(i + 1) * 128, j * 128:(j + 1) * 128] = jnp.where(same, 0.0, MASKED)
    acc[...] = jnp.zeros_like(acc)
    vg[...] = jnp.zeros_like(vg)

    for step in range(2):
        for m in (W_Q, W_K, W_V):
            z_serve(m, 0, step)
    z_send(W_OUT, 0)
    y_tok_here = xw.at[tok_rows(x, 1 - y)]
    remote(tok.at[1 - y], y_tok_here, done.at[0], yr.at[Y_TOK], at_y).wait_recv()
    go_on(x_copy(X_TOK, 1, y_tok_here, y_tok_here))
    for m in (W_Q, W_K, W_V):
        z_serve(m, 0, 2)
    y_send(W_OUT)
    z_serve(W_OUT, 0, 0)
    z_serve(W_OUT, 0, 1)
    z_send(W_UP, 0)
    for step in range(3):
        z_serve(W_VEC, 0, step)
    z_serve(W_OUT, 0, 2)
    y_send(W_UP)
    y_send(W_REST)
    for step in range(4):
        for m in (W_Q, W_K, W_V):
            y_serve(m, step)
    wait_weight(W_VEC)
    for d in range(8):
        vf[0:12, d * 128:(d + 1) * 128] = w_vec[d].astype(F32)
    local_x.wait()
    for j, yy in ((0, y), (1, 1 - y)):
        there = xw.at[tok_rows(1 - x, yy)]
        x_copy(X_TOK, j, there, there).wait_recv()
    for m in (W_Q, W_K, W_V):
        wait_weight(m)

    def head_bias(row):
        parts = [vf[row:row + 1, pl.ds(pl.multiple_of(yy * 512 + x * 256, 256), 256)] for yy in range(2)]
        return jnp.concatenate(parts, axis=1)

    for i in range(3):
        value = contract(xw[...], w_qkv[i], 1, 0)
        if i == 0:
            value = (value + head_bias(0)).astype(BF) * BF(HD ** -0.5)
        elif i == 2:
            value = value + head_bias(1)
        qkv[i] = value.astype(BF)

    low_half = lax.broadcasted_iota(jnp.int32, (1, 128), 1) < HD
    halves = (low_half, jnp.logical_not(low_half))
    none = jnp.zeros((), BF)

    def two_blocks(ref, t, lanes):
        return jnp.concatenate([ref[span(t, 128), lanes], ref[span(t + 2, 128), lanes]], axis=0)

    def attend(pair, carry):
        lanes = span(pair, 128)
        for t in range(2):
            keys = pl.ds(t * 128, WINDOW)
            query = two_blocks(qkv.at[0], t, lanes)
            key, value = qkv[1, keys, lanes], qkv[2, keys, lanes]
            total = jnp.zeros((ROWS, 128), F32)
            for h, half in enumerate(halves):
                scores = contract(jnp.where(half, query, none), key, 1, 1) + bias[t]
                top = jnp.max(scores, axis=1, keepdims=True)
                weight = jnp.exp(scores - top)
                share_of = 1.0 / jnp.sum(weight, axis=1, keepdims=True)
                weight = (weight * share_of).astype(BF)
                prob[pair * 4 + t * 2 + h] = weight
                total = total + contract(weight, jnp.where(half, value, none), 1, 0)
            total = total.astype(BF)
            ctx[t * 128:t * 128 + 128, lanes] = total[:128]
            ctx[t * 128 + 256:t * 128 + 384, lanes] = total[128:]
        return carry

    z_serve(W_UP, 0, 0)
    lax.fori_loop(0, 2, attend, 0)
    for step in range(4):
        y_serve(W_OUT, step)
    lax.fori_loop(2, 4, attend, 0)
    up_early, up_late = z_serve_split(W_UP, 0, 1, middle, edge)
    up_early()
    z_send(W_DOWN, 0)

    def rows_of(s):
        mine = jnp.where(s < 2, x, 1 - x)
        return pl.ds(pl.multiple_of(mine * ROWS + lax.rem(s, 2) * CHUNK, CHUNK), CHUNK)

    def x_sum(kind, j):
        return x_copy(kind, j, stage.at[span(j, CHUNK)], recv.at[span(j, CHUNK)])

    def x_rows(kind, j, buf):
        here = buf.at[pl.ds(pl.multiple_of(x * ROWS + j * CHUNK, CHUNK), CHUNK)]
        return x_copy(kind, j, here, here)

    def hand_over(kind, before, s, value):
        @pl.when(s < 2)
        def _():
            own[span(s, CHUNK), :] = value

        @pl.when(s >= 2)
        def _():
            if before is not None:
                x_sum(before, s - 2).wait_send()
            stage[span(s - 2, CHUNK), :] = value.astype(BF)
            x_sum(kind, s - 2).start()

    wait_weight(W_OUT)

    def mix(i, carry):
        s = lax.rem(i + 2, 4)
        hand_over(X_MIX, None, s, contract(ctx[rows_of(s), :], w_out[...], 1, 0))
        return carry

    lax.fori_loop(0, 4, mix, 0)
    up_late()
    z_serve(W_UP, 0, 2)
    y_serve(W_REST, 0)
    z_send(W_REST, 0)
    z_send(W_REST, 1)
    y_serve(W_UP, 0)
    z_serve(W_DOWN, 0, 0, keep=True)
    z_serve(W_DOWN, 0, 1, keep=True)

    def row_of(row):
        return vf[row:row + 1, :]

    def normed(value):
        centred = value - jnp.mean(value, axis=1, keepdims=True)
        inverse = lax.rsqrt(jnp.mean(centred * centred, axis=1, keepdims=True) + NORM_EPS)
        return centred * inverse, inverse

    def norm_back(normal, inverse, grad):
        first = jnp.mean(grad, axis=1, keepdims=True)
        second = jnp.mean(grad * normal, axis=1, keepdims=True)
        return inverse * (grad - first - normal * second)

    def tiles(j, body):
        def step(i, carry):
            body(pl.ds(pl.multiple_of(j * CHUNK + i * TILE, TILE), TILE),
                 pl.ds(pl.multiple_of(x * ROWS + j * CHUNK + i * TILE, TILE), TILE))
            return carry
        lax.fori_loop(0, CHUNK // TILE, step, 0)

    def first_norm(r, g):
        summed = xw[g, :].astype(F32) + own[r, :] + recv[r, :].astype(F32) + row_of(R_BO)
        normal, inverse = normed(summed)
        n1[r, :] = normal
        inv1[r, :] = jnp.broadcast_to(inverse, (TILE, 128))
        hw[g, :] = (normal * row_of(R_G1) + row_of(R_C1)).astype(BF)

    for j in range(2):
        x_sum(X_MIX, j).wait_recv()
        tiles(j, first_norm)
        x_rows(X_NORM, j, hw).start()

    y_send(W_DOWN)
    z_over(W_DOWN, 0)
    z_over(W_DOWN, 1)
    for step in range(1, 4):
        y_serve(W_UP, step)
    wait_weight(W_UP)

    def arrived(kind, s, buf):
        @pl.when(s >= 2)
        def _():
            there = buf.at[rows_of(s)]
            x_copy(kind, s - 2, there, there).wait_recv()

    def up_bias(n):
        return vf[pl.ds(8 + n * 2 + x, 1), :]

    def ffn_up(s, carry):
        rows = rows_of(s)
        arrived(X_NORM, s, hw)
        for n in range(2):
            pre = contract(hw[rows, :], w_up[:, n * 1024:(n + 1) * 1024], 1, 0) + up_bias(n)
            cdf = 0.5 * (1.0 + lax.erf(pre * SQRT_HALF))
            act[rows, n * 1024:(n + 1) * 1024] = (pre * cdf).astype(BF)
            slope[rows, n * 1024:(n + 1) * 1024] = (
                cdf + pre * INV_ROOT_TAU * jnp.exp(-0.5 * pre * pre)
            ).astype(BF)
        return carry

    lax.fori_loop(0, 2, ffn_up, 0)
    z_serve(W_DOWN, 0, 2)
    for r in range(2):
        z_serve(W_REST, r, 0)
        z_serve(W_REST, r, 1)
    y_serve(W_DOWN, 0)
    lax.fori_loop(2, 3, ffn_up, 0)
    y_serve(W_DOWN, 1)
    lax.fori_loop(3, 4, ffn_up, 0)
    y_serve(W_DOWN, 2)
    go_on(remote(cot.at[1 - y], cotb.at[span(y, CHUNK)], done.at[0], yr.at[Y_COT], at_y))

    def ffn_copy(step, j):
        cols = span(source_of(step), 256)
        return remote(
            stage.at[span(j, CHUNK), cols], recv.at[span(j, CHUNK), cols],
            fs.at[step, j], fr.at[step, j], at_x,
        )

    for j in range(2):
        x_sum(X_MIX, j).wait_send()
    for step in range(4):
        if step == 2:
            y_serve(W_DOWN, 3)
        if step == 3:
            z_serve(W_REST, 0, 2)
            z_serve(W_REST, 1, 2)
        wait_down(step)
        cols = span(source_of(step), 256)
        stage[:, cols] = contract(act[span(1 - x, ROWS), :], w_down[:, cols], 1, 0).astype(BF)
        for j in range(2):
            ffn_copy(step, j).start()
    for step in range(2):
        cols = span(step, 512)
        own[:, cols] = contract(act[span(x, ROWS), :], w_down[:, cols], 1, 0)

    def bump(row, value):
        acc[row] += fold_rows(value)

    def second_norm(r, g):
        h1 = n1[r, :] * row_of(R_G1) + row_of(R_C1)
        normal, inverse = normed(h1 + own[r, :] + recv[r, :].astype(F32) + row_of(R_BD))
        outb[r, :] = (normal * row_of(R_G2) + row_of(R_C2)).astype(BF)
        dy = cotb[r, :].astype(F32)
        bump(R_G2, dy * normal)
        bump(R_C2, dy)
        grad = norm_back(normal, inverse, dy * row_of(R_G2))
        bump(R_BD, grad)
        da[r, :] = grad
        aw[g, :] = grad.astype(BF)

    local_cot.wait()
    cot_here = cotb.at[span(1 - y, CHUNK)]
    remote(cot.at[1 - y], cot_here, done.at[0], yr.at[Y_COT], at_y).wait_recv()
    for j in range(2):
        for step in range(4):
            ffn_copy(step, j).wait()
        tiles(j, second_norm)
        x_rows(X_DA2, j, aw).start()
    out_here = pltpu.make_async_copy(outb.at[span(y, CHUNK)], out.at[y], os.at[0])
    out_here.start()
    go_on(remote(outb.at[span(1 - y, CHUNK)], out.at[y], done.at[0], yr.at[Y_OUT], at_y))

    def ffn_back(s, carry):
        rows = rows_of(s)
        arrived(X_DA2, s, aw)
        for n in range(2):
            cols = slice(n * 1024, (n + 1) * 1024)
            grad = contract(aw[rows, :], w_down[cols, :], 1, 1) * slope[rows, cols].astype(F32)
            bump(R_BU + n, grad)
            slope[rows, cols] = grad.astype(BF)
        hand_over(X_DH, None, s, contract(slope[rows, :], w_up[...], 1, 1))
        return carry

    lax.fori_loop(0, 4, ffn_back, 0)

    units = {
        U_DA: (g_down.at[0], c_down.at[0], y_da, z_da, h_da, o_down.at[0:512], gd.at[0:512]),
        U_DB: (g_down.at[1], c_down.at[1], y_db, z_db, h_db, o_down.at[512:1024], gd.at[512:1024]),
        U_OUT: (g_out, c_out, y_out, z_out, h_out, o_out, go),
    }
    for u, i in ((U_UA, 0), (U_UB, 1)):
        rows = slice(i * 64, (i + 1) * 64)
        units[u] = tuple(r.at[i] for r in (g_up, c_up, y_up, z_up, h_up)) + (o_up.at[rows], gu.at[rows])
    for u, i in ((U_Q, 0), (U_K, 1), (U_V, 2)):
        units[u] = tuple(r.at[i] for r in (g_qkv, c_qkv, y_qkv, z_qkv, h_qkv, o_qkv, gq))

    def piece_loop(rows, body):
        size = min(rows, CHUNK)

        def step(i, carry):
            body(span(i, size))
            return carry
        lax.fori_loop(0, rows // size, step, 0)

    def add_piece(g, yy, zz, other):
        def body(r):
            g[c, yy, zz, r, :] = (g[c, yy, zz, r, :].astype(F32) + other[r, :].astype(F32)).astype(BF)
        piece_loop(g.shape[3], body)

    def core_copy(u):
        g, rc = units[u][0], units[u][1]
        return remote(g.at[1 - c], rc, done.at[0], grc.at[u], at_c)

    def core_send(u):
        go_on(core_copy(u))

    def core_add(u, r):
        g, rc = units[u][0], units[u][1]
        for zz in range(ZS):
            add_piece(g, column(r), zz, rc.at[column(r), zz])

    def rs_y_copy(u):
        g, ry = units[u][0], units[u][2]
        source = g.at[c, 1 - y, pl.ds(z, 1)] if u in Z_FIRST else g.at[c, 1 - y]
        return remote(source, ry, done.at[0], gry.at[u], at_y)

    def rs_z_copy(u, r, k):
        g, rz = units[u][0], units[u][3]
        to = lax.rem(z + k, ZS)
        return remote(g.at[c, column(r), to], rz.at[r, k - 1], done.at[0], grz.at[u, r, k - 1], z_device(to))

    def rs_hand_on(u, r):
        g, rh = units[u][0], units[u][4]
        far = jnp.where(z == 0, ZS - 1, 0)
        return remote(g.at[c, column(r), far], rh.at[r], done.at[0], grz.at[u, r, 3], z_device(jnp.where(z == 0, 1, 2)))

    def z_hand_on(u, r):
        go_if(edge, rs_hand_on(u, r))

    def z_begin(u, r):
        go_if(z != ZS - 1, rs_z_copy(u, r, 1))
        go_if(z != 0, rs_z_copy(u, r, 3))
        go_if(edge, rs_z_copy(u, r, 2))

    def z_relay(u, r):
        g, rh = units[u][0], units[u][4]

        @pl.when(middle)
        def _():
            rs_hand_on(u, r).wait_recv()
            add_piece(g, column(r), lax.rem(z + 2, ZS), rh.at[r])
        go_if(middle, rs_z_copy(u, r, 2))

    def start(u):
        core_copy(u).wait_recv()
        core_add(u, 1)
        if u in Z_FIRST:
            z_hand_on(u, 1)
            core_add(u, 0)
            z_hand_on(u, 0)
            z_begin(u, 1)
            z_begin(u, 0)
        else:
            go_on(rs_y_copy(u))
            core_add(u, 0)

    def y_to_z(u):
        g, ry = units[u][0], units[u][2]
        rs_y_copy(u).wait_recv()
        for zz in range(ZS):
            add_piece(g, y, zz, ry.at[zz])
        z_hand_on(u, 0)
        z_begin(u, 0)

    def wait_z(u, r):
        rs_z_copy(u, r, 2).wait_recv()

        @pl.when(z != 0)
        def _():
            rs_z_copy(u, r, 1).wait_recv()

        @pl.when(z != ZS - 1)
        def _():
            rs_z_copy(u, r, 3).wait_recv()

    def z_total(u, r, rows):
        g, rz = units[u][0], units[u][3]
        value = g[c, column(r), z, rows, :].astype(F32)
        for k in range(ZS - 1):
            value = value + rz[r, k, rows, :].astype(F32)
        return value

    def z_to_y(u):
        g = units[u][0]
        wait_z(u, 1)

        def body(rows):
            g[c, 1 - y, z, rows, :] = z_total(u, 1, rows).astype(BF)
        piece_loop(g.shape[3], body)
        go_on(rs_y_copy(u))

    finals = []

    def finish(u):
        g, _, ry, _, _, o, dest = units[u]
        wait_z(u, 0)
        if u in Z_FIRST:
            rs_y_copy(u).wait_recv()

        def body(rows):
            value = z_total(u, 0, rows)
            if u in Z_FIRST:
                value = value + ry[0, rows, :].astype(F32)
            o[rows, :] = value
        piece_loop(g.shape[3], body)
        copy = pltpu.make_async_copy(o, dest, os.at[1 + u])
        copy.start()
        finals.append(copy)

    for u in units:
        for r in range(2 if u in Z_FIRST else 1):
            for k, alone in ((1, z == 0), (3, z == ZS - 1)):
                @pl.when(alone)
                def _(u=u, r=r, k=k):
                    rz = units[u][3]
                    rz[r, k - 1] = jnp.zeros(rz.shape[2:], BF)

    def grad_down(i, carry):
        half, yy = i // 2, i % 2
        value = contract(act[:, span(yy * 2 + half, 512)], aw[...], 0, 0).astype(BF)
        for d in range(8):
            g_down[half, d % 2, yy, d // 2] = value[:, d * 128:(d + 1) * 128]
        return carry

    lax.fori_loop(0, 2, grad_down, 0)
    core_send(U_DA)
    lax.fori_loop(2, 4, grad_down, 0)
    core_send(U_DB)
    start(U_DA)
    start(U_DB)

    def grad_up(index, carry):
        i, n = index // 2, index % 2
        value = contract(hw[:, span(i, 512)], slope[:, span(n, 1024)], 0, 0).astype(BF)
        for d in range(4):
            for part in range(2):
                r = d * 128 + part * 64
                g_up[part, d % 2, n, i * 2 + d // 2] = value[r:r + 64, :]
        return carry

    lax.fori_loop(0, 4, grad_up, 0)
    core_send(U_UA)
    core_send(U_UB)
    for u in (U_UA, U_UB):
        start(u)

    def back_norm(r, g):
        grad = da[r, :] + own[r, :] + recv[r, :].astype(F32)
        normal = n1[r, :]
        bump(R_G1, grad * normal)
        bump(R_C1, grad)
        grad = norm_back(normal, inv1[r, 0:1], grad * row_of(R_G1))
        bump(R_BO, grad)
        da[r, :] = grad
        a1w[g, :] = grad.astype(BF)

    for j in range(2):
        x_sum(X_DH, j).wait_recv()
        tiles(j, back_norm)
        x_rows(X_DA1, j, a1w).start()

    z_relay(U_DA, 1)
    z_relay(U_DA, 0)

    def ctx_back(s, carry):
        rows = rows_of(s)
        arrived(X_DA1, s, a1w)
        dctx[rows, :] = contract(a1w[rows, :], w_out[...], 1, 1).astype(BF)
        return carry

    lax.fori_loop(0, 2, ctx_back, 0)
    y_to_z(U_DB)
    lax.fori_loop(2, 4, ctx_back, 0)

    def attend_back(pair, carry):
        lanes = span(pair, 128)
        for t in range(2):
            keys = pl.ds(t * 128, WINDOW)
            query = two_blocks(qkv.at[0], t, lanes)
            key, value = qkv[1, keys, lanes], qkv[2, keys, lanes]
            grad = two_blocks(dctx, t, lanes)
            product = grad.astype(F32) * two_blocks(ctx, t, lanes).astype(F32)
            grad_q = jnp.zeros((ROWS, 128), F32)
            grad_k = jnp.zeros((WINDOW, 128), F32)
            grad_v = jnp.zeros((WINDOW, 128), F32)
            for h, half in enumerate(halves):
                grad_h = jnp.where(half, grad, none)
                weight = prob[pair * 4 + t * 2 + h]
                row_dot = jnp.sum(jnp.where(half, product, 0.0), axis=1, keepdims=True)
                score = (weight.astype(F32) * (contract(grad_h, value, 1, 1) - row_dot)).astype(BF)
                grad_q = grad_q + contract(score, jnp.where(half, key, none), 1, 0)
                grad_k = grad_k + contract(score, jnp.where(half, query, none), 0, 0)
                grad_v = grad_v + contract(weight, grad_h, 0, 0)
            grad_q = grad_q * (HD ** -0.5)
            acc[R_BQ, :, lanes] += fold_rows(grad_q)
            acc[R_BV, :, lanes] += fold_rows(grad_v)
            grad_q = grad_q.astype(BF)
            qkv[0, t * 128:t * 128 + 128, lanes] = grad_q[:128]
            qkv[0, t * 128 + 256:t * 128 + 384, lanes] = grad_q[128:]
            if t == 0:
                acc_k[0:WINDOW, :] = grad_k
                acc_v[0:WINDOW, :] = grad_v
                acc_k[WINDOW:SEQ, :] = jnp.zeros((128, 128), F32)
                acc_v[WINDOW:SEQ, :] = jnp.zeros((128, 128), F32)
            else:
                for i, total, more in ((1, acc_k, grad_k), (2, acc_v, grad_v)):
                    qkv[i, 0:128, lanes] = total[0:128, :].astype(BF)
                    qkv[i, 128:SEQ, lanes] = (total[128:SEQ, :] + more).astype(BF)
        return carry

    def grad_out():
        value = contract(ctx[...], a1w[...], 0, 0).astype(BF)
        for d in range(8):
            for yy in range(2):
                g_out[d % 2, yy, d // 2] = value[yy * 256:(yy + 1) * 256, d * 128:(d + 1) * 128]

    grad_out()
    core_send(U_OUT)
    lax.fori_loop(0, 2, attend_back, 0)
    start(U_OUT)
    z_relay(U_DB, 0)
    y_to_z(U_UA)
    lax.fori_loop(2, 4, attend_back, 0)

    for row in range(2, 8):
        line = jnp.sum(acc[row], axis=0, keepdims=True)
        for d in range(8):
            vg[d % 2, d // 2, row:row + 1, :] = line[:, d * 128:(d + 1) * 128]
    for n in range(2):
        line = jnp.sum(acc[R_BU + n], axis=0, keepdims=True)
        for d in range(8):
            vg[d % 2, d // 2, pl.ds(8 + n * 2 + x, 1), :] = line[:, d * 128:(d + 1) * 128]
    for row, source in ((0, R_BQ), (1, R_BV)):
        line = jnp.sum(acc[source], axis=0, keepdims=True)
        for yy in range(2):
            for half in range(2):
                vg[half, 2 * yy + x, row:row + 1, :] = (
                    line[:, yy * 256 + half * 128:yy * 256 + (half + 1) * 128]
                )
    vec_x = remote(vg, vgx, vs.at[0], vr.at[0], at_x)
    vec_c = remote(vg.at[1 - c], vgc, vs.at[1], vr.at[1], at_c)
    vec_y = remote(vg.at[c], vgy, vs.at[2], vr.at[2], at_y)

    def vec_z(k):
        to = lax.rem(z + k, ZS)
        return remote(vg.at[c, to], vgz.at[k - 1], vs.at[2 + k], vr.at[2 + k], z_device(to))

    vec_x.start()

    def input_back(i, carry):
        s = lax.rem(i + 2, 4)
        rows = rows_of(s)
        value = contract(qkv[0, rows, :], w_qkv[0], 1, 1)
        value = value + contract(qkv[1, rows, :], w_qkv[1], 1, 1)
        value = value + contract(qkv[2, rows, :], w_qkv[2], 1, 1)
        hand_over(X_DX, X_DH, s, value)
        return carry

    lax.fori_loop(0, 2, input_back, 0)
    vec_x.wait()
    vg[...] = vg[...] + vgx[...]
    vec_c.start()

    def grad_qkv(index, carry):
        kind, i = index // 2, index % 2
        value = contract(xw[:, span(i, 512)], qkv[kind], 0, 0).astype(BF)
        for d in range(4):
            for yy in range(2):
                g_qkv[kind, d % 2, yy, i * 2 + d // 2] = (
                    value[d * 128:(d + 1) * 128, yy * 256:(yy + 1) * 256]
                )
        return carry

    for kind, u in ((0, U_Q), (1, U_K), (2, U_V)):
        lax.fori_loop(kind * 2, kind * 2 + 2, grad_qkv, 0)
        core_send(u)
    vec_c.wait()
    vg[c] = vg[c] + vgc[...]
    vec_y.start()
    for u in (U_Q, U_K, U_V):
        start(u)
    z_relay(U_UA, 0)
    y_to_z(U_UB)
    lax.fori_loop(2, 4, input_back, 0)
    y_to_z(U_OUT)
    z_to_y(U_DA)
    vec_y.wait()
    vg[c] = vg[c] + vgy[...]
    for k in range(1, ZS):
        vec_z(k).start()

    def last_sum(j, other):
        x_sum(X_DX, j).wait_recv()

        def body(r, g):
            value = da[r, :] + own[r, :] + recv[r, :].astype(F32)
            if other:
                gts[pl.ds(pl.multiple_of(r.start - j * CHUNK, TILE), TILE), :] = value.astype(BF)
            else:
                da[r, :] = value
        tiles(j, body)

    last_sum(1 - y, True)
    go_on(remote(gts, gtr, done.at[0], yr.at[Y_GTOK], at_y))
    last_sum(y, False)
    gtok_here = pltpu.make_async_copy(da.at[span(y, CHUNK)], gtok.at[y], os.at[9])
    gtok_here.start()
    z_relay(U_UB, 0)
    y_to_z(U_Q)
    z_relay(U_OUT, 0)
    y_to_z(U_K)
    y_to_z(U_V)
    for u in (U_Q, U_K, U_V):
        z_relay(u, 0)
    for k in range(1, ZS):
        vec_z(k).wait()
    gvb[...] = vg[c, z] + vgz[0] + vgz[1] + vgz[2]
    vec_here = pltpu.make_async_copy(gvb.at[0:12], gv, os.at[10])
    vec_here.start()
    for u in (U_DA, U_DB, U_UA, U_UB):
        finish(u)
    remote(gts, gtr, done.at[0], yr.at[Y_GTOK], at_y).wait_recv()
    gtf[...] = gtr[...].astype(F32)
    gtok_there = pltpu.make_async_copy(gtf, gtok.at[1 - y], os.at[11])
    gtok_there.start()
    finish(U_OUT)
    finish(U_Q)
    finish(U_K)
    finish(U_V)
    remote(outb.at[span(1 - y, CHUNK)], out.at[1 - y], done.at[0], yr.at[Y_OUT], at_y).wait_recv()
    for kind, buf in ((X_NORM, hw), (X_DA2, aw), (X_DA1, a1w)):
        for j in range(2):
            x_rows(kind, j, buf).wait_send()
    for j in range(2):
        x_sum(X_DX, j).wait_send()
    for copy in sent:
        copy.wait_send()
    for condition, copy in later:
        @pl.when(condition)
        def _(copy=copy):
            copy.wait_send()
    for m in range(W_KINDS):
        remote(half_of(m), half_of(m), done.at[0], wrc.at[m], at_c).wait_send()
    for copy in finals + [out_here, gtok_here, gtok_there, vec_here]:
        copy.wait()


def settle_kernel(*refs):
    count = (len(refs) - 2) // 3
    sources, dests, held = refs[:count], refs[count:2 * count], refs[2 * count:3 * count]
    into, out_of = refs[3 * count:]
    first = [pltpu.make_async_copy(s, h, into.at[i]) for i, (s, h) in enumerate(zip(sources, held))]
    second = [pltpu.make_async_copy(h, d, out_of.at[i]) for i, (h, d) in enumerate(zip(held, dests))]
    for copy in first:
        copy.start()
    for before, after in zip(first, second):
        before.wait()
        after.start()
    for copy in second:
        copy.wait()


def settle(results):
    shapes = [jax.ShapeDtypeStruct(r.shape, r.dtype) for r in results]
    count = len(shapes)
    hbm = pl.BlockSpec(memory_space=pl.ANY)
    return pl.pallas_call(
        settle_kernel,
        out_shape=shapes,
        in_specs=[hbm] * count,
        out_specs=[hbm] * count,
        scratch_shapes=[pltpu.VMEM(r.shape, r.dtype) for r in shapes]
        + [pltpu.SemaphoreType.DMA((count,))] * 2,
    )(*results)


def layer(tokens, segment_ids, w_qkv, w_out, w_up, w_down, vectors, cotangent):
    vmem, dma = pltpu.VMEM, pltpu.SemaphoreType.DMA
    outs = (
        jax.ShapeDtypeStruct(tokens.shape, BF),
        jax.ShapeDtypeStruct(tokens.shape, F32),
        jax.ShapeDtypeStruct(w_qkv.shape, F32),
        jax.ShapeDtypeStruct(w_out.shape, F32),
        jax.ShapeDtypeStruct(w_up.shape, F32),
        jax.ShapeDtypeStruct(w_down.shape, F32),
        jax.ShapeDtypeStruct(vectors.shape, F32),
    )
    scratch = [
        vmem((3, D, COLS), BF), vmem((COLS, D), BF), vmem((D, HID), BF), vmem((HID, D), BF),
        vmem((8, 12, 128), BF), vmem((16, D), F32),
    ]
    half_down, half_up, piece_out, piece_qkv = (512, 128), (64, 1024), (256, 128), (128, 256)
    for shape in ((2, 2, 4), (2, 4)):
        scratch += [
            vmem((2,) + shape + half_down, BF), vmem((2,) + shape + half_up, BF),
            vmem(shape + piece_out, BF), vmem((3,) + shape + piece_qkv, BF),
        ]
    for y_shape, z_shape in (((4,), (1,)), ((1, 3), (2, 3)), ((1,), (2,))):
        scratch += [
            vmem(z_shape + half_down, BF), vmem(y_shape + half_down, BF),
            vmem((2,) + y_shape + half_up, BF), vmem(y_shape + piece_out, BF),
            vmem((3,) + y_shape + piece_qkv, BF),
        ]
    scratch += [vmem((3, 128, 256), F32), vmem((256, 128), F32), vmem((128, 1024), F32), vmem((1024, 128), F32)]
    scratch += [
        vmem((SEQ, D), BF), vmem((3, SEQ, COLS), BF), vmem((SEQ, COLS), BF),
        vmem((16, ROWS, WINDOW), BF), vmem((2, ROWS, WINDOW), F32), vmem((SEQ, D), BF),
        vmem((SEQ, HID), BF), vmem((SEQ, HID), BF), vmem((SEQ, D), BF), vmem((SEQ, D), BF),
        vmem((SEQ, COLS), BF),
        vmem((ROWS, D), F32), vmem((ROWS, D), F32), vmem((ROWS, D), F32), vmem((ROWS, 128), F32),
        vmem((ROWS, D), BF), vmem((ROWS, D), BF), vmem((ROWS, D), BF), vmem((ROWS, D), BF),
        vmem((CHUNK, D), BF), vmem((CHUNK, D), BF), vmem((CHUNK, D), F32),
        vmem((12, 8, D), F32),
        vmem((2, 4, 16, 128), F32), vmem((2, 4, 16, 128), F32), vmem((4, 16, 128), F32),
        vmem((4, 16, 128), F32), vmem((3, 16, 128), F32), vmem((16, 128), F32),
        vmem((SEQ, 128), F32), vmem((SEQ, 128), F32),
        dma((1,)), dma((8, 2, 3)), dma((8, 4)), dma((8,)), dma((2, 4)), dma((4, 2)), dma((4, 2)),
        dma((8, 2)), dma((8, 2)), dma((4,)),
        dma((8,)), dma((8,)), dma((8, 2, 4)),
        dma((6,)), dma((6,)), dma((10,)), dma((12,)),
    ]
    hbm = pl.BlockSpec(memory_space=pl.ANY)
    results = pl.pallas_call(
        layer_kernel,
        out_shape=outs,
        in_specs=[hbm, pl.BlockSpec(memory_space=pltpu.VMEM)] + [hbm] * 6,
        out_specs=[hbm] * 7,
        scratch_shapes=scratch,
        compiler_params=pltpu.CompilerParams(
            collective_id=0, has_side_effects=True, vmem_limit_bytes=67043328
        ),
    )(tokens, segment_ids, w_qkv, w_out, w_up, w_down, vectors, cotangent)
    return settle(results)


def solution(mesh):
    step = layer if (mesh.shape["dp"], mesh.shape["tensor"]) == (8, 4) else body
    return jax.shard_map(
        step,
        mesh=mesh,
        in_specs=(
            P("dp", "tensor", None),
            P("dp", None),
            P(None, "dp", "tensor"),
            P("tensor", "dp"),
            P("dp", "tensor"),
            P("tensor", "dp"),
            P(None, "dp"),
            P("dp", "tensor", None),
        ),
        out_specs=(
            P("dp", "tensor", None),
            P("dp", "tensor", None),
            P(None, "dp", "tensor"),
            P("tensor", "dp"),
            P("dp", "tensor"),
            P("tensor", "dp"),
            P(None, "dp"),
        ),
        check_vma=False,
    )
```

```python
import jax
import jax.numpy as jnp
from jax import lax
from jax.experimental import pallas as pl
from jax.experimental.pallas import tpu as pltpu
from jax.sharding import PartitionSpec as P

D = 1024
FF = 4096
HD = 64


NORM_EPS = 1e-06
SQRT_HALF = 0.7071067811865476
INV_ROOT_TAU = 0.3989422804014327
MASKED = -1e30


def gelu_value(pre_act):
    return 0.5 * pre_act * (1.0 + lax.erf(pre_act * SQRT_HALF))


def gelu_slope(pre_act):
    return 0.5 * (1.0 + lax.erf(pre_act * SQRT_HALF)) + pre_act * INV_ROOT_TAU * jnp.exp(
        -0.5 * pre_act * pre_act
    )


def norm_forward(summed, gain, shift):
    centred = summed - jnp.mean(summed, axis=-1, keepdims=True)
    inverse = lax.rsqrt(jnp.mean(centred * centred, axis=-1, keepdims=True) + NORM_EPS)
    normed = centred * inverse
    return (normed * gain + shift, normed, inverse)


def norm_backward(normed, inverse, grad_normed):
    first_mean = jnp.mean(grad_normed, axis=-1, keepdims=True)
    second_mean = jnp.mean(grad_normed * normed, axis=-1, keepdims=True)
    return inverse * (grad_normed - first_mean - normed * second_mean)


def attention_scores(query_heads, key_heads, segments):
    same_doc = segments[:, None] == segments[None, :]
    scores = jnp.einsum(
        "qhe,khe->hqk", query_heads, key_heads, preferred_element_type=jnp.float32
    ) * HD ** (-0.5)
    return jnp.where(same_doc[None], scores, MASKED)


def collect(w_qkv, w_out, w_up, w_down, vectors):
    return (
        lax.all_gather(w_qkv, "dp", axis=1, tiled=True),
        lax.all_gather(w_out, "dp", axis=1, tiled=True),
        lax.all_gather(w_up, "dp", axis=0, tiled=True),
        lax.all_gather(w_down, "dp", axis=1, tiled=True),
        lax.all_gather(vectors, "dp", axis=1, tiled=True),
    )


def share(gradients):
    return (
        lax.psum_scatter(
            gradients[0].astype(jnp.bfloat16), "dp", scatter_dimension=1, tiled=True
        ).astype(jnp.float32),
        lax.psum_scatter(
            gradients[1].astype(jnp.bfloat16), "dp", scatter_dimension=1, tiled=True
        ).astype(jnp.float32),
        lax.psum_scatter(
            gradients[2].astype(jnp.bfloat16), "dp", scatter_dimension=0, tiled=True
        ).astype(jnp.float32),
        lax.psum_scatter(
            gradients[3].astype(jnp.bfloat16), "dp", scatter_dimension=1, tiled=True
        ).astype(jnp.float32),
        lax.psum_scatter(
            gradients[4].astype(jnp.bfloat16), "dp", scatter_dimension=1, tiled=True
        ).astype(jnp.float32),
    )


def body(tokens, segment_ids, w_qkv, w_out, w_up, w_down, vectors, cotangent):
    tensor_rank = lax.axis_index("tensor")
    local_cols = w_qkv.shape[2]
    head_count = local_cols // HD
    hidden = w_up.shape[1]
    col_start = tensor_rank * local_cols
    ffn_start = tensor_rank * hidden

    def forward(weights, tok_block, segments):
        qkv_w, out_w, up_w, down_w, vec_b = weights
        vec_f32 = vec_b.astype(jnp.float32)
        whole = lax.all_gather(tok_block, "tensor", axis=0, tiled=True)
        seq_len = whole.shape[0]
        projected = jnp.einsum("sd,tdc->tsc", whole, qkv_w, preferred_element_type=jnp.float32)
        bias_q = lax.dynamic_slice_in_dim(vec_f32[0], col_start, local_cols)
        bias_v = lax.dynamic_slice_in_dim(vec_f32[1], col_start, local_cols)
        query_heads = (projected[0] + bias_q).astype(jnp.bfloat16).reshape(seq_len, head_count, HD)
        key_heads = projected[1].astype(jnp.bfloat16).reshape(seq_len, head_count, HD)
        value_heads = (projected[2] + bias_v).astype(jnp.bfloat16).reshape(seq_len, head_count, HD)
        scores = attention_scores(query_heads, key_heads, segments)
        row_top = jnp.max(scores, axis=-1, keepdims=True)
        log_total = row_top + jnp.log(jnp.sum(jnp.exp(scores - row_top), axis=-1, keepdims=True))
        attn_probs = jnp.exp(scores - log_total).astype(jnp.bfloat16)
        context = jnp.einsum(
            "hqk,khe->qhe", attn_probs, value_heads, preferred_element_type=jnp.float32
        )
        context = context.reshape(seq_len, local_cols).astype(jnp.bfloat16)
        piece = context
        attn_mixed = lax.psum_scatter(
            jnp.dot(piece, out_w, preferred_element_type=jnp.float32).astype(jnp.bfloat16),
            "tensor",
            scatter_dimension=0,
            tiled=True,
        ).astype(jnp.float32)
        summed_one = tok_block.astype(jnp.float32) + attn_mixed + vec_f32[2]
        normed_out, normed_one, inverse_one = norm_forward(summed_one, vec_f32[3], vec_f32[4])
        normed_b = normed_out.astype(jnp.bfloat16)
        normed_whole = lax.all_gather(normed_b, "tensor", axis=0, tiled=True)
        bias_up = lax.dynamic_slice_in_dim(vec_f32[8:12].reshape(FF), ffn_start, hidden)
        pre_act = jnp.dot(normed_whole, up_w, preferred_element_type=jnp.float32) + bias_up
        activated = gelu_value(pre_act).astype(jnp.bfloat16)
        piece = activated
        summed_two = (
            normed_out
            + lax.psum_scatter(
                jnp.dot(piece, down_w, preferred_element_type=jnp.float32).astype(jnp.bfloat16),
                "tensor",
                scatter_dimension=0,
                tiled=True,
            ).astype(jnp.float32)
            + vec_f32[5]
        )
        final, normed_two, inverse_two = norm_forward(summed_two, vec_f32[6], vec_f32[7])
        saved = (
            whole,
            query_heads,
            key_heads,
            value_heads,
            log_total,
            context,
            normed_one,
            inverse_one,
            normed_whole,
            pre_act,
            activated,
            normed_two,
            inverse_two,
        )
        return (final.astype(jnp.bfloat16), saved)

    def backward(weights, saved, segments, grad_block):
        qkv_w, out_w, up_w, down_w, vec_b = weights
        vec_f32 = vec_b.astype(jnp.float32)
        (
            whole,
            query_heads,
            key_heads,
            value_heads,
            log_total,
            context,
            normed_one,
            inverse_one,
            normed_whole,
            pre_act,
            activated,
            normed_two,
            inverse_two,
        ) = saved
        seq_len = whole.shape[0]
        grad_final = grad_block.astype(jnp.float32)
        g_gain2 = jnp.sum(grad_final * normed_two, axis=0)
        g_shift2 = jnp.sum(grad_final, axis=0)
        grad_two = norm_backward(normed_two, inverse_two, grad_final * vec_f32[6])
        grad_two_b = grad_two.astype(jnp.bfloat16)
        g_bdown = jnp.sum(grad_two, axis=0)
        grad_two_whole = lax.all_gather(grad_two_b, "tensor", axis=0, tiled=True)
        g_down = jnp.dot(activated.T, grad_two_whole, preferred_element_type=jnp.float32)
        grad_pre = jnp.dot(
            grad_two_whole, down_w.T, preferred_element_type=jnp.float32
        ) * gelu_slope(pre_act)
        grad_pre_b = grad_pre.astype(jnp.bfloat16)
        g_bup = jnp.sum(grad_pre, axis=0)
        g_up = jnp.dot(normed_whole.T, grad_pre_b, preferred_element_type=jnp.float32)
        piece = grad_pre_b
        grad_one_in = grad_two + lax.psum_scatter(
            jnp.dot(piece, up_w.T, preferred_element_type=jnp.float32).astype(jnp.bfloat16),
            "tensor",
            scatter_dimension=0,
            tiled=True,
        ).astype(jnp.float32)
        g_gain1 = jnp.sum(grad_one_in * normed_one, axis=0)
        g_shift1 = jnp.sum(grad_one_in, axis=0)
        grad_one = norm_backward(normed_one, inverse_one, grad_one_in * vec_f32[3])
        grad_one_b = grad_one.astype(jnp.bfloat16)
        g_bout = jnp.sum(grad_one, axis=0)
        grad_one_whole = lax.all_gather(grad_one_b, "tensor", axis=0, tiled=True)
        g_out = jnp.dot(context.T, grad_one_whole, preferred_element_type=jnp.float32)
        grad_context = jnp.dot(grad_one_whole, out_w.T, preferred_element_type=jnp.float32).astype(
            jnp.bfloat16
        )
        grad_context = grad_context.reshape(seq_len, head_count, HD)
        scores = attention_scores(query_heads, key_heads, segments)
        attn_exact = jnp.exp(scores - log_total)
        attn_probs = attn_exact.astype(jnp.bfloat16)
        grad_probs = jnp.einsum(
            "qhe,khe->hqk", grad_context, value_heads, preferred_element_type=jnp.float32
        )
        row_dot = jnp.sum(attn_exact * grad_probs, axis=-1, keepdims=True)
        grad_scores = (attn_exact * (grad_probs - row_dot) * HD ** (-0.5)).astype(jnp.bfloat16)
        grad_value = jnp.einsum(
            "hqk,qhe->khe", attn_probs, grad_context, preferred_element_type=jnp.float32
        )
        grad_value = grad_value.reshape(seq_len, local_cols)
        grad_query = jnp.einsum(
            "hqk,khe->qhe", grad_scores, key_heads, preferred_element_type=jnp.float32
        )
        grad_query = grad_query.reshape(seq_len, local_cols)
        grad_key = jnp.einsum(
            "hqk,qhe->khe", grad_scores, query_heads, preferred_element_type=jnp.float32
        )
        grad_key = grad_key.reshape(seq_len, local_cols)
        grad_qkv = jnp.stack([grad_query, grad_key, grad_value]).astype(jnp.bfloat16)
        g_qkv = jnp.einsum("sd,tsc->tdc", whole, grad_qkv, preferred_element_type=jnp.float32)
        piece = grad_qkv
        grad_input = grad_one + lax.psum_scatter(
            jnp.einsum("tsc,tdc->sd", piece, qkv_w, preferred_element_type=jnp.float32).astype(
                jnp.bfloat16
            ),
            "tensor",
            scatter_dimension=0,
            tiled=True,
        ).astype(jnp.float32)
        zero_row = jnp.zeros((D,), jnp.float32)
        row_q = lax.dynamic_update_slice_in_dim(zero_row, jnp.sum(grad_query, axis=0), col_start, 0)
        row_v = lax.dynamic_update_slice_in_dim(zero_row, jnp.sum(grad_value, axis=0), col_start, 0)
        up_rows = lax.dynamic_update_slice_in_dim(
            jnp.zeros((FF,), jnp.float32), g_bup, ffn_start, 0
        ).reshape(4, D)
        first_rows = jnp.stack(
            [row_q, row_v, g_bout, g_gain1, g_shift1, g_bdown, g_gain2, g_shift2]
        )
        g_vec = jnp.concatenate([first_rows, up_rows], axis=0)
        return ((g_qkv, g_out, g_up, g_down, g_vec), grad_input)

    def one_batch(carried, batch_item):
        tok_block, segments, grad_block = batch_item
        forward_w = collect(w_qkv, w_out, w_up, w_down, vectors)
        final_b, saved = forward(forward_w, tok_block, segments)
        second = collect(w_qkv, w_out, w_up, w_down, vectors)
        gradients, grad_input = backward(second, saved, segments, grad_block)
        updated = jax.tree.map(jnp.add, carried, gradients)
        return (updated, (final_b, grad_input))

    initial = (
        jnp.zeros((3, D, local_cols), jnp.float32),
        jnp.zeros((local_cols, D), jnp.float32),
        jnp.zeros((D, hidden), jnp.float32),
        jnp.zeros((hidden, D), jnp.float32),
        jnp.zeros((12, D), jnp.float32),
    )
    carried, stacked = lax.scan(one_batch, initial, (tokens, segment_ids, cotangent))
    totals = share(carried)
    vector_grads = lax.psum(totals[4], "tensor")
    return (stacked[0], stacked[1], totals[0], totals[1], totals[2], totals[3], vector_grads)


Y_TOK, Y_COT, Y_OUT, Y_GTOK = range(4)
X_MIX, X_DH, X_DX, X_TOK, X_NORM, X_DA2, X_DA1 = range(7)
W_Q, W_K, W_V, W_OUT, W_UP, W_DOWN, W_REST, W_VEC = range(8)
W_KINDS = 8
Y_FIRST = (W_REST,)
DIRECT = (W_VEC,)
FAR_FIRST = ()
U_DA, U_DB, U_UA, U_UB, U_OUT, U_V, U_K, U_Q = range(8)
Z_FIRST = (U_DA,)
DA_ROWS = 640
R_BQ, R_BV, R_BO, R_G1, R_C1, R_BD, R_G2, R_C2, R_BU = range(9)
ZS = 4
SEQ = 512
ROWS = 256
CHUNK = 128
TILE = 32
COLS = 512
HID = 2048
WINDOW = 384
BF = jnp.bfloat16
F32 = jnp.float32
MESH = pl.DeviceIdType.MESH


def span(index, size):
    return pl.ds(pl.multiple_of(index * size, size), size)


def contract(a, b, a_dim, b_dim):
    return lax.dot_general(a, b, (((a_dim,), (b_dim,)), ((), ())), preferred_element_type=F32)


def fold_rows(value):
    return jnp.sum(value.reshape(value.shape[0] // 8, 8, value.shape[1]), axis=0)


def layer_kernel(
    tok, seg, wq, wo, wu, wd, vec, cot,
    out, gtok, gq, go, gu, gd, gv,
    w_qkv, w_out, w_up, w_down, w_vec, vf,
    g_da, g_db, g_up, g_out, g_qkv,
    c_da, c_db, c_up, c_out, c_qkv,
    y_da, y_db, y_up, y_out, y_qkv,
    z_da, z_db, z_up, z_out, z_qkv,
    h_da, h_db, h_up, h_out, h_qkv,
    o_qkv, o_out, o_up, o_down,
    xw, qkv, ctx, prob, bias, hw, act, slope, aw, a1w, dctx,
    own, n1, da, inv1, recv, stage, cotb, outb, gts, gtr, gtf,
    acc, vg, vgx, vgc, vgy, vgz, gvb, acc_k, acc_v,
    done, wrz, wry, wrc, wrd, fs, fr, xs, xr, yr,
    grc, gry, grz, vs, vr, ls, os,
):
    dp = lax.axis_index("dp")
    tensor = lax.axis_index("tensor")
    z, c = dp // 2, dp % 2
    y, x = tensor // 2, tensor % 2
    at_x = {"dp": dp, "tensor": y * 2 + (1 - x)}
    at_y = {"dp": dp, "tensor": (1 - y) * 2 + x}
    at_c = {"dp": z * 2 + (1 - c), "tensor": tensor}

    def remote(src, dst, send, recv_sem, where):
        return pltpu.make_async_remote_copy(
            src_ref=src, dst_ref=dst, send_sem=send, recv_sem=recv_sem,
            device_id=where, device_id_type=MESH,
        )

    barrier = pltpu.get_barrier_semaphore()
    for where in [at_x, at_y, at_c] + [{"dp": lax.rem(z + k, ZS) * 2 + c, "tensor": tensor} for k in range(1, ZS)]:
        pl.semaphore_signal(barrier, inc=1, device_id=where, device_id_type=MESH)
    pl.semaphore_wait(barrier, 6)

    sent = []

    quiet = []

    def go_on(copy):
        copy.start()
        if not quiet:
            sent.append(copy)

    args = [wq.at[0], wq.at[1], wq.at[2], wo, wu, wd.at[0:512], wd.at[512:1024], vec]
    edge = jnp.logical_or(z == 0, z == ZS - 1)
    middle = jnp.logical_not(edge)
    later = []

    def z_device(where):
        return {"dp": where * 2 + c, "tensor": tensor}

    def go_if(condition, copy):
        @pl.when(condition)
        def _():
            copy.start()
        if not quiet:
            later.append((condition, copy))

    def place(m, yy, d):
        if m <= W_V:
            return w_qkv.at[m, span(d, 128), span(yy, 256)]
        if m == W_OUT:
            return w_out.at[span(yy, 256), span(d, 128)]
        if m == W_UP:
            return w_up.at[span(d, 128), span(yy, 1024)]
        if m == W_DOWN or m == W_REST:
            return w_down.at[span(yy * 2 + m - W_DOWN, 512), span(d, 128)]
        return w_vec.at[d]

    even = lax.rem(z, 2) == 0
    near_first = (jnp.where(even, 3, 1), 2, jnp.where(even, 1, 3))

    def from_z(k):
        return lax.rem(z + ZS - k, ZS)

    def z_slot(m, r):
        return 24 if r else m * 3

    def column(r):
        return y if r == 0 else 1 - y

    def z_send(m, r):
        source = args[m] if r == 0 else place(m, 1 - y, dp)
        steps = ((1, z != ZS - 1), (3, z != 0), (2, None))
        for k, there in (steps[2:] + steps[:2] if m in FAR_FIRST else steps):
            there = None if m in DIRECT else there
            copy = remote(
                source, place(m, column(r), dp), done.at[0], wrz.at[z_slot(m, r) + k - 1],
                z_device(lax.rem(z + k, ZS)),
            )
            if there is None:
                go_on(copy)
            else:
                go_if(there, copy)

    def z_serve(m, r, step, keep=False):
        z_take(m, r, step, keep)
        z_note(m, r, step)

    def z_serve_split(m, r, step, early, late):
        def first():
            @pl.when(early)
            def _():
                z_take(m, r, step)

        def second():
            @pl.when(late)
            def _():
                z_take(m, r, step)
            z_note(m, r, step)
        return first, second

    def z_parts(m, r, step):
        k = near_first[step]
        here = place(m, column(r), from_z(k) * 2 + c)
        slot = jnp.where(z == 1, 0, 2)
        hand_on = None
        if step == 1 and m not in DIRECT:
            hand_on = remote(
                here, here, done.at[0], wrz.at[z_slot(m, r) + slot], z_device(jnp.where(z == 1, 0, 3)),
            )
        over_y = None
        if r == 0 and m not in Y_FIRST and m != W_VEC:
            over_y = remote(here, here, done.at[0], wry.at[m, from_z(k)], at_y)
        return k, here, hand_on, over_y

    def z_over(m, step):
        z_parts(m, 0, step)[3].start()

    def z_take(m, r, step, keep=False):
        k, here, hand_on, over_y = z_parts(m, r, step)
        remote(here, here, done.at[0], wrz.at[z_slot(m, r) + k - 1], at_x).wait_recv()
        if hand_on is not None:
            @pl.when(middle)
            def _():
                hand_on.start()
        if over_y is not None and not keep:
            over_y.start()
        c_send(m, here, step + 1)

    def z_note(m, r, step):
        _, _, hand_on, over_y = z_parts(m, r, step)
        if hand_on is not None:
            later.append((middle, hand_on))
        if over_y is not None:
            sent.append(over_y)

    def y_send(m):
        go_on(remote(args[m], place(m, y, dp), done.at[0], wry.at[m, z], at_y))

    def source_of(step):
        return z if step == 0 else from_z(near_first[step - 1])

    def y_serve(m, step):
        zz = source_of(step)
        here = place(m, 1 - y, zz * 2 + c)
        remote(here, here, done.at[0], wry.at[m, zz], at_y).wait_recv()
        c_send(m, here, step)

    def c_send(m, source, step, dest=None):
        dest = source if dest is None else dest
        into = wrd.at[m - W_DOWN, step] if m in (W_DOWN, W_REST) else wrc.at[m]
        remote(source, dest, done.at[0], into, at_c).start()

    def own_send(m):
        c_send(m, args[m], 0, place(m, y, dp))
        pltpu.make_async_copy(args[m], place(m, y, dp), ls.at[m]).start()

    def half_of(m):
        if m <= W_V:
            return w_qkv.at[m, :, 0:256]
        return (
            w_out.at[0:256], w_up.at[:, 0:1024], w_down.at[0:512], w_down.at[0:512], w_vec.at[0:4]
        )[m - W_OUT]

    def wait_down(step):
        for m in (W_DOWN, W_REST):
            if step == 0:
                pltpu.make_async_copy(args[m], place(m, y, dp), ls.at[m]).wait()
            two = w_down.at[0:1024, 0:128]
            remote(two, two, done.at[0], wrd.at[m - W_DOWN, step], at_c).wait_recv()

    def wait_weight(m):
        pltpu.make_async_copy(args[m], place(m, y, dp), ls.at[m]).wait()
        remote(half_of(m), half_of(m), done.at[0], wrc.at[m], at_c).wait_recv()

    def x_copy(kind, j, src, dst):
        return remote(src, dst, xs.at[kind, j] if kind <= X_DX else done.at[0], xr.at[kind, j], at_x)

    def tok_rows(xx, yy):
        return pl.ds(pl.multiple_of(xx * ROWS + yy * CHUNK, CHUNK), CHUNK)

    for m in (W_Q, W_K, W_V):
        y_send(m)
        z_send(m, 0)
    go_on(remote(tok.at[1 - y], xw.at[tok_rows(x, y)], done.at[0], yr.at[Y_TOK], at_y))
    go_on(x_copy(X_TOK, 0, tok.at[y], xw.at[tok_rows(x, y)]))
    z_send(W_VEC, 0)
    for m in range(W_KINDS):
        own_send(m)
    local_x = pltpu.make_async_copy(tok.at[y], xw.at[tok_rows(x, y)], ls.at[8])
    local_x.start()
    local_cot = pltpu.make_async_copy(cot.at[y], cotb.at[span(y, CHUNK)], ls.at[9])
    local_cot.start()

    seg_row = seg[pl.ds(y, 1), :].astype(F32)
    blocks = [(p % 2) * 2 + p // 2 for p in range(4)]
    across = [jnp.broadcast_to(seg_row[:, n * 128:(n + 1) * 128], (128, 128)) for n in blocks]
    down = [b.T for b in across]
    for t in range(2):
        for i, q in enumerate((t, t + 2)):
            for j in range(3):
                same = down[q] == across[t + j]
                bias[t, i * 128:(i + 1) * 128, j * 128:(j + 1) * 128] = jnp.where(same, 0.0, MASKED)
    acc[...] = jnp.zeros_like(acc)
    vg[...] = jnp.zeros_like(vg)

    for step in range(2):
        for m in (W_Q, W_K, W_V):
            z_serve(m, 0, step)
    z_send(W_OUT, 0)
    y_tok_here = xw.at[tok_rows(x, 1 - y)]
    remote(tok.at[1 - y], y_tok_here, done.at[0], yr.at[Y_TOK], at_y).wait_recv()
    go_on(x_copy(X_TOK, 1, y_tok_here, y_tok_here))
    for m in (W_Q, W_K, W_V):
        z_serve(m, 0, 2)
    y_send(W_OUT)
    z_serve(W_OUT, 0, 0)
    z_serve(W_OUT, 0, 1)
    z_send(W_UP, 0)
    for step in range(3):
        z_serve(W_VEC, 0, step)
    z_serve(W_OUT, 0, 2)
    y_send(W_UP)
    y_send(W_REST)
    for step in range(4):
        for m in (W_Q, W_K, W_V):
            y_serve(m, step)
    wait_weight(W_VEC)
    for d in range(8):
        vf[0:12, d * 128:(d + 1) * 128] = w_vec[d].astype(F32)
    local_x.wait()
    for j, yy in ((0, y), (1, 1 - y)):
        there = xw.at[tok_rows(1 - x, yy)]
        x_copy(X_TOK, j, there, there).wait_recv()
    for m in (W_Q, W_K, W_V):
        wait_weight(m)

    def head_bias(row):
        parts = [vf[row:row + 1, pl.ds(pl.multiple_of(yy * 512 + x * 256, 256), 256)] for yy in range(2)]
        return jnp.concatenate(parts, axis=1)

    for i in range(3):
        value = contract(xw[...], w_qkv[i], 1, 0)
        if i == 0:
            value = (value + head_bias(0)).astype(BF) * BF(HD ** -0.5)
        elif i == 2:
            value = value + head_bias(1)
        qkv[i] = value.astype(BF)

    low_half = lax.broadcasted_iota(jnp.int32, (1, 128), 1) < HD
    halves = (low_half, jnp.logical_not(low_half))
    none = jnp.zeros((), BF)

    def two_blocks(ref, t, lanes):
        return jnp.concatenate([ref[span(t, 128), lanes], ref[span(t + 2, 128), lanes]], axis=0)

    def attend(pair, carry):
        lanes = span(pair, 128)
        for t in range(2):
            keys = pl.ds(t * 128, WINDOW)
            query = two_blocks(qkv.at[0], t, lanes)
            key, value = qkv[1, keys, lanes], qkv[2, keys, lanes]
            total = jnp.zeros((ROWS, 128), F32)
            for h, half in enumerate(halves):
                scores = contract(jnp.where(half, query, none), key, 1, 1) + bias[t]
                top = jnp.max(scores, axis=1, keepdims=True)
                weight = jnp.exp(scores - top)
                share_of = 1.0 / jnp.sum(weight, axis=1, keepdims=True)
                weight = (weight * share_of).astype(BF)
                prob[pair * 4 + t * 2 + h] = weight
                total = total + contract(weight, jnp.where(half, value, none), 1, 0)
            total = total.astype(BF)
            ctx[t * 128:t * 128 + 128, lanes] = total[:128]
            ctx[t * 128 + 256:t * 128 + 384, lanes] = total[128:]
        return carry

    z_serve(W_UP, 0, 0)
    lax.fori_loop(0, 2, attend, 0)
    for step in range(4):
        y_serve(W_OUT, step)
    lax.fori_loop(2, 4, attend, 0)
    up_early, up_late = z_serve_split(W_UP, 0, 1, middle, edge)
    up_early()
    z_send(W_DOWN, 0)

    def rows_of(s):
        mine = jnp.where(s < 2, x, 1 - x)
        return pl.ds(pl.multiple_of(mine * ROWS + lax.rem(s, 2) * CHUNK, CHUNK), CHUNK)

    def x_sum(kind, j):
        return x_copy(kind, j, stage.at[span(j, CHUNK)], recv.at[span(j, CHUNK)])

    def x_rows(kind, j, buf):
        here = buf.at[pl.ds(pl.multiple_of(x * ROWS + j * CHUNK, CHUNK), CHUNK)]
        return x_copy(kind, j, here, here)

    def hand_over(kind, before, s, value):
        @pl.when(s < 2)
        def _():
            own[span(s, CHUNK), :] = value

        @pl.when(s >= 2)
        def _():
            if before is not None:
                x_sum(before, s - 2).wait_send()
            stage[span(s - 2, CHUNK), :] = value.astype(BF)
            x_sum(kind, s - 2).start()

    wait_weight(W_OUT)

    def mix(i, carry):
        s = lax.rem(i + 2, 4)
        hand_over(X_MIX, None, s, contract(ctx[rows_of(s), :], w_out[...], 1, 0))
        return carry

    lax.fori_loop(0, 4, mix, 0)
    up_late()
    z_serve(W_UP, 0, 2)
    y_serve(W_REST, 0)
    z_send(W_REST, 0)
    z_send(W_REST, 1)
    y_serve(W_UP, 0)
    z_serve(W_DOWN, 0, 0, keep=True)
    z_serve(W_DOWN, 0, 1, keep=True)

    def row_of(row):
        return vf[row:row + 1, :]

    def normed(value):
        centred = value - jnp.mean(value, axis=1, keepdims=True)
        inverse = lax.rsqrt(jnp.mean(centred * centred, axis=1, keepdims=True) + NORM_EPS)
        return centred * inverse, inverse

    def norm_back(normal, inverse, grad):
        first = jnp.mean(grad, axis=1, keepdims=True)
        second = jnp.mean(grad * normal, axis=1, keepdims=True)
        return inverse * (grad - first - normal * second)

    def tiles(j, body):
        def step(i, carry):
            body(pl.ds(pl.multiple_of(j * CHUNK + i * TILE, TILE), TILE),
                 pl.ds(pl.multiple_of(x * ROWS + j * CHUNK + i * TILE, TILE), TILE))
            return carry
        lax.fori_loop(0, CHUNK // TILE, step, 0)

    def first_norm(r, g):
        summed = xw[g, :].astype(F32) + own[r, :] + recv[r, :].astype(F32) + row_of(R_BO)
        normal, inverse = normed(summed)
        n1[r, :] = normal
        inv1[r, :] = jnp.broadcast_to(inverse, (TILE, 128))
        hw[g, :] = (normal * row_of(R_G1) + row_of(R_C1)).astype(BF)

    for j in range(2):
        x_sum(X_MIX, j).wait_recv()
        tiles(j, first_norm)
        x_rows(X_NORM, j, hw).start()

    y_send(W_DOWN)
    z_over(W_DOWN, 0)
    z_over(W_DOWN, 1)
    for step in range(1, 4):
        y_serve(W_UP, step)
    wait_weight(W_UP)

    def arrived(kind, s, buf):
        @pl.when(s >= 2)
        def _():
            there = buf.at[rows_of(s)]
            x_copy(kind, s - 2, there, there).wait_recv()

    def up_bias(n):
        return vf[pl.ds(8 + n * 2 + x, 1), :]

    def ffn_up(s, carry):
        rows = rows_of(s)
        arrived(X_NORM, s, hw)
        for n in range(2):
            pre = contract(hw[rows, :], w_up[:, n * 1024:(n + 1) * 1024], 1, 0) + up_bias(n)
            cdf = 0.5 * (1.0 + lax.erf(pre * SQRT_HALF))
            act[rows, n * 1024:(n + 1) * 1024] = (pre * cdf).astype(BF)
            slope[rows, n * 1024:(n + 1) * 1024] = (
                cdf + pre * INV_ROOT_TAU * jnp.exp(-0.5 * pre * pre)
            ).astype(BF)
        return carry

    lax.fori_loop(0, 2, ffn_up, 0)
    z_serve(W_DOWN, 0, 2)
    for r in range(2):
        z_serve(W_REST, r, 0)
        z_serve(W_REST, r, 1)
    y_serve(W_DOWN, 0)
    lax.fori_loop(2, 3, ffn_up, 0)
    y_serve(W_DOWN, 1)
    lax.fori_loop(3, 4, ffn_up, 0)
    y_serve(W_DOWN, 2)
    go_on(remote(cot.at[1 - y], cotb.at[span(y, CHUNK)], done.at[0], yr.at[Y_COT], at_y))

    def ffn_copy(step, j):
        cols = span(source_of(step), 256)
        return remote(
            stage.at[span(j, CHUNK), cols], recv.at[span(j, CHUNK), cols],
            fs.at[0], fr.at[j], at_x,
        )

    for j in range(2):
        x_sum(X_MIX, j).wait_send()
    for step in range(4):
        if step == 2:
            y_serve(W_DOWN, 3)
        if step == 3:
            z_serve(W_REST, 0, 2)
            z_serve(W_REST, 1, 2)
        wait_down(step)
        cols = span(source_of(step), 256)
        stage[:, cols] = contract(act[span(1 - x, ROWS), :], w_down[:, cols], 1, 0).astype(BF)
        for j in range(2):
            ffn_copy(step, j).start()
    for step in range(2):
        cols = span(step, 512)
        own[:, cols] = contract(act[span(x, ROWS), :], w_down[:, cols], 1, 0)

    def bump(row, value):
        acc[row] += fold_rows(value)

    def second_norm(r, g):
        h1 = n1[r, :] * row_of(R_G1) + row_of(R_C1)
        normal, inverse = normed(h1 + own[r, :] + recv[r, :].astype(F32) + row_of(R_BD))
        own[r, :] = normal
        grad = norm_back(normal, inverse, cotb[r, :].astype(F32) * row_of(R_G2))
        da[r, :] = grad
        aw[g, :] = grad.astype(BF)

    def second_rest(r, g):
        normal, dy = own[r, :], cotb[r, :].astype(F32)
        outb[r, :] = (normal * row_of(R_G2) + row_of(R_C2)).astype(BF)
        bump(R_G2, dy * normal)
        bump(R_C2, dy)
        bump(R_BD, da[r, :])

    local_cot.wait()
    cot_here = cotb.at[span(1 - y, CHUNK)]
    remote(cot.at[1 - y], cot_here, done.at[0], yr.at[Y_COT], at_y).wait_recv()
    for j in range(2):
        half = recv.at[span(j, CHUNK)]
        remote(half, half, fs.at[0], fr.at[j], at_x).wait_recv()
        tiles(j, second_norm)
        x_rows(X_DA2, j, aw).start()
    for j in range(2):
        tiles(j, second_rest)
    out_here = pltpu.make_async_copy(outb.at[span(y, CHUNK)], out.at[y], os.at[0])
    out_here.start()
    go_on(remote(outb.at[span(1 - y, CHUNK)], out.at[y], done.at[0], yr.at[Y_OUT], at_y))

    def ffn_back(s, carry):
        rows = rows_of(s)
        arrived(X_DA2, s, aw)
        for n in range(2):
            cols = slice(n * 1024, (n + 1) * 1024)
            grad = contract(aw[rows, :], w_down[cols, :], 1, 1) * slope[rows, cols].astype(F32)
            bump(R_BU + n, grad)
            slope[rows, cols] = grad.astype(BF)
        hand_over(X_DH, None, s, contract(slope[rows, :], w_up[...], 1, 1))
        return carry

    remote(stage, stage, fs.at[0], fr.at[0], at_x).wait_send()
    lax.fori_loop(0, 4, ffn_back, 0)

    units = {
        U_DA: (g_da, c_da, y_da, z_da, h_da, o_down.at[0:DA_ROWS], gd.at[0:DA_ROWS]),
        U_DB: (g_db, c_db, y_db, z_db, h_db, o_down.at[DA_ROWS:1024], gd.at[DA_ROWS:1024]),
        U_OUT: (g_out, c_out, y_out, z_out, h_out, o_out, go),
    }
    for u, i in ((U_UA, 0), (U_UB, 1)):
        rows = slice(i * 64, (i + 1) * 64)
        units[u] = tuple(r.at[i] for r in (g_up, c_up, y_up, z_up, h_up)) + (o_up.at[rows], gu.at[rows])
    for u, i in ((U_Q, 0), (U_K, 1), (U_V, 2)):
        units[u] = tuple(r.at[i] for r in (g_qkv, c_qkv, y_qkv, z_qkv, h_qkv, o_qkv, gq))

    def piece_loop(rows, body):
        size = min(rows, CHUNK)

        def step(i, carry):
            body(span(i, size))
            return carry
        lax.fori_loop(0, rows // size, step, 0)

    def add_piece(g, yy, zz, other):
        def body(r):
            g[c, yy, zz, r, :] = (g[c, yy, zz, r, :].astype(F32) + other[r, :].astype(F32)).astype(BF)
        piece_loop(g.shape[3], body)

    def core_copy(u):
        g, rc = units[u][0], units[u][1]
        return remote(g.at[1 - c], rc, done.at[0], grc.at[u], at_c)

    def core_send(u):
        go_on(core_copy(u))

    def core_add(u, r):
        g, rc = units[u][0], units[u][1]
        for zz in range(ZS):
            add_piece(g, column(r), zz, rc.at[column(r), zz])

    def rs_y_copy(u):
        g, ry = units[u][0], units[u][2]
        source = g.at[c, 1 - y, pl.ds(z, 1)] if u in Z_FIRST else g.at[c, 1 - y]
        return remote(source, ry, done.at[0], gry.at[u], at_y)

    def rs_z_copy(u, r, k):
        g, rz = units[u][0], units[u][3]
        to = lax.rem(z + k, ZS)
        return remote(g.at[c, column(r), to], rz.at[r, k - 1], done.at[0], grz.at[(32 if r else u * 4) + k - 1], z_device(to))

    def rs_hand_on(u, r):
        g, rh = units[u][0], units[u][4]
        far = jnp.where(z == 0, ZS - 1, 0)
        return remote(g.at[c, column(r), far], rh.at[r], done.at[0], grz.at[(32 if r else u * 4) + 3], z_device(jnp.where(z == 0, 1, 2)))

    def z_hand_on(u, r):
        go_if(edge, rs_hand_on(u, r))

    def z_begin(u, r):
        go_if(z != ZS - 1, rs_z_copy(u, r, 1))
        go_if(z != 0, rs_z_copy(u, r, 3))
        go_if(edge, rs_z_copy(u, r, 2))

    def z_relay(u, r):
        g, rh = units[u][0], units[u][4]

        @pl.when(middle)
        def _():
            rs_hand_on(u, r).wait_recv()
            add_piece(g, column(r), lax.rem(z + 2, ZS), rh.at[r])
        go_if(middle, rs_z_copy(u, r, 2))

    def start(u):
        core_copy(u).wait_recv()
        core_add(u, 1)
        if u in Z_FIRST:
            z_hand_on(u, 1)
            core_add(u, 0)
            z_hand_on(u, 0)
            z_begin(u, 1)
            z_begin(u, 0)
        else:
            go_on(rs_y_copy(u))
            core_add(u, 0)

    def y_to_z(u):
        g, ry = units[u][0], units[u][2]
        rs_y_copy(u).wait_recv()
        for zz in range(ZS):
            add_piece(g, y, zz, ry.at[zz])
        z_hand_on(u, 0)
        z_begin(u, 0)

    def wait_z(u, r):
        rs_z_copy(u, r, 2).wait_recv()

        @pl.when(z != 0)
        def _():
            rs_z_copy(u, r, 1).wait_recv()

        @pl.when(z != ZS - 1)
        def _():
            rs_z_copy(u, r, 3).wait_recv()

    def z_total(u, r, rows):
        g, rz = units[u][0], units[u][3]
        value = g[c, column(r), z, rows, :].astype(F32)
        for k in range(ZS - 1):
            value = value + rz[r, k, rows, :].astype(F32)
        return value

    def z_to_y(u):
        g = units[u][0]
        wait_z(u, 1)

        def body(rows):
            g[c, 1 - y, z, rows, :] = z_total(u, 1, rows).astype(BF)
        piece_loop(g.shape[3], body)
        go_on(rs_y_copy(u))

    finals = []

    def finish(u):
        g, _, ry, _, _, o, dest = units[u]
        wait_z(u, 0)
        if u in Z_FIRST:
            rs_y_copy(u).wait_recv()

        def body(rows):
            value = z_total(u, 0, rows)
            if u in Z_FIRST:
                value = value + ry[0, rows, :].astype(F32)
            o[rows, :] = value
        piece_loop(g.shape[3], body)
        copy = pltpu.make_async_copy(o, dest, os.at[0])
        copy.start()
        finals.append(copy)

    for u in units:
        for r in range(2 if u in Z_FIRST else 1):
            for k, alone in ((1, z == 0), (3, z == ZS - 1)):
                @pl.when(alone)
                def _(u=u, r=r, k=k):
                    rz = units[u][3]
                    rz[r, k - 1] = jnp.zeros(rz.shape[2:], BF)

    def grad_down(u):
        g, first, count = (g_da, 0, DA_ROWS) if u == U_DA else (g_db, DA_ROWS, 1024 - DA_ROWS)

        def step(yy, carry):
            rows = pl.ds(pl.multiple_of(yy * 1024 + first, 128), count)
            value = contract(act[:, rows], aw[...], 0, 0).astype(BF)
            for d in range(8):
                g[d % 2, yy, d // 2] = value[:, d * 128:(d + 1) * 128]
            return carry

        lax.fori_loop(0, 2, step, 0)
        core_send(u)

    def grad_up():
        def step(index, carry):
            i, n = index // 2, index % 2
            value = contract(hw[:, span(i, 512)], slope[:, span(n, 1024)], 0, 0).astype(BF)
            for d in range(4):
                for part in range(2):
                    r = d * 128 + part * 64
                    g_up[part, d % 2, n, i * 2 + d // 2] = value[r:r + 64, :]
            return carry

        lax.fori_loop(0, 4, step, 0)
        core_send(U_UA)
        core_send(U_UB)

    quiet.append(True)

    @pl.when(c == 0)
    def _():
        grad_down(U_DB)
        start(U_DB)
        grad_down(U_DA)
        start(U_DA)
        grad_up()

    @pl.when(c == 1)
    def _():
        grad_down(U_DB)
        grad_down(U_DA)
        grad_up()
        start(U_DB)
        start(U_DA)

    quiet.clear()
    for u in (U_DB, U_DA, U_UA, U_UB):
        sent.append(core_copy(u))
    sent.append(rs_y_copy(U_DB))
    for r in (1, 0):
        later.append((edge, rs_hand_on(U_DA, r)))
        later.append((z != ZS - 1, rs_z_copy(U_DA, r, 1)))
        later.append((z != 0, rs_z_copy(U_DA, r, 3)))
        later.append((edge, rs_z_copy(U_DA, r, 2)))
    for u in (U_UA, U_UB):
        start(u)

    def back_norm(r, g):
        grad = da[r, :] + own[r, :] + recv[r, :].astype(F32)
        own[r, :] = grad
        grad = norm_back(n1[r, :], inv1[r, 0:1], grad * row_of(R_G1))
        da[r, :] = grad
        a1w[g, :] = grad.astype(BF)

    def back_rest(r, g):
        grad = own[r, :]
        bump(R_G1, grad * n1[r, :])
        bump(R_C1, grad)
        bump(R_BO, da[r, :])

    for j in range(2):
        x_sum(X_DH, j).wait_recv()
        tiles(j, back_norm)
        x_rows(X_DA1, j, a1w).start()
    for j in range(2):
        tiles(j, back_rest)

    z_relay(U_DA, 1)
    z_relay(U_DA, 0)

    def ctx_back(s, carry):
        rows = rows_of(s)
        arrived(X_DA1, s, a1w)
        dctx[rows, :] = contract(a1w[rows, :], w_out[...], 1, 1).astype(BF)
        return carry

    lax.fori_loop(0, 2, ctx_back, 0)
    y_to_z(U_DB)
    lax.fori_loop(2, 4, ctx_back, 0)

    def attend_back(pair, carry):
        lanes = span(pair, 128)
        for t in range(2):
            keys = pl.ds(t * 128, WINDOW)
            query = two_blocks(qkv.at[0], t, lanes)
            key, value = qkv[1, keys, lanes], qkv[2, keys, lanes]
            grad = two_blocks(dctx, t, lanes)
            product = grad.astype(F32) * two_blocks(ctx, t, lanes).astype(F32)
            grad_q = jnp.zeros((ROWS, 128), F32)
            grad_k = jnp.zeros((WINDOW, 128), F32)
            grad_v = jnp.zeros((WINDOW, 128), F32)
            for h, half in enumerate(halves):
                grad_h = jnp.where(half, grad, none)
                weight = prob[pair * 4 + t * 2 + h]
                row_dot = jnp.sum(jnp.where(half, product, 0.0), axis=1, keepdims=True)
                score = (weight.astype(F32) * (contract(grad_h, value, 1, 1) - row_dot)).astype(BF)
                grad_q = grad_q + contract(score, jnp.where(half, key, none), 1, 0)
                grad_k = grad_k + contract(score, jnp.where(half, query, none), 0, 0)
                grad_v = grad_v + contract(weight, grad_h, 0, 0)
            grad_q = grad_q * (HD ** -0.5)
            acc[R_BQ, :, lanes] += fold_rows(grad_q)
            acc[R_BV, :, lanes] += fold_rows(grad_v)
            grad_q = grad_q.astype(BF)
            qkv[0, t * 128:t * 128 + 128, lanes] = grad_q[:128]
            qkv[0, t * 128 + 256:t * 128 + 384, lanes] = grad_q[128:]
            if t == 0:
                acc_k[0:WINDOW, :] = grad_k
                acc_v[0:WINDOW, :] = grad_v
                acc_k[WINDOW:SEQ, :] = jnp.zeros((128, 128), F32)
                acc_v[WINDOW:SEQ, :] = jnp.zeros((128, 128), F32)
            else:
                for i, total, more in ((1, acc_k, grad_k), (2, acc_v, grad_v)):
                    qkv[i, 0:128, lanes] = total[0:128, :].astype(BF)
                    qkv[i, 128:SEQ, lanes] = (total[128:SEQ, :] + more).astype(BF)
        return carry

    def grad_out():
        value = contract(ctx[...], a1w[...], 0, 0).astype(BF)
        for d in range(8):
            for yy in range(2):
                g_out[d % 2, yy, d // 2] = value[yy * 256:(yy + 1) * 256, d * 128:(d + 1) * 128]

    grad_out()
    core_send(U_OUT)
    lax.fori_loop(0, 2, attend_back, 0)
    start(U_OUT)
    y_to_z(U_UA)
    lax.fori_loop(2, 4, attend_back, 0)

    for row in range(2, 8):
        line = jnp.sum(acc[row], axis=0, keepdims=True)
        for d in range(8):
            vg[d % 2, d // 2, row:row + 1, :] = line[:, d * 128:(d + 1) * 128]
    for n in range(2):
        line = jnp.sum(acc[R_BU + n], axis=0, keepdims=True)
        for d in range(8):
            vg[d % 2, d // 2, pl.ds(8 + n * 2 + x, 1), :] = line[:, d * 128:(d + 1) * 128]
    for row, source in ((0, R_BQ), (1, R_BV)):
        line = jnp.sum(acc[source], axis=0, keepdims=True)
        for yy in range(2):
            for half in range(2):
                vg[half, 2 * yy + x, row:row + 1, :] = (
                    line[:, yy * 256 + half * 128:yy * 256 + (half + 1) * 128]
                )
    vec_x = remote(vg, vgx, vs.at[0], vr.at[0], at_x)
    vec_c = remote(vg.at[1 - c], vgc, vs.at[1], vr.at[1], at_c)
    vec_y = remote(vg.at[c], vgy, vs.at[2], vr.at[2], at_y)

    def vec_z(k):
        to = lax.rem(z + k, ZS)
        return remote(vg.at[c, to], vgz.at[k - 1], done.at[0], vr.at[2 + k], z_device(to))

    vec_x.start()

    def input_back(i, carry):
        s = lax.rem(i + 2, 4)
        rows = rows_of(s)
        value = contract(qkv[0, rows, :], w_qkv[0], 1, 1)
        value = value + contract(qkv[1, rows, :], w_qkv[1], 1, 1)
        value = value + contract(qkv[2, rows, :], w_qkv[2], 1, 1)
        hand_over(X_DX, X_DH, s, value)
        return carry

    lax.fori_loop(0, 2, input_back, 0)
    vec_x.wait()
    vg[...] = vg[...] + vgx[...]
    vec_c.start()

    def grad_qkv(index, carry):
        kind, i = index // 2, index % 2
        value = contract(xw[:, span(i, 512)], qkv[kind], 0, 0).astype(BF)
        for d in range(4):
            for yy in range(2):
                g_qkv[kind, d % 2, yy, i * 2 + d // 2] = (
                    value[d * 128:(d + 1) * 128, yy * 256:(yy + 1) * 256]
                )
        return carry

    for kind, u in ((0, U_Q), (1, U_K), (2, U_V)):
        lax.fori_loop(kind * 2, kind * 2 + 2, grad_qkv, 0)
        core_send(u)
    z_relay(U_DB, 0)
    vec_c.wait()
    vg[c] = vg[c] + vgc[...]
    vec_y.start()
    for u in (U_Q, U_K, U_V):
        start(u)
    z_relay(U_UA, 0)
    y_to_z(U_UB)
    lax.fori_loop(2, 4, input_back, 0)
    y_to_z(U_OUT)
    z_to_y(U_DA)
    vec_y.wait()
    vg[c] = vg[c] + vgy[...]
    for k in range(1, ZS):
        go_on(vec_z(k))

    def last_sum(j, other):
        x_sum(X_DX, j).wait_recv()

        def body(r, g):
            value = da[r, :] + own[r, :] + recv[r, :].astype(F32)
            if other:
                gts[pl.ds(pl.multiple_of(r.start - j * CHUNK, TILE), TILE), :] = value.astype(BF)
            else:
                da[r, :] = value
        tiles(j, body)

    last_sum(1 - y, True)
    go_on(remote(gts, gtr, done.at[0], yr.at[Y_GTOK], at_y))
    last_sum(y, False)
    gtok_here = pltpu.make_async_copy(da.at[span(y, CHUNK)], gtok.at[y], os.at[0])
    gtok_here.start()
    z_relay(U_UB, 0)
    y_to_z(U_Q)
    z_relay(U_OUT, 0)
    y_to_z(U_K)
    y_to_z(U_V)
    for u in (U_Q, U_K, U_V):
        z_relay(u, 0)
    for k in range(1, ZS):
        vec_z(k).wait_recv()
    gvb[...] = vg[c, z] + vgz[0] + vgz[1] + vgz[2]
    vec_here = pltpu.make_async_copy(gvb.at[0:12], gv, os.at[0])
    vec_here.start()
    for u in (U_DA, U_DB, U_UA, U_UB):
        finish(u)
    remote(gts, gtr, done.at[0], yr.at[Y_GTOK], at_y).wait_recv()
    gtf[...] = gtr[...].astype(F32)
    gtok_there = pltpu.make_async_copy(gtf, gtok.at[1 - y], os.at[0])
    gtok_there.start()
    finish(U_OUT)
    finish(U_Q)
    finish(U_K)
    finish(U_V)
    remote(outb.at[span(1 - y, CHUNK)], out.at[1 - y], done.at[0], yr.at[Y_OUT], at_y).wait_recv()
    for kind, buf in ((X_NORM, hw), (X_DA2, aw), (X_DA1, a1w)):
        for j in range(2):
            x_rows(kind, j, buf).wait_send()
    for j in range(2):
        x_sum(X_DX, j).wait_send()
    for copy in sent:
        copy.wait_send()
    for condition, copy in later:
        @pl.when(condition)
        def _(copy=copy):
            copy.wait_send()
    for m in range(W_KINDS):
        remote(half_of(m), half_of(m), done.at[0], wrc.at[m], at_c).wait_send()
    for copy in finals + [out_here, gtok_here, gtok_there, vec_here]:
        copy.wait()


def settle_kernel(*refs):
    count = (len(refs) - 2) // 3
    sources, dests, held = refs[:count], refs[count:2 * count], refs[2 * count:3 * count]
    into, out_of = refs[3 * count:]
    first = [pltpu.make_async_copy(s, h, into.at[i]) for i, (s, h) in enumerate(zip(sources, held))]
    second = [pltpu.make_async_copy(h, d, out_of.at[i]) for i, (h, d) in enumerate(zip(held, dests))]
    for copy in first:
        copy.start()
    for before, after in zip(first, second):
        before.wait()
        after.start()
    for copy in second:
        copy.wait()


def settle(results):
    shapes = [jax.ShapeDtypeStruct(r.shape, r.dtype) for r in results]
    count = len(shapes)
    hbm = pl.BlockSpec(memory_space=pl.ANY)
    return pl.pallas_call(
        settle_kernel,
        out_shape=shapes,
        in_specs=[hbm] * count,
        out_specs=[hbm] * count,
        scratch_shapes=[pltpu.VMEM(r.shape, r.dtype) for r in shapes]
        + [pltpu.SemaphoreType.DMA((count,))] * 2,
    )(*results)


def layer(tokens, segment_ids, w_qkv, w_out, w_up, w_down, vectors, cotangent):
    vmem, dma = pltpu.VMEM, pltpu.SemaphoreType.DMA
    outs = (
        jax.ShapeDtypeStruct(tokens.shape, BF),
        jax.ShapeDtypeStruct(tokens.shape, F32),
        jax.ShapeDtypeStruct(w_qkv.shape, F32),
        jax.ShapeDtypeStruct(w_out.shape, F32),
        jax.ShapeDtypeStruct(w_up.shape, F32),
        jax.ShapeDtypeStruct(w_down.shape, F32),
        jax.ShapeDtypeStruct(vectors.shape, F32),
    )
    scratch = [
        vmem((3, D, COLS), BF), vmem((COLS, D), BF), vmem((D, HID), BF), vmem((HID, D), BF),
        vmem((8, 12, 128), BF), vmem((16, D), F32),
    ]
    part_da, part_db = (DA_ROWS, 128), (1024 - DA_ROWS, 128)
    half_up, piece_out, piece_qkv = (64, 1024), (256, 128), (128, 256)
    for shape in ((2, 2, 4), (2, 4)):
        scratch += [
            vmem(shape + part_da, BF), vmem(shape + part_db, BF), vmem((2,) + shape + half_up, BF),
            vmem(shape + piece_out, BF), vmem((3,) + shape + piece_qkv, BF),
        ]
    for y_shape, z_shape in (((4,), (1,)), ((1, 3), (2, 3)), ((1,), (2,))):
        scratch += [
            vmem(z_shape + part_da, BF), vmem(y_shape + part_db, BF),
            vmem((2,) + y_shape + half_up, BF), vmem(y_shape + piece_out, BF),
            vmem((3,) + y_shape + piece_qkv, BF),
        ]
    scratch += [vmem((3, 128, 256), F32), vmem((256, 128), F32), vmem((128, 1024), F32), vmem((1024, 128), F32)]
    scratch += [
        vmem((SEQ, D), BF), vmem((3, SEQ, COLS), BF), vmem((SEQ, COLS), BF),
        vmem((16, ROWS, WINDOW), BF), vmem((2, ROWS, WINDOW), F32), vmem((SEQ, D), BF),
        vmem((SEQ, HID), BF), vmem((SEQ, HID), BF), vmem((SEQ, D), BF), vmem((SEQ, D), BF),
        vmem((SEQ, COLS), BF),
        vmem((ROWS, D), F32), vmem((ROWS, D), F32), vmem((ROWS, D), F32), vmem((ROWS, 128), F32),
        vmem((ROWS, D), BF), vmem((ROWS, D), BF), vmem((ROWS, D), BF), vmem((ROWS, D), BF),
        vmem((CHUNK, D), BF), vmem((CHUNK, D), BF), vmem((CHUNK, D), F32),
        vmem((12, 8, D), F32),
        vmem((2, 4, 16, 128), F32), vmem((2, 4, 16, 128), F32), vmem((4, 16, 128), F32),
        vmem((4, 16, 128), F32), vmem((3, 16, 128), F32), vmem((16, 128), F32),
        vmem((SEQ, 128), F32), vmem((SEQ, 128), F32),
        dma((1,)), dma((27,)), dma((7, 4)), dma((8,)), dma((2, 4)), dma((1,)), dma((2,)),
        dma((3, 2)), dma((7, 2)), dma((4,)),
        dma((8,)), dma((8,)), dma((36,)),
        dma((3,)), dma((6,)), dma((10,)), dma((1,)),
    ]
    hbm = pl.BlockSpec(memory_space=pl.ANY)
    results = pl.pallas_call(
        layer_kernel,
        out_shape=outs,
        in_specs=[hbm, pl.BlockSpec(memory_space=pltpu.VMEM)] + [hbm] * 6,
        out_specs=[hbm] * 7,
        scratch_shapes=scratch,
        compiler_params=pltpu.CompilerParams(
            collective_id=0, has_side_effects=True, vmem_limit_bytes=67043328
        ),
    )(tokens, segment_ids, w_qkv, w_out, w_up, w_down, vectors, cotangent)
    return settle(results)


def solution(mesh):
    step = layer if (mesh.shape["dp"], mesh.shape["tensor"]) == (8, 4) else body
    return jax.shard_map(
        step,
        mesh=mesh,
        in_specs=(
            P("dp", "tensor", None),
            P("dp", None),
            P(None, "dp", "tensor"),
            P("tensor", "dp"),
            P("dp", "tensor"),
            P("tensor", "dp"),
            P(None, "dp"),
            P("dp", "tensor", None),
        ),
        out_specs=(
            P("dp", "tensor", None),
            P("dp", "tensor", None),
            P(None, "dp", "tensor"),
            P("tensor", "dp"),
            P("dp", "tensor"),
            P("tensor", "dp"),
            P(None, "dp"),
        ),
        check_vma=False,
    )
```

```python
import jax
import jax.numpy as jnp
from jax import lax
from jax.experimental import pallas as pl
from jax.experimental.pallas import tpu as pltpu
from jax.sharding import PartitionSpec as P

D = 1024
FF = 4096
HD = 64


NORM_EPS = 1e-06
SQRT_HALF = 0.7071067811865476
INV_ROOT_TAU = 0.3989422804014327
MASKED = -1e30


def gelu_value(pre_act):
    return 0.5 * pre_act * (1.0 + lax.erf(pre_act * SQRT_HALF))


def gelu_slope(pre_act):
    return 0.5 * (1.0 + lax.erf(pre_act * SQRT_HALF)) + pre_act * INV_ROOT_TAU * jnp.exp(
        -0.5 * pre_act * pre_act
    )


def norm_forward(summed, gain, shift):
    centred = summed - jnp.mean(summed, axis=-1, keepdims=True)
    inverse = lax.rsqrt(jnp.mean(centred * centred, axis=-1, keepdims=True) + NORM_EPS)
    normed = centred * inverse
    return (normed * gain + shift, normed, inverse)


def norm_backward(normed, inverse, grad_normed):
    first_mean = jnp.mean(grad_normed, axis=-1, keepdims=True)
    second_mean = jnp.mean(grad_normed * normed, axis=-1, keepdims=True)
    return inverse * (grad_normed - first_mean - normed * second_mean)


def attention_scores(query_heads, key_heads, segments):
    same_doc = segments[:, None] == segments[None, :]
    scores = jnp.einsum(
        "qhe,khe->hqk", query_heads, key_heads, preferred_element_type=jnp.float32
    ) * HD ** (-0.5)
    return jnp.where(same_doc[None], scores, MASKED)


def collect(w_qkv, w_out, w_up, w_down, vectors):
    return (
        lax.all_gather(w_qkv, "dp", axis=1, tiled=True),
        lax.all_gather(w_out, "dp", axis=1, tiled=True),
        lax.all_gather(w_up, "dp", axis=0, tiled=True),
        lax.all_gather(w_down, "dp", axis=1, tiled=True),
        lax.all_gather(vectors, "dp", axis=1, tiled=True),
    )


def share(gradients):
    return (
        lax.psum_scatter(
            gradients[0].astype(jnp.bfloat16), "dp", scatter_dimension=1, tiled=True
        ).astype(jnp.float32),
        lax.psum_scatter(
            gradients[1].astype(jnp.bfloat16), "dp", scatter_dimension=1, tiled=True
        ).astype(jnp.float32),
        lax.psum_scatter(
            gradients[2].astype(jnp.bfloat16), "dp", scatter_dimension=0, tiled=True
        ).astype(jnp.float32),
        lax.psum_scatter(
            gradients[3].astype(jnp.bfloat16), "dp", scatter_dimension=1, tiled=True
        ).astype(jnp.float32),
        lax.psum_scatter(
            gradients[4].astype(jnp.bfloat16), "dp", scatter_dimension=1, tiled=True
        ).astype(jnp.float32),
    )


def body(tokens, segment_ids, w_qkv, w_out, w_up, w_down, vectors, cotangent):
    tensor_rank = lax.axis_index("tensor")
    local_cols = w_qkv.shape[2]
    head_count = local_cols // HD
    hidden = w_up.shape[1]
    col_start = tensor_rank * local_cols
    ffn_start = tensor_rank * hidden

    def forward(weights, tok_block, segments):
        qkv_w, out_w, up_w, down_w, vec_b = weights
        vec_f32 = vec_b.astype(jnp.float32)
        whole = lax.all_gather(tok_block, "tensor", axis=0, tiled=True)
        seq_len = whole.shape[0]
        projected = jnp.einsum("sd,tdc->tsc", whole, qkv_w, preferred_element_type=jnp.float32)
        bias_q = lax.dynamic_slice_in_dim(vec_f32[0], col_start, local_cols)
        bias_v = lax.dynamic_slice_in_dim(vec_f32[1], col_start, local_cols)
        query_heads = (projected[0] + bias_q).astype(jnp.bfloat16).reshape(seq_len, head_count, HD)
        key_heads = projected[1].astype(jnp.bfloat16).reshape(seq_len, head_count, HD)
        value_heads = (projected[2] + bias_v).astype(jnp.bfloat16).reshape(seq_len, head_count, HD)
        scores = attention_scores(query_heads, key_heads, segments)
        row_top = jnp.max(scores, axis=-1, keepdims=True)
        log_total = row_top + jnp.log(jnp.sum(jnp.exp(scores - row_top), axis=-1, keepdims=True))
        attn_probs = jnp.exp(scores - log_total).astype(jnp.bfloat16)
        context = jnp.einsum(
            "hqk,khe->qhe", attn_probs, value_heads, preferred_element_type=jnp.float32
        )
        context = context.reshape(seq_len, local_cols).astype(jnp.bfloat16)
        piece = context
        attn_mixed = lax.psum_scatter(
            jnp.dot(piece, out_w, preferred_element_type=jnp.float32).astype(jnp.bfloat16),
            "tensor",
            scatter_dimension=0,
            tiled=True,
        ).astype(jnp.float32)
        summed_one = tok_block.astype(jnp.float32) + attn_mixed + vec_f32[2]
        normed_out, normed_one, inverse_one = norm_forward(summed_one, vec_f32[3], vec_f32[4])
        normed_b = normed_out.astype(jnp.bfloat16)
        normed_whole = lax.all_gather(normed_b, "tensor", axis=0, tiled=True)
        bias_up = lax.dynamic_slice_in_dim(vec_f32[8:12].reshape(FF), ffn_start, hidden)
        pre_act = jnp.dot(normed_whole, up_w, preferred_element_type=jnp.float32) + bias_up
        activated = gelu_value(pre_act).astype(jnp.bfloat16)
        piece = activated
        summed_two = (
            normed_out
            + lax.psum_scatter(
                jnp.dot(piece, down_w, preferred_element_type=jnp.float32).astype(jnp.bfloat16),
                "tensor",
                scatter_dimension=0,
                tiled=True,
            ).astype(jnp.float32)
            + vec_f32[5]
        )
        final, normed_two, inverse_two = norm_forward(summed_two, vec_f32[6], vec_f32[7])
        saved = (
            whole,
            query_heads,
            key_heads,
            value_heads,
            log_total,
            context,
            normed_one,
            inverse_one,
            normed_whole,
            pre_act,
            activated,
            normed_two,
            inverse_two,
        )
        return (final.astype(jnp.bfloat16), saved)

    def backward(weights, saved, segments, grad_block):
        qkv_w, out_w, up_w, down_w, vec_b = weights
        vec_f32 = vec_b.astype(jnp.float32)
        (
            whole,
            query_heads,
            key_heads,
            value_heads,
            log_total,
            context,
            normed_one,
            inverse_one,
            normed_whole,
            pre_act,
            activated,
            normed_two,
            inverse_two,
        ) = saved
        seq_len = whole.shape[0]
        grad_final = grad_block.astype(jnp.float32)
        g_gain2 = jnp.sum(grad_final * normed_two, axis=0)
        g_shift2 = jnp.sum(grad_final, axis=0)
        grad_two = norm_backward(normed_two, inverse_two, grad_final * vec_f32[6])
        grad_two_b = grad_two.astype(jnp.bfloat16)
        g_bdown = jnp.sum(grad_two, axis=0)
        grad_two_whole = lax.all_gather(grad_two_b, "tensor", axis=0, tiled=True)
        g_down = jnp.dot(activated.T, grad_two_whole, preferred_element_type=jnp.float32)
        grad_pre = jnp.dot(
            grad_two_whole, down_w.T, preferred_element_type=jnp.float32
        ) * gelu_slope(pre_act)
        grad_pre_b = grad_pre.astype(jnp.bfloat16)
        g_bup = jnp.sum(grad_pre, axis=0)
        g_up = jnp.dot(normed_whole.T, grad_pre_b, preferred_element_type=jnp.float32)
        piece = grad_pre_b
        grad_one_in = grad_two + lax.psum_scatter(
            jnp.dot(piece, up_w.T, preferred_element_type=jnp.float32).astype(jnp.bfloat16),
            "tensor",
            scatter_dimension=0,
            tiled=True,
        ).astype(jnp.float32)
        g_gain1 = jnp.sum(grad_one_in * normed_one, axis=0)
        g_shift1 = jnp.sum(grad_one_in, axis=0)
        grad_one = norm_backward(normed_one, inverse_one, grad_one_in * vec_f32[3])
        grad_one_b = grad_one.astype(jnp.bfloat16)
        g_bout = jnp.sum(grad_one, axis=0)
        grad_one_whole = lax.all_gather(grad_one_b, "tensor", axis=0, tiled=True)
        g_out = jnp.dot(context.T, grad_one_whole, preferred_element_type=jnp.float32)
        grad_context = jnp.dot(grad_one_whole, out_w.T, preferred_element_type=jnp.float32).astype(
            jnp.bfloat16
        )
        grad_context = grad_context.reshape(seq_len, head_count, HD)
        scores = attention_scores(query_heads, key_heads, segments)
        attn_exact = jnp.exp(scores - log_total)
        attn_probs = attn_exact.astype(jnp.bfloat16)
        grad_probs = jnp.einsum(
            "qhe,khe->hqk", grad_context, value_heads, preferred_element_type=jnp.float32
        )
        row_dot = jnp.sum(attn_exact * grad_probs, axis=-1, keepdims=True)
        grad_scores = (attn_exact * (grad_probs - row_dot) * HD ** (-0.5)).astype(jnp.bfloat16)
        grad_value = jnp.einsum(
            "hqk,qhe->khe", attn_probs, grad_context, preferred_element_type=jnp.float32
        )
        grad_value = grad_value.reshape(seq_len, local_cols)
        grad_query = jnp.einsum(
            "hqk,khe->qhe", grad_scores, key_heads, preferred_element_type=jnp.float32
        )
        grad_query = grad_query.reshape(seq_len, local_cols)
        grad_key = jnp.einsum(
            "hqk,qhe->khe", grad_scores, query_heads, preferred_element_type=jnp.float32
        )
        grad_key = grad_key.reshape(seq_len, local_cols)
        grad_qkv = jnp.stack([grad_query, grad_key, grad_value]).astype(jnp.bfloat16)
        g_qkv = jnp.einsum("sd,tsc->tdc", whole, grad_qkv, preferred_element_type=jnp.float32)
        piece = grad_qkv
        grad_input = grad_one + lax.psum_scatter(
            jnp.einsum("tsc,tdc->sd", piece, qkv_w, preferred_element_type=jnp.float32).astype(
                jnp.bfloat16
            ),
            "tensor",
            scatter_dimension=0,
            tiled=True,
        ).astype(jnp.float32)
        zero_row = jnp.zeros((D,), jnp.float32)
        row_q = lax.dynamic_update_slice_in_dim(zero_row, jnp.sum(grad_query, axis=0), col_start, 0)
        row_v = lax.dynamic_update_slice_in_dim(zero_row, jnp.sum(grad_value, axis=0), col_start, 0)
        up_rows = lax.dynamic_update_slice_in_dim(
            jnp.zeros((FF,), jnp.float32), g_bup, ffn_start, 0
        ).reshape(4, D)
        first_rows = jnp.stack(
            [row_q, row_v, g_bout, g_gain1, g_shift1, g_bdown, g_gain2, g_shift2]
        )
        g_vec = jnp.concatenate([first_rows, up_rows], axis=0)
        return ((g_qkv, g_out, g_up, g_down, g_vec), grad_input)

    def one_batch(carried, batch_item):
        tok_block, segments, grad_block = batch_item
        forward_w = collect(w_qkv, w_out, w_up, w_down, vectors)
        final_b, saved = forward(forward_w, tok_block, segments)
        second = collect(w_qkv, w_out, w_up, w_down, vectors)
        gradients, grad_input = backward(second, saved, segments, grad_block)
        updated = jax.tree.map(jnp.add, carried, gradients)
        return (updated, (final_b, grad_input))

    initial = (
        jnp.zeros((3, D, local_cols), jnp.float32),
        jnp.zeros((local_cols, D), jnp.float32),
        jnp.zeros((D, hidden), jnp.float32),
        jnp.zeros((hidden, D), jnp.float32),
        jnp.zeros((12, D), jnp.float32),
    )
    carried, stacked = lax.scan(one_batch, initial, (tokens, segment_ids, cotangent))
    totals = share(carried)
    vector_grads = lax.psum(totals[4], "tensor")
    return (stacked[0], stacked[1], totals[0], totals[1], totals[2], totals[3], vector_grads)


Y_TOK, Y_COT, Y_OUT, Y_GTOK = range(4)
X_MIX, X_DH, X_DX, X_TOK, X_NORM, X_DA2, X_DA1 = range(7)
W_Q, W_K, W_V, W_OUT, W_UP, W_DOWN, W_REST, W_VEC = range(8)
W_KINDS = 8
Y_FIRST = (W_REST,)
DIRECT = (W_VEC,)
FAR_FIRST = ()
U_DA, U_DB, U_UA, U_UB, U_OUT, U_V, U_K, U_Q = range(8)
Z_FIRST = (U_DA,)
DA_ROWS = 640
R_BQ, R_BV, R_BO, R_G1, R_C1, R_BD, R_G2, R_C2, R_BU = range(9)
ZS = 4
SEQ = 512
ROWS = 256
CHUNK = 128
TILE = 32
COLS = 512
HID = 2048
WINDOW = 384
BF = jnp.bfloat16
F32 = jnp.float32
MESH = pl.DeviceIdType.MESH


def span(index, size):
    return pl.ds(pl.multiple_of(index * size, size), size)


def contract(a, b, a_dim, b_dim):
    return lax.dot_general(a, b, (((a_dim,), (b_dim,)), ((), ())), preferred_element_type=F32)


def fold_rows(value):
    return jnp.sum(value.reshape(value.shape[0] // 8, 8, value.shape[1]), axis=0)


def layer_kernel(
    tok, seg, wq, wo, wu, wd, vec, cot,
    out, gtok, gq, go, gu, gd, gv,
    w_qkv, w_out, w_up, w_down, w_vec, vf,
    g_da, g_db, g_up, g_out, g_qkv,
    c_da, c_db, c_up, c_out, c_qkv,
    y_da, y_db, y_up, y_out, y_qkv,
    z_da, z_db, z_up, z_out, z_qkv,
    h_da, h_db, h_up, h_out, h_qkv,
    o_qkv, o_out, o_up, o_down,
    xw, qkv, ctx, prob, bias, hw, act, slope, aw, a1w, dctx,
    own, n1, da, inv1, recv, stage, cotb, outb, gts, gtr, gtf,
    acc, vg, vgx, vgc, vgy, vgz, gvb, acc_k, acc_v,
    done, wrz, wry, wrc, wrd, fs, fr, xs, xr, yr,
    grc, gry, grz, vs, vr, ls, os,
):
    dp = lax.axis_index("dp")
    tensor = lax.axis_index("tensor")
    z, c = dp // 2, dp % 2
    y, x = tensor // 2, tensor % 2
    at_x = {"dp": dp, "tensor": y * 2 + (1 - x)}
    at_y = {"dp": dp, "tensor": (1 - y) * 2 + x}
    at_c = {"dp": z * 2 + (1 - c), "tensor": tensor}

    def remote(src, dst, send, recv_sem, where):
        return pltpu.make_async_remote_copy(
            src_ref=src, dst_ref=dst, send_sem=send, recv_sem=recv_sem,
            device_id=where, device_id_type=MESH,
        )

    barrier = pltpu.get_barrier_semaphore()
    for where in [at_x, at_y, at_c] + [{"dp": lax.rem(z + k, ZS) * 2 + c, "tensor": tensor} for k in range(1, ZS)]:
        pl.semaphore_signal(barrier, inc=1, device_id=where, device_id_type=MESH)
    pl.semaphore_wait(barrier, 6)

    sent = []

    quiet = []

    def go_on(copy):
        copy.start()
        if not quiet:
            sent.append(copy)

    args = [wq.at[0], wq.at[1], wq.at[2], wo, wu, wd.at[0:512], wd.at[512:1024], vec]
    edge = jnp.logical_or(z == 0, z == ZS - 1)
    middle = jnp.logical_not(edge)
    later = []

    def z_device(where):
        return {"dp": where * 2 + c, "tensor": tensor}

    def go_if(condition, copy):
        @pl.when(condition)
        def _():
            copy.start()
        if not quiet:
            later.append((condition, copy))

    def place(m, yy, d):
        if m <= W_V:
            return w_qkv.at[m, span(d, 128), span(yy, 256)]
        if m == W_OUT:
            return w_out.at[span(yy, 256), span(d, 128)]
        if m == W_UP:
            return w_up.at[span(d, 128), span(yy, 1024)]
        if m == W_DOWN or m == W_REST:
            return w_down.at[span(yy * 2 + m - W_DOWN, 512), span(d, 128)]
        return w_vec.at[d]

    even = lax.rem(z, 2) == 0
    near_first = (jnp.where(even, 3, 1), 2, jnp.where(even, 1, 3))

    def from_z(k):
        return lax.rem(z + ZS - k, ZS)

    def z_slot(m, r):
        return 24 if r else m * 3

    def column(r):
        return y if r == 0 else 1 - y

    def z_send(m, r):
        source = args[m] if r == 0 else place(m, 1 - y, dp)
        steps = ((1, z != ZS - 1), (3, z != 0), (2, None))
        for k, there in (steps[2:] + steps[:2] if m in FAR_FIRST else steps):
            there = None if m in DIRECT else there
            copy = remote(
                source, place(m, column(r), dp), done.at[0], wrz.at[z_slot(m, r) + k - 1],
                z_device(lax.rem(z + k, ZS)),
            )
            if there is None:
                go_on(copy)
            else:
                go_if(there, copy)

    def z_serve(m, r, step, keep=False):
        z_take(m, r, step, keep)
        z_note(m, r, step)

    def z_serve_split(m, r, step, early, late):
        def first():
            @pl.when(early)
            def _():
                z_take(m, r, step)

        def second():
            @pl.when(late)
            def _():
                z_take(m, r, step)
            z_note(m, r, step)
        return first, second

    def z_parts(m, r, step):
        k = near_first[step]
        here = place(m, column(r), from_z(k) * 2 + c)
        slot = jnp.where(z == 1, 0, 2)
        hand_on = None
        if step == 1 and m not in DIRECT:
            hand_on = remote(
                here, here, done.at[0], wrz.at[z_slot(m, r) + slot], z_device(jnp.where(z == 1, 0, 3)),
            )
        over_y = None
        if r == 0 and m not in Y_FIRST and m != W_VEC:
            over_y = remote(here, here, done.at[0], wry.at[m, from_z(k)], at_y)
        return k, here, hand_on, over_y

    def z_over(m, step):
        z_parts(m, 0, step)[3].start()

    def z_take(m, r, step, keep=False):
        k, here, hand_on, over_y = z_parts(m, r, step)
        remote(here, here, done.at[0], wrz.at[z_slot(m, r) + k - 1], at_x).wait_recv()
        if hand_on is not None:
            @pl.when(middle)
            def _():
                hand_on.start()
        if over_y is not None and not keep:
            over_y.start()
        c_send(m, here, step + 1)

    def z_note(m, r, step):
        _, _, hand_on, over_y = z_parts(m, r, step)
        if hand_on is not None:
            later.append((middle, hand_on))
        if over_y is not None:
            sent.append(over_y)

    def y_send(m):
        go_on(remote(args[m], place(m, y, dp), done.at[0], wry.at[m, z], at_y))

    def source_of(step):
        return z if step == 0 else from_z(near_first[step - 1])

    def y_serve(m, step):
        zz = source_of(step)
        here = place(m, 1 - y, zz * 2 + c)
        remote(here, here, done.at[0], wry.at[m, zz], at_y).wait_recv()
        c_send(m, here, step)

    def c_send(m, source, step, dest=None):
        dest = source if dest is None else dest
        into = wrd.at[m - W_DOWN, step] if m in (W_DOWN, W_REST) else wrc.at[m]
        remote(source, dest, done.at[0], into, at_c).start()

    def own_send(m):
        c_send(m, args[m], 0, place(m, y, dp))
        pltpu.make_async_copy(args[m], place(m, y, dp), ls.at[m]).start()

    def half_of(m):
        if m <= W_V:
            return w_qkv.at[m, :, 0:256]
        return (
            w_out.at[0:256], w_up.at[:, 0:1024], w_down.at[0:512], w_down.at[0:512], w_vec.at[0:4]
        )[m - W_OUT]

    def wait_down(step):
        for m in (W_DOWN, W_REST):
            if step == 0:
                pltpu.make_async_copy(args[m], place(m, y, dp), ls.at[m]).wait()
            two = w_down.at[0:1024, 0:128]
            remote(two, two, done.at[0], wrd.at[m - W_DOWN, step], at_c).wait_recv()

    def wait_weight(m):
        pltpu.make_async_copy(args[m], place(m, y, dp), ls.at[m]).wait()
        remote(half_of(m), half_of(m), done.at[0], wrc.at[m], at_c).wait_recv()

    def x_copy(kind, j, src, dst):
        return remote(src, dst, xs.at[kind, j] if kind <= X_DX else done.at[0], xr.at[kind, j], at_x)

    def tok_rows(xx, yy):
        return pl.ds(pl.multiple_of(xx * ROWS + yy * CHUNK, CHUNK), CHUNK)

    for m in (W_Q, W_K, W_V):
        y_send(m)
        z_send(m, 0)
    go_on(remote(tok.at[1 - y], xw.at[tok_rows(x, y)], done.at[0], yr.at[Y_TOK], at_y))
    go_on(x_copy(X_TOK, 0, tok.at[y], xw.at[tok_rows(x, y)]))
    z_send(W_VEC, 0)
    for m in range(W_KINDS):
        own_send(m)
    local_x = pltpu.make_async_copy(tok.at[y], xw.at[tok_rows(x, y)], ls.at[8])
    local_x.start()
    local_cot = pltpu.make_async_copy(cot.at[y], cotb.at[span(y, CHUNK)], ls.at[9])
    local_cot.start()

    seg_row = seg[pl.ds(y, 1), :].astype(F32)
    blocks = [(p % 2) * 2 + p // 2 for p in range(4)]
    across = [jnp.broadcast_to(seg_row[:, n * 128:(n + 1) * 128], (128, 128)) for n in blocks]
    down = [b.T for b in across]
    for t in range(2):
        for i, q in enumerate((t, t + 2)):
            for j in range(3):
                same = down[q] == across[t + j]
                bias[t, i * 128:(i + 1) * 128, j * 128:(j + 1) * 128] = jnp.where(same, 0.0, MASKED)
    acc[...] = jnp.zeros_like(acc)
    vg[...] = jnp.zeros_like(vg)

    for step in range(2):
        for m in (W_Q, W_K, W_V):
            z_serve(m, 0, step)
    z_send(W_OUT, 0)
    y_tok_here = xw.at[tok_rows(x, 1 - y)]
    remote(tok.at[1 - y], y_tok_here, done.at[0], yr.at[Y_TOK], at_y).wait_recv()
    go_on(x_copy(X_TOK, 1, y_tok_here, y_tok_here))
    for m in (W_Q, W_K, W_V):
        z_serve(m, 0, 2)
    y_send(W_OUT)
    z_serve(W_OUT, 0, 0)
    z_serve(W_OUT, 0, 1)
    z_send(W_UP, 0)
    for step in range(3):
        z_serve(W_VEC, 0, step)
    z_serve(W_OUT, 0, 2)
    y_send(W_UP)
    y_send(W_REST)
    for step in range(4):
        for m in (W_Q, W_K, W_V):
            y_serve(m, step)
    wait_weight(W_VEC)
    for d in range(8):
        vf[0:12, d * 128:(d + 1) * 128] = w_vec[d].astype(F32)
    local_x.wait()
    for j, yy in ((0, y), (1, 1 - y)):
        there = xw.at[tok_rows(1 - x, yy)]
        x_copy(X_TOK, j, there, there).wait_recv()
    for m in (W_Q, W_K, W_V):
        wait_weight(m)

    def head_bias(row):
        parts = [vf[row:row + 1, pl.ds(pl.multiple_of(yy * 512 + x * 256, 256), 256)] for yy in range(2)]
        return jnp.concatenate(parts, axis=1)

    for i in range(3):
        value = contract(xw[...], w_qkv[i], 1, 0)
        if i == 0:
            value = (value + head_bias(0)).astype(BF) * BF(HD ** -0.5)
        elif i == 2:
            value = value + head_bias(1)
        qkv[i] = value.astype(BF)

    low_half = lax.broadcasted_iota(jnp.int32, (1, 128), 1) < HD
    halves = (low_half, jnp.logical_not(low_half))
    none = jnp.zeros((), BF)

    def two_blocks(ref, t, lanes):
        return jnp.concatenate([ref[span(t, 128), lanes], ref[span(t + 2, 128), lanes]], axis=0)

    def attend(pair, carry):
        lanes = span(pair, 128)
        for t in range(2):
            keys = pl.ds(t * 128, WINDOW)
            query = two_blocks(qkv.at[0], t, lanes)
            key, value = qkv[1, keys, lanes], qkv[2, keys, lanes]
            total = jnp.zeros((ROWS, 128), F32)
            for h, half in enumerate(halves):
                scores = contract(jnp.where(half, query, none), key, 1, 1) + bias[t]
                top = jnp.max(scores, axis=1, keepdims=True)
                weight = jnp.exp(scores - top)
                share_of = 1.0 / jnp.sum(weight, axis=1, keepdims=True)
                weight = (weight * share_of).astype(BF)
                prob[pair * 4 + t * 2 + h] = weight
                total = total + contract(weight, jnp.where(half, value, none), 1, 0)
            total = total.astype(BF)
            ctx[t * 128:t * 128 + 128, lanes] = total[:128]
            ctx[t * 128 + 256:t * 128 + 384, lanes] = total[128:]
        return carry

    z_serve(W_UP, 0, 0)
    lax.fori_loop(0, 2, attend, 0)
    for step in range(4):
        y_serve(W_OUT, step)
    lax.fori_loop(2, 4, attend, 0)
    up_early, up_late = z_serve_split(W_UP, 0, 1, middle, edge)
    up_early()
    z_send(W_DOWN, 0)

    def rows_of(s):
        mine = jnp.where(s < 2, x, 1 - x)
        return pl.ds(pl.multiple_of(mine * ROWS + lax.rem(s, 2) * CHUNK, CHUNK), CHUNK)

    def x_sum(kind, j):
        return x_copy(kind, j, stage.at[span(j, CHUNK)], recv.at[span(j, CHUNK)])

    def x_rows(kind, j, buf):
        here = buf.at[pl.ds(pl.multiple_of(x * ROWS + j * CHUNK, CHUNK), CHUNK)]
        return x_copy(kind, j, here, here)

    def hand_over(kind, before, s, value):
        @pl.when(s < 2)
        def _():
            own[span(s, CHUNK), :] = value

        @pl.when(s >= 2)
        def _():
            if before is not None:
                x_sum(before, s - 2).wait_send()
            stage[span(s - 2, CHUNK), :] = value.astype(BF)
            x_sum(kind, s - 2).start()

    wait_weight(W_OUT)

    def mix(i, carry):
        s = lax.rem(i + 2, 4)
        hand_over(X_MIX, None, s, contract(ctx[rows_of(s), :], w_out[...], 1, 0))
        return carry

    lax.fori_loop(0, 4, mix, 0)
    up_late()
    z_serve(W_UP, 0, 2)
    y_serve(W_REST, 0)
    z_send(W_REST, 0)
    z_send(W_REST, 1)
    y_serve(W_UP, 0)
    z_serve(W_DOWN, 0, 0, keep=True)
    z_serve(W_DOWN, 0, 1, keep=True)

    def row_of(row):
        return vf[row:row + 1, :]

    def normed(value):
        centred = value - jnp.mean(value, axis=1, keepdims=True)
        inverse = lax.rsqrt(jnp.mean(centred * centred, axis=1, keepdims=True) + NORM_EPS)
        return centred * inverse, inverse

    def norm_back(normal, inverse, grad):
        first = jnp.mean(grad, axis=1, keepdims=True)
        second = jnp.mean(grad * normal, axis=1, keepdims=True)
        return inverse * (grad - first - normal * second)

    def tiles(j, body):
        def step(i, carry):
            body(pl.ds(pl.multiple_of(j * CHUNK + i * TILE, TILE), TILE),
                 pl.ds(pl.multiple_of(x * ROWS + j * CHUNK + i * TILE, TILE), TILE))
            return carry
        lax.fori_loop(0, CHUNK // TILE, step, 0)

    def first_norm(r, g):
        summed = xw[g, :].astype(F32) + own[r, :] + recv[r, :].astype(F32) + row_of(R_BO)
        normal, inverse = normed(summed)
        n1[r, :] = normal
        inv1[r, :] = jnp.broadcast_to(inverse, (TILE, 128))
        hw[g, :] = (normal * row_of(R_G1) + row_of(R_C1)).astype(BF)

    for j in range(2):
        x_sum(X_MIX, j).wait_recv()
        tiles(j, first_norm)
        x_rows(X_NORM, j, hw).start()

    y_send(W_DOWN)
    z_over(W_DOWN, 0)
    z_over(W_DOWN, 1)
    for step in range(1, 4):
        y_serve(W_UP, step)
    wait_weight(W_UP)

    def arrived(kind, s, buf):
        @pl.when(s >= 2)
        def _():
            there = buf.at[rows_of(s)]
            x_copy(kind, s - 2, there, there).wait_recv()

    def up_bias(n):
        return vf[pl.ds(8 + n * 2 + x, 1), :]

    def ffn_up(s, carry):
        rows = rows_of(s)
        arrived(X_NORM, s, hw)
        for n in range(2):
            pre = contract(hw[rows, :], w_up[:, n * 1024:(n + 1) * 1024], 1, 0) + up_bias(n)
            cdf = 0.5 * (1.0 + lax.erf(pre * SQRT_HALF))
            act[rows, n * 1024:(n + 1) * 1024] = (pre * cdf).astype(BF)
            slope[rows, n * 1024:(n + 1) * 1024] = (
                cdf + pre * INV_ROOT_TAU * jnp.exp(-0.5 * pre * pre)
            ).astype(BF)
        return carry

    lax.fori_loop(0, 2, ffn_up, 0)
    z_serve(W_DOWN, 0, 2)
    for r in range(2):
        z_serve(W_REST, r, 0)
        z_serve(W_REST, r, 1)
    y_serve(W_DOWN, 0)
    lax.fori_loop(2, 3, ffn_up, 0)
    y_serve(W_DOWN, 1)
    lax.fori_loop(3, 4, ffn_up, 0)
    y_serve(W_DOWN, 2)
    go_on(remote(cot.at[1 - y], cotb.at[span(y, CHUNK)], done.at[0], yr.at[Y_COT], at_y))

    def ffn_copy(step, j):
        cols = span(source_of(step), 256)
        return remote(
            stage.at[span(j, CHUNK), cols], recv.at[span(j, CHUNK), cols],
            fs.at[0], fr.at[j], at_x,
        )

    for j in range(2):
        x_sum(X_MIX, j).wait_send()
    for step in range(4):
        if step == 2:
            y_serve(W_DOWN, 3)
        if step == 3:
            z_serve(W_REST, 0, 2)
            z_serve(W_REST, 1, 2)
        wait_down(step)
        cols = span(source_of(step), 256)
        stage[:, cols] = contract(act[span(1 - x, ROWS), :], w_down[:, cols], 1, 0).astype(BF)
        for j in range(2):
            ffn_copy(step, j).start()
    for step in range(2):
        cols = span(step, 512)
        own[:, cols] = contract(act[span(x, ROWS), :], w_down[:, cols], 1, 0)

    def bump(row, value):
        acc[row] += fold_rows(value)

    def second_norm(r, g):
        h1 = n1[r, :] * row_of(R_G1) + row_of(R_C1)
        normal, inverse = normed(h1 + own[r, :] + recv[r, :].astype(F32) + row_of(R_BD))
        own[r, :] = normal
        grad = norm_back(normal, inverse, cotb[r, :].astype(F32) * row_of(R_G2))
        da[r, :] = grad
        aw[g, :] = grad.astype(BF)

    def second_rest(r, g):
        normal, dy = own[r, :], cotb[r, :].astype(F32)
        outb[r, :] = (normal * row_of(R_G2) + row_of(R_C2)).astype(BF)
        bump(R_G2, dy * normal)
        bump(R_C2, dy)
        bump(R_BD, da[r, :])

    local_cot.wait()
    cot_here = cotb.at[span(1 - y, CHUNK)]
    remote(cot.at[1 - y], cot_here, done.at[0], yr.at[Y_COT], at_y).wait_recv()
    for j in range(2):
        half = recv.at[span(j, CHUNK)]
        remote(half, half, fs.at[0], fr.at[j], at_x).wait_recv()
        tiles(j, second_norm)
        x_rows(X_DA2, j, aw).start()
    for j in range(2):
        tiles(j, second_rest)
    out_here = pltpu.make_async_copy(outb.at[span(y, CHUNK)], out.at[y], os.at[0])
    out_here.start()
    go_on(remote(outb.at[span(1 - y, CHUNK)], out.at[y], done.at[0], yr.at[Y_OUT], at_y))

    def ffn_back(s, carry):
        rows = rows_of(s)
        arrived(X_DA2, s, aw)
        for n in range(2):
            cols = slice(n * 1024, (n + 1) * 1024)
            grad = contract(aw[rows, :], w_down[cols, :], 1, 1) * slope[rows, cols].astype(F32)
            bump(R_BU + n, grad)
            slope[rows, cols] = grad.astype(BF)
        hand_over(X_DH, None, s, contract(slope[rows, :], w_up[...], 1, 1))
        return carry

    remote(stage, stage, fs.at[0], fr.at[0], at_x).wait_send()
    lax.fori_loop(0, 4, ffn_back, 0)

    units = {
        U_DA: (g_da, c_da, y_da, z_da, h_da, o_down.at[0:DA_ROWS], gd.at[0:DA_ROWS]),
        U_DB: (g_db, c_db, y_db, z_db, h_db, o_down.at[DA_ROWS:1024], gd.at[DA_ROWS:1024]),
        U_OUT: (g_out, c_out, y_out, z_out, h_out, o_out, go),
    }
    for u, i in ((U_UA, 0), (U_UB, 1)):
        rows = slice(i * 64, (i + 1) * 64)
        units[u] = tuple(r.at[i] for r in (g_up, c_up, y_up, z_up, h_up)) + (o_up.at[rows], gu.at[rows])
    for u, i in ((U_Q, 0), (U_K, 1), (U_V, 2)):
        units[u] = tuple(r.at[i] for r in (g_qkv, c_qkv, y_qkv, z_qkv, h_qkv, o_qkv, gq))

    def piece_loop(rows, body):
        size = min(rows, CHUNK)

        def step(i, carry):
            body(span(i, size))
            return carry
        lax.fori_loop(0, rows // size, step, 0)

    def add_piece(g, yy, zz, other):
        def body(r):
            g[c, yy, zz, r, :] = (g[c, yy, zz, r, :].astype(F32) + other[r, :].astype(F32)).astype(BF)
        piece_loop(g.shape[3], body)

    def core_copy(u):
        g, rc = units[u][0], units[u][1]
        return remote(g.at[1 - c], rc, done.at[0], grc.at[u], at_c)

    def core_send(u):
        go_on(core_copy(u))

    def core_add(u, r):
        g, rc = units[u][0], units[u][1]
        for zz in range(ZS):
            add_piece(g, column(r), zz, rc.at[column(r), zz])

    def rs_y_copy(u):
        g, ry = units[u][0], units[u][2]
        source = g.at[c, 1 - y, pl.ds(z, 1)] if u in Z_FIRST else g.at[c, 1 - y]
        return remote(source, ry, done.at[0], gry.at[u], at_y)

    def rs_z_copy(u, r, k):
        g, rz = units[u][0], units[u][3]
        to = lax.rem(z + k, ZS)
        return remote(g.at[c, column(r), to], rz.at[r, k - 1], done.at[0], grz.at[(32 if r else u * 4) + k - 1], z_device(to))

    def rs_hand_on(u, r):
        g, rh = units[u][0], units[u][4]
        far = jnp.where(z == 0, ZS - 1, 0)
        return remote(g.at[c, column(r), far], rh.at[r], done.at[0], grz.at[(32 if r else u * 4) + 3], z_device(jnp.where(z == 0, 1, 2)))

    def z_hand_on(u, r):
        go_if(edge, rs_hand_on(u, r))

    def z_begin(u, r):
        go_if(z != ZS - 1, rs_z_copy(u, r, 1))
        go_if(z != 0, rs_z_copy(u, r, 3))
        go_if(edge, rs_z_copy(u, r, 2))

    def z_relay(u, r):
        g, rh = units[u][0], units[u][4]

        @pl.when(middle)
        def _():
            rs_hand_on(u, r).wait_recv()
            add_piece(g, column(r), lax.rem(z + 2, ZS), rh.at[r])
        go_if(middle, rs_z_copy(u, r, 2))

    def start(u):
        core_copy(u).wait_recv()
        core_add(u, 1)
        if u in Z_FIRST:
            z_hand_on(u, 1)
            core_add(u, 0)
            z_hand_on(u, 0)
            z_begin(u, 1)
            z_begin(u, 0)
        else:
            go_on(rs_y_copy(u))
            core_add(u, 0)

    def y_to_z(u):
        g, ry = units[u][0], units[u][2]
        rs_y_copy(u).wait_recv()
        for zz in range(ZS):
            add_piece(g, y, zz, ry.at[zz])
        z_hand_on(u, 0)
        z_begin(u, 0)

    def wait_z(u, r):
        rs_z_copy(u, r, 2).wait_recv()

        @pl.when(z != 0)
        def _():
            rs_z_copy(u, r, 1).wait_recv()

        @pl.when(z != ZS - 1)
        def _():
            rs_z_copy(u, r, 3).wait_recv()

    def z_total(u, r, rows):
        g, rz = units[u][0], units[u][3]
        value = g[c, column(r), z, rows, :].astype(F32)
        for k in range(ZS - 1):
            value = value + rz[r, k, rows, :].astype(F32)
        return value

    def z_to_y(u):
        g = units[u][0]
        wait_z(u, 1)

        def body(rows):
            g[c, 1 - y, z, rows, :] = z_total(u, 1, rows).astype(BF)
        piece_loop(g.shape[3], body)
        go_on(rs_y_copy(u))

    finals = []

    def finish(u):
        g, _, ry, _, _, o, dest = units[u]
        wait_z(u, 0)
        if u in Z_FIRST:
            rs_y_copy(u).wait_recv()

        def body(rows):
            value = z_total(u, 0, rows)
            if u in Z_FIRST:
                value = value + ry[0, rows, :].astype(F32)
            o[rows, :] = value
        piece_loop(g.shape[3], body)
        copy = pltpu.make_async_copy(o, dest, os.at[0])
        copy.start()
        finals.append(copy)

    for u in units:
        for r in range(2 if u in Z_FIRST else 1):
            for k, alone in ((1, z == 0), (3, z == ZS - 1)):
                @pl.when(alone)
                def _(u=u, r=r, k=k):
                    rz = units[u][3]
                    rz[r, k - 1] = jnp.zeros(rz.shape[2:], BF)

    def grad_down(u):
        g, first, count = (g_da, 0, DA_ROWS) if u == U_DA else (g_db, DA_ROWS, 1024 - DA_ROWS)

        def step(yy, carry):
            rows = pl.ds(pl.multiple_of(yy * 1024 + first, 128), count)
            value = contract(act[:, rows], aw[...], 0, 0).astype(BF)
            for d in range(8):
                g[d % 2, yy, d // 2] = value[:, d * 128:(d + 1) * 128]
            return carry

        lax.fori_loop(0, 2, step, 0)
        core_send(u)

    def grad_up():
        def step(index, carry):
            i, n = index // 2, index % 2
            value = contract(hw[:, span(i, 512)], slope[:, span(n, 1024)], 0, 0).astype(BF)
            for d in range(4):
                for part in range(2):
                    r = d * 128 + part * 64
                    g_up[part, d % 2, n, i * 2 + d // 2] = value[r:r + 64, :]
            return carry

        lax.fori_loop(0, 4, step, 0)
        core_send(U_UA)
        core_send(U_UB)

    quiet.append(True)

    @pl.when(c == 0)
    def _():
        grad_down(U_DB)
        start(U_DB)
        grad_down(U_DA)
        start(U_DA)
        grad_up()

    @pl.when(c == 1)
    def _():
        grad_down(U_DB)
        grad_down(U_DA)
        grad_up()
        start(U_DB)
        start(U_DA)

    quiet.clear()
    for u in (U_DB, U_DA, U_UA, U_UB):
        sent.append(core_copy(u))
    sent.append(rs_y_copy(U_DB))
    for r in (1, 0):
        later.append((edge, rs_hand_on(U_DA, r)))
        later.append((z != ZS - 1, rs_z_copy(U_DA, r, 1)))
        later.append((z != 0, rs_z_copy(U_DA, r, 3)))
        later.append((edge, rs_z_copy(U_DA, r, 2)))
    quiet.append(True)

    @pl.when(c == 0)
    def _():
        start(U_UA)
        start(U_UB)

    def back_norm(r, g):
        grad = da[r, :] + own[r, :] + recv[r, :].astype(F32)
        own[r, :] = grad
        grad = norm_back(n1[r, :], inv1[r, 0:1], grad * row_of(R_G1))
        da[r, :] = grad
        a1w[g, :] = grad.astype(BF)

    def back_rest(r, g):
        grad = own[r, :]
        bump(R_G1, grad * n1[r, :])
        bump(R_C1, grad)
        bump(R_BO, da[r, :])

    for j in range(2):
        x_sum(X_DH, j).wait_recv()
        tiles(j, back_norm)
        x_rows(X_DA1, j, a1w).start()

    @pl.when(c == 1)
    def _():
        start(U_UA)
        start(U_UB)

    quiet.clear()
    sent.append(rs_y_copy(U_UA))
    sent.append(rs_y_copy(U_UB))
    for j in range(2):
        tiles(j, back_rest)

    z_relay(U_DA, 1)
    z_relay(U_DA, 0)

    def ctx_back(s, carry):
        rows = rows_of(s)
        arrived(X_DA1, s, a1w)
        dctx[rows, :] = contract(a1w[rows, :], w_out[...], 1, 1).astype(BF)
        return carry

    lax.fori_loop(0, 2, ctx_back, 0)
    y_to_z(U_DB)
    lax.fori_loop(2, 4, ctx_back, 0)

    def attend_back(pair, carry):
        lanes = span(pair, 128)
        for t in range(2):
            keys = pl.ds(t * 128, WINDOW)
            query = two_blocks(qkv.at[0], t, lanes)
            key, value = qkv[1, keys, lanes], qkv[2, keys, lanes]
            grad = two_blocks(dctx, t, lanes)
            product = grad.astype(F32) * two_blocks(ctx, t, lanes).astype(F32)
            grad_q = jnp.zeros((ROWS, 128), F32)
            grad_k = jnp.zeros((WINDOW, 128), F32)
            grad_v = jnp.zeros((WINDOW, 128), F32)
            for h, half in enumerate(halves):
                grad_h = jnp.where(half, grad, none)
                weight = prob[pair * 4 + t * 2 + h]
                row_dot = jnp.sum(jnp.where(half, product, 0.0), axis=1, keepdims=True)
                score = (weight.astype(F32) * (contract(grad_h, value, 1, 1) - row_dot)).astype(BF)
                grad_q = grad_q + contract(score, jnp.where(half, key, none), 1, 0)
                grad_k = grad_k + contract(score, jnp.where(half, query, none), 0, 0)
                grad_v = grad_v + contract(weight, grad_h, 0, 0)
            grad_q = grad_q * (HD ** -0.5)
            acc[R_BQ, :, lanes] += fold_rows(grad_q)
            acc[R_BV, :, lanes] += fold_rows(grad_v)
            grad_q = grad_q.astype(BF)
            qkv[0, t * 128:t * 128 + 128, lanes] = grad_q[:128]
            qkv[0, t * 128 + 256:t * 128 + 384, lanes] = grad_q[128:]
            if t == 0:
                acc_k[0:WINDOW, :] = grad_k
                acc_v[0:WINDOW, :] = grad_v
                acc_k[WINDOW:SEQ, :] = jnp.zeros((128, 128), F32)
                acc_v[WINDOW:SEQ, :] = jnp.zeros((128, 128), F32)
            else:
                for i, total, more in ((1, acc_k, grad_k), (2, acc_v, grad_v)):
                    qkv[i, 0:128, lanes] = total[0:128, :].astype(BF)
                    qkv[i, 128:SEQ, lanes] = (total[128:SEQ, :] + more).astype(BF)
        return carry

    def grad_out():
        value = contract(ctx[...], a1w[...], 0, 0).astype(BF)
        for d in range(8):
            for yy in range(2):
                g_out[d % 2, yy, d // 2] = value[yy * 256:(yy + 1) * 256, d * 128:(d + 1) * 128]

    grad_out()
    core_send(U_OUT)
    lax.fori_loop(0, 2, attend_back, 0)
    start(U_OUT)
    y_to_z(U_UA)
    lax.fori_loop(2, 4, attend_back, 0)

    for row in range(2, 8):
        line = jnp.sum(acc[row], axis=0, keepdims=True)
        for d in range(8):
            vg[d % 2, d // 2, row:row + 1, :] = line[:, d * 128:(d + 1) * 128]
    for n in range(2):
        line = jnp.sum(acc[R_BU + n], axis=0, keepdims=True)
        for d in range(8):
            vg[d % 2, d // 2, pl.ds(8 + n * 2 + x, 1), :] = line[:, d * 128:(d + 1) * 128]
    for row, source in ((0, R_BQ), (1, R_BV)):
        line = jnp.sum(acc[source], axis=0, keepdims=True)
        for yy in range(2):
            for half in range(2):
                vg[half, 2 * yy + x, row:row + 1, :] = (
                    line[:, yy * 256 + half * 128:yy * 256 + (half + 1) * 128]
                )
    vec_x = remote(vg, vgx, vs.at[0], vr.at[0], at_x)
    vec_c = remote(vg.at[1 - c], vgc, vs.at[1], vr.at[1], at_c)
    vec_y = remote(vg.at[c], vgy, vs.at[2], vr.at[2], at_y)

    def vec_z(k):
        to = lax.rem(z + k, ZS)
        return remote(vg.at[c, to], vgz.at[k - 1], done.at[0], vr.at[2 + k], z_device(to))

    vec_x.start()

    def input_back(i, carry):
        s = lax.rem(i + 2, 4)
        rows = rows_of(s)
        value = contract(qkv[0, rows, :], w_qkv[0], 1, 1)
        value = value + contract(qkv[1, rows, :], w_qkv[1], 1, 1)
        value = value + contract(qkv[2, rows, :], w_qkv[2], 1, 1)
        hand_over(X_DX, X_DH, s, value)
        return carry

    lax.fori_loop(0, 2, input_back, 0)
    vec_x.wait()
    vg[...] = vg[...] + vgx[...]
    vec_c.start()

    def grad_qkv(index, carry):
        kind, i = index // 2, index % 2
        value = contract(xw[:, span(i, 512)], qkv[kind], 0, 0).astype(BF)
        for d in range(4):
            for yy in range(2):
                g_qkv[kind, d % 2, yy, i * 2 + d // 2] = (
                    value[d * 128:(d + 1) * 128, yy * 256:(yy + 1) * 256]
                )
        return carry

    for kind, u in ((0, U_Q), (1, U_K), (2, U_V)):
        lax.fori_loop(kind * 2, kind * 2 + 2, grad_qkv, 0)
        core_send(u)
    z_relay(U_DB, 0)
    vec_c.wait()
    vg[c] = vg[c] + vgc[...]
    vec_y.start()
    for u in (U_Q, U_K, U_V):
        start(u)
    z_relay(U_UA, 0)
    y_to_z(U_UB)
    lax.fori_loop(2, 4, input_back, 0)
    y_to_z(U_OUT)
    z_to_y(U_DA)
    vec_y.wait()
    vg[c] = vg[c] + vgy[...]
    for k in range(1, ZS):
        go_on(vec_z(k))

    def last_sum(j, other):
        x_sum(X_DX, j).wait_recv()

        def body(r, g):
            value = da[r, :] + own[r, :] + recv[r, :].astype(F32)
            if other:
                gts[pl.ds(pl.multiple_of(r.start - j * CHUNK, TILE), TILE), :] = value.astype(BF)
            else:
                da[r, :] = value
        tiles(j, body)

    last_sum(1 - y, True)
    go_on(remote(gts, gtr, done.at[0], yr.at[Y_GTOK], at_y))
    last_sum(y, False)
    gtok_here = pltpu.make_async_copy(da.at[span(y, CHUNK)], gtok.at[y], os.at[0])
    gtok_here.start()
    y_to_z(U_Q)
    z_relay(U_UB, 0)
    y_to_z(U_K)
    z_relay(U_OUT, 0)
    y_to_z(U_V)
    for u in (U_Q, U_K, U_V):
        z_relay(u, 0)
    for k in range(1, ZS):
        vec_z(k).wait_recv()
    gvb[...] = vg[c, z] + vgz[0] + vgz[1] + vgz[2]
    vec_here = pltpu.make_async_copy(gvb.at[0:12], gv, os.at[0])
    vec_here.start()
    for u in (U_DA, U_DB, U_UA, U_UB):
        finish(u)
    remote(gts, gtr, done.at[0], yr.at[Y_GTOK], at_y).wait_recv()
    gtf[...] = gtr[...].astype(F32)
    gtok_there = pltpu.make_async_copy(gtf, gtok.at[1 - y], os.at[0])
    gtok_there.start()
    finish(U_OUT)
    finish(U_Q)
    finish(U_K)
    finish(U_V)
    remote(outb.at[span(1 - y, CHUNK)], out.at[1 - y], done.at[0], yr.at[Y_OUT], at_y).wait_recv()
    for kind, buf in ((X_NORM, hw), (X_DA2, aw), (X_DA1, a1w)):
        for j in range(2):
            x_rows(kind, j, buf).wait_send()
    for j in range(2):
        x_sum(X_DX, j).wait_send()
    for copy in sent:
        copy.wait_send()
    for condition, copy in later:
        @pl.when(condition)
        def _(copy=copy):
            copy.wait_send()
    for m in range(W_KINDS):
        remote(half_of(m), half_of(m), done.at[0], wrc.at[m], at_c).wait_send()
    for copy in finals + [out_here, gtok_here, gtok_there, vec_here]:
        copy.wait()


def settle_kernel(*refs):
    count = (len(refs) - 2) // 3
    sources, dests, held = refs[:count], refs[count:2 * count], refs[2 * count:3 * count]
    into, out_of = refs[3 * count:]
    first = [pltpu.make_async_copy(s, h, into.at[i]) for i, (s, h) in enumerate(zip(sources, held))]
    second = [pltpu.make_async_copy(h, d, out_of.at[i]) for i, (h, d) in enumerate(zip(held, dests))]
    for copy in first:
        copy.start()
    for before, after in zip(first, second):
        before.wait()
        after.start()
    for copy in second:
        copy.wait()


def settle(results):
    shapes = [jax.ShapeDtypeStruct(r.shape, r.dtype) for r in results]
    count = len(shapes)
    hbm = pl.BlockSpec(memory_space=pl.ANY)
    return pl.pallas_call(
        settle_kernel,
        out_shape=shapes,
        in_specs=[hbm] * count,
        out_specs=[hbm] * count,
        scratch_shapes=[pltpu.VMEM(r.shape, r.dtype) for r in shapes]
        + [pltpu.SemaphoreType.DMA((count,))] * 2,
    )(*results)


def layer(tokens, segment_ids, w_qkv, w_out, w_up, w_down, vectors, cotangent):
    vmem, dma = pltpu.VMEM, pltpu.SemaphoreType.DMA
    outs = (
        jax.ShapeDtypeStruct(tokens.shape, BF),
        jax.ShapeDtypeStruct(tokens.shape, F32),
        jax.ShapeDtypeStruct(w_qkv.shape, F32),
        jax.ShapeDtypeStruct(w_out.shape, F32),
        jax.ShapeDtypeStruct(w_up.shape, F32),
        jax.ShapeDtypeStruct(w_down.shape, F32),
        jax.ShapeDtypeStruct(vectors.shape, F32),
    )
    scratch = [
        vmem((3, D, COLS), BF), vmem((COLS, D), BF), vmem((D, HID), BF), vmem((HID, D), BF),
        vmem((8, 12, 128), BF), vmem((16, D), F32),
    ]
    part_da, part_db = (DA_ROWS, 128), (1024 - DA_ROWS, 128)
    half_up, piece_out, piece_qkv = (64, 1024), (256, 128), (128, 256)
    for shape in ((2, 2, 4), (2, 4)):
        scratch += [
            vmem(shape + part_da, BF), vmem(shape + part_db, BF), vmem((2,) + shape + half_up, BF),
            vmem(shape + piece_out, BF), vmem((3,) + shape + piece_qkv, BF),
        ]
    for y_shape, z_shape in (((4,), (1,)), ((1, 3), (2, 3)), ((1,), (2,))):
        scratch += [
            vmem(z_shape + part_da, BF), vmem(y_shape + part_db, BF),
            vmem((2,) + y_shape + half_up, BF), vmem(y_shape + piece_out, BF),
            vmem((3,) + y_shape + piece_qkv, BF),
        ]
    scratch += [vmem((3, 128, 256), F32), vmem((256, 128), F32), vmem((128, 1024), F32), vmem((1024, 128), F32)]
    scratch += [
        vmem((SEQ, D), BF), vmem((3, SEQ, COLS), BF), vmem((SEQ, COLS), BF),
        vmem((16, ROWS, WINDOW), BF), vmem((2, ROWS, WINDOW), F32), vmem((SEQ, D), BF),
        vmem((SEQ, HID), BF), vmem((SEQ, HID), BF), vmem((SEQ, D), BF), vmem((SEQ, D), BF),
        vmem((SEQ, COLS), BF),
        vmem((ROWS, D), F32), vmem((ROWS, D), F32), vmem((ROWS, D), F32), vmem((ROWS, 128), F32),
        vmem((ROWS, D), BF), vmem((ROWS, D), BF), vmem((ROWS, D), BF), vmem((ROWS, D), BF),
        vmem((CHUNK, D), BF), vmem((CHUNK, D), BF), vmem((CHUNK, D), F32),
        vmem((12, 8, D), F32),
        vmem((2, 4, 16, 128), F32), vmem((2, 4, 16, 128), F32), vmem((4, 16, 128), F32),
        vmem((4, 16, 128), F32), vmem((3, 16, 128), F32), vmem((16, 128), F32),
        vmem((SEQ, 128), F32), vmem((SEQ, 128), F32),
        dma((1,)), dma((27,)), dma((7, 4)), dma((8,)), dma((2, 4)), dma((1,)), dma((2,)),
        dma((3, 2)), dma((7, 2)), dma((4,)),
        dma((8,)), dma((8,)), dma((36,)),
        dma((3,)), dma((6,)), dma((10,)), dma((1,)),
    ]
    hbm = pl.BlockSpec(memory_space=pl.ANY)
    results = pl.pallas_call(
        layer_kernel,
        out_shape=outs,
        in_specs=[hbm, pl.BlockSpec(memory_space=pltpu.VMEM)] + [hbm] * 6,
        out_specs=[hbm] * 7,
        scratch_shapes=scratch,
        compiler_params=pltpu.CompilerParams(
            collective_id=0, has_side_effects=True, vmem_limit_bytes=67043328
        ),
    )(tokens, segment_ids, w_qkv, w_out, w_up, w_down, vectors, cotangent)
    return settle(results)


def solution(mesh):
    step = layer if (mesh.shape["dp"], mesh.shape["tensor"]) == (8, 4) else body
    return jax.shard_map(
        step,
        mesh=mesh,
        in_specs=(
            P("dp", "tensor", None),
            P("dp", None),
            P(None, "dp", "tensor"),
            P("tensor", "dp"),
            P("dp", "tensor"),
            P("tensor", "dp"),
            P(None, "dp"),
            P("dp", "tensor", None),
        ),
        out_specs=(
            P("dp", "tensor", None),
            P("dp", "tensor", None),
            P(None, "dp", "tensor"),
            P("tensor", "dp"),
            P("dp", "tensor"),
            P("tensor", "dp"),
            P(None, "dp"),
        ),
        check_vma=False,
    )
```

```python
import functools

import jax
import jax.numpy as jnp
from jax import lax
from jax.experimental import pallas as pl
from jax.experimental.pallas import tpu as pltpu
from jax.sharding import PartitionSpec as P

D = 1024
FF = 4096
HD = 64


NORM_EPS = 1e-06
SQRT_HALF = 0.7071067811865476
INV_ROOT_TAU = 0.3989422804014327
MASKED = -1e30


def gelu_value(pre_act):
    return 0.5 * pre_act * (1.0 + lax.erf(pre_act * SQRT_HALF))


def gelu_slope(pre_act):
    return 0.5 * (1.0 + lax.erf(pre_act * SQRT_HALF)) + pre_act * INV_ROOT_TAU * jnp.exp(
        -0.5 * pre_act * pre_act
    )


def norm_forward(summed, gain, shift):
    centred = summed - jnp.mean(summed, axis=-1, keepdims=True)
    inverse = lax.rsqrt(jnp.mean(centred * centred, axis=-1, keepdims=True) + NORM_EPS)
    normed = centred * inverse
    return (normed * gain + shift, normed, inverse)


def norm_backward(normed, inverse, grad_normed):
    first_mean = jnp.mean(grad_normed, axis=-1, keepdims=True)
    second_mean = jnp.mean(grad_normed * normed, axis=-1, keepdims=True)
    return inverse * (grad_normed - first_mean - normed * second_mean)


def attention_scores(query_heads, key_heads, segments):
    same_doc = segments[:, None] == segments[None, :]
    scores = jnp.einsum(
        "qhe,khe->hqk", query_heads, key_heads, preferred_element_type=jnp.float32
    ) * HD ** (-0.5)
    return jnp.where(same_doc[None], scores, MASKED)


def collect(w_qkv, w_out, w_up, w_down, vectors):
    return (
        lax.all_gather(w_qkv, "dp", axis=1, tiled=True),
        lax.all_gather(w_out, "dp", axis=1, tiled=True),
        lax.all_gather(w_up, "dp", axis=0, tiled=True),
        lax.all_gather(w_down, "dp", axis=1, tiled=True),
        lax.all_gather(vectors, "dp", axis=1, tiled=True),
    )


def share(gradients):
    return (
        lax.psum_scatter(
            gradients[0].astype(jnp.bfloat16), "dp", scatter_dimension=1, tiled=True
        ).astype(jnp.float32),
        lax.psum_scatter(
            gradients[1].astype(jnp.bfloat16), "dp", scatter_dimension=1, tiled=True
        ).astype(jnp.float32),
        lax.psum_scatter(
            gradients[2].astype(jnp.bfloat16), "dp", scatter_dimension=0, tiled=True
        ).astype(jnp.float32),
        lax.psum_scatter(
            gradients[3].astype(jnp.bfloat16), "dp", scatter_dimension=1, tiled=True
        ).astype(jnp.float32),
        lax.psum_scatter(
            gradients[4].astype(jnp.bfloat16), "dp", scatter_dimension=1, tiled=True
        ).astype(jnp.float32),
    )


def body(tokens, segment_ids, w_qkv, w_out, w_up, w_down, vectors, cotangent):
    tensor_rank = lax.axis_index("tensor")
    local_cols = w_qkv.shape[2]
    head_count = local_cols // HD
    hidden = w_up.shape[1]
    col_start = tensor_rank * local_cols
    ffn_start = tensor_rank * hidden

    def forward(weights, tok_block, segments):
        qkv_w, out_w, up_w, down_w, vec_b = weights
        vec_f32 = vec_b.astype(jnp.float32)
        whole = lax.all_gather(tok_block, "tensor", axis=0, tiled=True)
        seq_len = whole.shape[0]
        projected = jnp.einsum("sd,tdc->tsc", whole, qkv_w, preferred_element_type=jnp.float32)
        bias_q = lax.dynamic_slice_in_dim(vec_f32[0], col_start, local_cols)
        bias_v = lax.dynamic_slice_in_dim(vec_f32[1], col_start, local_cols)
        query_heads = (projected[0] + bias_q).astype(jnp.bfloat16).reshape(seq_len, head_count, HD)
        key_heads = projected[1].astype(jnp.bfloat16).reshape(seq_len, head_count, HD)
        value_heads = (projected[2] + bias_v).astype(jnp.bfloat16).reshape(seq_len, head_count, HD)
        scores = attention_scores(query_heads, key_heads, segments)
        row_top = jnp.max(scores, axis=-1, keepdims=True)
        log_total = row_top + jnp.log(jnp.sum(jnp.exp(scores - row_top), axis=-1, keepdims=True))
        attn_probs = jnp.exp(scores - log_total).astype(jnp.bfloat16)
        context = jnp.einsum(
            "hqk,khe->qhe", attn_probs, value_heads, preferred_element_type=jnp.float32
        )
        context = context.reshape(seq_len, local_cols).astype(jnp.bfloat16)
        piece = context
        attn_mixed = lax.psum_scatter(
            jnp.dot(piece, out_w, preferred_element_type=jnp.float32).astype(jnp.bfloat16),
            "tensor",
            scatter_dimension=0,
            tiled=True,
        ).astype(jnp.float32)
        summed_one = tok_block.astype(jnp.float32) + attn_mixed + vec_f32[2]
        normed_out, normed_one, inverse_one = norm_forward(summed_one, vec_f32[3], vec_f32[4])
        normed_b = normed_out.astype(jnp.bfloat16)
        normed_whole = lax.all_gather(normed_b, "tensor", axis=0, tiled=True)
        bias_up = lax.dynamic_slice_in_dim(vec_f32[8:12].reshape(FF), ffn_start, hidden)
        pre_act = jnp.dot(normed_whole, up_w, preferred_element_type=jnp.float32) + bias_up
        activated = gelu_value(pre_act).astype(jnp.bfloat16)
        piece = activated
        summed_two = (
            normed_out
            + lax.psum_scatter(
                jnp.dot(piece, down_w, preferred_element_type=jnp.float32).astype(jnp.bfloat16),
                "tensor",
                scatter_dimension=0,
                tiled=True,
            ).astype(jnp.float32)
            + vec_f32[5]
        )
        final, normed_two, inverse_two = norm_forward(summed_two, vec_f32[6], vec_f32[7])
        saved = (
            whole,
            query_heads,
            key_heads,
            value_heads,
            log_total,
            context,
            normed_one,
            inverse_one,
            normed_whole,
            pre_act,
            activated,
            normed_two,
            inverse_two,
        )
        return (final.astype(jnp.bfloat16), saved)

    def backward(weights, saved, segments, grad_block):
        qkv_w, out_w, up_w, down_w, vec_b = weights
        vec_f32 = vec_b.astype(jnp.float32)
        (
            whole,
            query_heads,
            key_heads,
            value_heads,
            log_total,
            context,
            normed_one,
            inverse_one,
            normed_whole,
            pre_act,
            activated,
            normed_two,
            inverse_two,
        ) = saved
        seq_len = whole.shape[0]
        grad_final = grad_block.astype(jnp.float32)
        g_gain2 = jnp.sum(grad_final * normed_two, axis=0)
        g_shift2 = jnp.sum(grad_final, axis=0)
        grad_two = norm_backward(normed_two, inverse_two, grad_final * vec_f32[6])
        grad_two_b = grad_two.astype(jnp.bfloat16)
        g_bdown = jnp.sum(grad_two, axis=0)
        grad_two_whole = lax.all_gather(grad_two_b, "tensor", axis=0, tiled=True)
        g_down = jnp.dot(activated.T, grad_two_whole, preferred_element_type=jnp.float32)
        grad_pre = jnp.dot(
            grad_two_whole, down_w.T, preferred_element_type=jnp.float32
        ) * gelu_slope(pre_act)
        grad_pre_b = grad_pre.astype(jnp.bfloat16)
        g_bup = jnp.sum(grad_pre, axis=0)
        g_up = jnp.dot(normed_whole.T, grad_pre_b, preferred_element_type=jnp.float32)
        piece = grad_pre_b
        grad_one_in = grad_two + lax.psum_scatter(
            jnp.dot(piece, up_w.T, preferred_element_type=jnp.float32).astype(jnp.bfloat16),
            "tensor",
            scatter_dimension=0,
            tiled=True,
        ).astype(jnp.float32)
        g_gain1 = jnp.sum(grad_one_in * normed_one, axis=0)
        g_shift1 = jnp.sum(grad_one_in, axis=0)
        grad_one = norm_backward(normed_one, inverse_one, grad_one_in * vec_f32[3])
        grad_one_b = grad_one.astype(jnp.bfloat16)
        g_bout = jnp.sum(grad_one, axis=0)
        grad_one_whole = lax.all_gather(grad_one_b, "tensor", axis=0, tiled=True)
        g_out = jnp.dot(context.T, grad_one_whole, preferred_element_type=jnp.float32)
        grad_context = jnp.dot(grad_one_whole, out_w.T, preferred_element_type=jnp.float32).astype(
            jnp.bfloat16
        )
        grad_context = grad_context.reshape(seq_len, head_count, HD)
        scores = attention_scores(query_heads, key_heads, segments)
        attn_exact = jnp.exp(scores - log_total)
        attn_probs = attn_exact.astype(jnp.bfloat16)
        grad_probs = jnp.einsum(
            "qhe,khe->hqk", grad_context, value_heads, preferred_element_type=jnp.float32
        )
        row_dot = jnp.sum(attn_exact * grad_probs, axis=-1, keepdims=True)
        grad_scores = (attn_exact * (grad_probs - row_dot) * HD ** (-0.5)).astype(jnp.bfloat16)
        grad_value = jnp.einsum(
            "hqk,qhe->khe", attn_probs, grad_context, preferred_element_type=jnp.float32
        )
        grad_value = grad_value.reshape(seq_len, local_cols)
        grad_query = jnp.einsum(
            "hqk,khe->qhe", grad_scores, key_heads, preferred_element_type=jnp.float32
        )
        grad_query = grad_query.reshape(seq_len, local_cols)
        grad_key = jnp.einsum(
            "hqk,qhe->khe", grad_scores, query_heads, preferred_element_type=jnp.float32
        )
        grad_key = grad_key.reshape(seq_len, local_cols)
        grad_qkv = jnp.stack([grad_query, grad_key, grad_value]).astype(jnp.bfloat16)
        g_qkv = jnp.einsum("sd,tsc->tdc", whole, grad_qkv, preferred_element_type=jnp.float32)
        piece = grad_qkv
        grad_input = grad_one + lax.psum_scatter(
            jnp.einsum("tsc,tdc->sd", piece, qkv_w, preferred_element_type=jnp.float32).astype(
                jnp.bfloat16
            ),
            "tensor",
            scatter_dimension=0,
            tiled=True,
        ).astype(jnp.float32)
        zero_row = jnp.zeros((D,), jnp.float32)
        row_q = lax.dynamic_update_slice_in_dim(zero_row, jnp.sum(grad_query, axis=0), col_start, 0)
        row_v = lax.dynamic_update_slice_in_dim(zero_row, jnp.sum(grad_value, axis=0), col_start, 0)
        up_rows = lax.dynamic_update_slice_in_dim(
            jnp.zeros((FF,), jnp.float32), g_bup, ffn_start, 0
        ).reshape(4, D)
        first_rows = jnp.stack(
            [row_q, row_v, g_bout, g_gain1, g_shift1, g_bdown, g_gain2, g_shift2]
        )
        g_vec = jnp.concatenate([first_rows, up_rows], axis=0)
        return ((g_qkv, g_out, g_up, g_down, g_vec), grad_input)

    def one_batch(carried, batch_item):
        tok_block, segments, grad_block = batch_item
        forward_w = collect(w_qkv, w_out, w_up, w_down, vectors)
        final_b, saved = forward(forward_w, tok_block, segments)
        second = collect(w_qkv, w_out, w_up, w_down, vectors)
        gradients, grad_input = backward(second, saved, segments, grad_block)
        updated = jax.tree.map(jnp.add, carried, gradients)
        return (updated, (final_b, grad_input))

    initial = (
        jnp.zeros((3, D, local_cols), jnp.float32),
        jnp.zeros((local_cols, D), jnp.float32),
        jnp.zeros((D, hidden), jnp.float32),
        jnp.zeros((hidden, D), jnp.float32),
        jnp.zeros((12, D), jnp.float32),
    )
    carried, stacked = lax.scan(one_batch, initial, (tokens, segment_ids, cotangent))
    totals = share(carried)
    vector_grads = lax.psum(totals[4], "tensor")
    return (stacked[0], stacked[1], totals[0], totals[1], totals[2], totals[3], vector_grads)


Y_TOK, Y_COT, Y_OUT, Y_GTOK = range(4)
X_MIX, X_DH, X_DX, X_TOK, X_NORM, X_DA2, X_DA1 = range(7)
W_Q, W_K, W_V, W_OUT, W_UP, W_DOWN, W_REST, W_VEC = range(8)
W_KINDS = 8
Y_FIRST = (W_REST,)
DIRECT = (W_VEC,)
FAR_FIRST = ()
U_DA, U_DB, U_UA, U_UB, U_OUT, U_V, U_K, U_Q = range(8)
Z_FIRST = (U_DA,)
DA_ROWS = 640
R_BQ, R_BV, R_BO, R_G1, R_C1, R_BD, R_G2, R_C2, R_BU = range(9)
ZS = 4
SEQ = 512
ROWS = 256
CHUNK = 128
TILE = 32
COLS = 512
HID = 2048
WINDOW = 384
BF = jnp.bfloat16
F32 = jnp.float32
MESH = pl.DeviceIdType.MESH


def span(index, size):
    return pl.ds(pl.multiple_of(index * size, size), size)


def contract(a, b, a_dim, b_dim):
    return lax.dot_general(a, b, (((a_dim,), (b_dim,)), ((), ())), preferred_element_type=F32)


def fold_rows(value):
    return jnp.sum(value.reshape(value.shape[0] // 8, 8, value.shape[1]), axis=0)


def layer_kernel(
    tok, seg, wq, wo, wu, wd, vec, cot,
    out, gtok, gq, go, gu, gd, gv,
    w_qkv, w_out, w_up, w_down, w_vec, vf,
    g_da, g_db, g_up, g_out, g_qkv,
    c_da, c_db, c_up, c_out, c_qkv,
    y_da, y_db, y_up, y_out, y_qkv,
    z_da, z_db, z_up, z_out, z_qkv,
    h_da, h_db, h_up, h_out, h_qkv,
    o_qkv, o_out, o_up, o_down,
    xw, qkv, ctx, prob, bias, hw, act, slope, aw, a1w, dctx,
    own, n1, da, inv1, recv, stage, cotb, outb, gts, gtr, gtf,
    acc, vg, vgx, vgc, vgy, vgz, gvb, acc_k, acc_v,
    done, wrz, wry, wrc, wrd, fs, fr, xs, xr, yr,
    grc, gry, grz, vs, vr, ls, os,
):
    dp = lax.axis_index("dp")
    tensor = lax.axis_index("tensor")
    z, c = dp // 2, dp % 2
    y, x = tensor // 2, tensor % 2
    at_x = {"dp": dp, "tensor": y * 2 + (1 - x)}
    at_y = {"dp": dp, "tensor": (1 - y) * 2 + x}
    at_c = {"dp": z * 2 + (1 - c), "tensor": tensor}

    def remote(src, dst, send, recv_sem, where):
        return pltpu.make_async_remote_copy(
            src_ref=src, dst_ref=dst, send_sem=send, recv_sem=recv_sem,
            device_id=where, device_id_type=MESH,
        )

    barrier = pltpu.get_barrier_semaphore()
    for where in [at_x, at_y, at_c] + [{"dp": lax.rem(z + k, ZS) * 2 + c, "tensor": tensor} for k in range(1, ZS)]:
        pl.semaphore_signal(barrier, inc=1, device_id=where, device_id_type=MESH)
    pl.semaphore_wait(barrier, 6)

    sent = []

    quiet = []

    def go_on(copy):
        copy.start()
        if not quiet:
            sent.append(copy)

    args = [wq.at[0], wq.at[1], wq.at[2], wo, wu, wd.at[0:512], wd.at[512:1024], vec]
    edge = jnp.logical_or(z == 0, z == ZS - 1)
    middle = jnp.logical_not(edge)
    later = []

    def z_device(where):
        return {"dp": where * 2 + c, "tensor": tensor}

    def go_if(condition, copy):
        @pl.when(condition)
        def _():
            copy.start()
        if not quiet:
            later.append((condition, copy))

    def place(m, yy, d):
        if m <= W_V:
            return w_qkv.at[m, span(d, 128), span(yy, 256)]
        if m == W_OUT:
            return w_out.at[span(yy, 256), span(d, 128)]
        if m == W_UP:
            return w_up.at[span(d, 128), span(yy, 1024)]
        if m == W_DOWN or m == W_REST:
            return w_down.at[span(yy * 2 + m - W_DOWN, 512), span(d, 128)]
        return w_vec.at[d]

    even = lax.rem(z, 2) == 0
    near_first = (jnp.where(even, 3, 1), 2, jnp.where(even, 1, 3))

    def from_z(k):
        return lax.rem(z + ZS - k, ZS)

    def z_slot(m, r):
        return 24 if r else m * 3

    def column(r):
        return y if r == 0 else 1 - y

    def z_send(m, r):
        source = args[m] if r == 0 else place(m, 1 - y, dp)
        steps = ((1, z != ZS - 1), (3, z != 0), (2, None))
        for k, there in (steps[2:] + steps[:2] if m in FAR_FIRST else steps):
            there = None if m in DIRECT else there
            copy = remote(
                source, place(m, column(r), dp), done.at[0], wrz.at[z_slot(m, r) + k - 1],
                z_device(lax.rem(z + k, ZS)),
            )
            if there is None:
                go_on(copy)
            else:
                go_if(there, copy)

    def z_serve(m, r, step, keep=False):
        z_take(m, r, step, keep)
        z_note(m, r, step)

    def z_serve_split(m, r, step, early, late):
        def first():
            @pl.when(early)
            def _():
                z_take(m, r, step)

        def second():
            @pl.when(late)
            def _():
                z_take(m, r, step)
            z_note(m, r, step)
        return first, second

    def z_parts(m, r, step):
        k = near_first[step]
        here = place(m, column(r), from_z(k) * 2 + c)
        slot = jnp.where(z == 1, 0, 2)
        hand_on = None
        if step == 1 and m not in DIRECT:
            hand_on = remote(
                here, here, done.at[0], wrz.at[z_slot(m, r) + slot], z_device(jnp.where(z == 1, 0, 3)),
            )
        over_y = None
        if r == 0 and m not in Y_FIRST and m != W_VEC:
            over_y = remote(here, here, done.at[0], wry.at[m, from_z(k)], at_y)
        return k, here, hand_on, over_y

    def z_over(m, step):
        z_parts(m, 0, step)[3].start()

    def z_take(m, r, step, keep=False):
        k, here, hand_on, over_y = z_parts(m, r, step)
        remote(here, here, done.at[0], wrz.at[z_slot(m, r) + k - 1], at_x).wait_recv()
        if hand_on is not None:
            @pl.when(middle)
            def _():
                hand_on.start()
        if over_y is not None and not keep:
            over_y.start()
        c_send(m, here, step + 1)

    def z_note(m, r, step):
        _, _, hand_on, over_y = z_parts(m, r, step)
        if hand_on is not None:
            later.append((middle, hand_on))
        if over_y is not None:
            sent.append(over_y)

    def y_send(m):
        go_on(remote(args[m], place(m, y, dp), done.at[0], wry.at[m, z], at_y))

    def source_of(step):
        return z if step == 0 else from_z(near_first[step - 1])

    def y_serve(m, step):
        zz = source_of(step)
        here = place(m, 1 - y, zz * 2 + c)
        remote(here, here, done.at[0], wry.at[m, zz], at_y).wait_recv()
        c_send(m, here, step)

    def c_send(m, source, step, dest=None):
        dest = source if dest is None else dest
        into = wrd.at[m - W_DOWN, step] if m in (W_DOWN, W_REST) else wrc.at[m]
        remote(source, dest, done.at[0], into, at_c).start()

    def own_send(m):
        c_send(m, args[m], 0, place(m, y, dp))
        pltpu.make_async_copy(args[m], place(m, y, dp), ls.at[m]).start()

    def half_of(m):
        if m <= W_V:
            return w_qkv.at[m, :, 0:256]
        return (
            w_out.at[0:256], w_up.at[:, 0:1024], w_down.at[0:512], w_down.at[0:512], w_vec.at[0:4]
        )[m - W_OUT]

    def wait_down(step):
        for m in (W_DOWN, W_REST):
            if step == 0:
                pltpu.make_async_copy(args[m], place(m, y, dp), ls.at[m]).wait()
            two = w_down.at[0:1024, 0:128]
            remote(two, two, done.at[0], wrd.at[m - W_DOWN, step], at_c).wait_recv()

    def wait_weight(m):
        pltpu.make_async_copy(args[m], place(m, y, dp), ls.at[m]).wait()
        remote(half_of(m), half_of(m), done.at[0], wrc.at[m], at_c).wait_recv()

    def x_copy(kind, j, src, dst):
        return remote(src, dst, xs.at[kind, j] if kind <= X_DX else done.at[0], xr.at[kind, j], at_x)

    def tok_rows(xx, yy):
        return pl.ds(pl.multiple_of(xx * ROWS + yy * CHUNK, CHUNK), CHUNK)

    for m in (W_Q, W_K, W_V):
        y_send(m)
        z_send(m, 0)
    go_on(remote(tok.at[1 - y], xw.at[tok_rows(x, y)], done.at[0], yr.at[Y_TOK], at_y))
    go_on(x_copy(X_TOK, 0, tok.at[y], xw.at[tok_rows(x, y)]))
    z_send(W_VEC, 0)
    for m in range(W_KINDS):
        own_send(m)
    local_x = pltpu.make_async_copy(tok.at[y], xw.at[tok_rows(x, y)], ls.at[8])
    local_x.start()
    local_cot = pltpu.make_async_copy(cot.at[y], cotb.at[span(y, CHUNK)], ls.at[9])
    local_cot.start()

    seg_row = seg[pl.ds(y, 1), :].astype(F32)
    blocks = [(p % 2) * 2 + p // 2 for p in range(4)]
    across = [jnp.broadcast_to(seg_row[:, n * 128:(n + 1) * 128], (128, 128)) for n in blocks]
    down = [b.T for b in across]
    for t in range(2):
        for i, q in enumerate((t, t + 2)):
            for j in range(3):
                same = down[q] == across[t + j]
                bias[t, i * 128:(i + 1) * 128, j * 128:(j + 1) * 128] = jnp.where(same, 0.0, MASKED)
    acc[...] = jnp.zeros_like(acc)
    vg[...] = jnp.zeros_like(vg)

    for step in range(2):
        for m in (W_Q, W_K, W_V):
            z_serve(m, 0, step)
    z_send(W_OUT, 0)
    y_tok_here = xw.at[tok_rows(x, 1 - y)]
    remote(tok.at[1 - y], y_tok_here, done.at[0], yr.at[Y_TOK], at_y).wait_recv()
    go_on(x_copy(X_TOK, 1, y_tok_here, y_tok_here))
    for m in (W_Q, W_K, W_V):
        z_serve(m, 0, 2)
    y_send(W_OUT)
    z_serve(W_OUT, 0, 0)
    z_serve(W_OUT, 0, 1)
    z_send(W_UP, 0)
    for step in range(3):
        z_serve(W_VEC, 0, step)
    z_serve(W_OUT, 0, 2)
    y_send(W_UP)
    y_send(W_REST)
    for step in range(4):
        for m in (W_Q, W_K, W_V):
            y_serve(m, step)
    wait_weight(W_VEC)
    for d in range(8):
        vf[0:12, d * 128:(d + 1) * 128] = w_vec[d].astype(F32)
    local_x.wait()
    for j, yy in ((0, y), (1, 1 - y)):
        there = xw.at[tok_rows(1 - x, yy)]
        x_copy(X_TOK, j, there, there).wait_recv()
    for m in (W_Q, W_K, W_V):
        wait_weight(m)

    def head_bias(row):
        parts = [vf[row:row + 1, pl.ds(pl.multiple_of(yy * 512 + x * 256, 256), 256)] for yy in range(2)]
        return jnp.concatenate(parts, axis=1)

    for i in range(3):
        value = contract(xw[...], w_qkv[i], 1, 0)
        if i == 0:
            value = (value + head_bias(0)).astype(BF) * BF(HD ** -0.5)
        elif i == 2:
            value = value + head_bias(1)
        qkv[i] = value.astype(BF)

    low_half = lax.broadcasted_iota(jnp.int32, (1, 128), 1) < HD
    halves = (low_half, jnp.logical_not(low_half))
    none = jnp.zeros((), BF)

    def two_blocks(ref, t, lanes):
        return jnp.concatenate([ref[span(t, 128), lanes], ref[span(t + 2, 128), lanes]], axis=0)

    def attend(pair, carry):
        lanes = span(pair, 128)
        for t in range(2):
            keys = pl.ds(t * 128, WINDOW)
            query = two_blocks(qkv.at[0], t, lanes)
            key, value = qkv[1, keys, lanes], qkv[2, keys, lanes]
            total = jnp.zeros((ROWS, 128), F32)
            for h, half in enumerate(halves):
                scores = contract(jnp.where(half, query, none), key, 1, 1) + bias[t]
                top = jnp.max(scores, axis=1, keepdims=True)
                weight = jnp.exp(scores - top)
                share_of = 1.0 / jnp.sum(weight, axis=1, keepdims=True)
                weight = (weight * share_of).astype(BF)
                prob[pair * 4 + t * 2 + h] = weight
                total = total + contract(weight, jnp.where(half, value, none), 1, 0)
            total = total.astype(BF)
            ctx[t * 128:t * 128 + 128, lanes] = total[:128]
            ctx[t * 128 + 256:t * 128 + 384, lanes] = total[128:]
        return carry

    z_serve(W_UP, 0, 0)
    lax.fori_loop(0, 2, attend, 0)
    for step in range(4):
        y_serve(W_OUT, step)
    lax.fori_loop(2, 4, attend, 0)
    up_early, up_late = z_serve_split(W_UP, 0, 1, middle, edge)
    up_early()
    z_send(W_DOWN, 0)

    def rows_of(s):
        mine = jnp.where(s < 2, x, 1 - x)
        return pl.ds(pl.multiple_of(mine * ROWS + lax.rem(s, 2) * CHUNK, CHUNK), CHUNK)

    def x_sum(kind, j):
        return x_copy(kind, j, stage.at[span(j, CHUNK)], recv.at[span(j, CHUNK)])

    def x_rows(kind, j, buf):
        here = buf.at[pl.ds(pl.multiple_of(x * ROWS + j * CHUNK, CHUNK), CHUNK)]
        return x_copy(kind, j, here, here)

    def hand_over(kind, before, s, value):
        @pl.when(s < 2)
        def _():
            own[span(s, CHUNK), :] = value

        @pl.when(s >= 2)
        def _():
            if before is not None:
                x_sum(before, s - 2).wait_send()
            stage[span(s - 2, CHUNK), :] = value.astype(BF)
            x_sum(kind, s - 2).start()

    wait_weight(W_OUT)

    def mix(i, carry):
        s = lax.rem(i + 2, 4)
        hand_over(X_MIX, None, s, contract(ctx[rows_of(s), :], w_out[...], 1, 0))
        return carry

    lax.fori_loop(0, 4, mix, 0)
    up_late()
    z_serve(W_UP, 0, 2)
    y_serve(W_REST, 0)
    z_send(W_REST, 0)
    z_send(W_REST, 1)
    y_serve(W_UP, 0)
    z_serve(W_DOWN, 0, 0, keep=True)
    z_serve(W_DOWN, 0, 1, keep=True)

    def row_of(row):
        return vf[row:row + 1, :]

    def normed(value):
        centred = value - jnp.mean(value, axis=1, keepdims=True)
        inverse = lax.rsqrt(jnp.mean(centred * centred, axis=1, keepdims=True) + NORM_EPS)
        return centred * inverse, inverse

    def norm_back(normal, inverse, grad):
        first = jnp.mean(grad, axis=1, keepdims=True)
        second = jnp.mean(grad * normal, axis=1, keepdims=True)
        return inverse * (grad - first - normal * second)

    def tiles(j, body):
        def step(i, carry):
            body(pl.ds(pl.multiple_of(j * CHUNK + i * TILE, TILE), TILE),
                 pl.ds(pl.multiple_of(x * ROWS + j * CHUNK + i * TILE, TILE), TILE))
            return carry
        lax.fori_loop(0, CHUNK // TILE, step, 0)

    def first_norm(r, g):
        summed = xw[g, :].astype(F32) + own[r, :] + recv[r, :].astype(F32) + row_of(R_BO)
        normal, inverse = normed(summed)
        n1[r, :] = normal
        inv1[r, :] = jnp.broadcast_to(inverse, (TILE, 128))
        hw[g, :] = (normal * row_of(R_G1) + row_of(R_C1)).astype(BF)

    for j in range(2):
        x_sum(X_MIX, j).wait_recv()
        tiles(j, first_norm)
        x_rows(X_NORM, j, hw).start()

    y_send(W_DOWN)
    z_over(W_DOWN, 0)
    z_over(W_DOWN, 1)
    for step in range(1, 4):
        y_serve(W_UP, step)
    wait_weight(W_UP)

    def arrived(kind, s, buf):
        @pl.when(s >= 2)
        def _():
            there = buf.at[rows_of(s)]
            x_copy(kind, s - 2, there, there).wait_recv()

    def up_bias(n):
        return vf[pl.ds(8 + n * 2 + x, 1), :]

    def ffn_up(s, carry):
        rows = rows_of(s)
        arrived(X_NORM, s, hw)
        for n in range(2):
            pre = contract(hw[rows, :], w_up[:, n * 1024:(n + 1) * 1024], 1, 0) + up_bias(n)
            cdf = 0.5 * (1.0 + lax.erf(pre * SQRT_HALF))
            act[rows, n * 1024:(n + 1) * 1024] = (pre * cdf).astype(BF)
            slope[rows, n * 1024:(n + 1) * 1024] = (
                cdf + pre * INV_ROOT_TAU * jnp.exp(-0.5 * pre * pre)
            ).astype(BF)
        return carry

    lax.fori_loop(0, 2, ffn_up, 0)
    z_serve(W_DOWN, 0, 2)
    for r in range(2):
        z_serve(W_REST, r, 0)
        z_serve(W_REST, r, 1)
    y_serve(W_DOWN, 0)
    lax.fori_loop(2, 3, ffn_up, 0)
    y_serve(W_DOWN, 1)
    lax.fori_loop(3, 4, ffn_up, 0)
    y_serve(W_DOWN, 2)
    go_on(remote(cot.at[1 - y], cotb.at[span(y, CHUNK)], done.at[0], yr.at[Y_COT], at_y))

    def ffn_copy(step, j):
        cols = span(source_of(step), 256)
        return remote(
            stage.at[span(j, CHUNK), cols], recv.at[span(j, CHUNK), cols],
            fs.at[0], fr.at[j], at_x,
        )

    for j in range(2):
        x_sum(X_MIX, j).wait_send()
    for step in range(4):
        if step == 2:
            y_serve(W_DOWN, 3)
        if step == 3:
            z_serve(W_REST, 0, 2)
            z_serve(W_REST, 1, 2)
        wait_down(step)
        cols = span(source_of(step), 256)
        stage[:, cols] = contract(act[span(1 - x, ROWS), :], w_down[:, cols], 1, 0).astype(BF)
        for j in range(2):
            ffn_copy(step, j).start()
    for step in range(2):
        cols = span(step, 512)
        own[:, cols] = contract(act[span(x, ROWS), :], w_down[:, cols], 1, 0)

    def bump(row, value):
        acc[row] += fold_rows(value)

    def second_norm(r, g):
        h1 = n1[r, :] * row_of(R_G1) + row_of(R_C1)
        normal, inverse = normed(h1 + own[r, :] + recv[r, :].astype(F32) + row_of(R_BD))
        own[r, :] = normal
        grad = norm_back(normal, inverse, cotb[r, :].astype(F32) * row_of(R_G2))
        da[r, :] = grad
        aw[g, :] = grad.astype(BF)

    def second_rest(r, g):
        normal, dy = own[r, :], cotb[r, :].astype(F32)
        outb[r, :] = (normal * row_of(R_G2) + row_of(R_C2)).astype(BF)
        bump(R_G2, dy * normal)
        bump(R_C2, dy)
        bump(R_BD, da[r, :])

    local_cot.wait()
    cot_here = cotb.at[span(1 - y, CHUNK)]
    remote(cot.at[1 - y], cot_here, done.at[0], yr.at[Y_COT], at_y).wait_recv()
    for j in range(2):
        half = recv.at[span(j, CHUNK)]
        remote(half, half, fs.at[0], fr.at[j], at_x).wait_recv()
        tiles(j, second_norm)
        x_rows(X_DA2, j, aw).start()
    for j in range(2):
        tiles(j, second_rest)
    out_here = pltpu.make_async_copy(outb.at[span(y, CHUNK)], out.at[y], os.at[0])
    out_here.start()
    go_on(remote(outb.at[span(1 - y, CHUNK)], out.at[y], done.at[0], yr.at[Y_OUT], at_y))

    def ffn_back(s, carry, wait=True):
        rows = rows_of(s)
        if wait:
            arrived(X_DA2, s, aw)
        for n in range(2):
            cols = slice(n * 1024, (n + 1) * 1024)
            grad = contract(aw[rows, :], w_down[cols, :], 1, 1) * slope[rows, cols].astype(F32)
            bump(R_BU + n, grad)
            slope[rows, cols] = grad.astype(BF)
        hand_over(X_DH, None, s, contract(slope[rows, :], w_up[...], 1, 1))
        return carry

    remote(stage, stage, fs.at[0], fr.at[0], at_x).wait_send()
    lax.fori_loop(0, 3, ffn_back, 0)
    last_rows = aw.at[rows_of(jnp.int32(3))]
    x_copy(X_DA2, 1, last_rows, last_rows).wait_recv()

    def last_back():
        lax.fori_loop(3, 4, functools.partial(ffn_back, wait=False), 0)

    units = {
        U_DA: (g_da, c_da, y_da, z_da, h_da, o_down.at[0:DA_ROWS], gd.at[0:DA_ROWS]),
        U_DB: (g_db, c_db, y_db, z_db, h_db, o_down.at[DA_ROWS:1024], gd.at[DA_ROWS:1024]),
        U_OUT: (g_out, c_out, y_out, z_out, h_out, o_out, go),
    }
    for u, i in ((U_UA, 0), (U_UB, 1)):
        rows = slice(i * 64, (i + 1) * 64)
        units[u] = tuple(r.at[i] for r in (g_up, c_up, y_up, z_up, h_up)) + (o_up.at[rows], gu.at[rows])
    for u, i in ((U_Q, 0), (U_K, 1), (U_V, 2)):
        units[u] = tuple(r.at[i] for r in (g_qkv, c_qkv, y_qkv, z_qkv, h_qkv, o_qkv, gq))

    def piece_loop(rows, body):
        size = min(rows, CHUNK)

        def step(i, carry):
            body(span(i, size))
            return carry
        lax.fori_loop(0, rows // size, step, 0)

    def add_piece(g, yy, zz, other):
        def body(r):
            g[c, yy, zz, r, :] = (g[c, yy, zz, r, :].astype(F32) + other[r, :].astype(F32)).astype(BF)
        piece_loop(g.shape[3], body)

    def core_copy(u):
        g, rc = units[u][0], units[u][1]
        return remote(g.at[1 - c], rc, done.at[0], grc.at[u], at_c)

    def core_send(u):
        go_on(core_copy(u))

    def core_add(u, r):
        g, rc = units[u][0], units[u][1]
        for zz in range(ZS):
            add_piece(g, column(r), zz, rc.at[column(r), zz])

    def rs_y_copy(u):
        g, ry = units[u][0], units[u][2]
        source = g.at[c, 1 - y, pl.ds(z, 1)] if u in Z_FIRST else g.at[c, 1 - y]
        return remote(source, ry, done.at[0], gry.at[u], at_y)

    def rs_z_copy(u, r, k):
        g, rz = units[u][0], units[u][3]
        to = lax.rem(z + k, ZS)
        return remote(g.at[c, column(r), to], rz.at[r, k - 1], done.at[0], grz.at[(32 if r else u * 4) + k - 1], z_device(to))

    def rs_hand_on(u, r):
        g, rh = units[u][0], units[u][4]
        far = jnp.where(z == 0, ZS - 1, 0)
        return remote(g.at[c, column(r), far], rh.at[r], done.at[0], grz.at[(32 if r else u * 4) + 3], z_device(jnp.where(z == 0, 1, 2)))

    def z_hand_on(u, r):
        go_if(edge, rs_hand_on(u, r))

    def z_begin(u, r):
        go_if(z != ZS - 1, rs_z_copy(u, r, 1))
        go_if(z != 0, rs_z_copy(u, r, 3))
        go_if(edge, rs_z_copy(u, r, 2))

    def z_relay(u, r):
        g, rh = units[u][0], units[u][4]

        @pl.when(middle)
        def _():
            rs_hand_on(u, r).wait_recv()
            add_piece(g, column(r), lax.rem(z + 2, ZS), rh.at[r])
        go_if(middle, rs_z_copy(u, r, 2))

    def start(u):
        core_copy(u).wait_recv()
        core_add(u, 1)
        if u in Z_FIRST:
            z_hand_on(u, 1)
            core_add(u, 0)
            z_hand_on(u, 0)
            z_begin(u, 1)
            z_begin(u, 0)
        else:
            go_on(rs_y_copy(u))
            core_add(u, 0)

    def y_to_z(u):
        g, ry = units[u][0], units[u][2]
        rs_y_copy(u).wait_recv()
        for zz in range(ZS):
            add_piece(g, y, zz, ry.at[zz])
        z_hand_on(u, 0)
        z_begin(u, 0)

    def wait_z(u, r):
        rs_z_copy(u, r, 2).wait_recv()

        @pl.when(z != 0)
        def _():
            rs_z_copy(u, r, 1).wait_recv()

        @pl.when(z != ZS - 1)
        def _():
            rs_z_copy(u, r, 3).wait_recv()

    def z_total(u, r, rows):
        g, rz = units[u][0], units[u][3]
        value = g[c, column(r), z, rows, :].astype(F32)
        for k in range(ZS - 1):
            value = value + rz[r, k, rows, :].astype(F32)
        return value

    def z_to_y(u):
        g = units[u][0]
        wait_z(u, 1)

        def body(rows):
            g[c, 1 - y, z, rows, :] = z_total(u, 1, rows).astype(BF)
        piece_loop(g.shape[3], body)
        go_on(rs_y_copy(u))

    finals = []

    def finish(u):
        g, _, ry, _, _, o, dest = units[u]
        wait_z(u, 0)
        if u in Z_FIRST:
            rs_y_copy(u).wait_recv()

        def body(rows):
            value = z_total(u, 0, rows)
            if u in Z_FIRST:
                value = value + ry[0, rows, :].astype(F32)
            o[rows, :] = value
        piece_loop(g.shape[3], body)
        copy = pltpu.make_async_copy(o, dest, os.at[0])
        copy.start()
        finals.append(copy)

    for u in units:
        for r in range(2 if u in Z_FIRST else 1):
            for k, alone in ((1, z == 0), (3, z == ZS - 1)):
                @pl.when(alone)
                def _(u=u, r=r, k=k):
                    rz = units[u][3]
                    rz[r, k - 1] = jnp.zeros(rz.shape[2:], BF)

    def grad_down(u):
        g, first, count = (g_da, 0, DA_ROWS) if u == U_DA else (g_db, DA_ROWS, 1024 - DA_ROWS)

        def step(yy, carry):
            rows = pl.ds(pl.multiple_of(yy * 1024 + first, 128), count)
            value = contract(act[:, rows], aw[...], 0, 0).astype(BF)
            for d in range(8):
                g[d % 2, yy, d // 2] = value[:, d * 128:(d + 1) * 128]
            return carry

        lax.fori_loop(0, 2, step, 0)
        core_send(u)

    def grad_up():
        def step(index, carry):
            i, n = index // 2, index % 2
            value = contract(hw[:, span(i, 512)], slope[:, span(n, 1024)], 0, 0).astype(BF)
            for d in range(4):
                for part in range(2):
                    r = d * 128 + part * 64
                    g_up[part, d % 2, n, i * 2 + d // 2] = value[r:r + 64, :]
            return carry

        lax.fori_loop(0, 4, step, 0)
        core_send(U_UA)
        core_send(U_UB)

    quiet.append(True)

    @pl.when(c == 0)
    def _():
        grad_down(U_DB)
        start(U_DB)
        last_back()
        grad_down(U_DA)
        start(U_DA)
        grad_up()

    @pl.when(c == 1)
    def _():
        grad_down(U_DB)
        last_back()
        grad_down(U_DA)
        grad_up()
        start(U_DB)
        start(U_DA)

    quiet.clear()
    for u in (U_DB, U_DA, U_UA, U_UB):
        sent.append(core_copy(u))
    sent.append(rs_y_copy(U_DB))
    for r in (1, 0):
        later.append((edge, rs_hand_on(U_DA, r)))
        later.append((z != ZS - 1, rs_z_copy(U_DA, r, 1)))
        later.append((z != 0, rs_z_copy(U_DA, r, 3)))
        later.append((edge, rs_z_copy(U_DA, r, 2)))
    quiet.append(True)

    @pl.when(c == 0)
    def _():
        start(U_UA)
        start(U_UB)

    def back_norm(r, g):
        grad = da[r, :] + own[r, :] + recv[r, :].astype(F32)
        own[r, :] = grad
        grad = norm_back(n1[r, :], inv1[r, 0:1], grad * row_of(R_G1))
        da[r, :] = grad
        a1w[g, :] = grad.astype(BF)

    def back_rest(r, g):
        grad = own[r, :]
        bump(R_G1, grad * n1[r, :])
        bump(R_C1, grad)
        bump(R_BO, da[r, :])

    for j in range(2):
        x_sum(X_DH, j).wait_recv()
        tiles(j, back_norm)
        x_rows(X_DA1, j, a1w).start()

    @pl.when(c == 1)
    def _():
        start(U_UA)
        start(U_UB)

    quiet.clear()
    sent.append(rs_y_copy(U_UA))
    sent.append(rs_y_copy(U_UB))
    for j in range(2):
        tiles(j, back_rest)

    z_relay(U_DA, 1)
    z_relay(U_DA, 0)

    def ctx_back(s, carry):
        rows = rows_of(s)
        arrived(X_DA1, s, a1w)
        dctx[rows, :] = contract(a1w[rows, :], w_out[...], 1, 1).astype(BF)
        return carry

    lax.fori_loop(0, 2, ctx_back, 0)
    y_to_z(U_DB)
    lax.fori_loop(2, 4, ctx_back, 0)

    def attend_back(pair, carry):
        lanes = span(pair, 128)
        for t in range(2):
            keys = pl.ds(t * 128, WINDOW)
            query = two_blocks(qkv.at[0], t, lanes)
            key, value = qkv[1, keys, lanes], qkv[2, keys, lanes]
            grad = two_blocks(dctx, t, lanes)
            product = grad.astype(F32) * two_blocks(ctx, t, lanes).astype(F32)
            grad_q = jnp.zeros((ROWS, 128), F32)
            grad_k = jnp.zeros((WINDOW, 128), F32)
            grad_v = jnp.zeros((WINDOW, 128), F32)
            for h, half in enumerate(halves):
                grad_h = jnp.where(half, grad, none)
                weight = prob[pair * 4 + t * 2 + h]
                row_dot = jnp.sum(jnp.where(half, product, 0.0), axis=1, keepdims=True)
                score = (weight.astype(F32) * (contract(grad_h, value, 1, 1) - row_dot)).astype(BF)
                grad_q = grad_q + contract(score, jnp.where(half, key, none), 1, 0)
                grad_k = grad_k + contract(score, jnp.where(half, query, none), 0, 0)
                grad_v = grad_v + contract(weight, grad_h, 0, 0)
            grad_q = grad_q * (HD ** -0.5)
            acc[R_BQ, :, lanes] += fold_rows(grad_q)
            acc[R_BV, :, lanes] += fold_rows(grad_v)
            grad_q = grad_q.astype(BF)
            qkv[0, t * 128:t * 128 + 128, lanes] = grad_q[:128]
            qkv[0, t * 128 + 256:t * 128 + 384, lanes] = grad_q[128:]
            if t == 0:
                acc_k[0:WINDOW, :] = grad_k
                acc_v[0:WINDOW, :] = grad_v
                acc_k[WINDOW:SEQ, :] = jnp.zeros((128, 128), F32)
                acc_v[WINDOW:SEQ, :] = jnp.zeros((128, 128), F32)
            else:
                for i, total, more in ((1, acc_k, grad_k), (2, acc_v, grad_v)):
                    qkv[i, 0:128, lanes] = total[0:128, :].astype(BF)
                    qkv[i, 128:SEQ, lanes] = (total[128:SEQ, :] + more).astype(BF)
        return carry

    def grad_out():
        value = contract(ctx[...], a1w[...], 0, 0).astype(BF)
        for d in range(8):
            for yy in range(2):
                g_out[d % 2, yy, d // 2] = value[yy * 256:(yy + 1) * 256, d * 128:(d + 1) * 128]

    grad_out()
    core_send(U_OUT)
    lax.fori_loop(0, 2, attend_back, 0)
    start(U_OUT)
    y_to_z(U_UA)
    lax.fori_loop(2, 4, attend_back, 0)

    for row in range(2, 8):
        line = jnp.sum(acc[row], axis=0, keepdims=True)
        for d in range(8):
            vg[d % 2, d // 2, row:row + 1, :] = line[:, d * 128:(d + 1) * 128]
    for n in range(2):
        line = jnp.sum(acc[R_BU + n], axis=0, keepdims=True)
        for d in range(8):
            vg[d % 2, d // 2, pl.ds(8 + n * 2 + x, 1), :] = line[:, d * 128:(d + 1) * 128]
    for row, source in ((0, R_BQ), (1, R_BV)):
        line = jnp.sum(acc[source], axis=0, keepdims=True)
        for yy in range(2):
            for half in range(2):
                vg[half, 2 * yy + x, row:row + 1, :] = (
                    line[:, yy * 256 + half * 128:yy * 256 + (half + 1) * 128]
                )
    vec_x = remote(vg, vgx, vs.at[0], vr.at[0], at_x)
    vec_c = remote(vg.at[1 - c], vgc, vs.at[1], vr.at[1], at_c)
    vec_y = remote(vg.at[c], vgy, vs.at[2], vr.at[2], at_y)

    def vec_z(k):
        to = lax.rem(z + k, ZS)
        return remote(vg.at[c, to], vgz.at[k - 1], done.at[0], vr.at[2 + k], z_device(to))

    vec_x.start()

    def input_back(i, carry):
        s = lax.rem(i + 2, 4)
        rows = rows_of(s)
        value = contract(qkv[0, rows, :], w_qkv[0], 1, 1)
        value = value + contract(qkv[1, rows, :], w_qkv[1], 1, 1)
        value = value + contract(qkv[2, rows, :], w_qkv[2], 1, 1)
        hand_over(X_DX, X_DH, s, value)
        return carry

    lax.fori_loop(0, 2, input_back, 0)
    vec_x.wait()
    vg[...] = vg[...] + vgx[...]
    vec_c.start()

    def grad_qkv(index, carry):
        kind, i = index // 2, index % 2
        value = contract(xw[:, span(i, 512)], qkv[kind], 0, 0).astype(BF)
        for d in range(4):
            for yy in range(2):
                g_qkv[kind, d % 2, yy, i * 2 + d // 2] = (
                    value[d * 128:(d + 1) * 128, yy * 256:(yy + 1) * 256]
                )
        return carry

    for kind, u in ((0, U_Q), (1, U_K), (2, U_V)):
        lax.fori_loop(kind * 2, kind * 2 + 2, grad_qkv, 0)
        core_send(u)
    z_relay(U_DB, 0)
    vec_c.wait()
    vg[c] = vg[c] + vgc[...]
    vec_y.start()
    for u in (U_Q, U_K, U_V):
        start(u)
    z_relay(U_UA, 0)
    y_to_z(U_UB)
    lax.fori_loop(2, 4, input_back, 0)
    y_to_z(U_OUT)
    z_to_y(U_DA)
    vec_y.wait()
    vg[c] = vg[c] + vgy[...]
    for k in range(1, ZS):
        go_on(vec_z(k))

    def last_sum(j, other):
        x_sum(X_DX, j).wait_recv()

        def body(r, g):
            value = da[r, :] + own[r, :] + recv[r, :].astype(F32)
            if other:
                gts[pl.ds(pl.multiple_of(r.start - j * CHUNK, TILE), TILE), :] = value.astype(BF)
            else:
                da[r, :] = value
        tiles(j, body)

    last_sum(1 - y, True)
    go_on(remote(gts, gtr, done.at[0], yr.at[Y_GTOK], at_y))
    last_sum(y, False)
    gtok_here = pltpu.make_async_copy(da.at[span(y, CHUNK)], gtok.at[y], os.at[0])
    gtok_here.start()
    y_to_z(U_Q)
    z_relay(U_UB, 0)
    y_to_z(U_K)
    z_relay(U_OUT, 0)
    y_to_z(U_V)
    for u in (U_Q, U_K, U_V):
        z_relay(u, 0)
    for k in range(1, ZS):
        vec_z(k).wait_recv()
    gvb[...] = vg[c, z] + vgz[0] + vgz[1] + vgz[2]
    vec_here = pltpu.make_async_copy(gvb.at[0:12], gv, os.at[0])
    vec_here.start()
    for u in (U_DA, U_DB, U_UA, U_UB):
        finish(u)
    remote(gts, gtr, done.at[0], yr.at[Y_GTOK], at_y).wait_recv()
    gtf[...] = gtr[...].astype(F32)
    gtok_there = pltpu.make_async_copy(gtf, gtok.at[1 - y], os.at[0])
    gtok_there.start()
    finish(U_OUT)
    finish(U_Q)
    finish(U_K)
    finish(U_V)
    remote(outb.at[span(1 - y, CHUNK)], out.at[1 - y], done.at[0], yr.at[Y_OUT], at_y).wait_recv()
    for kind, buf in ((X_NORM, hw), (X_DA2, aw), (X_DA1, a1w)):
        for j in range(2):
            x_rows(kind, j, buf).wait_send()
    for j in range(2):
        x_sum(X_DX, j).wait_send()
    for copy in sent:
        copy.wait_send()
    for condition, copy in later:
        @pl.when(condition)
        def _(copy=copy):
            copy.wait_send()
    for m in range(W_KINDS):
        remote(half_of(m), half_of(m), done.at[0], wrc.at[m], at_c).wait_send()
    for copy in finals + [out_here, gtok_here, gtok_there, vec_here]:
        copy.wait()


def settle_kernel(*refs):
    count = (len(refs) - 2) // 3
    sources, dests, held = refs[:count], refs[count:2 * count], refs[2 * count:3 * count]
    into, out_of = refs[3 * count:]
    first = [pltpu.make_async_copy(s, h, into.at[i]) for i, (s, h) in enumerate(zip(sources, held))]
    second = [pltpu.make_async_copy(h, d, out_of.at[i]) for i, (h, d) in enumerate(zip(held, dests))]
    for copy in first:
        copy.start()
    for before, after in zip(first, second):
        before.wait()
        after.start()
    for copy in second:
        copy.wait()


def settle(results):
    shapes = [jax.ShapeDtypeStruct(r.shape, r.dtype) for r in results]
    count = len(shapes)
    hbm = pl.BlockSpec(memory_space=pl.ANY)
    return pl.pallas_call(
        settle_kernel,
        out_shape=shapes,
        in_specs=[hbm] * count,
        out_specs=[hbm] * count,
        scratch_shapes=[pltpu.VMEM(r.shape, r.dtype) for r in shapes]
        + [pltpu.SemaphoreType.DMA((count,))] * 2,
    )(*results)


def layer(tokens, segment_ids, w_qkv, w_out, w_up, w_down, vectors, cotangent):
    vmem, dma = pltpu.VMEM, pltpu.SemaphoreType.DMA
    outs = (
        jax.ShapeDtypeStruct(tokens.shape, BF),
        jax.ShapeDtypeStruct(tokens.shape, F32),
        jax.ShapeDtypeStruct(w_qkv.shape, F32),
        jax.ShapeDtypeStruct(w_out.shape, F32),
        jax.ShapeDtypeStruct(w_up.shape, F32),
        jax.ShapeDtypeStruct(w_down.shape, F32),
        jax.ShapeDtypeStruct(vectors.shape, F32),
    )
    scratch = [
        vmem((3, D, COLS), BF), vmem((COLS, D), BF), vmem((D, HID), BF), vmem((HID, D), BF),
        vmem((8, 12, 128), BF), vmem((16, D), F32),
    ]
    part_da, part_db = (DA_ROWS, 128), (1024 - DA_ROWS, 128)
    half_up, piece_out, piece_qkv = (64, 1024), (256, 128), (128, 256)
    for shape in ((2, 2, 4), (2, 4)):
        scratch += [
            vmem(shape + part_da, BF), vmem(shape + part_db, BF), vmem((2,) + shape + half_up, BF),
            vmem(shape + piece_out, BF), vmem((3,) + shape + piece_qkv, BF),
        ]
    for y_shape, z_shape in (((4,), (1,)), ((1, 3), (2, 3)), ((1,), (2,))):
        scratch += [
            vmem(z_shape + part_da, BF), vmem(y_shape + part_db, BF),
            vmem((2,) + y_shape + half_up, BF), vmem(y_shape + piece_out, BF),
            vmem((3,) + y_shape + piece_qkv, BF),
        ]
    scratch += [vmem((3, 128, 256), F32), vmem((256, 128), F32), vmem((128, 1024), F32), vmem((1024, 128), F32)]
    scratch += [
        vmem((SEQ, D), BF), vmem((3, SEQ, COLS), BF), vmem((SEQ, COLS), BF),
        vmem((16, ROWS, WINDOW), BF), vmem((2, ROWS, WINDOW), F32), vmem((SEQ, D), BF),
        vmem((SEQ, HID), BF), vmem((SEQ, HID), BF), vmem((SEQ, D), BF), vmem((SEQ, D), BF),
        vmem((SEQ, COLS), BF),
        vmem((ROWS, D), F32), vmem((ROWS, D), F32), vmem((ROWS, D), F32), vmem((ROWS, 128), F32),
        vmem((ROWS, D), BF), vmem((ROWS, D), BF), vmem((ROWS, D), BF), vmem((ROWS, D), BF),
        vmem((CHUNK, D), BF), vmem((CHUNK, D), BF), vmem((CHUNK, D), F32),
        vmem((12, 8, D), F32),
        vmem((2, 4, 16, 128), F32), vmem((2, 4, 16, 128), F32), vmem((4, 16, 128), F32),
        vmem((4, 16, 128), F32), vmem((3, 16, 128), F32), vmem((16, 128), F32),
        vmem((SEQ, 128), F32), vmem((SEQ, 128), F32),
        dma((1,)), dma((27,)), dma((7, 4)), dma((8,)), dma((2, 4)), dma((1,)), dma((2,)),
        dma((3, 2)), dma((7, 2)), dma((4,)),
        dma((8,)), dma((8,)), dma((36,)),
        dma((3,)), dma((6,)), dma((10,)), dma((1,)),
    ]
    hbm = pl.BlockSpec(memory_space=pl.ANY)
    results = pl.pallas_call(
        layer_kernel,
        out_shape=outs,
        in_specs=[hbm, pl.BlockSpec(memory_space=pltpu.VMEM)] + [hbm] * 6,
        out_specs=[hbm] * 7,
        scratch_shapes=scratch,
        compiler_params=pltpu.CompilerParams(
            collective_id=0, has_side_effects=True, vmem_limit_bytes=67043328
        ),
    )(tokens, segment_ids, w_qkv, w_out, w_up, w_down, vectors, cotangent)
    return settle(results)


def solution(mesh):
    step = layer if (mesh.shape["dp"], mesh.shape["tensor"]) == (8, 4) else body
    return jax.shard_map(
        step,
        mesh=mesh,
        in_specs=(
            P("dp", "tensor", None),
            P("dp", None),
            P(None, "dp", "tensor"),
            P("tensor", "dp"),
            P("dp", "tensor"),
            P("tensor", "dp"),
            P(None, "dp"),
            P("dp", "tensor", None),
        ),
        out_specs=(
            P("dp", "tensor", None),
            P("dp", "tensor", None),
            P(None, "dp", "tensor"),
            P("tensor", "dp"),
            P("dp", "tensor"),
            P("tensor", "dp"),
            P(None, "dp"),
        ),
        check_vma=False,
    )
```
